32 devices in a mesh: stream: 32 (over z, y, x, core), item: 1.
Axes of the slice: x: 2, y: 2, z: 4, core: 2. Of those that a mesh axis runs over, the one named last changes fastest.
Arguments:
- event_items: int32 [131072], P('stream'), may hold values from 0 to 262143, as said below
- event_sessions: int32 [131072], P('stream'), may hold values from 0 to 8191, never falling along the last dimension, each value on 1 to 64 neighbouring positions
- sketch_bits: int32 [15, 262144], P(None, 'item'), may hold values from 0 to 262143
Outputs:
- sketch: float32 [128, 256], P('stream')
The draws below stay inside these ranges and needn't reach their ends.
Inputs may be any that keep to these rules, and one draw needn't show every extreme that they name: `event_items`: item 262144 - 1 occurs at least once.
All inputs are finite; a program needn't handle non-finite values.
Results may differ from the reference program's by a relative error of at most 0.0006.
Values may be sent and summed in bfloat16 or wider, within the bound.
A program may use at most 128 MiB of HBM per device.

```python
import math
import jax
import jax.numpy as jnp
import numpy as np
from jax import lax

ITEMS = 262144
SKETCH = 256
WINDOW = 15
WORDS = 15
EVENTS = 131072
ROWS = 128


def draw_event_items(key, part):
    first_key, second_key, third_key = jax.random.split(jax.random.fold_in(key, 7), 3)
    picker = jax.random.randint(first_key, (EVENTS,), 0, 2)
    row_items = jax.random.randint(second_key, (EVENTS,), 0, ROWS)
    wide_items = jax.random.randint(third_key, (EVENTS,), 0, ITEMS)
    chosen = jnp.where(picker == 0, row_items, wide_items)
    return chosen.at[EVENTS // 2].set(ITEMS - 1).astype(jnp.int32)


def place_ends(values, own_key, low, high):
    dims = values.shape
    index_at = [jax.random.randint(jax.random.fold_in(own_key, axis), (), 0, dims[axis]) for axis in range(len(dims))]
    values = values.at[tuple(index_at)].set(low)
    longest = dims.index(max(dims))
    index_at[longest] = (index_at[longest] + 1) % dims[longest]
    return values.at[tuple(index_at)].set(high)


def split_up(count, total, most, slope):
    weights = [(1 << 20) // math.isqrt(rank ** slope) + 1 for rank in range(2, count + 1)]
    rest, given = total - most - (count - 1), [1] * (count - 1)
    while rest > 0:
        candidates = [i for i in range(count - 1) if given[i] < most]
        pool, remaining = sum([weights[i] for i in candidates]), rest
        for i in candidates:
            more = min(most - given[i], max(1, remaining * weights[i] // pool), rest)
            given[i] = given[i] + more
            rest = rest - more
    return np.array([most] + given)


def uneven(rng, count, total, bound, lean):
    if count == 2:
        one = jax.random.randint(rng, (), max(1, total - bound), min(bound, total - 1) + 1)
        return jnp.stack([one, total - one])
    tallies = jnp.asarray(split_up(count, total, bound, lean), jnp.int32)
    pairs = (count - 1) // 2
    giver, receiver = tallies[1:1 + 2 * pairs:2], tallies[2:2 + 2 * pairs:2]
    room = jnp.minimum(giver - 1, bound - receiver)
    passed = jax.random.randint(jax.random.fold_in(rng, 1), (pairs,), 0, 1 << 20) % (room + 1)
    tallies = tallies.at[1:1 + 2 * pairs:2].set(giver - passed).at[2:2 + 2 * pairs:2].set(receiver + passed)
    return tallies[jax.random.permutation(jax.random.fold_in(rng, 2), count)]


def setup_inputs(seed: int = 0) -> dict:
    key_of = jax.random.split(jax.random.key(seed), 4)
    return {
        "event_items": draw_event_items(jax.random.fold_in(key_of[3], 71), 0),
        "event_sessions": jnp.searchsorted(jnp.cumsum(uneven(key_of[1], EVENTS // 16, EVENTS, 64, 0)), jnp.arange(EVENTS), side="right").astype(jnp.int32),
        "sketch_bits": place_ends(jax.random.randint(key_of[2], (WORDS, ITEMS), 0, 2 ** 18), jax.random.fold_in(key_of[2], 1), 0, (2 ** 18) - 1).astype(jnp.int32),
    }


def pointwise(count_block, row_margin, col_margin, pair_total):
    log_ratio = jnp.log(jnp.maximum(count_block, 1.0)) + jnp.log(pair_total) - jnp.log(jnp.maximum(row_margin, 1.0)) - jnp.log(jnp.maximum(col_margin, 1.0))
    return jnp.where(count_block > 0, jnp.maximum(log_ratio, 0.0), 0.0)

def sign_table(bit_block, sketch_width):
    word_count = bit_block.shape[0]
    spread = jnp.repeat(bit_block, 18, axis=0, total_repeat_length=word_count * 18)[:sketch_width]
    bit_shift = (jnp.arange(sketch_width, dtype=jnp.int32) % 18)[:, None]
    return (2 * jnp.bitwise_and(jnp.right_shift(spread, bit_shift), 1) - 1).astype(jnp.float32)

def reference(event_items, event_sessions, sketch_bits):
    position = jnp.arange(EVENTS, dtype=jnp.int32)
    partners = []
    weights = []
    for offset in range(1, WINDOW + 1):
        for direction in (1, -1):
            other_pos = position + direction * offset
            inside = (other_pos >= 0) & (other_pos < EVENTS)
            clipped = jnp.clip(other_pos, 0, EVENTS - 1).astype(jnp.int32)
            linked = inside & (event_sessions[clipped] == event_sessions)
            partners.append(event_items[clipped])
            weights.append(linked.astype(jnp.float32))
    partner_all = jnp.concatenate(partners)
    weight_all = jnp.concatenate(weights)
    owner_all = jnp.tile(event_items, 2 * WINDOW)
    margin = jnp.zeros((ITEMS,), jnp.float32).at[partner_all].add(weight_all)
    hit_row = owner_all < ROWS
    counts = jnp.zeros((ROWS, ITEMS), jnp.float32).at[jnp.where(hit_row, owner_all, 0), partner_all].add(jnp.where(hit_row, weight_all, 0.0))
    pair_total = jnp.sum(margin)
    row_margin = margin[:ROWS]
    block_width = math.gcd(ITEMS, 8192)

    def accumulate(block_index, summed):
        first_col = (block_index * block_width).astype(jnp.int32)
        count_block = lax.dynamic_slice_in_dim(counts, first_col, block_width, 1)
        col_margin = lax.dynamic_slice_in_dim(margin, first_col, block_width, 0)
        bit_block = lax.dynamic_slice_in_dim(sketch_bits, first_col, block_width, 1)
        positive = pointwise(count_block, row_margin[:, None], col_margin[None, :], pair_total)
        sign_rows = sign_table(bit_block, SKETCH)
        return summed + lax.dot_general(positive, sign_rows, (((1,), (1,)), ((), ())), precision=lax.Precision.HIGHEST, preferred_element_type=jnp.float32)
    summed = lax.fori_loop(0, ITEMS // block_width, accumulate, jnp.zeros((ROWS, SKETCH), jnp.float32))
    return summed / math.sqrt(EVENTS)
```

```python
import functools
import math

import jax
import jax.numpy as jnp
from jax import lax
from jax.experimental import pallas as pl
from jax.experimental.pallas import tpu as pltpu
from jax.sharding import PartitionSpec as P

WINDOW = 15
ITEM_BITS = 18
LANES = 128
BITS_PER_WORD = 18
BIG = 1.0e6
PLANE = 8
VMEM_GRANT = 45 * 1024 * 1024
NT = (((1,), (1,)), ((), ()))
VMEM = pl.BlockSpec(memory_space=pltpu.VMEM)


def one_where(mask):
    return jnp.where(mask, 1.0, 0.0).astype(jnp.bfloat16)


def hot_columns(ids, values):
    row = jnp.broadcast_to(values, (16, values.shape[1])).astype(jnp.bfloat16)
    one, zero = jnp.ones((), jnp.bfloat16), jnp.zeros((), jnp.bfloat16)
    return jnp.concatenate(
        [jnp.where(ids[n : n + 16] == row, one, zero) for n in range(0, ids.shape[0], 16)], axis=0
    )


def greet_all(slabs, me):
    barrier = pltpu.get_barrier_semaphore()

    for k in range(1, slabs):
        pl.semaphore_signal(
            barrier, inc=1, device_id={"stream": lax.rem(me + k, slabs)}, device_id_type=pl.DeviceIdType.MESH
        )
    return barrier


def send(src, dst, send_sem, recv_sem, to):
    return pltpu.make_async_remote_copy(
        src_ref=src,
        dst_ref=dst,
        send_sem=send_sem,
        recv_sem=recv_sem,
        device_id={"stream": to},
        device_id_type=pl.DeviceIdType.MESH,
    )


def each(low, high, do):
    for k in range(low, high):
        do(k)


def exchange(slabs, me, out_ref, in_ref, send_sems, recv_sems, start):
    def copy(k):
        to = lax.rem(me + k, slabs)
        return send(out_ref.at[to], in_ref.at[me], send_sems.at[k], recv_sems.at[k], to)

    if start:
        each(1, slabs, lambda k: copy(k).start())
        in_ref[me] = out_ref[me]
    else:
        each(1, slabs, lambda k: copy(k).wait())


def gather_kernel(
    slabs, rows, blocks, items_ref, sessions_ref, all_items, all_sessions, head_ref,
    own_items, own_sessions, short_ref, halo_ref, item_ref, session_ref, links_ref, total_ref,
    pair_out, pair_in, plane_out, plane_in, line_out, line_in,
    load_sems, halo_send, halo_recv, line_send, line_recv, plane_send, plane_recv, near_send, near_recv,
    pair_sems, head_plane_send, head_plane_recv, head_line_send, head_line_recv,
):
    me = lax.axis_index("stream")
    depth = slabs // PLANE
    layer, low = me // PLANE, lax.rem(me, PLANE)
    parity, quad = lax.rem(me, 2), lax.rem(me // 2, 4)

    def flip(bit):
        return bit - 2 * bit * lax.rem(me // bit, 2)

    partner = me + flip(1)
    steps = (flip(2), flip(4), flip(2) + flip(4))
    after, before = lax.rem(me + 1, slabs), lax.rem(me + slabs - 1, slabs)

    def other_layer(k):
        rising = k + (k - layer + depth) // depth
        mirrored = depth - 1 - layer
        falling = depth - 1 - k - (k - mirrored + depth) // depth
        high = layer // ((depth + 1) // 2)
        return rising + (falling - rising) * lax.rem(high, 2)

    others = [other_layer(k) for k in range(depth - 1)]
    loads = [
        pltpu.make_async_copy(items_ref, own_items, load_sems.at[0]),
        pltpu.make_async_copy(sessions_ref, own_sessions, load_sems.at[1]),
    ]
    for copy in loads:
        copy.start()
    barrier = pltpu.get_barrier_semaphore()
    greeted = [partner, after, before] + [me + step for step in steps] + [o * PLANE + low for o in others]
    for to in greeted:
        pl.semaphore_signal(
            barrier, inc=1, device_id={"stream": to}, device_id_type=pl.DeviceIdType.MESH
        )
    for copy in loads:
        copy.wait()
    short_ref[...] = own_sessions[...].astype(jnp.int16)
    item_ref[8 : 8 + blocks] = own_items[...]
    session_ref[8 : 8 + blocks] = own_sessions[...]
    all_items[me] = own_items[...]
    all_sessions[me] = short_ref[...]
    pl.semaphore_wait(barrier, len(greeted))

    halos = []
    for n, ref in enumerate((own_items, own_sessions)):
        for side, to, rows_sent in ((0, after, ref.at[blocks - 8 : blocks]), (1, before, ref.at[0:8])):
            at = 2 * n + side
            halos.append(send(rows_sent, halo_ref.at[at], halo_send.at[at], halo_recv.at[at], to))

    def do_all(copies, act):
        for copy in copies:
            act(copy)

    def source(n, slab, own):
        every = (all_items, all_sessions)[n]
        return (own_items, short_ref)[n] if own else every.at[slab]

    def along_line(there, here):
        return [
            send(
                source(n, me, True), (all_items, all_sessions)[n].at[me],
                line_send.at[n * depth + there], line_recv.at[n * depth + here], there * PLANE + low,
            )
            for n in range(2)
        ]

    def in_plane(d, at_layer, own=False):
        slab = at_layer * PLANE + low
        copies = []
        for n in range(2):
            sem = (2 * d + n) * depth + at_layer
            copies.append(
                send(
                    source(n, slab, own), (all_items, all_sessions)[n].at[slab],
                    plane_send.at[sem], plane_recv.at[sem], me + steps[d],
                )
            )
        return copies

    def to_partner(r, at_layer, own=False):
        slab = at_layer * PLANE + low + ((0,) + steps)[r]
        copies = []
        for n in range(2):
            sem = (2 * r + n) * depth + at_layer
            copies.append(
                send(
                    source(n, slab, own), (all_items, all_sessions)[n].at[slab],
                    near_send.at[sem], near_recv.at[sem], partner,
                )
            )
        return copies

    def start(copies):
        do_all(copies, lambda c: c.start())

    start(halos)
    for o in reversed(others):
        start(along_line(o, layer))
    for d in range(3):
        start(in_plane(d, layer, True))
    start(to_partner(0, layer, True))

    sub = lax.broadcasted_iota(jnp.int32, (LANES, LANES), 0)
    lane = lax.broadcasted_iota(jnp.int32, (LANES, LANES), 1)
    low_lane = lax.broadcasted_iota(jnp.int32, (1, LANES), 1) < LANES // 2
    ids = lax.broadcasted_iota(jnp.int32, (rows, LANES), 0)
    gaps = (sub - LANES // 2 - lane, sub + LANES // 2 - lane)
    in_reach = [(jnp.abs(gap) <= WINDOW) & (gap != 0) for gap in gaps]
    ones = jnp.ones((8, 2 * LANES), jnp.float32).astype(jnp.bfloat16)
    links_ref[...] = jnp.zeros_like(links_ref)
    total_ref[...] = jnp.zeros_like(total_ref)

    def block(b, unused):
        def around(ref):
            turned = [pltpu.roll(ref[pl.ds(b + o, 1)], LANES // 2, 1) for o in (7, 8, 9)]
            return (
                jnp.where(low_lane, turned[0], turned[1]),
                jnp.where(low_lane, turned[1], turned[2]),
            )

        own_item, own_session = item_ref[pl.ds(b + 8, 1)], session_ref[pl.ds(b + 8, 1)]
        hot = jnp.concatenate([one_where(ids == item) for item in around(item_ref)], axis=1)
        linked = jnp.concatenate(
            [
                one_where((jnp.broadcast_to(session, (LANES, LANES)).T == own_session) & reach)
                for session, reach in zip(around(session_ref), in_reach)
            ],
            axis=0,
        )
        links = jnp.dot(jnp.concatenate([hot, ones], axis=0), linked, preferred_element_type=jnp.float32)
        links_ref[...] += lax.dot_general(
            links.astype(jnp.bfloat16), one_where(ids == own_item), NT, preferred_element_type=jnp.float32
        )
        total_ref[...] += links[rows:]
        return unused

    def forward_line(k):
        do_all(along_line(layer, others[k]), lambda c: c.wait_recv())
        for d in range(3):
            start(in_plane(d, others[k]))
        start(to_partner(0, others[k]))

    def forward_plane(at_layer):
        for d in range(3):
            do_all(in_plane(d, at_layer), lambda c: c.wait_recv())
            start(to_partner(d + 1, at_layer))

    cuts = [1 + (blocks - 2) * n // depth for n in range(depth + 1)]
    for n in range(depth):
        lax.fori_loop(cuts[n], cuts[n + 1], block, 0, unroll=4)
        if n < depth - 1:
            forward_line(n)
    for copy in halos:
        copy.wait()
    item_ref[0:8] = halo_ref[0]
    item_ref[8 + blocks : 16 + blocks] = halo_ref[1]
    session_ref[0:8] = jnp.where(me == 0, -1, halo_ref[2])
    session_ref[8 + blocks : 16 + blocks] = jnp.where(me == slabs - 1, -1, halo_ref[3])
    block(0, 0)
    block(blocks - 1, 0)

    share = rows // slabs
    tail = jnp.concatenate(
        [links_ref[rows : rows + 1], total_ref[0:1], jnp.zeros((6 - share, LANES), jnp.float32)], axis=0
    )
    for d in range(slabs):
        at = (d % 2, d // 2 % 4, d // PLANE)
        pair_out[at + (slice(0, share),)] = links_ref[d * share : (d + 1) * share]
        pair_out[at + (slice(share, 8),)] = tail

    pair = send(pair_out.at[1 - parity], pair_in, pair_sems.at[0], pair_sems.at[1], partner)
    pair.start()
    forward_plane(layer)
    pair.wait()
    plane_out[...] = pair_out[parity] + pair_in[...]

    def head_plane(d):
        to = me + steps[d]
        return send(
            plane_out.at[lax.rem(to // 2, 4)], plane_in.at[d], head_plane_send.at[d], head_plane_recv.at[d], to
        )

    for d in range(3):
        head_plane(d).start()
    for k in range(depth - 2):
        forward_plane(others[k])
    for d in range(3):
        head_plane(d).wait()
    line_out[...] = plane_out[quad] + plane_in[0] + plane_in[1] + plane_in[2]

    def head_line(there, here):
        return send(
            line_out.at[there], line_in.at[layer], head_line_send.at[there], head_line_recv.at[here],
            there * PLANE + low,
        )

    for o in others:
        head_line(o, layer).start()
    line_in[layer] = line_out[layer]
    for k in range(max(0, depth - 2), depth - 1):
        forward_plane(others[k])
    for o in others:
        head_line(o, o).wait_recv()
    head_ref[...] = jnp.sum(line_in[...], axis=0)
    for at_layer in [layer] + others:
        for r in range(4):
            do_all(to_partner(r, at_layer), lambda c: c.wait())
        for d in range(3):
            do_all(in_plane(d, at_layer), lambda c: c.wait_send())
    for o in others:
        do_all(along_line(o, layer), lambda c: c.wait_send())
        head_line(o, o).wait_send()


def take_windows(code_ref, length, start):
    whole, part = start >> 3, start & 7
    bits = max(1, (length // 8 - 1).bit_length())
    keep = 8 * ((1 << (bits - 1)) + 4)
    value = None
    for bit in reversed(range(bits)):
        step = 8 << bit
        keep = 8 * ((1 << bit) + 4)
        chosen = ((whole >> bit) & 1) == 1
        if value is None:
            low, high = code_ref[0:keep, :], code_ref[step : step + keep, :]
        else:
            low, high = value[0:keep], value[step : step + keep]
        value = jnp.where(chosen, high, low)
    for bit in (2, 1, 0):
        chosen = ((part >> bit) & 1) == 1
        value = jnp.where(chosen, pltpu.roll(value, value.shape[0] - (1 << bit), 0), value)
    return value[0:32]


def tile_kernel(rows, length, half, base_ref, all_items, all_sessions, count_ref, margin_ref, flat_ref, code_ref, key_ref):
    item_mask = (1 << ITEM_BITS) - 1
    base = base_ref[0]
    count_ref[...] = jnp.zeros_like(count_ref)
    margin_ref[...] = jnp.zeros_like(margin_ref)
    band = 2 * half
    band_rows = band // LANES
    chunk = 8 * math.gcd(length // 8, 16)
    slabs, blocks, unused_lanes = all_items.shape
    for n in range(slabs):
        flat_ref[n * blocks : (n + 1) * blocks] = all_items[n] | (all_sessions[n].astype(jnp.int32) << ITEM_BITS)
    per = length // LANES
    for r in range(per):
        code_ref[16 + r * LANES : 16 + (r + 1) * LANES] = flat_ref[pl.ds(r, LANES, stride=per), :].T
    lane = lax.broadcasted_iota(jnp.int32, (16, LANES), 1)
    code_ref[0:16] = jnp.where(lane == 0, -1, pltpu.roll(code_ref[length : length + 16], 1, 1))
    code_ref[length + 16 : length + 32] = jnp.where(
        lane == LANES - 1, -1, pltpu.roll(code_ref[16:32], LANES - 1, 1)
    )

    def fill(c, tops):
        at = pl.multiple_of(c * chunk, chunk)
        item = code_ref[pl.ds(at + 16, chunk), :] & item_mask
        place = (at + lax.broadcasted_iota(jnp.int32, (chunk, LANES), 0)).astype(jnp.float32)
        new = []
        for s in range(2):
            local = item - base - s * band
            mine = (local >= 0) & (local < band) & (item >= rows)
            key_ref[s, pl.ds(at, chunk), :] = jnp.where(mine, place, BIG)
            new.append(tops[s] + jnp.sum(mine.astype(jnp.int32), axis=0, keepdims=True))
        return tuple(new)

    none = jnp.zeros((1, LANES), jnp.int32)
    tally = lax.fori_loop(0, length // chunk, fill, (none, none))
    trips = (jnp.max(jnp.maximum(tally[0], tally[1])) + 1) // 2

    row_ids = lax.broadcasted_iota(jnp.int32, (rows, 2 * LANES), 0).astype(jnp.float32).astype(jnp.bfloat16)
    d_ids = lax.broadcasted_iota(jnp.int32, (32, LANES), 0)
    near = (d_ids >= 1) & (d_ids != 16)
    m_ids = lax.broadcasted_iota(jnp.int32, (max(8, band_rows), 2 * LANES), 0)
    l_ids = lax.broadcasted_iota(jnp.int32, (LANES, 2 * LANES), 0)
    tile = 256
    t_ids = lax.broadcasted_iota(jnp.int32, (tile, 2 * LANES), 0).astype(jnp.float32).astype(jnp.bfloat16)

    def body(unused, state):
        out = []
        for s in range(2):
            first, last = state[2 * s], state[2 * s + 1]
            key = key_ref[s]
            next_first = jnp.min(jnp.where(key > first, key, BIG), axis=0, keepdims=True)
            next_last = jnp.max(jnp.where(key < last, key, -1.0), axis=0, keepdims=True)
            first_ok = next_first < last
            last_ok = next_last > next_first
            out += [next_first, next_last]
            heads, weights, locals_ = [], [], []
            for at, ok in ((next_first, first_ok), (next_last, last_ok)):
                start = jnp.where(ok, at, 0.0).astype(jnp.int32)
                window = take_windows(code_ref, length, start)
                item, session = window & item_mask, window >> ITEM_BITS
                linked = (session == session[16:17]) & near & ok
                heads.append(jnp.where(linked & (item < rows), item, -1).astype(jnp.float32))
                weights.append(jnp.sum(jnp.where(linked, 1.0, 0.0), axis=0, keepdims=True))
                locals_.append(item[16:17] - base - s * band)
            head = jnp.concatenate(heads, axis=1)
            weight = jnp.concatenate(weights, axis=1)
            local = jnp.concatenate(locals_, axis=1)
            links = jnp.zeros((rows, 2 * LANES), jnp.bfloat16)
            for d in range(1, 32):
                if d != 16:
                    links += hot_columns(row_ids, head[d : d + 1])
            upper = local >= half
            side = jnp.broadcast_to(jnp.where(upper, 1.0, 0.0), (16, 2 * LANES)).astype(jnp.bfloat16)
            high_part = jnp.concatenate([links[n : n + 16] * side for n in range(0, rows, 16)], axis=0)
            pair = jnp.concatenate([links - high_part, high_part], axis=0)
            inner = jnp.where(upper, local - half, local)
            for t in range(half // tile):
                inside = (inner >= t * tile) & (inner < (t + 1) * tile)
                hot = hot_columns(t_ids, jnp.where(inside, inner - t * tile, -1).astype(jnp.float32))
                count_ref[s, :, t * tile : (t + 1) * tile] += lax.dot_general(
                    pair, hot, NT, preferred_element_type=jnp.float32
                )
            coarse = jnp.where(m_ids == (local >> 7), weight, 0.0).astype(jnp.bfloat16)
            fine = one_where(l_ids == (local & (LANES - 1)))
            margin_ref[s] += lax.dot_general(coarse, fine, NT, preferred_element_type=jnp.float32)
        return tuple(out)

    low = jnp.full((1, LANES), -1.0, jnp.float32)
    high = jnp.full((1, LANES), BIG, jnp.float32)
    lax.fori_loop(0, trips, body, (low, high, low, high))


def sketch_kernel(
    slabs, rows, half, width, scale, count_ref, margin_ref, head_ref, bits_ref, out_ref,
    log_ref, own_bits, head_bits, acc_ref, send_ref, recv_ref, bit_sems, send_sems, recv_sems,
):
    me = lax.axis_index("stream")
    barrier = greet_all(slabs, me)
    owned = 4 * half
    share = rows // slabs
    tile = min(half, 512)
    bit_copy = pltpu.make_async_copy(
        bits_ref.at[:, pl.ds(pl.multiple_of(me * owned, owned), owned)], own_bits, bit_sems.at[0]
    )
    head_copy = pltpu.make_async_copy(bits_ref.at[:, 0:rows], head_bits, bit_sems.at[1])
    bit_copy.start()
    head_copy.start()

    log_ref[...] = jnp.log(jnp.maximum(margin_ref[...], 1.0))
    row_log = jnp.log(jnp.maximum(head_ref[share : share + 1], 1.0))
    column_log = jnp.broadcast_to(row_log, (rows, LANES)).T
    total_log = jnp.log(jnp.sum(head_ref[share + 1 : share + 2], axis=1, keepdims=True))
    row_term = total_log - column_log[:, 0:1]
    groups = []
    for g in range(width // 8):
        word = 8 * g // BITS_PER_WORD
        groups.append((word, (word + 1) * BITS_PER_WORD - 8 * g, 8 * g - word * BITS_PER_WORD))

    def product(positive, words):
        size = words.shape[1]

        def wide(value):
            return jnp.concatenate([value] * (size // LANES), axis=1)

        shift = lax.broadcasted_iota(jnp.int32, (8, LANES), 0)
        upper = positive.astype(jnp.bfloat16)
        lower = (positive - upper.astype(jnp.float32)).astype(jnp.bfloat16)
        parts = []
        for word, split, offset in groups:
            now = jnp.broadcast_to(words[word : word + 1], (8, size))
            where_bit = jnp.left_shift(1, shift + offset)
            if split < 8:
                later = jnp.broadcast_to(words[word + 1 : word + 2], (8, size))
                now = jnp.where(wide(shift) >= split, later, now)
                place = jnp.where(shift >= split, shift - split, shift + offset)
                where_bit = jnp.left_shift(1, place)
            parts.append(jnp.where((now & wide(where_bit)) != 0, 1.0, -1.0))
        signs = jnp.concatenate(parts, axis=0).astype(jnp.bfloat16)
        both = jnp.concatenate([upper, lower], axis=0)
        value = lax.dot_general(both, signs, NT, preferred_element_type=jnp.float32)
        return value[0:rows] + value[rows:]

    head_copy.wait()
    row = lax.broadcasted_iota(jnp.int32, (8, LANES), 0)
    shared = jnp.concatenate(
        [jnp.where(row < share, head_ref[...], 0.0), jnp.zeros((rows - 8, LANES), jnp.float32)], axis=0
    )
    shared = pltpu.roll(shared, me * share, 0)
    ratio = jnp.log(jnp.maximum(shared, 1.0)) + total_log - row_log - column_log
    first_band = jnp.where(lax.axis_index("item") == 0, 1.0, 0.0)
    positive = jnp.where(shared > 0, jnp.maximum(ratio, 0.0), 0.0) * first_band
    acc_ref[...] = product(positive.T, head_bits[...])
    bit_copy.wait()

    for s in range(2):
        for h in range(2):

            def step(t, unused, s=s, h=h):
                at = pl.multiple_of(t * tile, tile)
                counts = count_ref[s, h * rows : (h + 1) * rows, pl.ds(at, tile)]
                first_log = h * (half // LANES) + t * (tile // LANES)
                col_log = jnp.concatenate(
                    [log_ref[s, pl.ds(first_log + n, 1), :] for n in range(tile // LANES)], axis=1
                )
                ratio = jnp.log(jnp.maximum(counts, 1.0)) + row_term - col_log
                positive = jnp.where(counts > 0, jnp.maximum(ratio, 0.0), 0.0)
                bit_at = pl.multiple_of(s * 2 * half + h * half + t * tile, tile)
                acc_ref[...] += product(positive, own_bits[:, pl.ds(bit_at, tile)])
                return unused

            lax.fori_loop(0, half // tile, step, 0, unroll=True)

    cuts = width // LANES
    for d in range(slabs):
        for c in range(cuts):
            send_ref[d, c * share : (c + 1) * share] = (
                acc_ref[d * share : (d + 1) * share, c * LANES : (c + 1) * LANES] * scale
            )
    pl.semaphore_wait(barrier, slabs - 1)
    exchange(slabs, me, send_ref, recv_ref, send_sems, recv_sems, True)
    exchange(slabs, me, send_ref, recv_ref, send_sems, recv_sems, False)
    summed = jnp.sum(recv_ref[...], axis=0)
    out_ref[...] = jnp.concatenate([summed[c * share : (c + 1) * share] for c in range(cuts)], axis=1)


def local(event_items, event_sessions, sketch_bits):
    slabs = lax.axis_size("stream")
    slab = event_items.shape[0]
    total_events = slab * slabs
    words, band_size = sketch_bits.shape
    owned = band_size // slabs
    rows, width, half = 128, 256, owned // 4
    me = lax.axis_index("stream")
    own_start = me * owned
    first_id = lax.axis_index("item") * band_size + own_start
    blocks = slab // LANES
    length = total_events // LANES

    dma = pltpu.SemaphoreType.DMA
    depth = slabs // PLANE
    any_space = pl.BlockSpec(memory_space=pltpu.HBM)
    all_items, all_sessions, head = pl.pallas_call(
        functools.partial(gather_kernel, slabs, rows, blocks),
        out_shape=(
            jax.ShapeDtypeStruct((slabs, blocks, LANES), jnp.int32),
            jax.ShapeDtypeStruct((slabs, blocks, LANES), jnp.int16),
            jax.ShapeDtypeStruct((8, LANES), jnp.float32),
        ),
        in_specs=[any_space, any_space],
        out_specs=(VMEM, VMEM, VMEM),
        scratch_shapes=[
            pltpu.VMEM((blocks, LANES), jnp.int32),
            pltpu.VMEM((blocks, LANES), jnp.int32),
            pltpu.VMEM((blocks, LANES), jnp.int16),
            pltpu.VMEM((4, 8, LANES), jnp.int32),
            pltpu.VMEM((blocks + 16, LANES), jnp.int32),
            pltpu.VMEM((blocks + 16, LANES), jnp.int32),
            pltpu.VMEM((rows + 8, LANES), jnp.float32),
            pltpu.VMEM((8, LANES), jnp.float32),
            pltpu.VMEM((2, 4, depth, 8, LANES), jnp.float32),
            pltpu.VMEM((4, depth, 8, LANES), jnp.float32),
            pltpu.VMEM((4, depth, 8, LANES), jnp.float32),
            pltpu.VMEM((3, depth, 8, LANES), jnp.float32),
            pltpu.VMEM((depth, 8, LANES), jnp.float32),
            pltpu.VMEM((depth, 8, LANES), jnp.float32),
            dma((2,)),
            dma((4,)),
            dma((4,)),
            dma((2 * depth,)),
            dma((2 * depth,)),
            dma((6 * depth,)),
            dma((6 * depth,)),
            dma((8 * depth,)),
            dma((8 * depth,)),
            dma((2,)),
            dma((3,)),
            dma((3,)),
            dma((depth,)),
            dma((depth,)),
        ],
        compiler_params=pltpu.CompilerParams(
            collective_id=0, has_side_effects=True, vmem_limit_bytes=VMEM_GRANT
        ),
        name="gather_events",
    )(event_items.reshape(blocks, LANES), event_sessions.reshape(blocks, LANES))

    band_rows = max(8, 2 * half // LANES)
    counts, margins = pl.pallas_call(
        functools.partial(tile_kernel, rows, length, half),
        out_shape=(
            jax.ShapeDtypeStruct((2, 2 * rows, half), jnp.float32),
            jax.ShapeDtypeStruct((2, band_rows, LANES), jnp.float32),
        ),
        in_specs=[pl.BlockSpec(memory_space=pltpu.SMEM), VMEM, VMEM],
        out_specs=(VMEM, VMEM),
        scratch_shapes=[
            pltpu.VMEM((length, LANES), jnp.int32),
            pltpu.VMEM((length + 32, LANES), jnp.int32),
            pltpu.VMEM((2, length, LANES), jnp.float32),
        ],
        compiler_params=pltpu.CompilerParams(vmem_limit_bytes=VMEM_GRANT),
        name="tile_counts",
    )(first_id.astype(jnp.int32)[None], all_items, all_sessions)

    own_rows = pl.pallas_call(
        functools.partial(sketch_kernel, slabs, rows, half, width, 1.0 / math.sqrt(total_events)),
        out_shape=jax.ShapeDtypeStruct((rows // slabs, width), jnp.float32),
        in_specs=[VMEM] * 3 + [pl.BlockSpec(memory_space=pl.ANY)],
        out_specs=VMEM,
        scratch_shapes=[
            pltpu.VMEM((2, band_rows, LANES), jnp.float32),
            pltpu.VMEM((words, owned), jnp.int32),
            pltpu.VMEM((words, rows), jnp.int32),
            pltpu.VMEM((rows, width), jnp.float32),
            pltpu.VMEM((slabs, 8, LANES), jnp.float32),
            pltpu.VMEM((slabs, 8, LANES), jnp.float32),
            dma((2,)),
            dma((slabs,)),
            dma((slabs,)),
        ],
        compiler_params=pltpu.CompilerParams(
            collective_id=1, has_side_effects=True, vmem_limit_bytes=VMEM_GRANT
        ),
        name="sketch_tile",
    )(counts, margins, head, sketch_bits)
    if lax.axis_size("item") > 1:
        own_rows = lax.psum(own_rows, "item")
    return own_rows


def solution(mesh):
    placed = (P("stream"), P("stream"), P(None, "item"))
    return jax.shard_map(
        local, mesh=mesh, in_specs=placed, out_specs=P("stream", None), check_vma=False
    )
```

```python
import functools
import math

import jax
import jax.numpy as jnp
from jax import lax
from jax.experimental import pallas as pl
from jax.experimental.pallas import tpu as pltpu
from jax.sharding import PartitionSpec as P

WINDOW = 15
ITEM_BITS = 18
LANES = 128
BITS_PER_WORD = 18
BIG = 1.0e6
PLANE = 8
VMEM_GRANT = 45 * 1024 * 1024
NT = (((1,), (1,)), ((), ()))
VMEM = pl.BlockSpec(memory_space=pltpu.VMEM)


def one_where(mask):
    return jnp.where(mask, 1.0, 0.0).astype(jnp.bfloat16)


def hot_columns(ids, values):
    row = jnp.broadcast_to(values, (16, values.shape[1])).astype(jnp.bfloat16)
    one, zero = jnp.ones((), jnp.bfloat16), jnp.zeros((), jnp.bfloat16)
    return jnp.concatenate(
        [jnp.where(ids[n : n + 16] == row, one, zero) for n in range(0, ids.shape[0], 16)], axis=0
    )


def greet_all(slabs, me):
    barrier = pltpu.get_barrier_semaphore()

    for k in range(1, slabs):
        pl.semaphore_signal(
            barrier, inc=1, device_id={"stream": lax.rem(me + k, slabs)}, device_id_type=pl.DeviceIdType.MESH
        )
    return barrier


def send(src, dst, send_sem, recv_sem, to):
    return pltpu.make_async_remote_copy(
        src_ref=src,
        dst_ref=dst,
        send_sem=send_sem,
        recv_sem=recv_sem,
        device_id={"stream": to},
        device_id_type=pl.DeviceIdType.MESH,
    )


def each(low, high, do):
    for k in range(low, high):
        do(k)


def exchange(slabs, me, out_ref, in_ref, send_sems, recv_sems, start):
    def copy(k):
        to = lax.rem(me + k, slabs)
        return send(out_ref.at[to], in_ref.at[me], send_sems.at[k], recv_sems.at[k], to)

    if start:
        each(1, slabs, lambda k: copy(k).start())
        in_ref[me] = out_ref[me]
    else:
        each(1, slabs, lambda k: copy(k).wait())


def gather_kernel(
    slabs, rows, blocks, own_ref, all_ref, head_ref,
    own_pack, halo_ref, item_ref, session_ref, links_ref, total_ref,
    pair_out, pair_in, plane_out, plane_in, line_out, line_in,
    halo_send, halo_recv, line_send, line_recv, plane_send, plane_recv, near_send, near_recv,
    pair_sems, head_plane_send, head_plane_recv, head_line_send, head_line_recv,
):
    me = lax.axis_index("stream")
    depth = slabs // PLANE
    layer, low = me // PLANE, lax.rem(me, PLANE)
    parity, quad = lax.rem(me, 2), lax.rem(me // 2, 4)

    def flip(bit):
        return bit - 2 * bit * lax.rem(me // bit, 2)

    partner = me + flip(1)
    steps = (flip(2), flip(4), flip(2) + flip(4))
    after, before = lax.rem(me + 1, slabs), lax.rem(me + slabs - 1, slabs)

    def other_layer(k):
        rising = k + (k - layer + depth) // depth
        mirrored = depth - 1 - layer
        falling = depth - 1 - k - (k - mirrored + depth) // depth
        high = layer // ((depth + 1) // 2)
        return rising + (falling - rising) * lax.rem(high, 2)

    others = [other_layer(k) for k in range(depth - 1)]
    own_items, own_sessions = own_ref.at[0], own_ref.at[1]
    barrier = pltpu.get_barrier_semaphore()
    greeted = [partner, after, before] + [me + step for step in steps] + [o * PLANE + low for o in others]
    for to in greeted:
        pl.semaphore_signal(
            barrier, inc=1, device_id={"stream": to}, device_id_type=pl.DeviceIdType.MESH
        )
    half = blocks // 2
    own_pack[0:blocks] = own_items[...]
    own_pack[blocks : blocks + half] = own_sessions[0:half] | (own_sessions[half:blocks] << 16)
    all_ref[me] = own_pack[...]
    item_ref[8 : 8 + blocks] = own_items[...]
    session_ref[8 : 8 + blocks] = own_sessions[...]
    sub = lax.broadcasted_iota(jnp.int32, (LANES, LANES), 0)
    lane = lax.broadcasted_iota(jnp.int32, (LANES, LANES), 1)
    low_lane = lax.broadcasted_iota(jnp.int32, (1, LANES), 1) < LANES // 2
    ids = lax.broadcasted_iota(jnp.int32, (rows, LANES), 0)
    gaps = (sub - LANES // 2 - lane, sub + LANES // 2 - lane)
    in_reach = [(jnp.abs(gap) <= WINDOW) & (gap != 0) for gap in gaps]
    ones = jnp.ones((8, 2 * LANES), jnp.float32).astype(jnp.bfloat16)
    links_ref[...] = jnp.zeros_like(links_ref)
    total_ref[...] = jnp.zeros_like(total_ref)

    def block(b, unused):
        def around(ref):
            turned = [pltpu.roll(ref[pl.ds(b + o, 1)], LANES // 2, 1) for o in (7, 8, 9)]
            return (
                jnp.where(low_lane, turned[0], turned[1]),
                jnp.where(low_lane, turned[1], turned[2]),
            )

        own_item, own_session = item_ref[pl.ds(b + 8, 1)], session_ref[pl.ds(b + 8, 1)]
        hot = jnp.concatenate([one_where(ids == item) for item in around(item_ref)], axis=1)
        linked = jnp.concatenate(
            [
                one_where((jnp.broadcast_to(session, (LANES, LANES)).T == own_session) & reach)
                for session, reach in zip(around(session_ref), in_reach)
            ],
            axis=0,
        )
        links = jnp.dot(jnp.concatenate([hot, ones], axis=0), linked, preferred_element_type=jnp.float32)
        links_ref[...] += lax.dot_general(
            links.astype(jnp.bfloat16), one_where(ids == own_item), NT, preferred_element_type=jnp.float32
        )
        total_ref[...] += links[rows:]
        return unused

    inner = [1 + (blocks - 2) * n // 30 for n in (0, 15, 30)]

    def blocks_of(n):
        lax.fori_loop(inner[n], inner[n + 1], block, 0, unroll=5)

    blocks_of(0)
    pl.semaphore_wait(barrier, len(greeted))

    halos = []
    for n, ref in enumerate((own_items, own_sessions)):
        for side, to, rows_sent in ((0, after, ref.at[blocks - 8 : blocks]), (1, before, ref.at[0:8])):
            at = 2 * n + side
            halos.append(send(rows_sent, halo_ref.at[at], halo_send.at[at], halo_recv.at[at], to))

    def do_all(copies, act):
        for copy in copies:
            act(copy)

    def along_line(there, here):
        return send(
            own_pack, all_ref.at[me], line_send.at[there], line_recv.at[here], there * PLANE + low
        )

    def in_plane(d, at_layer, own=False):
        slab = all_ref.at[at_layer * PLANE + low]
        sem = d * depth + at_layer
        return send(own_pack if own else slab, slab, plane_send.at[sem], plane_recv.at[sem], me + steps[d])

    def to_partner(r, at_layer, own=False):
        slab = all_ref.at[at_layer * PLANE + low + ((0,) + steps)[r]]
        sem = r * depth + at_layer
        return send(own_pack if own else slab, slab, near_send.at[sem], near_recv.at[sem], partner)

    do_all(halos, lambda c: c.start())
    for o in reversed(others):
        along_line(o, layer).start()
    for d in range(3):
        in_plane(d, layer, True).start()
    to_partner(0, layer, True).start()

    def forward_line(k):
        along_line(layer, others[k]).wait_recv()
        for d in range(3):
            in_plane(d, others[k]).start()
        to_partner(0, others[k]).start()

    def forward_plane(at_layer):
        for d in range(3):
            in_plane(d, at_layer).wait_recv()
            to_partner(d + 1, at_layer).start()

    blocks_of(1)
    forward_line(0)
    for copy in halos:
        copy.wait()
    item_ref[0:8] = halo_ref[0]
    item_ref[8 + blocks : 16 + blocks] = halo_ref[1]
    session_ref[0:8] = jnp.where(me == 0, -1, halo_ref[2])
    session_ref[8 + blocks : 16 + blocks] = jnp.where(me == slabs - 1, -1, halo_ref[3])
    block(0, 0)
    block(blocks - 1, 0)

    share = rows // slabs
    tail = jnp.concatenate(
        [links_ref[rows : rows + 1], total_ref[0:1], jnp.zeros((6 - share, LANES), jnp.float32)], axis=0
    )
    for d in range(slabs):
        at = (d % 2, d // PLANE, d // 2 % 4)
        pair_out[at + (slice(0, share),)] = links_ref[d * share : (d + 1) * share]
        pair_out[at + (slice(share, 8),)] = tail

    pair = send(pair_out.at[1 - parity], pair_in, pair_sems.at[0], pair_sems.at[1], partner)
    pair.start()
    forward_line(1)
    forward_plane(layer)
    pair.wait()
    line_out[...] = pair_out[parity] + pair_in[...]

    def head_line(there, here):
        return send(
            line_out.at[there], line_in.at[layer], head_line_send.at[there], head_line_recv.at[here],
            there * PLANE + low,
        )

    for o in others:
        head_line(o, layer).start()
    line_in[layer] = line_out[layer]
    for k in range(2, depth - 1):
        forward_line(k)
    for o in others[:-1]:
        forward_plane(o)
    for o in others:
        head_line(o, o).wait_recv()
    plane_out[...] = jnp.sum(line_in[...], axis=0)

    def head_plane(d):
        to = me + steps[d]
        return send(
            plane_out.at[lax.rem(to // 2, 4)], plane_in.at[d], head_plane_send.at[d], head_plane_recv.at[d], to
        )

    for d in range(3):
        head_plane(d).start()
    for o in others[-1:]:
        forward_plane(o)
    for at_layer in [layer] + others:
        for r in range(4):
            to_partner(r, at_layer).wait()
        for d in range(3):
            in_plane(d, at_layer).wait_send()
    for o in others:
        along_line(o, layer).wait_send()
        head_line(o, o).wait_send()
    for d in range(3):
        head_plane(d).wait()
    head_ref[...] = plane_out[quad] + plane_in[0] + plane_in[1] + plane_in[2]


def take_windows(code_ref, length, start):
    whole, part = start >> 3, start & 7
    bits = max(1, (length // 8 - 1).bit_length())
    keep = 8 * ((1 << (bits - 1)) + 4)
    value = None
    for bit in reversed(range(bits)):
        step = 8 << bit
        keep = 8 * ((1 << bit) + 4)
        chosen = ((whole >> bit) & 1) == 1
        if value is None:
            low, high = code_ref[0:keep, :], code_ref[step : step + keep, :]
        else:
            low, high = value[0:keep], value[step : step + keep]
        value = jnp.where(chosen, high, low)
    for bit in (2, 1, 0):
        chosen = ((part >> bit) & 1) == 1
        value = jnp.where(chosen, pltpu.roll(value, value.shape[0] - (1 << bit), 0), value)
    return value[0:32]


def tile_kernel(rows, length, half, base_ref, all_ref, count_ref, margin_ref, flat_ref, code_ref, key_ref):
    item_mask = (1 << ITEM_BITS) - 1
    base = base_ref[0]
    count_ref[...] = jnp.zeros_like(count_ref)
    margin_ref[...] = jnp.zeros_like(margin_ref)
    band = 2 * half
    band_rows = band // LANES
    chunk = 8 * math.gcd(length // 8, 16)
    slabs, blocks = all_ref.shape[0], all_ref.shape[1] * 2 // 3
    for n in range(slabs):
        paired = all_ref[n, blocks:]
        sessions = jnp.concatenate([paired & 0xFFFF, paired >> 16], axis=0)
        flat_ref[n * blocks : (n + 1) * blocks] = all_ref[n, 0:blocks] | (sessions << ITEM_BITS)
    per = length // LANES
    for r in range(per):
        code_ref[16 + r * LANES : 16 + (r + 1) * LANES] = flat_ref[pl.ds(r, LANES, stride=per), :].T
    lane = lax.broadcasted_iota(jnp.int32, (16, LANES), 1)
    code_ref[0:16] = jnp.where(lane == 0, -1, pltpu.roll(code_ref[length : length + 16], 1, 1))
    code_ref[length + 16 : length + 32] = jnp.where(
        lane == LANES - 1, -1, pltpu.roll(code_ref[16:32], LANES - 1, 1)
    )

    def fill(c, tops):
        at = pl.multiple_of(c * chunk, chunk)
        item = code_ref[pl.ds(at + 16, chunk), :] & item_mask
        place = (at + lax.broadcasted_iota(jnp.int32, (chunk, LANES), 0)).astype(jnp.float32)
        new = []
        for s in range(2):
            local = item - base - s * band
            mine = (local >= 0) & (local < band) & (item >= rows)
            key_ref[s, pl.ds(at, chunk), :] = jnp.where(mine, place, BIG)
            new.append(tops[s] + jnp.sum(mine.astype(jnp.int32), axis=0, keepdims=True))
        return tuple(new)

    none = jnp.zeros((1, LANES), jnp.int32)
    tally = lax.fori_loop(0, length // chunk, fill, (none, none))
    trips = (jnp.max(jnp.maximum(tally[0], tally[1])) + 1) // 2

    row_ids = lax.broadcasted_iota(jnp.int32, (rows, 2 * LANES), 0).astype(jnp.float32).astype(jnp.bfloat16)
    d_ids = lax.broadcasted_iota(jnp.int32, (32, LANES), 0)
    near = (d_ids >= 1) & (d_ids != 16)
    m_ids = lax.broadcasted_iota(jnp.int32, (max(8, band_rows), 2 * LANES), 0)
    l_ids = lax.broadcasted_iota(jnp.int32, (LANES, 2 * LANES), 0)
    tile = 256
    t_ids = lax.broadcasted_iota(jnp.int32, (tile, 2 * LANES), 0).astype(jnp.float32).astype(jnp.bfloat16)

    def body(unused, state):
        out = []
        for s in range(2):
            first, last = state[2 * s], state[2 * s + 1]
            key = key_ref[s]
            next_first = jnp.min(jnp.where(key > first, key, BIG), axis=0, keepdims=True)
            next_last = jnp.max(jnp.where(key < last, key, -1.0), axis=0, keepdims=True)
            first_ok = next_first < last
            last_ok = next_last > next_first
            out += [next_first, next_last]
            heads, weights, locals_ = [], [], []
            for at, ok in ((next_first, first_ok), (next_last, last_ok)):
                start = jnp.where(ok, at, 0.0).astype(jnp.int32)
                window = take_windows(code_ref, length, start)
                item, session = window & item_mask, window >> ITEM_BITS
                linked = (session == session[16:17]) & near & ok
                heads.append(jnp.where(linked & (item < rows), item, -1).astype(jnp.float32))
                weights.append(jnp.sum(jnp.where(linked, 1.0, 0.0), axis=0, keepdims=True))
                locals_.append(item[16:17] - base - s * band)
            head = jnp.concatenate(heads, axis=1)
            weight = jnp.concatenate(weights, axis=1)
            local = jnp.concatenate(locals_, axis=1)
            links = jnp.zeros((rows, 2 * LANES), jnp.bfloat16)
            for d in range(1, 32):
                if d != 16:
                    links += hot_columns(row_ids, head[d : d + 1])
            upper = local >= half
            side = jnp.broadcast_to(jnp.where(upper, 1.0, 0.0), (16, 2 * LANES)).astype(jnp.bfloat16)
            high_part = jnp.concatenate([links[n : n + 16] * side for n in range(0, rows, 16)], axis=0)
            pair = jnp.concatenate([links - high_part, high_part], axis=0)
            inner = jnp.where(upper, local - half, local)
            for t in range(half // tile):
                inside = (inner >= t * tile) & (inner < (t + 1) * tile)
                hot = hot_columns(t_ids, jnp.where(inside, inner - t * tile, -1).astype(jnp.float32))
                count_ref[s, :, t * tile : (t + 1) * tile] += lax.dot_general(
                    pair, hot, NT, preferred_element_type=jnp.float32
                )
            coarse = jnp.where(m_ids == (local >> 7), weight, 0.0).astype(jnp.bfloat16)
            fine = one_where(l_ids == (local & (LANES - 1)))
            margin_ref[s] += lax.dot_general(coarse, fine, NT, preferred_element_type=jnp.float32)
        return tuple(out)

    low = jnp.full((1, LANES), -1.0, jnp.float32)
    high = jnp.full((1, LANES), BIG, jnp.float32)
    lax.fori_loop(0, trips, body, (low, high, low, high))


def sketch_kernel(
    slabs, rows, half, width, scale, count_ref, margin_ref, head_ref, bits_ref, out_ref,
    log_ref, own_bits, head_bits, acc_ref, send_ref, recv_ref, bit_sems, send_sems, recv_sems,
):
    me = lax.axis_index("stream")
    barrier = greet_all(slabs, me)
    owned = 4 * half
    share = rows // slabs
    tile = min(half, 512)
    bit_copy = pltpu.make_async_copy(
        bits_ref.at[:, pl.ds(pl.multiple_of(me * owned, owned), owned)], own_bits, bit_sems.at[0]
    )
    head_copy = pltpu.make_async_copy(bits_ref.at[:, 0:rows], head_bits, bit_sems.at[1])
    bit_copy.start()
    head_copy.start()

    log_ref[...] = jnp.log(jnp.maximum(margin_ref[...], 1.0))
    row_log = jnp.log(jnp.maximum(head_ref[share : share + 1], 1.0))
    column_log = jnp.broadcast_to(row_log, (rows, LANES)).T
    total_log = jnp.log(jnp.sum(head_ref[share + 1 : share + 2], axis=1, keepdims=True))
    row_term = total_log - column_log[:, 0:1]
    groups = []
    for g in range(width // 8):
        word = 8 * g // BITS_PER_WORD
        groups.append((word, (word + 1) * BITS_PER_WORD - 8 * g, 8 * g - word * BITS_PER_WORD))

    def product(positive, words):
        size = words.shape[1]

        def wide(value):
            return jnp.concatenate([value] * (size // LANES), axis=1)

        shift = lax.broadcasted_iota(jnp.int32, (8, LANES), 0)
        upper = positive.astype(jnp.bfloat16)
        lower = (positive - upper.astype(jnp.float32)).astype(jnp.bfloat16)
        parts = []
        for word, split, offset in groups:
            now = jnp.broadcast_to(words[word : word + 1], (8, size))
            where_bit = jnp.left_shift(1, shift + offset)
            if split < 8:
                later = jnp.broadcast_to(words[word + 1 : word + 2], (8, size))
                now = jnp.where(wide(shift) >= split, later, now)
                place = jnp.where(shift >= split, shift - split, shift + offset)
                where_bit = jnp.left_shift(1, place)
            parts.append(jnp.where((now & wide(where_bit)) != 0, 1.0, -1.0))
        signs = jnp.concatenate(parts, axis=0).astype(jnp.bfloat16)
        both = jnp.concatenate([upper, lower], axis=0)
        value = lax.dot_general(both, signs, NT, preferred_element_type=jnp.float32)
        return value[0:rows] + value[rows:]

    head_copy.wait()
    row = lax.broadcasted_iota(jnp.int32, (8, LANES), 0)
    shared = jnp.concatenate(
        [jnp.where(row < share, head_ref[...], 0.0), jnp.zeros((rows - 8, LANES), jnp.float32)], axis=0
    )
    shared = pltpu.roll(shared, me * share, 0)
    ratio = jnp.log(jnp.maximum(shared, 1.0)) + total_log - row_log - column_log
    first_band = jnp.where(lax.axis_index("item") == 0, 1.0, 0.0)
    positive = jnp.where(shared > 0, jnp.maximum(ratio, 0.0), 0.0) * first_band
    acc_ref[...] = product(positive.T, head_bits[...])
    bit_copy.wait()

    for s in range(2):
        for h in range(2):

            def step(t, unused, s=s, h=h):
                at = pl.multiple_of(t * tile, tile)
                counts = count_ref[s, h * rows : (h + 1) * rows, pl.ds(at, tile)]
                first_log = h * (half // LANES) + t * (tile // LANES)
                col_log = jnp.concatenate(
                    [log_ref[s, pl.ds(first_log + n, 1), :] for n in range(tile // LANES)], axis=1
                )
                ratio = jnp.log(jnp.maximum(counts, 1.0)) + row_term - col_log
                positive = jnp.where(counts > 0, jnp.maximum(ratio, 0.0), 0.0)
                bit_at = pl.multiple_of(s * 2 * half + h * half + t * tile, tile)
                acc_ref[...] += product(positive, own_bits[:, pl.ds(bit_at, tile)])
                return unused

            lax.fori_loop(0, half // tile, step, 0, unroll=True)

    cuts = width // LANES
    for d in range(slabs):
        for c in range(cuts):
            send_ref[d, c * share : (c + 1) * share] = (
                acc_ref[d * share : (d + 1) * share, c * LANES : (c + 1) * LANES] * scale
            )
    pl.semaphore_wait(barrier, slabs - 1)
    exchange(slabs, me, send_ref, recv_ref, send_sems, recv_sems, True)
    exchange(slabs, me, send_ref, recv_ref, send_sems, recv_sems, False)
    summed = jnp.sum(recv_ref[...], axis=0)
    out_ref[...] = jnp.concatenate([summed[c * share : (c + 1) * share] for c in range(cuts)], axis=1)


def local(event_items, event_sessions, sketch_bits):
    slabs = lax.axis_size("stream")
    slab = event_items.shape[0]
    total_events = slab * slabs
    words, band_size = sketch_bits.shape
    owned = band_size // slabs
    rows, width, half = 128, 256, owned // 4
    me = lax.axis_index("stream")
    own_start = me * owned
    first_id = lax.axis_index("item") * band_size + own_start
    blocks = slab // LANES
    length = total_events // LANES

    dma = pltpu.SemaphoreType.DMA
    depth = slabs // PLANE
    events, head = pl.pallas_call(
        functools.partial(gather_kernel, slabs, rows, blocks),
        out_shape=(
            jax.ShapeDtypeStruct((slabs, blocks * 3 // 2, LANES), jnp.int32),
            jax.ShapeDtypeStruct((8, LANES), jnp.float32),
        ),
        in_specs=[VMEM],
        out_specs=(VMEM, VMEM),
        scratch_shapes=[
            pltpu.VMEM((blocks * 3 // 2, LANES), jnp.int32),
            pltpu.VMEM((4, 8, LANES), jnp.int32),
            pltpu.VMEM((blocks + 16, LANES), jnp.int32),
            pltpu.VMEM((blocks + 16, LANES), jnp.int32),
            pltpu.VMEM((rows + 8, LANES), jnp.float32),
            pltpu.VMEM((8, LANES), jnp.float32),
            pltpu.VMEM((2, depth, 4, 8, LANES), jnp.float32),
            pltpu.VMEM((depth, 4, 8, LANES), jnp.float32),
            pltpu.VMEM((4, 8, LANES), jnp.float32),
            pltpu.VMEM((3, 8, LANES), jnp.float32),
            pltpu.VMEM((depth, 4, 8, LANES), jnp.float32),
            pltpu.VMEM((depth, 4, 8, LANES), jnp.float32),
            dma((4,)),
            dma((4,)),
            dma((depth,)),
            dma((depth,)),
            dma((3 * depth,)),
            dma((3 * depth,)),
            dma((4 * depth,)),
            dma((4 * depth,)),
            dma((2,)),
            dma((3,)),
            dma((3,)),
            dma((depth,)),
            dma((depth,)),
        ],
        compiler_params=pltpu.CompilerParams(
            collective_id=0, has_side_effects=True, vmem_limit_bytes=VMEM_GRANT
        ),
        name="gather_events",
    )(jnp.stack([event_items, event_sessions]).reshape(2, blocks, LANES))

    band_rows = max(8, 2 * half // LANES)
    counts, margins = pl.pallas_call(
        functools.partial(tile_kernel, rows, length, half),
        out_shape=(
            jax.ShapeDtypeStruct((2, 2 * rows, half), jnp.float32),
            jax.ShapeDtypeStruct((2, band_rows, LANES), jnp.float32),
        ),
        in_specs=[pl.BlockSpec(memory_space=pltpu.SMEM), VMEM],
        out_specs=(VMEM, VMEM),
        scratch_shapes=[
            pltpu.VMEM((length, LANES), jnp.int32),
            pltpu.VMEM((length + 32, LANES), jnp.int32),
            pltpu.VMEM((2, length, LANES), jnp.float32),
        ],
        compiler_params=pltpu.CompilerParams(vmem_limit_bytes=VMEM_GRANT),
        name="tile_counts",
    )(first_id.astype(jnp.int32)[None], events)

    own_rows = pl.pallas_call(
        functools.partial(sketch_kernel, slabs, rows, half, width, 1.0 / math.sqrt(total_events)),
        out_shape=jax.ShapeDtypeStruct((rows // slabs, width), jnp.float32),
        in_specs=[VMEM] * 3 + [pl.BlockSpec(memory_space=pl.ANY)],
        out_specs=VMEM,
        scratch_shapes=[
            pltpu.VMEM((2, band_rows, LANES), jnp.float32),
            pltpu.VMEM((words, owned), jnp.int32),
            pltpu.VMEM((words, rows), jnp.int32),
            pltpu.VMEM((rows, width), jnp.float32),
            pltpu.VMEM((slabs, 8, LANES), jnp.float32),
            pltpu.VMEM((slabs, 8, LANES), jnp.float32),
            dma((2,)),
            dma((slabs,)),
            dma((slabs,)),
        ],
        compiler_params=pltpu.CompilerParams(
            collective_id=1, has_side_effects=True, vmem_limit_bytes=VMEM_GRANT
        ),
        name="sketch_tile",
    )(counts, margins, head, sketch_bits)
    if lax.axis_size("item") > 1:
        own_rows = lax.psum(own_rows, "item")
    return own_rows


def solution(mesh):
    placed = (P("stream"), P("stream"), P(None, "item"))
    return jax.shard_map(
        local, mesh=mesh, in_specs=placed, out_specs=P("stream", None), check_vma=False
    )
```

```python
import functools
import math

import jax
import jax.numpy as jnp
from jax import lax
from jax.experimental import pallas as pl
from jax.experimental.pallas import tpu as pltpu
from jax.sharding import PartitionSpec as P

WINDOW = 15
ITEM_BITS = 18
LANES = 128
BITS_PER_WORD = 18
PLANE = 8
VMEM_GRANT = 45 * 1024 * 1024
NT = (((1,), (1,)), ((), ()))
VMEM = pl.BlockSpec(memory_space=pltpu.VMEM)


def one_where(mask):
    return jnp.where(mask, 1.0, 0.0).astype(jnp.bfloat16)


def hot_columns(ids, values):
    row = jnp.broadcast_to(values, (16, values.shape[1])).astype(jnp.bfloat16)
    one, zero = jnp.ones((), jnp.bfloat16), jnp.zeros((), jnp.bfloat16)
    return jnp.concatenate(
        [jnp.where(ids[n : n + 16] == row, one, zero) for n in range(0, ids.shape[0], 16)], axis=0
    )


def greet_all(slabs, me):
    barrier = pltpu.get_barrier_semaphore()

    for k in range(1, slabs):
        pl.semaphore_signal(
            barrier, inc=1, device_id={"stream": lax.rem(me + k, slabs)}, device_id_type=pl.DeviceIdType.MESH
        )
    return barrier


def send(src, dst, send_sem, recv_sem, to):
    return pltpu.make_async_remote_copy(
        src_ref=src,
        dst_ref=dst,
        send_sem=send_sem,
        recv_sem=recv_sem,
        device_id={"stream": to},
        device_id_type=pl.DeviceIdType.MESH,
    )


def each(low, high, do):
    for k in range(low, high):
        do(k)


def exchange(slabs, me, out_ref, in_ref, send_sems, recv_sems, start):
    def copy(k):
        to = lax.rem(me + k, slabs)
        return send(out_ref.at[to], in_ref.at[me], send_sems.at[k], recv_sems.at[k], to)

    if start:
        each(1, slabs, lambda k: copy(k).start())
        in_ref[me] = out_ref[me]
    else:
        each(1, slabs, lambda k: copy(k).wait())


def gather_kernel(
    slabs, rows, blocks, own_ref, all_ref, head_ref,
    own_pack, halo_ref, item_ref, session_ref, links_ref, total_ref,
    pair_out, pair_in, plane_out, plane_in, line_out, line_in,
    halo_send, halo_recv, line_send, line_recv, plane_send, plane_recv, near_send, near_recv,
    pair_sems, head_plane_send, head_plane_recv, head_line_send, head_line_recv,
):
    me = lax.axis_index("stream")
    depth = slabs // PLANE
    layer, low = me // PLANE, lax.rem(me, PLANE)
    parity, quad = lax.rem(me, 2), lax.rem(me // 2, 4)

    def flip(bit):
        return bit - 2 * bit * lax.rem(me // bit, 2)

    partner = me + flip(1)
    steps = (flip(2), flip(4), flip(2) + flip(4))
    after, before = lax.rem(me + 1, slabs), lax.rem(me + slabs - 1, slabs)

    def other_layer(k):
        rising = k + (k - layer + depth) // depth
        mirrored = depth - 1 - layer
        falling = depth - 1 - k - (k - mirrored + depth) // depth
        high = layer // ((depth + 1) // 2)
        return rising + (falling - rising) * lax.rem(high, 2)

    others = [other_layer(k) for k in range(depth - 1)]
    own_items, own_sessions = own_ref.at[0], own_ref.at[1]
    barrier = pltpu.get_barrier_semaphore()
    greeted = [partner, after, before] + [me + step for step in steps] + [o * PLANE + low for o in others]
    for to in greeted:
        pl.semaphore_signal(
            barrier, inc=1, device_id={"stream": to}, device_id_type=pl.DeviceIdType.MESH
        )
    half = blocks // 2
    own_pack[0:blocks] = own_items[...]
    own_pack[blocks : blocks + half] = own_sessions[0:half] | (own_sessions[half:blocks] << 16)
    all_ref[me] = own_pack[...]
    item_ref[8 : 8 + blocks] = own_items[...]
    session_ref[8 : 8 + blocks] = own_sessions[...]
    sub = lax.broadcasted_iota(jnp.int32, (LANES, LANES), 0)
    lane = lax.broadcasted_iota(jnp.int32, (LANES, LANES), 1)
    low_lane = lax.broadcasted_iota(jnp.int32, (1, LANES), 1) < LANES // 2
    ids = lax.broadcasted_iota(jnp.int32, (rows, LANES), 0)
    gaps = (sub - LANES // 2 - lane, sub + LANES // 2 - lane)
    in_reach = [(jnp.abs(gap) <= WINDOW) & (gap != 0) for gap in gaps]
    ones = jnp.ones((8, 2 * LANES), jnp.float32).astype(jnp.bfloat16)
    links_ref[...] = jnp.zeros_like(links_ref)
    total_ref[...] = jnp.zeros_like(total_ref)

    def block(b, unused):
        def around(ref):
            turned = [pltpu.roll(ref[pl.ds(b + o, 1)], LANES // 2, 1) for o in (7, 8, 9)]
            return (
                jnp.where(low_lane, turned[0], turned[1]),
                jnp.where(low_lane, turned[1], turned[2]),
            )

        own_item, own_session = item_ref[pl.ds(b + 8, 1)], session_ref[pl.ds(b + 8, 1)]
        hot = jnp.concatenate([one_where(ids == item) for item in around(item_ref)], axis=1)
        linked = jnp.concatenate(
            [
                one_where((jnp.broadcast_to(session, (LANES, LANES)).T == own_session) & reach)
                for session, reach in zip(around(session_ref), in_reach)
            ],
            axis=0,
        )
        links = jnp.dot(jnp.concatenate([hot, ones], axis=0), linked, preferred_element_type=jnp.float32)
        links_ref[...] += lax.dot_general(
            links.astype(jnp.bfloat16), one_where(ids == own_item), NT, preferred_element_type=jnp.float32
        )
        total_ref[...] += links[rows:]
        return unused

    inner = [1 + (blocks - 2) * n // 30 for n in (0, 15, 30)]

    def blocks_of(n):
        lax.fori_loop(inner[n], inner[n + 1], block, 0, unroll=5)

    blocks_of(0)
    pl.semaphore_wait(barrier, len(greeted))

    halos = []
    for n, ref in enumerate((own_items, own_sessions)):
        for side, to, rows_sent in ((0, after, ref.at[blocks - 8 : blocks]), (1, before, ref.at[0:8])):
            at = 2 * n + side
            halos.append(send(rows_sent, halo_ref.at[at], halo_send.at[at], halo_recv.at[at], to))

    def do_all(copies, act):
        for copy in copies:
            act(copy)

    def along_line(there, here):
        return send(
            own_pack, all_ref.at[me], line_send.at[there], line_recv.at[here], there * PLANE + low
        )

    def in_plane(d, at_layer, own=False):
        slab = all_ref.at[at_layer * PLANE + low]
        sem = d * depth + at_layer
        return send(own_pack if own else slab, slab, plane_send.at[sem], plane_recv.at[sem], me + steps[d])

    def to_partner(r, at_layer, own=False):
        slab = all_ref.at[at_layer * PLANE + low + ((0,) + steps)[r]]
        sem = r * depth + at_layer
        return send(own_pack if own else slab, slab, near_send.at[sem], near_recv.at[sem], partner)

    do_all(halos, lambda c: c.start())
    for o in reversed(others):
        along_line(o, layer).start()
    for d in range(3):
        in_plane(d, layer, True).start()
    to_partner(0, layer, True).start()

    def forward_line(k):
        along_line(layer, others[k]).wait_recv()
        for d in range(3):
            in_plane(d, others[k]).start()
        to_partner(0, others[k]).start()

    def forward_plane(at_layer):
        for d in range(3):
            in_plane(d, at_layer).wait_recv()
            to_partner(d + 1, at_layer).start()

    blocks_of(1)
    forward_line(0)
    for copy in halos:
        copy.wait()
    item_ref[0:8] = halo_ref[0]
    item_ref[8 + blocks : 16 + blocks] = halo_ref[1]
    session_ref[0:8] = jnp.where(me == 0, -1, halo_ref[2])
    session_ref[8 + blocks : 16 + blocks] = jnp.where(me == slabs - 1, -1, halo_ref[3])
    block(0, 0)
    block(blocks - 1, 0)

    share = rows // slabs
    tail = jnp.concatenate(
        [links_ref[rows : rows + 1], total_ref[0:1], jnp.zeros((6 - share, LANES), jnp.float32)], axis=0
    )
    for d in range(slabs):
        at = (d % 2, d // PLANE, d // 2 % 4)
        pair_out[at + (slice(0, share),)] = links_ref[d * share : (d + 1) * share]
        pair_out[at + (slice(share, 8),)] = tail

    pair = send(pair_out.at[1 - parity], pair_in, pair_sems.at[0], pair_sems.at[1], partner)
    pair.start()
    forward_line(1)
    forward_plane(layer)
    pair.wait()
    line_out[...] = pair_out[parity] + pair_in[...]

    def head_line(there, here):
        return send(
            line_out.at[there], line_in.at[layer], head_line_send.at[there], head_line_recv.at[here],
            there * PLANE + low,
        )

    for o in others:
        head_line(o, layer).start()
    line_in[layer] = line_out[layer]
    for k in range(2, depth - 1):
        forward_line(k)
    for o in others[:-1]:
        forward_plane(o)
    for o in others:
        head_line(o, o).wait_recv()
    plane_out[...] = jnp.sum(line_in[...], axis=0)

    def head_plane(d):
        to = me + steps[d]
        return send(
            plane_out.at[lax.rem(to // 2, 4)], plane_in.at[d], head_plane_send.at[d], head_plane_recv.at[d], to
        )

    for d in range(3):
        head_plane(d).start()
    for o in others[-1:]:
        forward_plane(o)
    for at_layer in [layer] + others:
        for r in range(4):
            to_partner(r, at_layer).wait()
        for d in range(3):
            in_plane(d, at_layer).wait_send()
    for o in others:
        along_line(o, layer).wait_send()
        head_line(o, o).wait_send()
    for d in range(3):
        head_plane(d).wait()
    head_ref[...] = plane_out[quad] + plane_in[0] + plane_in[1] + plane_in[2]


def take_windows(code_ref, length, start):
    whole, part = start >> 3, start & 7
    bits = max(1, (length // 8 - 1).bit_length())
    keep = 8 * ((1 << (bits - 1)) + 4)
    value = None
    for bit in reversed(range(bits)):
        step = 8 << bit
        keep = 8 * ((1 << bit) + 4)
        chosen = ((whole >> bit) & 1) == 1
        if value is None:
            low, high = code_ref[0:keep, :], code_ref[step : step + keep, :]
        else:
            low, high = value[0:keep], value[step : step + keep]
        value = jnp.where(chosen, high, low)
    for bit in (2, 1, 0):
        chosen = ((part >> bit) & 1) == 1
        value = jnp.where(chosen, pltpu.roll(value, value.shape[0] - (1 << bit), 0), value)
    return value[0:32]


def all_rows(value, combine):
    for shift in (4, 2, 1):
        value = combine(value, pltpu.roll(value, shift, 0))
    return value


def head_counts(window, ok, near, rows):
    center = window[16:17]
    linked = ((window ^ center) >> ITEM_BITS == 0) & near & ok
    item = window & ((1 << ITEM_BITS) - 1)
    tag = jnp.where(linked & (item < rows), item | rows, 0)
    packed = tag[0:8] | (tag[8:16] << 8) | (tag[16:24] << 16) | (tag[24:32] << 24)
    one = jnp.where(linked, 1, 0)
    weight = all_rows(one[0:8] + one[8:16] + one[16:24] + one[24:32], lambda x, y: x + y)
    sub = lax.broadcasted_iota(jnp.int32, (8, LANES), 0)

    def plane(k):
        spread = lax.shift_left(lax.shift_right_logical(packed, k) & 0x01010101, sub)
        return all_rows(spread, lambda x, y: x | y)

    bits = rows.bit_length() - 1
    node = plane(bits)
    for k in range(3):
        node = node & (plane(k) ^ (((sub >> k) & 1) - 1))
    nodes = [node]
    for k in reversed(range(3, bits)):
        word = plane(k)
        nodes = [part for node in nodes for part in (node & ~word, node & word)]
    counts = jnp.concatenate([lax.population_count(node).astype(jnp.float32) for node in nodes], axis=0)
    return counts.astype(jnp.bfloat16), weight[0:1].astype(jnp.float32), center & ((1 << ITEM_BITS) - 1)


def tile_kernel(rows, length, parts, base_ref, all_ref, count_ref, margin_ref, flat_ref, code_ref):
    item_mask = (1 << ITEM_BITS) - 1
    base = base_ref[0]
    count_ref[...] = jnp.zeros_like(count_ref)
    margin_ref[...] = jnp.zeros_like(margin_ref)
    width = count_ref.shape[2]
    band = parts * width
    slabs, blocks = all_ref.shape[0], all_ref.shape[1] * 2 // 3
    for n in range(slabs):
        paired = all_ref[n, blocks:]
        sessions = jnp.concatenate([paired & 0xFFFF, paired >> 16], axis=0)
        flat_ref[n * blocks : (n + 1) * blocks] = all_ref[n, 0:blocks] | (sessions << ITEM_BITS)
    per = length // LANES
    for r in range(per):
        code_ref[16 + r * LANES : 16 + (r + 1) * LANES] = flat_ref[pl.ds(r, LANES, stride=per), :].T
    lane = lax.broadcasted_iota(jnp.int32, (16, LANES), 1)
    code_ref[0:16] = jnp.where(lane == 0, -1, pltpu.roll(code_ref[length : length + 16], 1, 1))
    code_ref[length + 16 : length + 32] = jnp.where(
        lane == LANES - 1, -1, pltpu.roll(code_ref[16:32], LANES - 1, 1)
    )

    words = length // 32
    row_bit = jnp.left_shift(1, lax.broadcasted_iota(jnp.int32, (32, LANES), 0))
    masks = [[], []]
    for w in range(words):
        item = code_ref[16 + 32 * w : 48 + 32 * w] & item_mask
        for s in range(2):
            local = item - base - s * band
            mine = (local >= 0) & (local < band) & (item >= rows)
            masks[s].append(jnp.sum(jnp.where(mine, row_bit, 0), axis=0, keepdims=True))
    start_masks = tuple(jnp.concatenate(m, axis=0) for m in masks)
    tally = [jnp.sum(lax.population_count(m), axis=0, keepdims=True) for m in start_masks]
    trips = (jnp.max(jnp.maximum(tally[0], tally[1])) + 1) // 2

    word_ids = lax.broadcasted_iota(jnp.int32, (words, LANES), 0)
    d_ids = lax.broadcasted_iota(jnp.int32, (32, LANES), 0)
    near = (d_ids >= 1) & (d_ids != 16)
    tile = min(width, 256)
    t_ids = lax.broadcasted_iota(jnp.int32, (tile, 2 * LANES), 0).astype(jnp.float32).astype(jnp.bfloat16)
    p_ids = lax.broadcasted_iota(jnp.int32, (16, 2 * LANES), 0)

    def ends(mask):
        some = mask != 0
        first_row = jnp.min(jnp.where(some, word_ids, words), axis=0, keepdims=True)
        last_row = jnp.max(jnp.where(some, word_ids, -1), axis=0, keepdims=True)
        at_first, at_last = word_ids == first_row, word_ids == last_row
        first_word = jnp.sum(jnp.where(at_first, mask, 0), axis=0, keepdims=True)
        last_word = jnp.sum(jnp.where(at_last, mask, 0), axis=0, keepdims=True)
        first_bit = first_word & -first_word
        last_place = 31 - lax.clz(last_word)
        last_bit = jnp.where(last_word == 0, 0, jnp.left_shift(1, last_place & 31))
        first = 32 * first_row + lax.population_count(first_bit - 1)
        last = 32 * last_row + last_place
        first_ok = first_word != 0
        last_ok = first_ok & (last > first)
        mask = mask & ~(jnp.where(at_first, first_bit, 0) | jnp.where(at_last, last_bit, 0))
        return mask, ((first, first_ok), (last, last_ok))

    def body(unused, state):
        out = []
        for s in range(2):
            mask, found = ends(state[s])
            out.append(mask)
            links, weights, locals_ = [], [], []
            for at, ok in found:
                window = take_windows(code_ref, length, jnp.where(ok, at, 0))
                counts, weight, item = head_counts(window, ok, near, rows)
                links.append(counts)
                weights.append(weight)
                locals_.append(item - base - s * band)
            links = jnp.concatenate(links, axis=1)
            weight = jnp.concatenate(weights, axis=1)
            local = jnp.concatenate(locals_, axis=1)
            part = local >> (width.bit_length() - 1)
            inner = local & (width - 1)
            pieces = []
            for p in range(parts):
                chosen = jnp.broadcast_to(jnp.where(part == p, 1.0, 0.0), (16, 2 * LANES)).astype(jnp.bfloat16)
                pieces += [links[n : n + 16] * chosen for n in range(0, rows, 16)]
            pieces.append(jnp.where(p_ids == part, weight, 0.0).astype(jnp.bfloat16))
            left = jnp.concatenate(pieces, axis=0)
            for t in range(width // tile):
                inside = (inner >= t * tile) & (inner < (t + 1) * tile)
                hot = hot_columns(t_ids, jnp.where(inside, inner - t * tile, -1).astype(jnp.float32))
                cols = slice(t * tile, (t + 1) * tile)
                value = lax.dot_general(left, hot, NT, preferred_element_type=jnp.float32)
                count_ref[s, :, cols] += value[0 : parts * rows]
                margin_ref[s, :, cols] += value[parts * rows :]
        return tuple(out)

    lax.fori_loop(0, trips, body, start_masks)


def sketch_kernel(
    slabs, rows, parts, width, scale, count_ref, margin_ref, head_ref, bits_ref, out_ref,
    log_ref, own_bits, head_bits, acc_ref, send_ref, recv_ref, bit_sems, send_sems, recv_sems,
):
    me = lax.axis_index("stream")
    barrier = greet_all(slabs, me)
    part = count_ref.shape[2]
    owned = 2 * parts * part
    share = rows // slabs
    tile = min(part, 512)
    bit_copy = pltpu.make_async_copy(
        bits_ref.at[:, pl.ds(pl.multiple_of(me * owned, owned), owned)], own_bits, bit_sems.at[0]
    )
    head_copy = pltpu.make_async_copy(bits_ref.at[:, 0:rows], head_bits, bit_sems.at[1])
    bit_copy.start()
    head_copy.start()

    log_ref[...] = jnp.log(jnp.maximum(margin_ref[...], 1.0))
    row_log = jnp.log(jnp.maximum(head_ref[share : share + 1], 1.0))
    column_log = jnp.broadcast_to(row_log, (rows, LANES)).T
    total_log = jnp.log(jnp.sum(head_ref[share + 1 : share + 2], axis=1, keepdims=True))
    row_term = total_log - column_log[:, 0:1]
    groups = []
    for g in range(width // 8):
        word = 8 * g // BITS_PER_WORD
        groups.append((word, (word + 1) * BITS_PER_WORD - 8 * g, 8 * g - word * BITS_PER_WORD))

    def product(positive, words):
        size = words.shape[1]

        def wide(value):
            return jnp.concatenate([value] * (size // LANES), axis=1)

        shift = lax.broadcasted_iota(jnp.int32, (8, LANES), 0)
        upper = positive.astype(jnp.bfloat16)
        lower = (positive - upper.astype(jnp.float32)).astype(jnp.bfloat16)
        parts = []
        for word, split, offset in groups:
            now = jnp.broadcast_to(words[word : word + 1], (8, size))
            where_bit = jnp.left_shift(1, shift + offset)
            if split < 8:
                later = jnp.broadcast_to(words[word + 1 : word + 2], (8, size))
                now = jnp.where(wide(shift) >= split, later, now)
                place = jnp.where(shift >= split, shift - split, shift + offset)
                where_bit = jnp.left_shift(1, place)
            parts.append(jnp.where((now & wide(where_bit)) != 0, 1.0, -1.0))
        signs = jnp.concatenate(parts, axis=0).astype(jnp.bfloat16)
        both = jnp.concatenate([upper, lower], axis=0)
        value = lax.dot_general(both, signs, NT, preferred_element_type=jnp.float32)
        return value[0:rows] + value[rows:]

    head_copy.wait()
    row = lax.broadcasted_iota(jnp.int32, (8, LANES), 0)
    shared = jnp.concatenate(
        [jnp.where(row < share, head_ref[...], 0.0), jnp.zeros((rows - 8, LANES), jnp.float32)], axis=0
    )
    shared = pltpu.roll(shared, me * share, 0)
    ratio = jnp.log(jnp.maximum(shared, 1.0)) + total_log - row_log - column_log
    first_band = jnp.where(lax.axis_index("item") == 0, 1.0, 0.0)
    positive = jnp.where(shared > 0, jnp.maximum(ratio, 0.0), 0.0) * first_band
    acc_ref[...] = product(positive.T, head_bits[...])
    bit_copy.wait()

    for s in range(2):
        for h in range(parts):
            for at in range(0, part, tile):
                counts = count_ref[s, h * rows : (h + 1) * rows, at : at + tile]
                ratio = jnp.log(jnp.maximum(counts, 1.0)) + row_term - log_ref[s, h : h + 1, at : at + tile]
                positive = jnp.where(counts > 0, jnp.maximum(ratio, 0.0), 0.0)
                bit_at = (s * parts + h) * part + at
                acc_ref[...] += product(positive, own_bits[:, bit_at : bit_at + tile])

    cuts = width // LANES
    for d in range(slabs):
        for c in range(cuts):
            send_ref[d, c * share : (c + 1) * share] = (
                acc_ref[d * share : (d + 1) * share, c * LANES : (c + 1) * LANES] * scale
            )
    pl.semaphore_wait(barrier, slabs - 1)
    exchange(slabs, me, send_ref, recv_ref, send_sems, recv_sems, True)
    exchange(slabs, me, send_ref, recv_ref, send_sems, recv_sems, False)
    summed = jnp.sum(recv_ref[...], axis=0)
    out_ref[...] = jnp.concatenate([summed[c * share : (c + 1) * share] for c in range(cuts)], axis=1)


def local(event_items, event_sessions, sketch_bits):
    slabs = lax.axis_size("stream")
    slab = event_items.shape[0]
    total_events = slab * slabs
    words, band_size = sketch_bits.shape
    owned = band_size // slabs
    rows, width = 128, 256
    part = max(LANES, owned // 16)
    parts = owned // (2 * part)
    me = lax.axis_index("stream")
    own_start = me * owned
    first_id = lax.axis_index("item") * band_size + own_start
    blocks = slab // LANES
    length = total_events // LANES

    dma = pltpu.SemaphoreType.DMA
    depth = slabs // PLANE
    events, head = pl.pallas_call(
        functools.partial(gather_kernel, slabs, rows, blocks),
        out_shape=(
            jax.ShapeDtypeStruct((slabs, blocks * 3 // 2, LANES), jnp.int32),
            jax.ShapeDtypeStruct((8, LANES), jnp.float32),
        ),
        in_specs=[VMEM],
        out_specs=(VMEM, VMEM),
        scratch_shapes=[
            pltpu.VMEM((blocks * 3 // 2, LANES), jnp.int32),
            pltpu.VMEM((4, 8, LANES), jnp.int32),
            pltpu.VMEM((blocks + 16, LANES), jnp.int32),
            pltpu.VMEM((blocks + 16, LANES), jnp.int32),
            pltpu.VMEM((rows + 8, LANES), jnp.float32),
            pltpu.VMEM((8, LANES), jnp.float32),
            pltpu.VMEM((2, depth, 4, 8, LANES), jnp.float32),
            pltpu.VMEM((depth, 4, 8, LANES), jnp.float32),
            pltpu.VMEM((4, 8, LANES), jnp.float32),
            pltpu.VMEM((3, 8, LANES), jnp.float32),
            pltpu.VMEM((depth, 4, 8, LANES), jnp.float32),
            pltpu.VMEM((depth, 4, 8, LANES), jnp.float32),
            dma((4,)),
            dma((4,)),
            dma((depth,)),
            dma((depth,)),
            dma((3 * depth,)),
            dma((3 * depth,)),
            dma((4 * depth,)),
            dma((4 * depth,)),
            dma((2,)),
            dma((3,)),
            dma((3,)),
            dma((depth,)),
            dma((depth,)),
        ],
        compiler_params=pltpu.CompilerParams(
            collective_id=0, has_side_effects=True, vmem_limit_bytes=VMEM_GRANT
        ),
        name="gather_events",
    )(jnp.stack([event_items, event_sessions]).reshape(2, blocks, LANES))

    counts, margins = pl.pallas_call(
        functools.partial(tile_kernel, rows, length, parts),
        out_shape=(
            jax.ShapeDtypeStruct((2, parts * rows, part), jnp.float32),
            jax.ShapeDtypeStruct((2, 16, part), jnp.float32),
        ),
        in_specs=[pl.BlockSpec(memory_space=pltpu.SMEM), VMEM],
        out_specs=(VMEM, VMEM),
        scratch_shapes=[
            pltpu.VMEM((length, LANES), jnp.int32),
            pltpu.VMEM((length + 32, LANES), jnp.int32),
        ],
        compiler_params=pltpu.CompilerParams(vmem_limit_bytes=VMEM_GRANT),
        name="tile_counts",
    )(first_id.astype(jnp.int32)[None], events)

    own_rows = pl.pallas_call(
        functools.partial(sketch_kernel, slabs, rows, parts, width, 1.0 / math.sqrt(total_events)),
        out_shape=jax.ShapeDtypeStruct((rows // slabs, width), jnp.float32),
        in_specs=[VMEM] * 3 + [pl.BlockSpec(memory_space=pl.ANY)],
        out_specs=VMEM,
        scratch_shapes=[
            pltpu.VMEM((2, 16, part), jnp.float32),
            pltpu.VMEM((words, owned), jnp.int32),
            pltpu.VMEM((words, rows), jnp.int32),
            pltpu.VMEM((rows, width), jnp.float32),
            pltpu.VMEM((slabs, 8, LANES), jnp.float32),
            pltpu.VMEM((slabs, 8, LANES), jnp.float32),
            dma((2,)),
            dma((slabs,)),
            dma((slabs,)),
        ],
        compiler_params=pltpu.CompilerParams(
            collective_id=1, has_side_effects=True, vmem_limit_bytes=VMEM_GRANT
        ),
        name="sketch_tile",
    )(counts, margins, head, sketch_bits)
    if lax.axis_size("item") > 1:
        own_rows = lax.psum(own_rows, "item")
    return own_rows


def solution(mesh):
    placed = (P("stream"), P("stream"), P(None, "item"))
    return jax.shard_map(
        local, mesh=mesh, in_specs=placed, out_specs=P("stream", None), check_vma=False
    )
```

```python
import functools
import math

import jax
import jax.numpy as jnp
from jax import lax
from jax.experimental import pallas as pl
from jax.experimental.pallas import tpu as pltpu
from jax.sharding import PartitionSpec as P

WINDOW = 15
ITEM_BITS = 18
LANES = 128
BITS_PER_WORD = 18
PLANE = 8
VMEM_GRANT = 45 * 1024 * 1024
NT = (((1,), (1,)), ((), ()))
VMEM = pl.BlockSpec(memory_space=pltpu.VMEM)


def one_where(mask):
    return jnp.where(mask, 1.0, 0.0).astype(jnp.bfloat16)


def hot_columns(ids, values):
    row = jnp.broadcast_to(values, (16, values.shape[1])).astype(jnp.bfloat16)
    one, zero = jnp.ones((), jnp.bfloat16), jnp.zeros((), jnp.bfloat16)
    return jnp.concatenate(
        [jnp.where(ids[n : n + 16] == row, one, zero) for n in range(0, ids.shape[0], 16)], axis=0
    )


def greet_all(slabs, me):
    barrier = pltpu.get_barrier_semaphore()

    for k in range(1, slabs):
        pl.semaphore_signal(
            barrier, inc=1, device_id={"stream": lax.rem(me + k, slabs)}, device_id_type=pl.DeviceIdType.MESH
        )
    return barrier


def send(src, dst, send_sem, recv_sem, to):
    return pltpu.make_async_remote_copy(
        src_ref=src,
        dst_ref=dst,
        send_sem=send_sem,
        recv_sem=recv_sem,
        device_id={"stream": to},
        device_id_type=pl.DeviceIdType.MESH,
    )


def each(low, high, do):
    for k in range(low, high):
        do(k)


def exchange(slabs, me, out_ref, in_ref, send_sems, recv_sems, start):
    def copy(k):
        to = lax.rem(me + k, slabs)
        return send(out_ref.at[to], in_ref.at[me], send_sems.at[k], recv_sems.at[k], to)

    if start:
        each(1, slabs, lambda k: copy(k).start())
        in_ref[me] = out_ref[me]
    else:
        each(1, slabs, lambda k: copy(k).wait())


def gather_kernel(
    slabs, rows, blocks, own_ref, bits_ref, all_ref, head_ref, sign_ref,
    own_pack, own_bits, item_ref, session_ref, links_ref, total_ref,
    pair_out, pair_in, plane_out, plane_in, line_out, line_in,
    bit_sem, line_send, line_recv, plane_send, plane_recv, near_send, near_recv,
    pair_sems, head_plane_send, head_plane_recv, head_line_send, head_line_recv,
):
    me = lax.axis_index("stream")
    depth = slabs // PLANE
    layer, low = me // PLANE, lax.rem(me, PLANE)
    parity, quad = lax.rem(me, 2), lax.rem(me // 2, 4)

    def flip(bit):
        return bit - 2 * bit * lax.rem(me // bit, 2)

    partner = me + flip(1)
    steps = (flip(2), flip(4), flip(2) + flip(4))
    def other_layer(k):
        rising = k + (k - layer + depth) // depth
        mirrored = depth - 1 - layer
        falling = depth - 1 - k - (k - mirrored + depth) // depth
        high = layer // ((depth + 1) // 2)
        return rising + (falling - rising) * lax.rem(high, 2)

    others = [other_layer(k) for k in range(depth - 1)]
    own_items, own_sessions = own_ref.at[0], own_ref.at[1]
    barrier = pltpu.get_barrier_semaphore()
    owned = own_bits.shape[1]
    bit_copy = pltpu.make_async_copy(
        bits_ref.at[:, pl.ds(pl.multiple_of(me * owned, owned), owned)], own_bits, bit_sem.at[0]
    )
    bit_copy.start()
    greeted = [partner] + [me + step for step in steps] + [o * PLANE + low for o in others]
    for to in greeted:
        pl.semaphore_signal(
            barrier, inc=1, device_id={"stream": to}, device_id_type=pl.DeviceIdType.MESH
        )
    half = blocks // 2
    own_pack[0:blocks] = own_items[...]
    own_pack[blocks : blocks + half] = own_sessions[0:half] | (own_sessions[half:blocks] << 16)
    all_ref[me] = own_pack[...]
    item_ref[8 : 8 + blocks] = own_items[...]
    session_ref[8 : 8 + blocks] = own_sessions[...]
    for edge in (slice(0, 8), slice(8 + blocks, 16 + blocks)):
        item_ref[edge] = jnp.zeros((8, LANES), jnp.int32)
        session_ref[edge] = jnp.full((8, LANES), -1, jnp.int32)
    sub = lax.broadcasted_iota(jnp.int32, (LANES, LANES), 0)
    lane = lax.broadcasted_iota(jnp.int32, (LANES, LANES), 1)
    low_lane = lax.broadcasted_iota(jnp.int32, (1, LANES), 1) < LANES // 2
    ids = lax.broadcasted_iota(jnp.int32, (rows, LANES), 0)
    gaps = (sub - LANES // 2 - lane, sub + LANES // 2 - lane)
    in_reach = [(jnp.abs(gap) <= WINDOW) & (gap != 0) for gap in gaps]
    ones = jnp.ones((8, 2 * LANES), jnp.float32).astype(jnp.bfloat16)
    links_ref[...] = jnp.zeros_like(links_ref)
    total_ref[...] = jnp.zeros_like(total_ref)

    def block(b, unused):
        def around(ref):
            turned = [pltpu.roll(ref[pl.ds(b + o, 1)], LANES // 2, 1) for o in (7, 8, 9)]
            return (
                jnp.where(low_lane, turned[0], turned[1]),
                jnp.where(low_lane, turned[1], turned[2]),
            )

        own_item, own_session = item_ref[pl.ds(b + 8, 1)], session_ref[pl.ds(b + 8, 1)]
        hot = jnp.concatenate([one_where(ids == item) for item in around(item_ref)], axis=1)
        linked = jnp.concatenate(
            [
                one_where((jnp.broadcast_to(session, (LANES, LANES)).T == own_session) & reach)
                for session, reach in zip(around(session_ref), in_reach)
            ],
            axis=0,
        )
        links = jnp.dot(jnp.concatenate([hot, ones], axis=0), linked, preferred_element_type=jnp.float32)
        links_ref[...] += lax.dot_general(
            links.astype(jnp.bfloat16), one_where(ids == own_item), NT, preferred_element_type=jnp.float32
        )
        total_ref[...] += links[rows:]
        return unused

    inner = [blocks * n // 32 for n in (0, 16, 32)]

    def blocks_of(n):
        lax.fori_loop(inner[n], inner[n + 1], block, 0, unroll=4)

    step_columns = max(LANES, owned // 16)
    steps_in_all = owned // step_columns

    def signs(low_step, high_step):
        def step(t, unused):
            at = pl.multiple_of(t * step_columns, step_columns)
            sign_ref[:, pl.ds(at, step_columns)] = sign_table(own_bits[:, pl.ds(at, step_columns)], sign_ref.shape[0])
            return unused

        lax.fori_loop(low_step * steps_in_all // 16, high_step * steps_in_all // 16, step, 0)

    blocks_of(0)
    bit_copy.wait()
    pl.semaphore_wait(barrier, len(greeted))

    def along_line(there, here):
        return send(
            own_pack, all_ref.at[me], line_send.at[there], line_recv.at[here], there * PLANE + low
        )

    def in_plane(d, at_layer, own=False):
        slab = all_ref.at[at_layer * PLANE + low]
        sem = d * depth + at_layer
        return send(own_pack if own else slab, slab, plane_send.at[sem], plane_recv.at[sem], me + steps[d])

    def to_partner(r, at_layer, own=False):
        slab = all_ref.at[at_layer * PLANE + low + ((0,) + steps)[r]]
        sem = r * depth + at_layer
        return send(own_pack if own else slab, slab, near_send.at[sem], near_recv.at[sem], partner)

    for o in reversed(others):
        along_line(o, layer).start()
    for d in range(3):
        in_plane(d, layer, True).start()
    to_partner(0, layer, True).start()

    def forward_line(k):
        along_line(layer, others[k]).wait_recv()
        for d in range(3):
            in_plane(d, others[k]).start()
        to_partner(0, others[k]).start()

    def forward_plane(at_layer):
        for d in range(3):
            in_plane(d, at_layer).wait_recv()
            to_partner(d + 1, at_layer).start()

    blocks_of(1)
    share = rows // slabs
    tail = jnp.concatenate(
        [links_ref[rows : rows + 1], total_ref[0:1], jnp.zeros((6 - share, LANES), jnp.float32)], axis=0
    )
    for d in range(slabs):
        at = (d % 2, d // PLANE, d // 2 % 4)
        pair_out[at + (slice(0, share),)] = links_ref[d * share : (d + 1) * share]
        pair_out[at + (slice(share, 8),)] = tail

    pair = send(pair_out.at[1 - parity], pair_in, pair_sems.at[0], pair_sems.at[1], partner)
    pair.start()
    signs(0, 2)
    forward_line(0)
    pair.wait()
    line_out[...] = pair_out[parity] + pair_in[...]

    def head_line(there, here):
        return send(
            line_out.at[there], line_in.at[layer], head_line_send.at[there], head_line_recv.at[here],
            there * PLANE + low,
        )

    for o in others:
        head_line(o, layer).start()
    line_in[layer] = line_out[layer]
    forward_line(1)
    forward_plane(layer)
    for k in range(2, depth - 1):
        forward_line(k)
    signs(2, 6)
    forward_plane(others[0])
    signs(6, 9)
    for o in others[1:-1]:
        forward_plane(o)
    for o in others:
        head_line(o, o).wait_recv()
    plane_out[...] = jnp.sum(line_in[...], axis=0)

    def head_plane(d):
        to = me + steps[d]
        return send(
            plane_out.at[lax.rem(to // 2, 4)], plane_in.at[d], head_plane_send.at[d], head_plane_recv.at[d], to
        )

    for d in range(3):
        head_plane(d).start()
    signs(9, 12)
    for o in others[-1:]:
        forward_plane(o)
    signs(12, 16)
    for at_layer in [layer] + others:
        for r in range(4):
            to_partner(r, at_layer).wait()
        for d in range(3):
            in_plane(d, at_layer).wait_send()
    for o in others:
        along_line(o, layer).wait_send()
        head_line(o, o).wait_send()
    for d in range(3):
        head_plane(d).wait()

    last_items, last_sessions = all_ref[:, blocks - 1, :], all_ref[:, blocks + half - 1, :] >> 16
    next_items, next_sessions = all_ref[:, 0, :], all_ref[:, blocks, :] & 0xFFFF
    group = slabs // 4
    small = lax.broadcasted_iota(jnp.int32, (group, LANES), 1)

    def meet(last, following):
        joined = None
        for g in range(4):
            shift = 32 * g + 16
            pieces = (pltpu.roll(x[g * group : (g + 1) * group], shift % LANES, 1) for x in (last, following))
            both = jnp.where(lax.rem(small, 32) < 16, *pieces)
            joined = both if joined is None else jnp.where(small // 32 == g, both, joined)
        return joined

    slab_ids = lax.broadcasted_iota(jnp.int32, (slabs, LANES), 0)
    next_sessions = jnp.where(slab_ids == slabs - 1, -1, pltpu.roll(next_sessions, slabs - 1, 0))
    met_items = meet(last_items, pltpu.roll(next_items, slabs - 1, 0))
    met_sessions = meet(last_sessions, next_sessions)
    crossing = (sub // 32 == lane // 32) & ((lax.rem(sub, 32) < 16) != (lax.rem(lane, 32) < 16))
    crossing = crossing & (jnp.abs(sub - lane) <= WINDOW)
    extra = jnp.zeros((rows + 8, LANES), jnp.float32)
    extra_total = jnp.zeros((8, LANES), jnp.float32)
    for g in range(group):
        item, session = met_items[g : g + 1], met_sessions[g : g + 1]
        linked = one_where((jnp.broadcast_to(session, (LANES, LANES)).T == session) & crossing)
        hot = one_where(ids == item)
        links = jnp.dot(jnp.concatenate([hot, ones[:, 0:LANES]], axis=0), linked, preferred_element_type=jnp.float32)
        extra += lax.dot_general(links.astype(jnp.bfloat16), hot, NT, preferred_element_type=jnp.float32)
        extra_total += links[rows:]
    links_ref[...] = extra
    more = jnp.concatenate(
        [
            links_ref[pl.ds(me * share, share)],
            links_ref[rows : rows + 1],
            extra_total[0:1],
            jnp.zeros((6 - share, LANES), jnp.float32),
        ],
        axis=0,
    )
    head_ref[...] = plane_out[quad] + plane_in[0] + plane_in[1] + plane_in[2] + more


def take_windows(code_ref, length, start):
    whole, part = start >> 3, start & 7
    bits = max(1, (length // 8 - 1).bit_length())
    keep = 8 * ((1 << (bits - 1)) + 4)
    value = None
    for bit in reversed(range(bits)):
        step = 8 << bit
        keep = 8 * ((1 << bit) + 4)
        chosen = ((whole >> bit) & 1) == 1
        if value is None:
            low, high = code_ref[0:keep, :], code_ref[step : step + keep, :]
        else:
            low, high = value[0:keep], value[step : step + keep]
        value = jnp.where(chosen, high, low)
    for bit in (2, 1, 0):
        chosen = ((part >> bit) & 1) == 1
        value = jnp.where(chosen, pltpu.roll(value, value.shape[0] - (1 << bit), 0), value)
    return value[0:32]


def all_rows(value, combine):
    for shift in (4, 2, 1):
        value = combine(value, pltpu.roll(value, shift, 0))
    return value


def head_counts(window, ok, near, rows):
    center = window[16:17]
    linked = ((window ^ center) >> ITEM_BITS == 0) & near & ok
    item = window & ((1 << ITEM_BITS) - 1)
    tag = jnp.where(linked & (item < rows), item | rows, 0)
    packed = tag[0:8] | (tag[8:16] << 8) | (tag[16:24] << 16) | (tag[24:32] << 24)
    one = jnp.where(linked, 1, 0)
    weight = all_rows(one[0:8] + one[8:16] + one[16:24] + one[24:32], lambda x, y: x + y)
    sub = lax.broadcasted_iota(jnp.int32, (8, LANES), 0)

    def plane(k):
        spread = lax.shift_left(lax.shift_right_logical(packed, k) & 0x01010101, sub)
        return all_rows(spread, lambda x, y: x | y)

    bits = rows.bit_length() - 1
    node = plane(bits)
    for k in range(3):
        node = node & (plane(k) ^ (((sub >> k) & 1) - 1))
    nodes = [node]
    for k in reversed(range(3, bits)):
        word = plane(k)
        nodes = [part for node in nodes for part in (node & ~word, node & word)]
    counts = jnp.concatenate([lax.population_count(node).astype(jnp.float32) for node in nodes], axis=0)
    return counts.astype(jnp.bfloat16), weight[0:1].astype(jnp.float32), center & ((1 << ITEM_BITS) - 1)


def tile_kernel(rows, length, parts, base_ref, all_ref, count_ref, margin_ref, flat_ref, code_ref):
    item_mask = (1 << ITEM_BITS) - 1
    base = base_ref[0]
    count_ref[...] = jnp.zeros_like(count_ref)
    margin_ref[...] = jnp.zeros_like(margin_ref)
    width = count_ref.shape[2]
    band = parts * width
    slabs, blocks = all_ref.shape[0], all_ref.shape[1] * 2 // 3
    for n in range(slabs):
        paired = all_ref[n, blocks:]
        sessions = jnp.concatenate([paired & 0xFFFF, paired >> 16], axis=0)
        flat_ref[n * blocks : (n + 1) * blocks] = all_ref[n, 0:blocks] | (sessions << ITEM_BITS)
    per = length // LANES
    for r in range(per):
        code_ref[16 + r * LANES : 16 + (r + 1) * LANES] = flat_ref[pl.ds(r, LANES, stride=per), :].T
    lane = lax.broadcasted_iota(jnp.int32, (16, LANES), 1)
    code_ref[0:16] = jnp.where(lane == 0, -1, pltpu.roll(code_ref[length : length + 16], 1, 1))
    code_ref[length + 16 : length + 32] = jnp.where(
        lane == LANES - 1, -1, pltpu.roll(code_ref[16:32], LANES - 1, 1)
    )

    words = length // 32
    row_bit = jnp.left_shift(1, lax.broadcasted_iota(jnp.int32, (32, LANES), 0))
    masks = [[], []]
    for w in range(words):
        item = code_ref[16 + 32 * w : 48 + 32 * w] & item_mask
        for s in range(2):
            local = item - base - s * band
            mine = (local >= 0) & (local < band) & (item >= rows)
            masks[s].append(jnp.sum(jnp.where(mine, row_bit, 0), axis=0, keepdims=True))
    start_masks = tuple(jnp.concatenate(m, axis=0) for m in masks)
    tally = [jnp.sum(lax.population_count(m), axis=0, keepdims=True) for m in start_masks]
    trips = (jnp.max(jnp.maximum(tally[0], tally[1])) + 1) // 2

    word_ids = lax.broadcasted_iota(jnp.int32, (words, LANES), 0)
    d_ids = lax.broadcasted_iota(jnp.int32, (32, LANES), 0)
    near = (d_ids >= 1) & (d_ids != 16)
    tile = min(width, 256)
    t_ids = lax.broadcasted_iota(jnp.int32, (tile, 2 * LANES), 0).astype(jnp.float32).astype(jnp.bfloat16)
    p_ids = lax.broadcasted_iota(jnp.int32, (16, 2 * LANES), 0)

    def ends(mask):
        some = mask != 0
        first_row = jnp.min(jnp.where(some, word_ids, words), axis=0, keepdims=True)
        last_row = jnp.max(jnp.where(some, word_ids, -1), axis=0, keepdims=True)
        at_first, at_last = word_ids == first_row, word_ids == last_row
        first_word = jnp.sum(jnp.where(at_first, mask, 0), axis=0, keepdims=True)
        last_word = jnp.sum(jnp.where(at_last, mask, 0), axis=0, keepdims=True)
        first_bit = first_word & -first_word
        last_place = 31 - lax.clz(last_word)
        last_bit = jnp.where(last_word == 0, 0, jnp.left_shift(1, last_place & 31))
        first = 32 * first_row + lax.population_count(first_bit - 1)
        last = 32 * last_row + last_place
        first_ok = first_word != 0
        last_ok = first_ok & (last > first)
        mask = mask & ~(jnp.where(at_first, first_bit, 0) | jnp.where(at_last, last_bit, 0))
        return mask, ((first, first_ok), (last, last_ok))

    def body(unused, state):
        out = []
        for s in range(2):
            mask, found = ends(state[s])
            out.append(mask)
            links, weights, locals_ = [], [], []
            for at, ok in found:
                window = take_windows(code_ref, length, jnp.where(ok, at, 0))
                counts, weight, item = head_counts(window, ok, near, rows)
                links.append(counts)
                weights.append(weight)
                locals_.append(item - base - s * band)
            links = jnp.concatenate(links, axis=1)
            weight = jnp.concatenate(weights, axis=1)
            local = jnp.concatenate(locals_, axis=1)
            part = local >> (width.bit_length() - 1)
            inner = local & (width - 1)
            pieces = []
            for p in range(parts):
                chosen = jnp.broadcast_to(jnp.where(part == p, 1.0, 0.0), (16, 2 * LANES)).astype(jnp.bfloat16)
                pieces += [links[n : n + 16] * chosen for n in range(0, rows, 16)]
            pieces.append(jnp.where(p_ids == part, weight, 0.0).astype(jnp.bfloat16))
            left = jnp.concatenate(pieces, axis=0)
            for t in range(width // tile):
                inside = (inner >= t * tile) & (inner < (t + 1) * tile)
                hot = hot_columns(t_ids, jnp.where(inside, inner - t * tile, -1).astype(jnp.float32))
                cols = slice(t * tile, (t + 1) * tile)
                value = lax.dot_general(left, hot, NT, preferred_element_type=jnp.float32)
                count_ref[s, :, cols] += value[0 : parts * rows]
                margin_ref[s, :, cols] += value[parts * rows :]
        return tuple(out)

    lax.fori_loop(0, trips, body, start_masks)


def sign_table(words, width):
    size = words.shape[1]

    def wide(value):
        return jnp.concatenate([value] * (size // LANES), axis=1)

    shift = lax.broadcasted_iota(jnp.int32, (8, LANES), 0)
    parts = []
    for g in range(width // 8):
        word = 8 * g // BITS_PER_WORD
        split, offset = (word + 1) * BITS_PER_WORD - 8 * g, 8 * g - word * BITS_PER_WORD
        now = jnp.broadcast_to(words[word : word + 1], (8, size))
        where_bit = jnp.left_shift(1, shift + offset)
        if split < 8:
            later = jnp.broadcast_to(words[word + 1 : word + 2], (8, size))
            now = jnp.where(wide(shift) >= split, later, now)
            place = jnp.where(shift >= split, shift - split, shift + offset)
            where_bit = jnp.left_shift(1, place)
        parts.append(jnp.where((now & wide(where_bit)) != 0, 1.0, -1.0))
    return jnp.concatenate(parts, axis=0).astype(jnp.bfloat16)


def sketch_kernel(
    slabs, rows, parts, width, scale, count_ref, margin_ref, head_ref, sign_ref, bits_ref, out_ref,
    log_ref, head_bits, acc_ref, send_ref, recv_ref, bit_sem, send_sems, recv_sems,
):
    me = lax.axis_index("stream")
    barrier = greet_all(slabs, me)
    part = count_ref.shape[2]
    share = rows // slabs
    tile = min(part, 512)
    head_copy = pltpu.make_async_copy(bits_ref.at[:, 0:rows], head_bits, bit_sem.at[0])
    head_copy.start()

    log_ref[...] = jnp.log(jnp.maximum(margin_ref[...], 1.0))
    row_log = jnp.log(jnp.maximum(head_ref[share : share + 1], 1.0))
    column_log = jnp.broadcast_to(row_log, (rows, LANES)).T
    total_log = jnp.log(jnp.sum(head_ref[share + 1 : share + 2], axis=1, keepdims=True))
    row_term = total_log - column_log[:, 0:1]
    def product(positive, signs):
        upper = positive.astype(jnp.bfloat16)
        lower = (positive - upper.astype(jnp.float32)).astype(jnp.bfloat16)
        both = jnp.concatenate([upper, lower], axis=0)
        value = lax.dot_general(both, signs, NT, preferred_element_type=jnp.float32)
        return value[0:rows] + value[rows:]

    head_copy.wait()
    row = lax.broadcasted_iota(jnp.int32, (8, LANES), 0)
    shared = jnp.concatenate(
        [jnp.where(row < share, head_ref[...], 0.0), jnp.zeros((rows - 8, LANES), jnp.float32)], axis=0
    )
    shared = pltpu.roll(shared, me * share, 0)
    ratio = jnp.log(jnp.maximum(shared, 1.0)) + total_log - row_log - column_log
    first_band = jnp.where(lax.axis_index("item") == 0, 1.0, 0.0)
    positive = jnp.where(shared > 0, jnp.maximum(ratio, 0.0), 0.0) * first_band
    acc_ref[...] = product(positive.T, sign_table(head_bits[...], width))

    for s in range(2):
        for h in range(parts):
            for at in range(0, part, tile):
                counts = count_ref[s, h * rows : (h + 1) * rows, at : at + tile]
                ratio = jnp.log(jnp.maximum(counts, 1.0)) + row_term - log_ref[s, h : h + 1, at : at + tile]
                positive = jnp.where(counts > 0, jnp.maximum(ratio, 0.0), 0.0)
                bit_at = (s * parts + h) * part + at
                acc_ref[...] += product(positive, sign_ref[:, bit_at : bit_at + tile])

    cuts = width // LANES
    for d in range(slabs):
        for c in range(cuts):
            send_ref[d, c * share : (c + 1) * share] = (
                acc_ref[d * share : (d + 1) * share, c * LANES : (c + 1) * LANES] * scale
            )
    pl.semaphore_wait(barrier, slabs - 1)
    exchange(slabs, me, send_ref, recv_ref, send_sems, recv_sems, True)
    exchange(slabs, me, send_ref, recv_ref, send_sems, recv_sems, False)
    summed = jnp.sum(recv_ref[...], axis=0)
    out_ref[...] = jnp.concatenate([summed[c * share : (c + 1) * share] for c in range(cuts)], axis=1)


def local(event_items, event_sessions, sketch_bits):
    slabs = lax.axis_size("stream")
    slab = event_items.shape[0]
    total_events = slab * slabs
    words, band_size = sketch_bits.shape
    owned = band_size // slabs
    rows, width = 128, 256
    part = max(LANES, owned // 16)
    parts = owned // (2 * part)
    me = lax.axis_index("stream")
    own_start = me * owned
    first_id = lax.axis_index("item") * band_size + own_start
    blocks = slab // LANES
    length = total_events // LANES

    dma = pltpu.SemaphoreType.DMA
    depth = slabs // PLANE
    events, head, signs = pl.pallas_call(
        functools.partial(gather_kernel, slabs, rows, blocks),
        out_shape=(
            jax.ShapeDtypeStruct((slabs, blocks * 3 // 2, LANES), jnp.int32),
            jax.ShapeDtypeStruct((8, LANES), jnp.float32),
            jax.ShapeDtypeStruct((width, owned), jnp.bfloat16),
        ),
        in_specs=[VMEM, pl.BlockSpec(memory_space=pl.ANY)],
        out_specs=(VMEM, VMEM, VMEM),
        scratch_shapes=[
            pltpu.VMEM((blocks * 3 // 2, LANES), jnp.int32),
            pltpu.VMEM((words, owned), jnp.int32),
            pltpu.VMEM((blocks + 16, LANES), jnp.int32),
            pltpu.VMEM((blocks + 16, LANES), jnp.int32),
            pltpu.VMEM((rows + 8, LANES), jnp.float32),
            pltpu.VMEM((8, LANES), jnp.float32),
            pltpu.VMEM((2, depth, 4, 8, LANES), jnp.float32),
            pltpu.VMEM((depth, 4, 8, LANES), jnp.float32),
            pltpu.VMEM((4, 8, LANES), jnp.float32),
            pltpu.VMEM((3, 8, LANES), jnp.float32),
            pltpu.VMEM((depth, 4, 8, LANES), jnp.float32),
            pltpu.VMEM((depth, 4, 8, LANES), jnp.float32),
            dma((1,)),
            dma((depth,)),
            dma((depth,)),
            dma((3 * depth,)),
            dma((3 * depth,)),
            dma((4 * depth,)),
            dma((4 * depth,)),
            dma((2,)),
            dma((3,)),
            dma((3,)),
            dma((depth,)),
            dma((depth,)),
        ],
        compiler_params=pltpu.CompilerParams(
            collective_id=0, has_side_effects=True, vmem_limit_bytes=VMEM_GRANT
        ),
        name="gather_events",
    )(jnp.stack([event_items, event_sessions]).reshape(2, blocks, LANES), sketch_bits)

    counts, margins = pl.pallas_call(
        functools.partial(tile_kernel, rows, length, parts),
        out_shape=(
            jax.ShapeDtypeStruct((2, parts * rows, part), jnp.float32),
            jax.ShapeDtypeStruct((2, 16, part), jnp.float32),
        ),
        in_specs=[pl.BlockSpec(memory_space=pltpu.SMEM), VMEM],
        out_specs=(VMEM, VMEM),
        scratch_shapes=[
            pltpu.VMEM((length, LANES), jnp.int32),
            pltpu.VMEM((length + 32, LANES), jnp.int32),
        ],
        compiler_params=pltpu.CompilerParams(vmem_limit_bytes=VMEM_GRANT),
        name="tile_counts",
    )(first_id.astype(jnp.int32)[None], events)

    own_rows = pl.pallas_call(
        functools.partial(sketch_kernel, slabs, rows, parts, width, 1.0 / math.sqrt(total_events)),
        out_shape=jax.ShapeDtypeStruct((rows // slabs, width), jnp.float32),
        in_specs=[VMEM] * 4 + [pl.BlockSpec(memory_space=pl.ANY)],
        out_specs=VMEM,
        scratch_shapes=[
            pltpu.VMEM((2, 16, part), jnp.float32),
            pltpu.VMEM((words, rows), jnp.int32),
            pltpu.VMEM((rows, width), jnp.float32),
            pltpu.VMEM((slabs, 8, LANES), jnp.float32),
            pltpu.VMEM((slabs, 8, LANES), jnp.float32),
            dma((1,)),
            dma((slabs,)),
            dma((slabs,)),
        ],
        compiler_params=pltpu.CompilerParams(
            collective_id=1, has_side_effects=True, vmem_limit_bytes=VMEM_GRANT
        ),
        name="sketch_tile",
    )(counts, margins, head, signs, sketch_bits)
    if lax.axis_size("item") > 1:
        own_rows = lax.psum(own_rows, "item")
    return own_rows


def solution(mesh):
    placed = (P("stream"), P("stream"), P(None, "item"))
    return jax.shard_map(
        local, mesh=mesh, in_specs=placed, out_specs=P("stream", None), check_vma=False
    )
```

```python
import functools
import math

import jax
import jax.numpy as jnp
from jax import lax
from jax.experimental import pallas as pl
from jax.experimental.pallas import tpu as pltpu
from jax.sharding import PartitionSpec as P

WINDOW = 15
ITEM_BITS = 18
LANES = 128
BITS_PER_WORD = 18
PLANE = 8
BANDS = 4
VMEM_GRANT = 45 * 1024 * 1024
NT = (((1,), (1,)), ((), ()))
VMEM = pl.BlockSpec(memory_space=pltpu.VMEM)


def one_where(mask):
    return jnp.where(mask, 1.0, 0.0).astype(jnp.bfloat16)


def hot_columns(ids, values):
    row = jnp.broadcast_to(values, (16, values.shape[1])).astype(jnp.bfloat16)
    one, zero = jnp.ones((), jnp.bfloat16), jnp.zeros((), jnp.bfloat16)
    return jnp.concatenate(
        [jnp.where(ids[n : n + 16] == row, one, zero) for n in range(0, ids.shape[0], 16)], axis=0
    )


def greet_all(slabs, me):
    barrier = pltpu.get_barrier_semaphore()

    for k in range(1, slabs):
        pl.semaphore_signal(
            barrier, inc=1, device_id={"stream": lax.rem(me + k, slabs)}, device_id_type=pl.DeviceIdType.MESH
        )
    return barrier


def send(src, dst, send_sem, recv_sem, to):
    return pltpu.make_async_remote_copy(
        src_ref=src,
        dst_ref=dst,
        send_sem=send_sem,
        recv_sem=recv_sem,
        device_id={"stream": to},
        device_id_type=pl.DeviceIdType.MESH,
    )


def each(low, high, do):
    for k in range(low, high):
        do(k)


def exchange(slabs, me, out_ref, in_ref, send_sems, recv_sems, start):
    def copy(k):
        to = lax.rem(me + k, slabs)
        return send(out_ref.at[to], in_ref.at[me], send_sems.at[k], recv_sems.at[k], to)

    if start:
        each(1, slabs, lambda k: copy(k).start())
        in_ref[me] = out_ref[me]
    else:
        each(1, slabs, lambda k: copy(k).wait())


def gather_kernel(
    slabs, rows, blocks, own_ref, bits_ref, all_ref, head_ref, sign_ref,
    own_pack, own_bits, item_ref, session_ref, links_ref, total_ref,
    pair_out, pair_in, plane_out, plane_in, line_out, line_in,
    bit_sem, line_send, line_recv, plane_send, plane_recv, near_send, near_recv,
    pair_sems, head_plane_send, head_plane_recv, head_line_send, head_line_recv,
):
    me = lax.axis_index("stream")
    depth = slabs // PLANE
    layer, low = me // PLANE, lax.rem(me, PLANE)
    parity, quad = lax.rem(me, 2), lax.rem(me // 2, 4)

    def flip(bit):
        return bit - 2 * bit * lax.rem(me // bit, 2)

    partner = me + flip(1)
    steps = (flip(2), flip(4), flip(2) + flip(4))
    def other_layer(k):
        rising = k + (k - layer + depth) // depth
        mirrored = depth - 1 - layer
        falling = depth - 1 - k - (k - mirrored + depth) // depth
        high = layer // ((depth + 1) // 2)
        return rising + (falling - rising) * lax.rem(high, 2)

    others = [other_layer(k) for k in range(depth - 1)]
    own_items, own_sessions = own_ref.at[0], own_ref.at[1]
    barrier = pltpu.get_barrier_semaphore()
    owned = own_bits.shape[1]
    bit_copy = pltpu.make_async_copy(
        bits_ref.at[:, pl.ds(pl.multiple_of(me * owned, owned), owned)], own_bits, bit_sem.at[0]
    )
    bit_copy.start()
    greeted = [partner] + [me + step for step in steps] + [o * PLANE + low for o in others]
    for to in greeted:
        pl.semaphore_signal(
            barrier, inc=1, device_id={"stream": to}, device_id_type=pl.DeviceIdType.MESH
        )
    half = blocks // 2
    own_pack[0:blocks] = own_items[...]
    own_pack[blocks : blocks + half] = own_sessions[0:half] | (own_sessions[half:blocks] << 16)
    all_ref[me] = own_pack[...]
    item_ref[8 : 8 + blocks] = own_items[...]
    session_ref[8 : 8 + blocks] = own_sessions[...]
    for edge in (slice(0, 8), slice(8 + blocks, 16 + blocks)):
        item_ref[edge] = jnp.zeros((8, LANES), jnp.int32)
        session_ref[edge] = jnp.full((8, LANES), -1, jnp.int32)
    sub = lax.broadcasted_iota(jnp.int32, (LANES, LANES), 0)
    lane = lax.broadcasted_iota(jnp.int32, (LANES, LANES), 1)
    low_lane = lax.broadcasted_iota(jnp.int32, (1, LANES), 1) < LANES // 2
    ids = lax.broadcasted_iota(jnp.int32, (rows, LANES), 0)
    gaps = (sub - LANES // 2 - lane, sub + LANES // 2 - lane)
    in_reach = [(jnp.abs(gap) <= WINDOW) & (gap != 0) for gap in gaps]
    ones = jnp.ones((8, 2 * LANES), jnp.float32).astype(jnp.bfloat16)
    links_ref[...] = jnp.zeros_like(links_ref)
    total_ref[...] = jnp.zeros_like(total_ref)

    def block(b, unused):
        def around(ref):
            turned = [pltpu.roll(ref[pl.ds(b + o, 1)], LANES // 2, 1) for o in (7, 8, 9)]
            return (
                jnp.where(low_lane, turned[0], turned[1]),
                jnp.where(low_lane, turned[1], turned[2]),
            )

        own_item, own_session = item_ref[pl.ds(b + 8, 1)], session_ref[pl.ds(b + 8, 1)]
        hot = jnp.concatenate([one_where(ids == item) for item in around(item_ref)], axis=1)
        linked = jnp.concatenate(
            [
                one_where((jnp.broadcast_to(session, (LANES, LANES)).T == own_session) & reach)
                for session, reach in zip(around(session_ref), in_reach)
            ],
            axis=0,
        )
        links = jnp.dot(jnp.concatenate([hot, ones], axis=0), linked, preferred_element_type=jnp.float32)
        links_ref[...] += lax.dot_general(
            links.astype(jnp.bfloat16), one_where(ids == own_item), NT, preferred_element_type=jnp.float32
        )
        total_ref[...] += links[rows:]
        return unused

    inner = [blocks * n // 32 for n in (0, 8, 28, 32)]

    def blocks_of(n):
        lax.fori_loop(inner[n], inner[n + 1], block, 0, unroll=4)

    step_columns = max(LANES, owned // 16)
    steps_in_all = owned // step_columns

    def signs(low_step, high_step):
        def step(t, unused):
            at = pl.multiple_of(t * step_columns, step_columns)
            sign_ref[:, pl.ds(at, step_columns)] = sign_table(own_bits[:, pl.ds(at, step_columns)], sign_ref.shape[0])
            return unused

        lax.fori_loop(low_step * steps_in_all // 16, high_step * steps_in_all // 16, step, 0)

    blocks_of(0)
    bit_copy.wait()
    pl.semaphore_wait(barrier, len(greeted))

    def along_line(there, here):
        return send(
            own_pack, all_ref.at[me], line_send.at[there], line_recv.at[here], there * PLANE + low
        )

    def in_plane(d, at_layer, own=False):
        slab = all_ref.at[at_layer * PLANE + low]
        sem = d * depth + at_layer
        return send(own_pack if own else slab, slab, plane_send.at[sem], plane_recv.at[sem], me + steps[d])

    def to_partner(r, at_layer, own=False):
        slab = all_ref.at[at_layer * PLANE + low + ((0,) + steps)[r]]
        sem = r * depth + at_layer
        return send(own_pack if own else slab, slab, near_send.at[sem], near_recv.at[sem], partner)

    for o in reversed(others):
        along_line(o, layer).start()
    for d in range(3):
        in_plane(d, layer, True).start()
    to_partner(0, layer, True).start()

    def forward_line(k):
        along_line(layer, others[k]).wait_recv()
        for d in range(3):
            in_plane(d, others[k]).start()
        to_partner(0, others[k]).start()

    def forward_plane(at_layer):
        for d in range(3):
            in_plane(d, at_layer).wait_recv()
            to_partner(d + 1, at_layer).start()

    blocks_of(1)
    forward_line(0)
    blocks_of(2)
    share = rows // slabs
    tail = jnp.concatenate(
        [links_ref[rows : rows + 1], total_ref[0:1], jnp.zeros((6 - share, LANES), jnp.float32)], axis=0
    )
    for d in range(slabs):
        at = (d % 2, d // PLANE, d // 2 % 4)
        pair_out[at + (slice(0, share),)] = links_ref[d * share : (d + 1) * share]
        pair_out[at + (slice(share, 8),)] = tail

    pair = send(pair_out.at[1 - parity], pair_in, pair_sems.at[0], pair_sems.at[1], partner)
    pair.start()
    forward_line(1)
    signs(0, 2)
    pair.wait()
    line_out[...] = pair_out[parity] + pair_in[...]

    def head_line(there, here):
        return send(
            line_out.at[there], line_in.at[layer], head_line_send.at[there], head_line_recv.at[here],
            there * PLANE + low,
        )

    for o in others:
        head_line(o, layer).start()
    line_in[layer] = line_out[layer]
    forward_plane(layer)
    for k in range(2, depth - 1):
        forward_line(k)
    signs(2, 6)
    forward_plane(others[0])
    signs(6, 9)
    for o in others[1:-1]:
        forward_plane(o)
    for o in others:
        head_line(o, o).wait_recv()
    plane_out[...] = jnp.sum(line_in[...], axis=0)

    def head_plane(d):
        to = me + steps[d]
        return send(
            plane_out.at[lax.rem(to // 2, 4)], plane_in.at[d], head_plane_send.at[d], head_plane_recv.at[d], to
        )

    for d in range(3):
        head_plane(d).start()
    signs(9, 12)
    for o in others[-1:]:
        forward_plane(o)
    signs(12, 16)
    for at_layer in [layer] + others:
        for r in range(4):
            to_partner(r, at_layer).wait()
        for d in range(3):
            in_plane(d, at_layer).wait_send()
    for o in others:
        along_line(o, layer).wait_send()
        head_line(o, o).wait_send()
    for d in range(3):
        head_plane(d).wait()
    head_ref[...] = plane_out[quad] + plane_in[0] + plane_in[1] + plane_in[2]


def take_windows(code_ref, length, start):
    whole, part = start >> 3, start & 7
    bits = max(1, (length // 8 - 1).bit_length())
    keep = 8 * ((1 << (bits - 1)) + 4)
    value = None
    for bit in reversed(range(bits)):
        step = 8 << bit
        keep = 8 * ((1 << bit) + 4)
        chosen = ((whole >> bit) & 1) == 1
        if value is None:
            low, high = code_ref[0:keep, :], code_ref[step : step + keep, :]
        else:
            low, high = value[0:keep], value[step : step + keep]
        value = jnp.where(chosen, high, low)
    for bit in (2, 1, 0):
        chosen = ((part >> bit) & 1) == 1
        value = jnp.where(chosen, pltpu.roll(value, value.shape[0] - (1 << bit), 0), value)
    return value[0:32]


def all_rows(value, combine):
    for shift in (4, 2, 1):
        value = combine(value, pltpu.roll(value, shift, 0))
    return value


def bytes_of_rows(tag):
    return tag[0:8] | (tag[8:16] << 8) | (tag[16:24] << 16) | (tag[24:32] << 24)


def plane_word(packed, k):
    sub = lax.broadcasted_iota(jnp.int32, (8, LANES), 0)
    spread = lax.shift_left(lax.shift_right_logical(packed, k) & 0x01010101, sub)
    return all_rows(spread, lambda x, y: x | y)


def head_counts(window, ok, near, rows):
    center = window[16:17]
    linked = ((window ^ center) >> ITEM_BITS == 0) & near & ok
    item = window & ((1 << ITEM_BITS) - 1)
    tag = jnp.where(linked & (item < rows), item | rows, 0)
    packed = bytes_of_rows(tag)
    one = jnp.where(linked, 1, 0)
    weight = all_rows(one[0:8] + one[8:16] + one[16:24] + one[24:32], lambda x, y: x + y)
    sub = lax.broadcasted_iota(jnp.int32, (8, LANES), 0)

    def plane(k):
        return plane_word(packed, k)

    bits = rows.bit_length() - 1
    node = plane(bits)
    for k in range(3):
        node = node & (plane(k) ^ (((sub >> k) & 1) - 1))
    nodes = [node]
    for k in reversed(range(3, bits)):
        word = plane(k)
        nodes = [part for node in nodes for part in (node & ~word, node & word)]
    counts = jnp.concatenate([lax.population_count(node).astype(jnp.float32) for node in nodes], axis=0)
    return counts.astype(jnp.bfloat16), weight[0:1].astype(jnp.float32), center & ((1 << ITEM_BITS) - 1)


def tile_kernel(rows, length, parts, base_ref, all_ref, count_ref, margin_ref, flat_ref, code_ref, mask_ref):
    item_mask = (1 << ITEM_BITS) - 1
    base = base_ref[0]
    count_ref[...] = jnp.zeros_like(count_ref)
    margin_ref[...] = jnp.zeros_like(margin_ref)
    bands, unused_rows, width = count_ref.shape
    band = parts * width
    slabs, blocks = all_ref.shape[0], all_ref.shape[1] * 2 // 3
    for n in range(slabs):
        paired = all_ref[n, blocks:]
        sessions = jnp.concatenate([paired & 0xFFFF, paired >> 16], axis=0)
        flat_ref[n * blocks : (n + 1) * blocks] = all_ref[n, 0:blocks] | (sessions << ITEM_BITS)
    per = length // LANES
    for r in range(per):
        code_ref[16 + r * LANES : 16 + (r + 1) * LANES] = flat_ref[pl.ds(r, LANES, stride=per), :].T
    lane = lax.broadcasted_iota(jnp.int32, (16, LANES), 1)
    code_ref[0:16] = jnp.where(lane == 0, -1, pltpu.roll(code_ref[length : length + 16], 1, 1))
    code_ref[length + 16 : length + 32] = jnp.where(
        lane == LANES - 1, -1, pltpu.roll(code_ref[16:32], LANES - 1, 1)
    )

    words = length // 32
    band_bits = (bands - 1).bit_length()
    for w in range(words):
        item = code_ref[16 + 32 * w : 48 + 32 * w] & item_mask
        local = item - base
        mine = (local >= 0) & (local < bands * band) & (item >= rows)
        packed = bytes_of_rows(jnp.where(mine, (local >> (band.bit_length() - 1)) | bands, 0))
        for k in range(band_bits + 1):
            mask_ref[k, w : w + 1] = plane_word(packed, k)[0:1]
    planes = [mask_ref[k] for k in range(band_bits + 1)]
    for s in range(bands):
        mask = planes[band_bits]
        for k in range(band_bits):
            mask = mask & (planes[k] if s >> k & 1 else ~planes[k])
        mask_ref[s] = mask
    bounds = []
    for s in range(bands):
        tally = jnp.sum(lax.population_count(mask_ref[s]), axis=0, keepdims=True)
        bounds.append((jnp.max(tally) + 1) // 2 + (bounds[-1] if bounds else 0))

    word_ids = lax.broadcasted_iota(jnp.int32, (words, LANES), 0)
    d_ids = lax.broadcasted_iota(jnp.int32, (32, LANES), 0)
    near = (d_ids >= 1) & (d_ids != 16)
    tile = min(width, 256)
    t_ids = lax.broadcasted_iota(jnp.int32, (tile, 2 * LANES), 0).astype(jnp.float32).astype(jnp.bfloat16)
    p_ids = lax.broadcasted_iota(jnp.int32, (16, 2 * LANES), 0)

    def ends(mask):
        some = mask != 0
        first_row = jnp.min(jnp.where(some, word_ids, words), axis=0, keepdims=True)
        last_row = jnp.max(jnp.where(some, word_ids, -1), axis=0, keepdims=True)
        at_first, at_last = word_ids == first_row, word_ids == last_row
        first_word = jnp.sum(jnp.where(at_first, mask, 0), axis=0, keepdims=True)
        last_word = jnp.sum(jnp.where(at_last, mask, 0), axis=0, keepdims=True)
        first_bit = first_word & -first_word
        last_place = 31 - lax.clz(last_word)
        last_bit = jnp.where(last_word == 0, 0, jnp.left_shift(1, last_place & 31))
        first = 32 * first_row + lax.population_count(first_bit - 1)
        last = 32 * last_row + last_place
        first_ok = first_word != 0
        last_ok = first_ok & (last > first)
        mask = mask & ~(jnp.where(at_first, first_bit, 0) | jnp.where(at_last, last_bit, 0))
        return mask, ((first, first_ok), (last, last_ok))

    def find(s):
        mask, found = ends(mask_ref[s])
        mask_ref[s] = mask
        links, weights, locals_ = [], [], []
        for at, ok in found:
            window = take_windows(code_ref, length, jnp.where(ok, at, 0))
            counts, weight, item = head_counts(window, ok, near, rows)
            links.append(counts)
            weights.append(weight)
            locals_.append(item - base - s * band)
        return tuple(jnp.concatenate(x, axis=1) for x in (links, weights, locals_))

    def count(s, links, weight, local):
        part = local >> (width.bit_length() - 1)
        inner = local & (width - 1)
        pieces = []
        for p in range(parts):
            chosen = jnp.broadcast_to(jnp.where(part == p, 1.0, 0.0), (16, 2 * LANES)).astype(jnp.bfloat16)
            pieces += [links[n : n + 16] * chosen for n in range(0, rows, 16)]
        pieces.append(jnp.where(p_ids == part, weight, 0.0).astype(jnp.bfloat16))
        left = jnp.concatenate(pieces, axis=0)
        for t in range(width // tile):
            inside = (inner >= t * tile) & (inner < (t + 1) * tile)
            hot = hot_columns(t_ids, jnp.where(inside, inner - t * tile, -1).astype(jnp.float32))
            cols = slice(t * tile, (t + 1) * tile)
            value = lax.dot_general(left, hot, NT, preferred_element_type=jnp.float32)
            count_ref[s, :, cols] += value[0 : parts * rows]
            margin_ref[s, :, cols] += value[parts * rows :]

    def band_of(trip):
        s = jnp.int32(0)
        for bound in bounds[:-1]:
            s += jnp.where(trip >= bound, 1, 0)
        return s

    def body(trip, found):
        count(band_of(trip), *found)
        return find(band_of(trip + 1))

    lax.fori_loop(0, bounds[-1], body, find(band_of(0)))


def sign_table(words, width):
    size = words.shape[1]

    def wide(value):
        return jnp.concatenate([value] * (size // LANES), axis=1)

    shift = lax.broadcasted_iota(jnp.int32, (8, LANES), 0)
    parts = []
    for g in range(width // 8):
        word = 8 * g // BITS_PER_WORD
        split, offset = (word + 1) * BITS_PER_WORD - 8 * g, 8 * g - word * BITS_PER_WORD
        now = jnp.broadcast_to(words[word : word + 1], (8, size))
        where_bit = jnp.left_shift(1, shift + offset)
        if split < 8:
            later = jnp.broadcast_to(words[word + 1 : word + 2], (8, size))
            now = jnp.where(wide(shift) >= split, later, now)
            place = jnp.where(shift >= split, shift - split, shift + offset)
            where_bit = jnp.left_shift(1, place)
        parts.append(jnp.where((now & wide(where_bit)) != 0, 1.0, -1.0))
    return jnp.concatenate(parts, axis=0).astype(jnp.bfloat16)


def boundary_counts(rows, share, me, all_ref, extra_ref):
    slabs, blocks = all_ref.shape[0], all_ref.shape[1] * 2 // 3
    half = blocks // 2
    group = slabs // 4
    sub = lax.broadcasted_iota(jnp.int32, (LANES, LANES), 0)
    lane = lax.broadcasted_iota(jnp.int32, (LANES, LANES), 1)
    ids = lax.broadcasted_iota(jnp.int32, (rows, LANES), 0)
    small = lax.broadcasted_iota(jnp.int32, (group, LANES), 1)
    last_items, last_sessions = all_ref[:, blocks - 1, :], all_ref[:, blocks + half - 1, :] >> 16
    next_items, next_sessions = all_ref[:, 0, :], all_ref[:, blocks, :] & 0xFFFF

    def meet(last, following):
        joined = None
        for g in range(4):
            shift = 32 * g + 16
            pieces = (pltpu.roll(x[g * group : (g + 1) * group], shift, 1) for x in (last, following))
            both = jnp.where(small % 32 < 16, *pieces)
            joined = both if joined is None else jnp.where(small // 32 == g, both, joined)
        return joined

    slab_ids = lax.broadcasted_iota(jnp.int32, (slabs, LANES), 0)
    next_sessions = jnp.where(slab_ids == slabs - 1, -1, pltpu.roll(next_sessions, slabs - 1, 0))
    met_items = meet(last_items, pltpu.roll(next_items, slabs - 1, 0))
    met_sessions = meet(last_sessions, next_sessions)
    crossing = ((sub >> 5) == (lane >> 5)) & (((sub ^ lane) & 16) != 0) & (jnp.abs(sub - lane) <= WINDOW)
    ones = jnp.ones((8, LANES), jnp.float32).astype(jnp.bfloat16)
    extra = jnp.zeros((rows + 8, LANES), jnp.float32)
    total = jnp.zeros((8, LANES), jnp.float32)
    for g in range(group):
        item, session = met_items[g : g + 1], met_sessions[g : g + 1]
        linked = one_where((jnp.broadcast_to(session, (LANES, LANES)).T == session) & crossing)
        hot = one_where(ids == item)
        links = jnp.dot(jnp.concatenate([hot, ones], axis=0), linked, preferred_element_type=jnp.float32)
        extra += lax.dot_general(links.astype(jnp.bfloat16), hot, NT, preferred_element_type=jnp.float32)
        total += links[rows:]
    extra_ref[...] = extra
    return jnp.concatenate(
        [
            extra_ref[pl.ds(me * share, share)],
            extra_ref[rows : rows + 1],
            total[0:1],
            jnp.zeros((6 - share, LANES), jnp.float32),
        ],
        axis=0,
    )


def sketch_kernel(
    slabs, rows, parts, width, scale, count_ref, margin_ref, head_ref, sign_ref, all_ref, bits_ref, out_ref,
    extra_ref, log_ref, head_bits, acc_ref, send_ref, recv_ref, bit_sem, send_sems, recv_sems,
):
    me = lax.axis_index("stream")
    barrier = greet_all(slabs, me)
    bands, unused_rows, part = count_ref.shape
    share = rows // slabs
    tile = min(part, 512)
    head_copy = pltpu.make_async_copy(bits_ref.at[:, 0:rows], head_bits, bit_sem.at[0])
    head_copy.start()

    log_ref[...] = jnp.log(jnp.maximum(margin_ref[...], 1.0))
    head = head_ref[...] + boundary_counts(rows, share, me, all_ref, extra_ref)
    row_log = jnp.log(jnp.maximum(head[share : share + 1], 1.0))
    column_log = jnp.broadcast_to(row_log, (rows, LANES)).T
    total_log = jnp.log(jnp.sum(head[share + 1 : share + 2], axis=1, keepdims=True))
    row_term = total_log - column_log[:, 0:1]
    def product(positive, signs):
        upper = positive.astype(jnp.bfloat16)
        lower = (positive - upper.astype(jnp.float32)).astype(jnp.bfloat16)
        both = jnp.concatenate([upper, lower], axis=0)
        value = lax.dot_general(both, signs, NT, preferred_element_type=jnp.float32)
        return value[0:rows] + value[rows:]

    head_copy.wait()
    row = lax.broadcasted_iota(jnp.int32, (8, LANES), 0)
    shared = jnp.concatenate(
        [jnp.where(row < share, head, 0.0), jnp.zeros((rows - 8, LANES), jnp.float32)], axis=0
    )
    shared = pltpu.roll(shared, me * share, 0)
    ratio = jnp.log(jnp.maximum(shared, 1.0)) + total_log - row_log - column_log
    first_band = jnp.where(lax.axis_index("item") == 0, 1.0, 0.0)
    positive = jnp.where(shared > 0, jnp.maximum(ratio, 0.0), 0.0) * first_band
    acc_ref[...] = product(positive.T, sign_table(head_bits[...], width))

    for s in range(bands):
        for h in range(parts):
            for at in range(0, part, tile):
                counts = count_ref[s, h * rows : (h + 1) * rows, at : at + tile]
                ratio = jnp.log(jnp.maximum(counts, 1.0)) + row_term - log_ref[s, h : h + 1, at : at + tile]
                positive = jnp.where(counts > 0, jnp.maximum(ratio, 0.0), 0.0)
                bit_at = (s * parts + h) * part + at
                acc_ref[...] += product(positive, sign_ref[:, bit_at : bit_at + tile])

    cuts = width // LANES
    for d in range(slabs):
        for c in range(cuts):
            send_ref[d, c * share : (c + 1) * share] = (
                acc_ref[d * share : (d + 1) * share, c * LANES : (c + 1) * LANES] * scale
            )
    pl.semaphore_wait(barrier, slabs - 1)
    exchange(slabs, me, send_ref, recv_ref, send_sems, recv_sems, True)
    exchange(slabs, me, send_ref, recv_ref, send_sems, recv_sems, False)
    summed = jnp.sum(recv_ref[...], axis=0)
    out_ref[...] = jnp.concatenate([summed[c * share : (c + 1) * share] for c in range(cuts)], axis=1)


def local(event_items, event_sessions, sketch_bits):
    slabs = lax.axis_size("stream")
    slab = event_items.shape[0]
    total_events = slab * slabs
    words, band_size = sketch_bits.shape
    owned = band_size // slabs
    rows, width = 128, 256
    part = max(LANES, owned // 16)
    bands = BANDS
    parts = owned // (bands * part)
    me = lax.axis_index("stream")
    own_start = me * owned
    first_id = lax.axis_index("item") * band_size + own_start
    blocks = slab // LANES
    length = total_events // LANES

    dma = pltpu.SemaphoreType.DMA
    depth = slabs // PLANE
    events, head, signs = pl.pallas_call(
        functools.partial(gather_kernel, slabs, rows, blocks),
        out_shape=(
            jax.ShapeDtypeStruct((slabs, blocks * 3 // 2, LANES), jnp.int32),
            jax.ShapeDtypeStruct((8, LANES), jnp.float32),
            jax.ShapeDtypeStruct((width, owned), jnp.bfloat16),
        ),
        in_specs=[VMEM, pl.BlockSpec(memory_space=pl.ANY)],
        out_specs=(VMEM, VMEM, VMEM),
        scratch_shapes=[
            pltpu.VMEM((blocks * 3 // 2, LANES), jnp.int32),
            pltpu.VMEM((words, owned), jnp.int32),
            pltpu.VMEM((blocks + 16, LANES), jnp.int32),
            pltpu.VMEM((blocks + 16, LANES), jnp.int32),
            pltpu.VMEM((rows + 8, LANES), jnp.float32),
            pltpu.VMEM((8, LANES), jnp.float32),
            pltpu.VMEM((2, depth, 4, 8, LANES), jnp.float32),
            pltpu.VMEM((depth, 4, 8, LANES), jnp.float32),
            pltpu.VMEM((4, 8, LANES), jnp.float32),
            pltpu.VMEM((3, 8, LANES), jnp.float32),
            pltpu.VMEM((depth, 4, 8, LANES), jnp.float32),
            pltpu.VMEM((depth, 4, 8, LANES), jnp.float32),
            dma((1,)),
            dma((depth,)),
            dma((depth,)),
            dma((3 * depth,)),
            dma((3 * depth,)),
            dma((4 * depth,)),
            dma((4 * depth,)),
            dma((2,)),
            dma((3,)),
            dma((3,)),
            dma((depth,)),
            dma((depth,)),
        ],
        compiler_params=pltpu.CompilerParams(
            collective_id=0, has_side_effects=True, vmem_limit_bytes=VMEM_GRANT
        ),
        name="gather_events",
    )(jnp.stack([event_items, event_sessions]).reshape(2, blocks, LANES), sketch_bits)

    counts, margins = pl.pallas_call(
        functools.partial(tile_kernel, rows, length, parts),
        out_shape=(
            jax.ShapeDtypeStruct((bands, parts * rows, part), jnp.float32),
            jax.ShapeDtypeStruct((bands, 16, part), jnp.float32),
        ),
        in_specs=[pl.BlockSpec(memory_space=pltpu.SMEM), VMEM],
        out_specs=(VMEM, VMEM),
        scratch_shapes=[
            pltpu.VMEM((length, LANES), jnp.int32),
            pltpu.VMEM((length + 32, LANES), jnp.int32),
            pltpu.VMEM((bands, length // 32, LANES), jnp.int32),
        ],
        compiler_params=pltpu.CompilerParams(vmem_limit_bytes=VMEM_GRANT),
        name="tile_counts",
    )(first_id.astype(jnp.int32)[None], events)

    own_rows = pl.pallas_call(
        functools.partial(sketch_kernel, slabs, rows, parts, width, 1.0 / math.sqrt(total_events)),
        out_shape=jax.ShapeDtypeStruct((rows // slabs, width), jnp.float32),
        in_specs=[VMEM] * 5 + [pl.BlockSpec(memory_space=pl.ANY)],
        out_specs=VMEM,
        scratch_shapes=[
            pltpu.VMEM((rows + 8, LANES), jnp.float32),
            pltpu.VMEM((bands, 16, part), jnp.float32),
            pltpu.VMEM((words, rows), jnp.int32),
            pltpu.VMEM((rows, width), jnp.float32),
            pltpu.VMEM((slabs, 8, LANES), jnp.float32),
            pltpu.VMEM((slabs, 8, LANES), jnp.float32),
            dma((1,)),
            dma((slabs,)),
            dma((slabs,)),
        ],
        compiler_params=pltpu.CompilerParams(
            collective_id=1, has_side_effects=True, vmem_limit_bytes=VMEM_GRANT
        ),
        name="sketch_tile",
    )(counts, margins, head, signs, events, sketch_bits)
    if lax.axis_size("item") > 1:
        own_rows = lax.psum(own_rows, "item")
    return own_rows


def solution(mesh):
    placed = (P("stream"), P("stream"), P(None, "item"))
    return jax.shard_map(
        local, mesh=mesh, in_specs=placed, out_specs=P("stream", None), check_vma=False
    )
```

```python
import functools
import math

import jax
import jax.numpy as jnp
from jax import lax
from jax.experimental import pallas as pl
from jax.experimental.pallas import tpu as pltpu
from jax.sharding import PartitionSpec as P

WINDOW = 15
ITEM_BITS = 18
LANES = 128
BITS_PER_WORD = 18
PLANE = 8
BANDS = 4
VMEM_GRANT = 45 * 1024 * 1024
NT = (((1,), (1,)), ((), ()))
VMEM = pl.BlockSpec(memory_space=pltpu.VMEM)


def one_where(mask):
    return jnp.where(mask, 1.0, 0.0).astype(jnp.bfloat16)


def hot_columns(ids, values):
    row = jnp.broadcast_to(values, (16, values.shape[1])).astype(jnp.bfloat16)
    one, zero = jnp.ones((), jnp.bfloat16), jnp.zeros((), jnp.bfloat16)
    return jnp.concatenate(
        [jnp.where(ids[n : n + 16] == row, one, zero) for n in range(0, ids.shape[0], 16)], axis=0
    )


def greet_all(slabs, me):
    barrier = pltpu.get_barrier_semaphore()

    for k in range(1, slabs):
        pl.semaphore_signal(
            barrier, inc=1, device_id={"stream": lax.rem(me + k, slabs)}, device_id_type=pl.DeviceIdType.MESH
        )
    return barrier


def send(src, dst, send_sem, recv_sem, to):
    return pltpu.make_async_remote_copy(
        src_ref=src,
        dst_ref=dst,
        send_sem=send_sem,
        recv_sem=recv_sem,
        device_id={"stream": to},
        device_id_type=pl.DeviceIdType.MESH,
    )


def each(low, high, do):
    for k in range(low, high):
        do(k)


def exchange(slabs, me, out_ref, in_ref, send_sems, recv_sems, start):
    def copy(k):
        to = lax.rem(me + k, slabs)
        return send(out_ref.at[to], in_ref.at[me], send_sems.at[k], recv_sems.at[k], to)

    if start:
        each(1, slabs, lambda k: copy(k).start())
        in_ref[me] = out_ref[me]
    else:
        each(1, slabs, lambda k: copy(k).wait())


def gather_kernel(
    slabs, rows, blocks, own_ref, bits_ref, all_ref, head_ref, sign_ref,
    own_pack, own_bits, item_ref, session_ref, links_ref, total_ref,
    pair_out, pair_in, plane_out, plane_in, line_out, line_in,
    bit_sem, line_send, line_recv, plane_send, plane_recv, near_send, near_recv,
    pair_sems, head_plane_send, head_plane_recv, head_line_send, head_line_recv,
):
    me = lax.axis_index("stream")
    depth = slabs // PLANE
    layer, low = me // PLANE, lax.rem(me, PLANE)
    parity, quad = lax.rem(me, 2), lax.rem(me // 2, 4)

    def flip(bit):
        return bit - 2 * bit * lax.rem(me // bit, 2)

    partner = me + flip(1)
    steps = (flip(2), flip(4), flip(2) + flip(4))
    def other_layer(k):
        rising = k + (k - layer + depth) // depth
        mirrored = depth - 1 - layer
        falling = depth - 1 - k - (k - mirrored + depth) // depth
        high = layer // ((depth + 1) // 2)
        return rising + (falling - rising) * lax.rem(high, 2)

    others = [other_layer(k) for k in range(depth - 1)]
    own_items, own_sessions = own_ref.at[0], own_ref.at[1]
    barrier = pltpu.get_barrier_semaphore()
    owned = own_bits.shape[1]
    bit_copy = pltpu.make_async_copy(
        bits_ref.at[:, pl.ds(pl.multiple_of(me * owned, owned), owned)], own_bits, bit_sem.at[0]
    )
    bit_copy.start()
    greeted = [partner] + [me + step for step in steps] + [o * PLANE + low for o in others]
    for to in greeted:
        pl.semaphore_signal(
            barrier, inc=1, device_id={"stream": to}, device_id_type=pl.DeviceIdType.MESH
        )
    half = blocks // 2
    own_pack[0:blocks] = own_items[...]
    own_pack[blocks : blocks + half] = own_sessions[0:half] | (own_sessions[half:blocks] << 16)
    all_ref[me] = own_pack[...]
    item_ref[8 : 8 + blocks] = own_items[...]
    session_ref[8 : 8 + blocks] = own_sessions[...]
    for edge in (slice(0, 8), slice(8 + blocks, 16 + blocks)):
        item_ref[edge] = jnp.zeros((8, LANES), jnp.int32)
        session_ref[edge] = jnp.full((8, LANES), -1, jnp.int32)
    sub = lax.broadcasted_iota(jnp.int32, (LANES, LANES), 0)
    lane = lax.broadcasted_iota(jnp.int32, (LANES, LANES), 1)
    low_lane = lax.broadcasted_iota(jnp.int32, (1, LANES), 1) < LANES // 2
    ids = lax.broadcasted_iota(jnp.int32, (rows, LANES), 0)
    gaps = (sub - LANES // 2 - lane, sub + LANES // 2 - lane)
    in_reach = [(jnp.abs(gap) <= WINDOW) & (gap != 0) for gap in gaps]
    ones = jnp.ones((8, 2 * LANES), jnp.float32).astype(jnp.bfloat16)
    links_ref[...] = jnp.zeros_like(links_ref)
    total_ref[...] = jnp.zeros_like(total_ref)

    def block(b, unused):
        def around(ref):
            turned = [pltpu.roll(ref[pl.ds(b + o, 1)], LANES // 2, 1) for o in (7, 8, 9)]
            return (
                jnp.where(low_lane, turned[0], turned[1]),
                jnp.where(low_lane, turned[1], turned[2]),
            )

        own_item, own_session = item_ref[pl.ds(b + 8, 1)], session_ref[pl.ds(b + 8, 1)]
        hot = jnp.concatenate([one_where(ids == item) for item in around(item_ref)], axis=1)
        linked = jnp.concatenate(
            [
                one_where((jnp.broadcast_to(session, (LANES, LANES)).T == own_session) & reach)
                for session, reach in zip(around(session_ref), in_reach)
            ],
            axis=0,
        )
        links = jnp.dot(jnp.concatenate([hot, ones], axis=0), linked, preferred_element_type=jnp.float32)
        links_ref[...] += lax.dot_general(
            links.astype(jnp.bfloat16), one_where(ids == own_item), NT, preferred_element_type=jnp.float32
        )
        total_ref[...] += links[rows:]
        return unused

    inner = [blocks * n // 32 for n in (0, 8, 28, 32)]

    def blocks_of(n):
        lax.fori_loop(inner[n], inner[n + 1], block, 0, unroll=4)

    step_columns = max(LANES, owned // 16)
    steps_in_all = owned // step_columns

    def signs(low_step, high_step):
        def step(t, unused):
            at = pl.multiple_of(t * step_columns, step_columns)
            sign_ref[:, pl.ds(at, step_columns)] = sign_table(own_bits[:, pl.ds(at, step_columns)], sign_ref.shape[0])
            return unused

        lax.fori_loop(low_step * steps_in_all // 16, high_step * steps_in_all // 16, step, 0)

    blocks_of(0)
    bit_copy.wait()
    pl.semaphore_wait(barrier, len(greeted))

    def along_line(there, here):
        return send(
            own_pack, all_ref.at[me], line_send.at[there], line_recv.at[here], there * PLANE + low
        )

    def in_plane(d, at_layer, own=False):
        slab = all_ref.at[at_layer * PLANE + low]
        sem = d * depth + at_layer
        return send(own_pack if own else slab, slab, plane_send.at[sem], plane_recv.at[sem], me + steps[d])

    def to_partner(r, at_layer, own=False):
        slab = all_ref.at[at_layer * PLANE + low + ((0,) + steps)[r]]
        sem = r * depth + at_layer
        return send(own_pack if own else slab, slab, near_send.at[sem], near_recv.at[sem], partner)

    for o in reversed(others):
        along_line(o, layer).start()
    for d in range(3):
        in_plane(d, layer, True).start()
    to_partner(0, layer, True).start()

    def forward_line(k):
        along_line(layer, others[k]).wait_recv()
        for d in range(3):
            in_plane(d, others[k]).start()
        to_partner(0, others[k]).start()

    def forward_plane(at_layer):
        for d in range(3):
            in_plane(d, at_layer).wait_recv()
            to_partner(d + 1, at_layer).start()

    blocks_of(1)
    forward_line(0)
    blocks_of(2)
    share = rows // slabs
    tail = jnp.concatenate(
        [links_ref[rows : rows + 1], total_ref[0:1], jnp.zeros((6 - share, LANES), jnp.float32)], axis=0
    )
    for d in range(slabs):
        at = (d % 2, d // PLANE, d // 2 % 4)
        pair_out[at + (slice(0, share),)] = links_ref[d * share : (d + 1) * share]
        pair_out[at + (slice(share, 8),)] = tail

    pair = send(pair_out.at[1 - parity], pair_in, pair_sems.at[0], pair_sems.at[1], partner)
    pair.start()
    forward_line(1)
    signs(0, 2)
    pair.wait()
    line_out[...] = pair_out[parity] + pair_in[...]

    def head_line(there, here):
        return send(
            line_out.at[there], line_in.at[layer], head_line_send.at[there], head_line_recv.at[here],
            there * PLANE + low,
        )

    for o in others:
        head_line(o, layer).start()
    line_in[layer] = line_out[layer]
    forward_plane(layer)
    for k in range(2, depth - 1):
        forward_line(k)
    signs(2, 6)
    forward_plane(others[0])
    signs(6, 9)
    for o in others[1:-1]:
        forward_plane(o)
    for o in others:
        head_line(o, o).wait_recv()
    plane_out[...] = jnp.sum(line_in[...], axis=0)

    def head_plane(d):
        to = me + steps[d]
        return send(
            plane_out.at[lax.rem(to // 2, 4)], plane_in.at[d], head_plane_send.at[d], head_plane_recv.at[d], to
        )

    for d in range(3):
        head_plane(d).start()
    signs(9, 12)
    for o in others[-1:]:
        forward_plane(o)
    signs(12, 16)
    for at_layer in [layer] + others:
        for r in range(4):
            to_partner(r, at_layer).wait()
        for d in range(3):
            in_plane(d, at_layer).wait_send()
    for o in others:
        along_line(o, layer).wait_send()
        head_line(o, o).wait_send()
    for d in range(3):
        head_plane(d).wait()
    head_ref[...] = plane_out[quad] + plane_in[0] + plane_in[1] + plane_in[2]


def take_windows(code_ref, length, start):
    whole, part = start >> 3, start & 7
    bits = max(1, (length // 8 - 1).bit_length())
    keep = 8 * ((1 << (bits - 1)) + 4)
    value = None
    for bit in reversed(range(bits)):
        step = 8 << bit
        keep = 8 * ((1 << bit) + 4)
        chosen = ((whole >> bit) & 1) == 1
        if value is None:
            low, high = code_ref[0:keep, :], code_ref[step : step + keep, :]
        else:
            low, high = value[0:keep], value[step : step + keep]
        value = jnp.where(chosen, high, low)
    for bit in (2, 1, 0):
        chosen = ((part >> bit) & 1) == 1
        value = jnp.where(chosen, pltpu.roll(value, value.shape[0] - (1 << bit), 0), value)
    return value[0:32]


def all_rows(value, combine):
    for shift in (4, 2, 1):
        value = combine(value, pltpu.roll(value, shift, 0))
    return value


def bytes_of_rows(tag):
    return tag[0:8] | (tag[8:16] << 8) | (tag[16:24] << 16) | (tag[24:32] << 24)


def plane_word(packed, k):
    sub = lax.broadcasted_iota(jnp.int32, (8, LANES), 0)
    spread = lax.shift_left(lax.shift_right_logical(packed, k) & 0x01010101, sub)
    return all_rows(spread, lambda x, y: x | y)


def head_counts(window, ok, near, rows):
    center = window[16:17]
    linked = ((window ^ center) >> ITEM_BITS == 0) & near & ok
    item = window & ((1 << ITEM_BITS) - 1)
    tag = jnp.where(linked & (item < rows), item | rows, 0)
    packed = bytes_of_rows(tag)
    one = jnp.where(linked, 1, 0)
    weight = all_rows(one[0:8] + one[8:16] + one[16:24] + one[24:32], lambda x, y: x + y)
    sub = lax.broadcasted_iota(jnp.int32, (8, LANES), 0)

    def plane(k):
        return plane_word(packed, k)

    bits = rows.bit_length() - 1
    node = plane(bits)
    for k in range(3):
        node = node & (plane(k) ^ (((sub >> k) & 1) - 1))
    nodes = [node]
    for k in reversed(range(3, bits)):
        word = plane(k)
        nodes = [part for node in nodes for part in (node & ~word, node & word)]
    counts = jnp.concatenate([lax.population_count(node).astype(jnp.float32) for node in nodes], axis=0)
    return counts.astype(jnp.bfloat16), weight[0:1].astype(jnp.float32), center & ((1 << ITEM_BITS) - 1)


def tile_kernel(rows, length, parts, base_ref, all_ref, count_ref, margin_ref, flat_ref, code_ref, mask_ref):
    item_mask = (1 << ITEM_BITS) - 1
    base = base_ref[0]
    count_ref[...] = jnp.zeros_like(count_ref)
    margin_ref[...] = jnp.zeros_like(margin_ref)
    bands, unused_rows, width = count_ref.shape
    band = parts * width
    slabs, blocks = all_ref.shape[0], all_ref.shape[1] * 2 // 3
    for n in range(slabs):
        paired = all_ref[n, blocks:]
        sessions = jnp.concatenate([paired & 0xFFFF, paired >> 16], axis=0)
        flat_ref[n * blocks : (n + 1) * blocks] = all_ref[n, 0:blocks] | (sessions << ITEM_BITS)
    per = length // LANES
    for r in range(per):
        code_ref[16 + r * LANES : 16 + (r + 1) * LANES] = flat_ref[pl.ds(r, LANES, stride=per), :].T
    lane = lax.broadcasted_iota(jnp.int32, (16, LANES), 1)
    code_ref[0:16] = jnp.where(lane == 0, -1, pltpu.roll(code_ref[length : length + 16], 1, 1))
    code_ref[length + 16 : length + 32] = jnp.where(
        lane == LANES - 1, -1, pltpu.roll(code_ref[16:32], LANES - 1, 1)
    )

    words = length // 32
    band_bits = (bands - 1).bit_length()
    for w in range(words):
        item = code_ref[16 + 32 * w : 48 + 32 * w] & item_mask
        local = item - base
        mine = (local >= 0) & (local < bands * band) & (item >= rows)
        packed = bytes_of_rows(jnp.where(mine, (local >> (band.bit_length() - 1)) | bands, 0))
        for k in range(band_bits + 1):
            mask_ref[k, w : w + 1] = plane_word(packed, k)[0:1]
    planes = [mask_ref[k] for k in range(band_bits + 1)]
    for s in range(bands):
        mask = planes[band_bits]
        for k in range(band_bits):
            mask = mask & (planes[k] if s >> k & 1 else ~planes[k])
        mask_ref[s] = mask
    tallies = [jnp.sum(lax.population_count(mask_ref[s]), axis=0, keepdims=True) for s in range(bands)]

    word_ids = lax.broadcasted_iota(jnp.int32, (words, LANES), 0)
    d_ids = lax.broadcasted_iota(jnp.int32, (32, LANES), 0)
    near = (d_ids >= 1) & (d_ids != 16)
    tile = min(width, 256)
    t_ids = lax.broadcasted_iota(jnp.int32, (tile, 2 * LANES), 0).astype(jnp.float32).astype(jnp.bfloat16)
    p_ids = lax.broadcasted_iota(jnp.int32, (16, 2 * LANES), 0)

    def ends(mask):
        some = mask != 0
        first_row = jnp.min(jnp.where(some, word_ids, words), axis=0, keepdims=True)
        last_row = jnp.max(jnp.where(some, word_ids, -1), axis=0, keepdims=True)
        at_first, at_last = word_ids == first_row, word_ids == last_row
        first_word = jnp.sum(jnp.where(at_first, mask, 0), axis=0, keepdims=True)
        last_word = jnp.sum(jnp.where(at_last, mask, 0), axis=0, keepdims=True)
        first_bit = first_word & -first_word
        last_place = 31 - lax.clz(last_word)
        last_bit = jnp.where(last_word == 0, 0, jnp.left_shift(1, last_place & 31))
        first = 32 * first_row + lax.population_count(first_bit - 1)
        last = 32 * last_row + last_place
        first_ok = first_word != 0
        last_ok = first_ok & (last > first)
        mask = mask & ~(jnp.where(at_first, first_bit, 0) | jnp.where(at_last, last_bit, 0))
        return mask, ((first, first_ok), (last, last_ok))

    def find(s, mask):
        mask, found = ends(mask)
        links, weights, locals_ = [], [], []
        for at, ok in found:
            window = take_windows(code_ref, length, jnp.where(ok, at, 0))
            counts, weight, item = head_counts(window, ok, near, rows)
            links.append(counts)
            weights.append(weight)
            locals_.append(item - base - s * band)
        return mask, *(jnp.concatenate(x, axis=1) for x in (links, weights, locals_))

    def count(s, links, weight, local):
        part = local >> (width.bit_length() - 1)
        inner = local & (width - 1)
        pieces = []
        for p in range(parts):
            chosen = jnp.broadcast_to(jnp.where(part == p, 1.0, 0.0), (16, 2 * LANES)).astype(jnp.bfloat16)
            pieces += [links[n : n + 16] * chosen for n in range(0, rows, 16)]
        pieces.append(jnp.where(p_ids == part, weight, 0.0).astype(jnp.bfloat16))
        left = jnp.concatenate(pieces, axis=0)
        for t in range(width // tile):
            inside = (inner >= t * tile) & (inner < (t + 1) * tile)
            hot = hot_columns(t_ids, jnp.where(inside, inner - t * tile, -1).astype(jnp.float32))
            cols = slice(t * tile, (t + 1) * tile)
            value = lax.dot_general(left, hot, NT, preferred_element_type=jnp.float32)
            count_ref[s, :, cols] += value[0 : parts * rows]
            margin_ref[s, :, cols] += value[parts * rows :]

    for low in range(0, bands, 2):
        both = range(low, min(low + 2, bands))
        most = functools.reduce(jnp.maximum, [tallies[s] for s in both])

        def body(unused, masks, both=both):
            out = []
            for s, mask in zip(both, masks):
                mask, *found = find(s, mask)
                out.append(mask)
                count(s, *found)
            return tuple(out)

        lax.fori_loop(0, (jnp.max(most) + 1) // 2, body, tuple(mask_ref[s] for s in both))


def sign_table(words, width):
    size = words.shape[1]

    def wide(value):
        return jnp.concatenate([value] * (size // LANES), axis=1)

    shift = lax.broadcasted_iota(jnp.int32, (8, LANES), 0)
    parts = []
    for g in range(width // 8):
        word = 8 * g // BITS_PER_WORD
        split, offset = (word + 1) * BITS_PER_WORD - 8 * g, 8 * g - word * BITS_PER_WORD
        now = jnp.broadcast_to(words[word : word + 1], (8, size))
        where_bit = jnp.left_shift(1, shift + offset)
        if split < 8:
            later = jnp.broadcast_to(words[word + 1 : word + 2], (8, size))
            now = jnp.where(wide(shift) >= split, later, now)
            place = jnp.where(shift >= split, shift - split, shift + offset)
            where_bit = jnp.left_shift(1, place)
        parts.append(jnp.where((now & wide(where_bit)) != 0, 1.0, -1.0))
    return jnp.concatenate(parts, axis=0).astype(jnp.bfloat16)


def boundary_counts(rows, share, me, all_ref, extra_ref):
    slabs, blocks = all_ref.shape[0], all_ref.shape[1] * 2 // 3
    half = blocks // 2
    group = slabs // 4
    sub = lax.broadcasted_iota(jnp.int32, (LANES, LANES), 0)
    lane = lax.broadcasted_iota(jnp.int32, (LANES, LANES), 1)
    ids = lax.broadcasted_iota(jnp.int32, (rows, LANES), 0)
    small = lax.broadcasted_iota(jnp.int32, (group, LANES), 1)
    last_items, last_sessions = all_ref[:, blocks - 1, :], all_ref[:, blocks + half - 1, :] >> 16
    next_items, next_sessions = all_ref[:, 0, :], all_ref[:, blocks, :] & 0xFFFF

    def meet(last, following):
        joined = None
        for g in range(4):
            shift = 32 * g + 16
            pieces = (pltpu.roll(x[g * group : (g + 1) * group], shift, 1) for x in (last, following))
            both = jnp.where(small % 32 < 16, *pieces)
            joined = both if joined is None else jnp.where(small // 32 == g, both, joined)
        return joined

    slab_ids = lax.broadcasted_iota(jnp.int32, (slabs, LANES), 0)
    next_sessions = jnp.where(slab_ids == slabs - 1, -1, pltpu.roll(next_sessions, slabs - 1, 0))
    met_items = meet(last_items, pltpu.roll(next_items, slabs - 1, 0))
    met_sessions = meet(last_sessions, next_sessions)
    crossing = ((sub >> 5) == (lane >> 5)) & (((sub ^ lane) & 16) != 0) & (jnp.abs(sub - lane) <= WINDOW)
    ones = jnp.ones((8, LANES), jnp.float32).astype(jnp.bfloat16)
    extra = jnp.zeros((rows + 8, LANES), jnp.float32)
    total = jnp.zeros((8, LANES), jnp.float32)
    for g in range(group):
        item, session = met_items[g : g + 1], met_sessions[g : g + 1]
        linked = one_where((jnp.broadcast_to(session, (LANES, LANES)).T == session) & crossing)
        hot = one_where(ids == item)
        links = jnp.dot(jnp.concatenate([hot, ones], axis=0), linked, preferred_element_type=jnp.float32)
        extra += lax.dot_general(links.astype(jnp.bfloat16), hot, NT, preferred_element_type=jnp.float32)
        total += links[rows:]
    extra_ref[...] = extra
    return jnp.concatenate(
        [
            extra_ref[pl.ds(me * share, share)],
            extra_ref[rows : rows + 1],
            total[0:1],
            jnp.zeros((6 - share, LANES), jnp.float32),
        ],
        axis=0,
    )


def sketch_kernel(
    slabs, rows, parts, width, scale, count_ref, margin_ref, head_ref, sign_ref, all_ref, bits_ref, out_ref,
    extra_ref, log_ref, head_bits, acc_ref, send_ref, recv_ref, bit_sem, send_sems, recv_sems,
):
    me = lax.axis_index("stream")
    barrier = greet_all(slabs, me)
    bands, unused_rows, part = count_ref.shape
    share = rows // slabs
    tile = min(part, 512)
    head_copy = pltpu.make_async_copy(bits_ref.at[:, 0:rows], head_bits, bit_sem.at[0])
    head_copy.start()

    log_ref[...] = jnp.log(jnp.maximum(margin_ref[...], 1.0))
    head = head_ref[...] + boundary_counts(rows, share, me, all_ref, extra_ref)
    row_log = jnp.log(jnp.maximum(head[share : share + 1], 1.0))
    column_log = jnp.broadcast_to(row_log, (rows, LANES)).T
    total_log = jnp.log(jnp.sum(head[share + 1 : share + 2], axis=1, keepdims=True))
    row_term = total_log - column_log[:, 0:1]
    def product(positive, signs):
        upper = positive.astype(jnp.bfloat16)
        lower = (positive - upper.astype(jnp.float32)).astype(jnp.bfloat16)
        both = jnp.concatenate([upper, lower], axis=0)
        value = lax.dot_general(both, signs, NT, preferred_element_type=jnp.float32)
        return value[0:rows] + value[rows:]

    head_copy.wait()
    row = lax.broadcasted_iota(jnp.int32, (8, LANES), 0)
    shared = jnp.concatenate(
        [jnp.where(row < share, head, 0.0), jnp.zeros((rows - 8, LANES), jnp.float32)], axis=0
    )
    shared = pltpu.roll(shared, me * share, 0)
    ratio = jnp.log(jnp.maximum(shared, 1.0)) + total_log - row_log - column_log
    first_band = jnp.where(lax.axis_index("item") == 0, 1.0, 0.0)
    positive = jnp.where(shared > 0, jnp.maximum(ratio, 0.0), 0.0) * first_band
    acc_ref[...] = product(positive.T, sign_table(head_bits[...], width))

    for s in range(bands):
        for h in range(parts):
            for at in range(0, part, tile):
                counts = count_ref[s, h * rows : (h + 1) * rows, at : at + tile]
                ratio = jnp.log(jnp.maximum(counts, 1.0)) + row_term - log_ref[s, h : h + 1, at : at + tile]
                positive = jnp.where(counts > 0, jnp.maximum(ratio, 0.0), 0.0)
                bit_at = (s * parts + h) * part + at
                acc_ref[...] += product(positive, sign_ref[:, bit_at : bit_at + tile])

    cuts = width // LANES
    for d in range(slabs):
        for c in range(cuts):
            send_ref[d, c * share : (c + 1) * share] = (
                acc_ref[d * share : (d + 1) * share, c * LANES : (c + 1) * LANES] * scale
            )
    pl.semaphore_wait(barrier, slabs - 1)
    exchange(slabs, me, send_ref, recv_ref, send_sems, recv_sems, True)
    exchange(slabs, me, send_ref, recv_ref, send_sems, recv_sems, False)
    summed = jnp.sum(recv_ref[...], axis=0)
    out_ref[...] = jnp.concatenate([summed[c * share : (c + 1) * share] for c in range(cuts)], axis=1)


def local(event_items, event_sessions, sketch_bits):
    slabs = lax.axis_size("stream")
    slab = event_items.shape[0]
    total_events = slab * slabs
    words, band_size = sketch_bits.shape
    owned = band_size // slabs
    rows, width = 128, 256
    part = max(LANES, owned // 16)
    bands = BANDS
    parts = owned // (bands * part)
    me = lax.axis_index("stream")
    own_start = me * owned
    first_id = lax.axis_index("item") * band_size + own_start
    blocks = slab // LANES
    length = total_events // LANES

    dma = pltpu.SemaphoreType.DMA
    depth = slabs // PLANE
    events, head, signs = pl.pallas_call(
        functools.partial(gather_kernel, slabs, rows, blocks),
        out_shape=(
            jax.ShapeDtypeStruct((slabs, blocks * 3 // 2, LANES), jnp.int32),
            jax.ShapeDtypeStruct((8, LANES), jnp.float32),
            jax.ShapeDtypeStruct((width, owned), jnp.bfloat16),
        ),
        in_specs=[VMEM, pl.BlockSpec(memory_space=pl.ANY)],
        out_specs=(VMEM, VMEM, VMEM),
        scratch_shapes=[
            pltpu.VMEM((blocks * 3 // 2, LANES), jnp.int32),
            pltpu.VMEM((words, owned), jnp.int32),
            pltpu.VMEM((blocks + 16, LANES), jnp.int32),
            pltpu.VMEM((blocks + 16, LANES), jnp.int32),
            pltpu.VMEM((rows + 8, LANES), jnp.float32),
            pltpu.VMEM((8, LANES), jnp.float32),
            pltpu.VMEM((2, depth, 4, 8, LANES), jnp.float32),
            pltpu.VMEM((depth, 4, 8, LANES), jnp.float32),
            pltpu.VMEM((4, 8, LANES), jnp.float32),
            pltpu.VMEM((3, 8, LANES), jnp.float32),
            pltpu.VMEM((depth, 4, 8, LANES), jnp.float32),
            pltpu.VMEM((depth, 4, 8, LANES), jnp.float32),
            dma((1,)),
            dma((depth,)),
            dma((depth,)),
            dma((3 * depth,)),
            dma((3 * depth,)),
            dma((4 * depth,)),
            dma((4 * depth,)),
            dma((2,)),
            dma((3,)),
            dma((3,)),
            dma((depth,)),
            dma((depth,)),
        ],
        compiler_params=pltpu.CompilerParams(
            collective_id=0, has_side_effects=True, vmem_limit_bytes=VMEM_GRANT
        ),
        name="gather_events",
    )(jnp.stack([event_items, event_sessions]).reshape(2, blocks, LANES), sketch_bits)

    counts, margins = pl.pallas_call(
        functools.partial(tile_kernel, rows, length, parts),
        out_shape=(
            jax.ShapeDtypeStruct((bands, parts * rows, part), jnp.float32),
            jax.ShapeDtypeStruct((bands, 16, part), jnp.float32),
        ),
        in_specs=[pl.BlockSpec(memory_space=pltpu.SMEM), VMEM],
        out_specs=(VMEM, VMEM),
        scratch_shapes=[
            pltpu.VMEM((length, LANES), jnp.int32),
            pltpu.VMEM((length + 32, LANES), jnp.int32),
            pltpu.VMEM((bands, length // 32, LANES), jnp.int32),
        ],
        compiler_params=pltpu.CompilerParams(vmem_limit_bytes=VMEM_GRANT),
        name="tile_counts",
    )(first_id.astype(jnp.int32)[None], events)

    own_rows = pl.pallas_call(
        functools.partial(sketch_kernel, slabs, rows, parts, width, 1.0 / math.sqrt(total_events)),
        out_shape=jax.ShapeDtypeStruct((rows // slabs, width), jnp.float32),
        in_specs=[VMEM] * 5 + [pl.BlockSpec(memory_space=pl.ANY)],
        out_specs=VMEM,
        scratch_shapes=[
            pltpu.VMEM((rows + 8, LANES), jnp.float32),
            pltpu.VMEM((bands, 16, part), jnp.float32),
            pltpu.VMEM((words, rows), jnp.int32),
            pltpu.VMEM((rows, width), jnp.float32),
            pltpu.VMEM((slabs, 8, LANES), jnp.float32),
            pltpu.VMEM((slabs, 8, LANES), jnp.float32),
            dma((1,)),
            dma((slabs,)),
            dma((slabs,)),
        ],
        compiler_params=pltpu.CompilerParams(
            collective_id=1, has_side_effects=True, vmem_limit_bytes=VMEM_GRANT
        ),
        name="sketch_tile",
    )(counts, margins, head, signs, events, sketch_bits)
    if lax.axis_size("item") > 1:
        own_rows = lax.psum(own_rows, "item")
    return own_rows


def solution(mesh):
    placed = (P("stream"), P("stream"), P(None, "item"))
    return jax.shard_map(
        local, mesh=mesh, in_specs=placed, out_specs=P("stream", None), check_vma=False
    )
```

```python
import functools
import math

import jax
import jax.numpy as jnp
from jax import lax
from jax.experimental import pallas as pl
from jax.experimental.pallas import tpu as pltpu
from jax.sharding import PartitionSpec as P

WINDOW = 15
ITEM_BITS = 18
LANES = 128
BITS_PER_WORD = 18
PLANE = 8
BANDS = 4
NONE = 1.0e-30
VMEM_GRANT = 45 * 1024 * 1024
NT = (((1,), (1,)), ((), ()))
VMEM = pl.BlockSpec(memory_space=pltpu.VMEM)


def one_where(mask):
    return jnp.where(mask, 1.0, 0.0).astype(jnp.bfloat16)


def hot_columns(ids, values):
    row = jnp.broadcast_to(values, (16, values.shape[1])).astype(jnp.bfloat16)
    one, zero = jnp.ones((), jnp.bfloat16), jnp.zeros((), jnp.bfloat16)
    return jnp.concatenate(
        [jnp.where(ids[n : n + 16] == row, one, zero) for n in range(0, ids.shape[0], 16)], axis=0
    )


def greet_all(slabs, me):
    barrier = pltpu.get_barrier_semaphore()

    for k in range(1, slabs):
        pl.semaphore_signal(
            barrier, inc=1, device_id={"stream": lax.rem(me + k, slabs)}, device_id_type=pl.DeviceIdType.MESH
        )
    return barrier


def send(src, dst, send_sem, recv_sem, to):
    return pltpu.make_async_remote_copy(
        src_ref=src,
        dst_ref=dst,
        send_sem=send_sem,
        recv_sem=recv_sem,
        device_id={"stream": to},
        device_id_type=pl.DeviceIdType.MESH,
    )


def each(low, high, do):
    for k in range(low, high):
        do(k)


def exchange(slabs, me, out_ref, in_ref, send_sems, recv_sems, start):
    def copy(k):
        to = lax.rem(me + k, slabs)
        return send(out_ref.at[to], in_ref.at[me], send_sems.at[k], recv_sems.at[k], to)

    if start:
        each(1, slabs, lambda k: copy(k).start())
        in_ref[me] = out_ref[me]
    else:
        each(1, slabs, lambda k: copy(k).wait())


def gather_kernel(
    slabs, rows, blocks, own_ref, bits_ref, all_ref, head_ref, sign_ref, count_ref, margin_ref,
    own_pack, own_bits, item_ref, session_ref, links_ref, total_ref,
    pair_out, pair_in, plane_out, plane_in, line_out, line_in,
    bit_sem, line_send, line_recv, plane_send, plane_recv, near_send, near_recv,
    pair_sems, head_plane_send, head_plane_recv, head_line_send, head_line_recv,
):
    me = lax.axis_index("stream")
    depth = slabs // PLANE
    layer, low = me // PLANE, lax.rem(me, PLANE)
    parity, quad = lax.rem(me, 2), lax.rem(me // 2, 4)

    def flip(bit):
        return bit - 2 * bit * lax.rem(me // bit, 2)

    partner = me + flip(1)
    steps = (flip(2), flip(4), flip(2) + flip(4))
    def other_layer(k):
        rising = k + (k - layer + depth) // depth
        mirrored = depth - 1 - layer
        falling = depth - 1 - k - (k - mirrored + depth) // depth
        high = layer // ((depth + 1) // 2)
        return rising + (falling - rising) * lax.rem(high, 2)

    others = [other_layer(k) for k in range(depth - 1)]
    own_items, own_sessions = own_ref.at[0], own_ref.at[1]
    barrier = pltpu.get_barrier_semaphore()
    owned = own_bits.shape[1]
    bit_copy = pltpu.make_async_copy(
        bits_ref.at[:, pl.ds(pl.multiple_of(me * owned, owned), owned)], own_bits, bit_sem.at[0]
    )
    bit_copy.start()
    greeted = [partner] + [me + step for step in steps] + [o * PLANE + low for o in others]
    for to in greeted:
        pl.semaphore_signal(
            barrier, inc=1, device_id={"stream": to}, device_id_type=pl.DeviceIdType.MESH
        )
    half = blocks // 2
    own_pack[0:blocks] = own_items[...]
    own_pack[blocks : blocks + half] = own_sessions[0:half] | (own_sessions[half:blocks] << 16)
    all_ref[me] = own_pack[...]
    item_ref[8 : 8 + blocks] = own_items[...]
    session_ref[8 : 8 + blocks] = own_sessions[...]
    for edge in (slice(0, 8), slice(8 + blocks, 16 + blocks)):
        item_ref[edge] = jnp.zeros((8, LANES), jnp.int32)
        session_ref[edge] = jnp.full((8, LANES), -1, jnp.int32)
    sub = lax.broadcasted_iota(jnp.int32, (LANES, LANES), 0)
    lane = lax.broadcasted_iota(jnp.int32, (LANES, LANES), 1)
    low_lane = lax.broadcasted_iota(jnp.int32, (1, LANES), 1) < LANES // 2
    ids = lax.broadcasted_iota(jnp.int32, (rows, LANES), 0)
    gaps = (sub - LANES // 2 - lane, sub + LANES // 2 - lane)
    in_reach = [(jnp.abs(gap) <= WINDOW) & (gap != 0) for gap in gaps]
    ones = jnp.ones((8, 2 * LANES), jnp.float32).astype(jnp.bfloat16)
    links_ref[...] = jnp.zeros_like(links_ref)
    total_ref[...] = jnp.zeros_like(total_ref)

    together = 8

    def some_blocks(n, unused):
        first = n * together

        def shifted(ref):
            turned = [pltpu.roll(ref[pl.ds(first + 7 + o, 1)], LANES // 2, 1) for o in range(together + 2)]
            return [jnp.where(low_lane, turned[o], turned[o + 1]) for o in range(together + 1)]

        hots = [one_where(ids == item) for item in shifted(item_ref)]
        sessions = [jnp.broadcast_to(session, (LANES, LANES)).T for session in shifted(session_ref)]
        for o in range(together):
            own_item, own_session = item_ref[pl.ds(first + o + 8, 1)], session_ref[pl.ds(first + o + 8, 1)]
            hot = jnp.concatenate([hots[o], hots[o + 1]], axis=1)
            linked = jnp.concatenate(
                [one_where((sessions[o + side] == own_session) & in_reach[side]) for side in range(2)], axis=0
            )
            links = jnp.dot(jnp.concatenate([hot, ones], axis=0), linked, preferred_element_type=jnp.float32)
            links_ref[...] += lax.dot_general(
                links.astype(jnp.bfloat16), one_where(ids == own_item), NT, preferred_element_type=jnp.float32
            )
            total_ref[...] += links[rows:]
        return unused

    inner = [blocks * n // 32 for n in (0, 16, 32)]

    def blocks_of(n):
        lax.fori_loop(inner[n] // together, inner[n + 1] // together, some_blocks, 0)

    step_columns = max(LANES, owned // 16)
    steps_in_all = owned // step_columns

    def signs(low_step, high_step):
        def step(t, unused):
            at = pl.multiple_of(t * step_columns, step_columns)
            sign_ref[:, pl.ds(at, step_columns)] = sign_table(own_bits[:, pl.ds(at, step_columns)], sign_ref.shape[0])
            return unused

        lax.fori_loop(low_step * steps_in_all // 16, high_step * steps_in_all // 16, step, 0)

    blocks_of(0)
    bit_copy.wait()
    pl.semaphore_wait(barrier, len(greeted))

    def along_line(there, here):
        return send(
            own_pack, all_ref.at[me], line_send.at[there], line_recv.at[here], there * PLANE + low
        )

    def in_plane(d, at_layer, own=False):
        slab = all_ref.at[at_layer * PLANE + low]
        sem = d * depth + at_layer
        return send(own_pack if own else slab, slab, plane_send.at[sem], plane_recv.at[sem], me + steps[d])

    def to_partner(r, at_layer, own=False):
        slab = all_ref.at[at_layer * PLANE + low + ((0,) + steps)[r]]
        sem = r * depth + at_layer
        return send(own_pack if own else slab, slab, near_send.at[sem], near_recv.at[sem], partner)

    for o in reversed(others):
        along_line(o, layer).start()
    for d in range(3):
        in_plane(d, layer, True).start()
    to_partner(0, layer, True).start()

    def forward_line(k):
        along_line(layer, others[k]).wait_recv()
        for d in range(3):
            in_plane(d, others[k]).start()
        to_partner(0, others[k]).start()

    def forward_plane(at_layer):
        for d in range(3):
            in_plane(d, at_layer).wait_recv()
            to_partner(d + 1, at_layer).start()

    blocks_of(1)
    forward_line(0)
    share = rows // slabs
    tail = jnp.concatenate(
        [links_ref[rows : rows + 1], total_ref[0:1], jnp.zeros((6 - share, LANES), jnp.float32)], axis=0
    )
    for d in range(slabs):
        at = (d % 2, d // PLANE, d // 2 % 4)
        pair_out[at + (slice(0, share),)] = links_ref[d * share : (d + 1) * share]
        pair_out[at + (slice(share, 8),)] = tail

    pair = send(pair_out.at[1 - parity], pair_in, pair_sems.at[0], pair_sems.at[1], partner)
    pair.start()
    forward_line(1)
    pair.wait()
    line_out[...] = pair_out[parity] + pair_in[...]

    def head_line(there, here):
        return send(
            line_out.at[there], line_in.at[layer], head_line_send.at[there], head_line_recv.at[here],
            there * PLANE + low,
        )

    for o in others:
        head_line(o, layer).start()
    line_in[layer] = line_out[layer]
    forward_plane(layer)
    for k in range(2, depth - 1):
        forward_line(k)
    count_ref[...] = jnp.zeros_like(count_ref)
    margin_ref[...] = jnp.zeros_like(margin_ref)
    signs(0, 4)
    forward_plane(others[0])
    signs(4, 8)
    for o in others[1:-1]:
        forward_plane(o)
    for o in others:
        head_line(o, o).wait_recv()
    plane_out[...] = jnp.sum(line_in[...], axis=0)

    def head_plane(d):
        to = me + steps[d]
        return send(
            plane_out.at[lax.rem(to // 2, 4)], plane_in.at[d], head_plane_send.at[d], head_plane_recv.at[d], to
        )

    for d in range(3):
        head_plane(d).start()
    signs(8, 12)
    for o in others[-1:]:
        forward_plane(o)
    signs(12, 16)
    for at_layer in [layer] + others:
        for r in range(4):
            to_partner(r, at_layer).wait()
        for d in range(3):
            in_plane(d, at_layer).wait_send()
    for o in others:
        along_line(o, layer).wait_send()
        head_line(o, o).wait_send()
    for d in range(3):
        head_plane(d).wait()
    head_ref[...] = plane_out[quad] + plane_in[0] + plane_in[1] + plane_in[2]


def take_windows(code_ref, length, start):
    whole, part = start >> 3, start & 7
    bits = max(1, (length // 8 - 1).bit_length())
    keep = 8 * ((1 << (bits - 1)) + 4)
    value = None
    for bit in reversed(range(bits)):
        step = 8 << bit
        keep = 8 * ((1 << bit) + 4)
        chosen = ((whole >> bit) & 1) == 1
        if value is None:
            low, high = code_ref[0:keep, :], code_ref[step : step + keep, :]
        else:
            low, high = value[0:keep], value[step : step + keep]
        value = jnp.where(chosen, high, low)
    for bit in (2, 1, 0):
        chosen = ((part >> bit) & 1) == 1
        value = jnp.where(chosen, pltpu.roll(value, value.shape[0] - (1 << bit), 0), value)
    return value[0:32]


def all_rows(value, combine):
    for shift in (4, 2, 1):
        value = combine(value, pltpu.roll(value, shift, 0))
    return value


def bytes_of_rows(tag):
    return tag[0:8] | (tag[8:16] << 8) | (tag[16:24] << 16) | (tag[24:32] << 24)


def plane_word(packed, k):
    sub = lax.broadcasted_iota(jnp.int32, (8, LANES), 0)
    spread = lax.shift_left(lax.shift_right_logical(packed, k) & 0x01010101, sub)
    return all_rows(spread, lambda x, y: x | y)


def head_counts(window, ok, near, rows):
    center = window[16:17]
    linked = ((window ^ center) >> ITEM_BITS == 0) & near & ok
    item = window & ((1 << ITEM_BITS) - 1)
    tag = jnp.where(linked & (item < rows), item | rows, 0)
    packed = bytes_of_rows(tag)
    one = jnp.where(linked, 1, 0)
    weight = all_rows(one[0:8] + one[8:16] + one[16:24] + one[24:32], lambda x, y: x + y)
    sub = lax.broadcasted_iota(jnp.int32, (8, LANES), 0)

    def plane(k):
        return plane_word(packed, k)

    bits = rows.bit_length() - 1
    node = plane(bits)
    for k in range(3):
        node = node & (plane(k) ^ (((sub >> k) & 1) - 1))
    nodes = [node]
    for k in reversed(range(3, bits)):
        word = plane(k)
        nodes = [part for node in nodes for part in (node & ~word, node & word)]
    counts = jnp.concatenate([lax.population_count(node).astype(jnp.float32) for node in nodes], axis=0)
    return counts.astype(jnp.bfloat16), weight[0:1].astype(jnp.float32), center & ((1 << ITEM_BITS) - 1)


def tile_kernel(rows, length, parts, base_ref, all_ref, unused_counts, unused_margins, count_ref, margin_ref, flat_ref, code_ref, mask_ref):
    item_mask = (1 << ITEM_BITS) - 1
    base = base_ref[0]
    bands, unused_rows, width = count_ref.shape
    band = parts * width
    slabs, blocks = all_ref.shape[0], all_ref.shape[1] * 2 // 3
    for n in range(slabs):
        paired = all_ref[n, blocks:]
        sessions = jnp.concatenate([paired & 0xFFFF, paired >> 16], axis=0)
        flat_ref[n * blocks : (n + 1) * blocks] = all_ref[n, 0:blocks] | (sessions << ITEM_BITS)
    per = length // LANES
    for r in range(per):
        code_ref[16 + r * LANES : 16 + (r + 1) * LANES] = flat_ref[pl.ds(r, LANES, stride=per), :].T
    lane = lax.broadcasted_iota(jnp.int32, (16, LANES), 1)
    code_ref[0:16] = jnp.where(lane == 0, -1, pltpu.roll(code_ref[length : length + 16], 1, 1))
    code_ref[length + 16 : length + 32] = jnp.where(
        lane == LANES - 1, -1, pltpu.roll(code_ref[16:32], LANES - 1, 1)
    )

    words = length // 32
    band_bits = (bands - 1).bit_length()
    for w in range(words):
        item = code_ref[16 + 32 * w : 48 + 32 * w] & item_mask
        local = item - base
        mine = (local >= 0) & (local < bands * band) & (item >= rows)
        packed = bytes_of_rows(jnp.where(mine, (local >> (band.bit_length() - 1)) | bands, 0))
        for k in range(band_bits + 1):
            mask_ref[k, w : w + 1] = plane_word(packed, k)[0:1]
    planes = [mask_ref[k] for k in range(band_bits + 1)]
    for s in range(bands):
        mask = planes[band_bits]
        for k in range(band_bits):
            mask = mask & (planes[k] if s >> k & 1 else ~planes[k])
        mask_ref[s] = mask
    tallies = [jnp.sum(lax.population_count(mask_ref[s]), axis=0, keepdims=True) for s in range(bands)]

    word_ids = lax.broadcasted_iota(jnp.int32, (words, LANES), 0)
    d_ids = lax.broadcasted_iota(jnp.int32, (32, LANES), 0)
    near = (d_ids >= 1) & (d_ids != 16)
    tile = min(width, 256)
    t_ids = lax.broadcasted_iota(jnp.int32, (tile, 2 * LANES), 0).astype(jnp.float32).astype(jnp.bfloat16)
    p_ids = lax.broadcasted_iota(jnp.int32, (16, 2 * LANES), 0)

    def ends(mask):
        some = mask != 0
        first_row = jnp.min(jnp.where(some, word_ids, words), axis=0, keepdims=True)
        last_row = jnp.max(jnp.where(some, word_ids, -1), axis=0, keepdims=True)
        at_first, at_last = word_ids == first_row, word_ids == last_row
        first_word = jnp.sum(jnp.where(at_first, mask, 0), axis=0, keepdims=True)
        last_word = jnp.sum(jnp.where(at_last, mask, 0), axis=0, keepdims=True)
        first_bit = first_word & -first_word
        last_place = 31 - lax.clz(last_word)
        last_bit = jnp.where(last_word == 0, 0, jnp.left_shift(1, last_place & 31))
        first = 32 * first_row + lax.population_count(first_bit - 1)
        last = 32 * last_row + last_place
        first_ok = first_word != 0
        last_ok = first_ok & (last > first)
        mask = mask & ~(jnp.where(at_first, first_bit, 0) | jnp.where(at_last, last_bit, 0))
        return mask, ((first, first_ok), (last, last_ok))

    def find(s, mask):
        mask, found = ends(mask)
        links, weights, locals_ = [], [], []
        for at, ok in found:
            window = take_windows(code_ref, length, jnp.where(ok, at, 0))
            counts, weight, item = head_counts(window, ok, near, rows)
            links.append(counts)
            weights.append(weight)
            locals_.append(item - base - s * band)
        return mask, *(jnp.concatenate(x, axis=1) for x in (links, weights, locals_))

    def count(s, links, weight, local):
        part = local >> (width.bit_length() - 1)
        inner = local & (width - 1)
        pieces = []
        for p in range(parts):
            chosen = jnp.broadcast_to(jnp.where(part == p, 1.0, 0.0), (16, 2 * LANES)).astype(jnp.bfloat16)
            pieces += [links[n : n + 16] * chosen for n in range(0, rows, 16)]
        pieces.append(jnp.where(p_ids == part, weight, 0.0).astype(jnp.bfloat16))
        left = jnp.concatenate(pieces, axis=0)
        for t in range(width // tile):
            inside = (inner >= t * tile) & (inner < (t + 1) * tile)
            hot = hot_columns(t_ids, jnp.where(inside, inner - t * tile, -1).astype(jnp.float32))
            cols = slice(t * tile, (t + 1) * tile)
            value = lax.dot_general(left, hot, NT, preferred_element_type=jnp.float32)
            count_ref[s, :, cols] += value[0 : parts * rows]
            margin_ref[s, :, cols] += value[parts * rows :]

    for low in range(0, bands, 2):
        both = range(low, min(low + 2, bands))
        most = functools.reduce(jnp.maximum, [tallies[s] for s in both])

        def body(unused, masks, both=both):
            out = []
            for s, mask in zip(both, masks):
                mask, *found = find(s, mask)
                out.append(mask)
                count(s, *found)
            return tuple(out)

        lax.fori_loop(0, (jnp.max(most) + 1) // 2, body, tuple(mask_ref[s] for s in both))


def sign_table(words, width):
    size = words.shape[1]

    def wide(value):
        return jnp.concatenate([value] * (size // LANES), axis=1)

    shift = lax.broadcasted_iota(jnp.int32, (8, LANES), 0)
    parts = []
    for g in range(width // 8):
        word = 8 * g // BITS_PER_WORD
        split, offset = (word + 1) * BITS_PER_WORD - 8 * g, 8 * g - word * BITS_PER_WORD
        now = jnp.broadcast_to(words[word : word + 1], (8, size))
        where_bit = jnp.left_shift(1, shift + offset)
        if split < 8:
            later = jnp.broadcast_to(words[word + 1 : word + 2], (8, size))
            now = jnp.where(wide(shift) >= split, later, now)
            place = jnp.where(shift >= split, shift - split, shift + offset)
            where_bit = jnp.left_shift(1, place)
        parts.append(jnp.where((now & wide(where_bit)) != 0, 1.0, -1.0))
    return jnp.concatenate(parts, axis=0).astype(jnp.bfloat16)


def boundary_counts(rows, share, me, all_ref, extra_ref):
    slabs, blocks = all_ref.shape[0], all_ref.shape[1] * 2 // 3
    half = blocks // 2
    group = slabs // 4
    sub = lax.broadcasted_iota(jnp.int32, (LANES, LANES), 0)
    lane = lax.broadcasted_iota(jnp.int32, (LANES, LANES), 1)
    ids = lax.broadcasted_iota(jnp.int32, (rows, LANES), 0)
    small = lax.broadcasted_iota(jnp.int32, (group, LANES), 1)
    last_items, last_sessions = all_ref[:, blocks - 1, :], all_ref[:, blocks + half - 1, :] >> 16
    next_items, next_sessions = all_ref[:, 0, :], all_ref[:, blocks, :] & 0xFFFF

    def meet(last, following):
        joined = None
        for g in range(4):
            shift = 32 * g + 16
            pieces = (pltpu.roll(x[g * group : (g + 1) * group], shift, 1) for x in (last, following))
            both = jnp.where(small % 32 < 16, *pieces)
            joined = both if joined is None else jnp.where(small // 32 == g, both, joined)
        return joined

    slab_ids = lax.broadcasted_iota(jnp.int32, (slabs, LANES), 0)
    next_sessions = jnp.where(slab_ids == slabs - 1, -1, pltpu.roll(next_sessions, slabs - 1, 0))
    met_items = meet(last_items, pltpu.roll(next_items, slabs - 1, 0))
    met_sessions = meet(last_sessions, next_sessions)
    crossing = ((sub >> 5) == (lane >> 5)) & (((sub ^ lane) & 16) != 0) & (jnp.abs(sub - lane) <= WINDOW)
    ones = jnp.ones((8, LANES), jnp.float32).astype(jnp.bfloat16)
    extra = jnp.zeros((rows + 8, LANES), jnp.float32)
    total = jnp.zeros((8, LANES), jnp.float32)
    for g in range(group):
        item, session = met_items[g : g + 1], met_sessions[g : g + 1]
        linked = one_where((jnp.broadcast_to(session, (LANES, LANES)).T == session) & crossing)
        hot = one_where(ids == item)
        links = jnp.dot(jnp.concatenate([hot, ones], axis=0), linked, preferred_element_type=jnp.float32)
        extra += lax.dot_general(links.astype(jnp.bfloat16), hot, NT, preferred_element_type=jnp.float32)
        total += links[rows:]
    extra_ref[...] = extra
    return jnp.concatenate(
        [
            extra_ref[pl.ds(me * share, share)],
            extra_ref[rows : rows + 1],
            total[0:1],
            jnp.zeros((6 - share, LANES), jnp.float32),
        ],
        axis=0,
    )


def sketch_kernel(
    slabs, rows, parts, width, scale, count_ref, margin_ref, head_ref, sign_ref, all_ref, bits_ref, out_ref,
    extra_ref, log_ref, head_bits, acc_ref, send_ref, recv_ref, bit_sem, send_sems, recv_sems,
):
    me = lax.axis_index("stream")
    barrier = greet_all(slabs, me)
    bands, unused_rows, part = count_ref.shape
    share = rows // slabs
    tile = min(part, 512)
    head_copy = pltpu.make_async_copy(bits_ref.at[:, 0:rows], head_bits, bit_sem.at[0])
    head_copy.start()

    log_ref[...] = jnp.log(jnp.maximum(margin_ref[...], 1.0))
    head = head_ref[...] + boundary_counts(rows, share, me, all_ref, extra_ref)
    row_log = jnp.log(jnp.maximum(head[share : share + 1], 1.0))
    column_log = jnp.broadcast_to(row_log, (rows, LANES)).T
    total_log = jnp.log(jnp.sum(head[share + 1 : share + 2], axis=1, keepdims=True))
    row_term = total_log - column_log[:, 0:1]
    def product(positive, signs):
        upper = positive.astype(jnp.bfloat16)
        lower = (positive - upper.astype(jnp.float32)).astype(jnp.bfloat16)
        both = jnp.concatenate([upper, lower], axis=0)
        value = lax.dot_general(both, signs, NT, preferred_element_type=jnp.float32)
        return value[0:rows] + value[rows:]

    head_copy.wait()
    row = lax.broadcasted_iota(jnp.int32, (8, LANES), 0)
    shared = jnp.concatenate(
        [jnp.where(row < share, head, 0.0), jnp.zeros((rows - 8, LANES), jnp.float32)], axis=0
    )
    shared = pltpu.roll(shared, me * share, 0)
    ratio = jnp.log(jnp.maximum(shared, 1.0)) + total_log - row_log - column_log
    first_band = jnp.where(lax.axis_index("item") == 0, 1.0, 0.0)
    positive = jnp.where(shared > 0, jnp.maximum(ratio, 0.0), 0.0) * first_band
    acc_ref[...] = product(positive.T, sign_table(head_bits[...], width))

    for s in range(bands):
        for h in range(parts):
            for at in range(0, part, tile):
                counts = count_ref[s, h * rows : (h + 1) * rows, at : at + tile]
                ratio = jnp.log(jnp.maximum(counts, NONE)) + row_term - log_ref[s, h : h + 1, at : at + tile]
                positive = jnp.maximum(ratio, 0.0)
                bit_at = (s * parts + h) * part + at
                acc_ref[...] += product(positive, sign_ref[:, bit_at : bit_at + tile])

    cuts = width // LANES
    for d in range(slabs):
        for c in range(cuts):
            send_ref[d, c * share : (c + 1) * share] = (
                acc_ref[d * share : (d + 1) * share, c * LANES : (c + 1) * LANES] * scale
            )
    pl.semaphore_wait(barrier, slabs - 1)
    exchange(slabs, me, send_ref, recv_ref, send_sems, recv_sems, True)
    exchange(slabs, me, send_ref, recv_ref, send_sems, recv_sems, False)
    summed = jnp.sum(recv_ref[...], axis=0)
    out_ref[...] = jnp.concatenate([summed[c * share : (c + 1) * share] for c in range(cuts)], axis=1)


def local(event_items, event_sessions, sketch_bits):
    slabs = lax.axis_size("stream")
    slab = event_items.shape[0]
    total_events = slab * slabs
    words, band_size = sketch_bits.shape
    owned = band_size // slabs
    rows, width = 128, 256
    part = max(LANES, owned // 16)
    bands = BANDS
    parts = owned // (bands * part)
    me = lax.axis_index("stream")
    own_start = me * owned
    first_id = lax.axis_index("item") * band_size + own_start
    blocks = slab // LANES
    length = total_events // LANES

    dma = pltpu.SemaphoreType.DMA
    depth = slabs // PLANE
    count_shapes = (
        jax.ShapeDtypeStruct((bands, parts * rows, part), jnp.float32),
        jax.ShapeDtypeStruct((bands, 16, part), jnp.float32),
    )
    events, head, signs, no_counts, no_margins = pl.pallas_call(
        functools.partial(gather_kernel, slabs, rows, blocks),
        out_shape=(
            jax.ShapeDtypeStruct((slabs, blocks * 3 // 2, LANES), jnp.int32),
            jax.ShapeDtypeStruct((8, LANES), jnp.float32),
            jax.ShapeDtypeStruct((width, owned), jnp.bfloat16),
            *count_shapes,
        ),
        in_specs=[VMEM, pl.BlockSpec(memory_space=pl.ANY)],
        out_specs=(VMEM,) * 5,
        scratch_shapes=[
            pltpu.VMEM((blocks * 3 // 2, LANES), jnp.int32),
            pltpu.VMEM((words, owned), jnp.int32),
            pltpu.VMEM((blocks + 16, LANES), jnp.int32),
            pltpu.VMEM((blocks + 16, LANES), jnp.int32),
            pltpu.VMEM((rows + 8, LANES), jnp.float32),
            pltpu.VMEM((8, LANES), jnp.float32),
            pltpu.VMEM((2, depth, 4, 8, LANES), jnp.float32),
            pltpu.VMEM((depth, 4, 8, LANES), jnp.float32),
            pltpu.VMEM((4, 8, LANES), jnp.float32),
            pltpu.VMEM((3, 8, LANES), jnp.float32),
            pltpu.VMEM((depth, 4, 8, LANES), jnp.float32),
            pltpu.VMEM((depth, 4, 8, LANES), jnp.float32),
            dma((1,)),
            dma((depth,)),
            dma((depth,)),
            dma((3 * depth,)),
            dma((3 * depth,)),
            dma((4 * depth,)),
            dma((4 * depth,)),
            dma((2,)),
            dma((3,)),
            dma((3,)),
            dma((depth,)),
            dma((depth,)),
        ],
        compiler_params=pltpu.CompilerParams(
            collective_id=0, has_side_effects=True, vmem_limit_bytes=VMEM_GRANT
        ),
        name="gather_events",
    )(jnp.stack([event_items, event_sessions]).reshape(2, blocks, LANES), sketch_bits)

    counts, margins = pl.pallas_call(
        functools.partial(tile_kernel, rows, length, parts),
        out_shape=count_shapes,
        in_specs=[pl.BlockSpec(memory_space=pltpu.SMEM), VMEM, VMEM, VMEM],
        input_output_aliases={2: 0, 3: 1},
        out_specs=(VMEM, VMEM),
        scratch_shapes=[
            pltpu.VMEM((length, LANES), jnp.int32),
            pltpu.VMEM((length + 32, LANES), jnp.int32),
            pltpu.VMEM((bands, length // 32, LANES), jnp.int32),
        ],
        compiler_params=pltpu.CompilerParams(vmem_limit_bytes=VMEM_GRANT),
        name="tile_counts",
    )(first_id.astype(jnp.int32)[None], events, no_counts, no_margins)

    own_rows = pl.pallas_call(
        functools.partial(sketch_kernel, slabs, rows, parts, width, 1.0 / math.sqrt(total_events)),
        out_shape=jax.ShapeDtypeStruct((rows // slabs, width), jnp.float32),
        in_specs=[VMEM] * 5 + [pl.BlockSpec(memory_space=pl.ANY)],
        out_specs=VMEM,
        scratch_shapes=[
            pltpu.VMEM((rows + 8, LANES), jnp.float32),
            pltpu.VMEM((bands, 16, part), jnp.float32),
            pltpu.VMEM((words, rows), jnp.int32),
            pltpu.VMEM((rows, width), jnp.float32),
            pltpu.VMEM((slabs, 8, LANES), jnp.float32),
            pltpu.VMEM((slabs, 8, LANES), jnp.float32),
            dma((1,)),
            dma((slabs,)),
            dma((slabs,)),
        ],
        compiler_params=pltpu.CompilerParams(
            collective_id=1, has_side_effects=True, vmem_limit_bytes=VMEM_GRANT
        ),
        name="sketch_tile",
    )(counts, margins, head, signs, events, sketch_bits)
    if lax.axis_size("item") > 1:
        own_rows = lax.psum(own_rows, "item")
    return own_rows


def solution(mesh):
    placed = (P("stream"), P("stream"), P(None, "item"))
    return jax.shard_map(
        local, mesh=mesh, in_specs=placed, out_specs=P("stream", None), check_vma=False
    )
```

```python
import functools
import math

import jax
import jax.numpy as jnp
from jax import lax
from jax.experimental import pallas as pl
from jax.experimental.pallas import tpu as pltpu
from jax.sharding import PartitionSpec as P

WINDOW = 15
ITEM_BITS = 18
LANES = 128
BITS_PER_WORD = 18
PLANE = 8
BANDS = 4
NONE = 1.0e-30
VMEM_GRANT = 45 * 1024 * 1024
NT = (((1,), (1,)), ((), ()))
VMEM = pl.BlockSpec(memory_space=pltpu.VMEM)


def one_where(mask):
    return jnp.where(mask, 1.0, 0.0).astype(jnp.bfloat16)


def hot_columns(ids, values):
    row = jnp.broadcast_to(values, (16, values.shape[1])).astype(jnp.bfloat16)
    one, zero = jnp.ones((), jnp.bfloat16), jnp.zeros((), jnp.bfloat16)
    return jnp.concatenate(
        [jnp.where(ids[n : n + 16] == row, one, zero) for n in range(0, ids.shape[0], 16)], axis=0
    )


def greet_all(slabs, me):
    barrier = pltpu.get_barrier_semaphore()

    for k in range(1, slabs):
        pl.semaphore_signal(
            barrier, inc=1, device_id={"stream": lax.rem(me + k, slabs)}, device_id_type=pl.DeviceIdType.MESH
        )
    return barrier


def send(src, dst, send_sem, recv_sem, to):
    return pltpu.make_async_remote_copy(
        src_ref=src,
        dst_ref=dst,
        send_sem=send_sem,
        recv_sem=recv_sem,
        device_id={"stream": to},
        device_id_type=pl.DeviceIdType.MESH,
    )


def each(low, high, do):
    for k in range(low, high):
        do(k)


def exchange(slabs, me, out_ref, in_ref, send_sems, recv_sems, start):
    def copy(k):
        to = lax.rem(me + k, slabs)
        return send(out_ref.at[to], in_ref.at[me], send_sems.at[k], recv_sems.at[k], to)

    if start:
        each(1, slabs, lambda k: copy(k).start())
        in_ref[me] = out_ref[me]
    else:
        each(1, slabs, lambda k: copy(k).wait())


def gather_kernel(
    slabs, rows, blocks, items_ref, sessions_ref, bits_ref, all_ref, head_ref, sign_ref, count_ref, margin_ref,
    own_pack, own_bits, own_items, own_sessions, item_ref, session_ref, links_ref, total_ref,
    pair_out, pair_in, plane_out, plane_in, line_out, line_in,
    bit_sem, line_send, line_recv, plane_send, plane_recv, near_send, near_recv,
    pair_sems, head_plane_send, head_plane_recv, head_line_send, head_line_recv,
):
    me = lax.axis_index("stream")
    depth = slabs // PLANE
    layer, low = me // PLANE, lax.rem(me, PLANE)
    parity, quad = lax.rem(me, 2), lax.rem(me // 2, 4)

    def flip(bit):
        return bit - 2 * bit * lax.rem(me // bit, 2)

    partner = me + flip(1)
    steps = (flip(2), flip(4), flip(2) + flip(4))
    def other_layer(k):
        rising = k + (k - layer + depth) // depth
        mirrored = depth - 1 - layer
        falling = depth - 1 - k - (k - mirrored + depth) // depth
        high = layer // ((depth + 1) // 2)
        return rising + (falling - rising) * lax.rem(high, 2)

    others = [other_layer(k) for k in range(depth - 1)]
    loads = [
        pltpu.make_async_copy(items_ref, own_items, bit_sem.at[1]),
        pltpu.make_async_copy(sessions_ref, own_sessions, bit_sem.at[2]),
    ]
    for copy in loads:
        copy.start()
    barrier = pltpu.get_barrier_semaphore()
    owned = own_bits.shape[1]
    bit_copy = pltpu.make_async_copy(
        bits_ref.at[:, pl.ds(pl.multiple_of(me * owned, owned), owned)], own_bits, bit_sem.at[0]
    )
    bit_copy.start()
    greeted = [partner] + [me + step for step in steps] + [o * PLANE + low for o in others]
    for to in greeted:
        pl.semaphore_signal(
            barrier, inc=1, device_id={"stream": to}, device_id_type=pl.DeviceIdType.MESH
        )
    for copy in loads:
        copy.wait()
    half = blocks // 2
    own_pack[0:blocks] = own_items[...]
    own_pack[blocks : blocks + half] = own_sessions[0:half] | (own_sessions[half:blocks] << 16)
    all_ref[me] = own_pack[...]
    item_ref[8 : 8 + blocks] = own_items[...]
    session_ref[8 : 8 + blocks] = own_sessions[...]
    for edge in (slice(0, 8), slice(8 + blocks, 16 + blocks)):
        item_ref[edge] = jnp.zeros((8, LANES), jnp.int32)
        session_ref[edge] = jnp.full((8, LANES), -1, jnp.int32)
    sub = lax.broadcasted_iota(jnp.int32, (LANES, LANES), 0)
    lane = lax.broadcasted_iota(jnp.int32, (LANES, LANES), 1)
    low_lane = lax.broadcasted_iota(jnp.int32, (1, LANES), 1) < LANES // 2
    ids = lax.broadcasted_iota(jnp.int32, (rows, LANES), 0)
    gaps = (sub - LANES // 2 - lane, sub + LANES // 2 - lane)
    in_reach = [(jnp.abs(gap) <= WINDOW) & (gap != 0) for gap in gaps]
    ones = jnp.ones((8, 2 * LANES), jnp.float32).astype(jnp.bfloat16)
    links_ref[...] = jnp.zeros_like(links_ref)
    total_ref[...] = jnp.zeros_like(total_ref)

    together = 8

    def some_blocks(n, unused):
        first = n * together

        def shifted(ref):
            turned = [pltpu.roll(ref[pl.ds(first + 7 + o, 1)], LANES // 2, 1) for o in range(together + 2)]
            return [jnp.where(low_lane, turned[o], turned[o + 1]) for o in range(together + 1)]

        hots = [one_where(ids == item) for item in shifted(item_ref)]
        sessions = [jnp.broadcast_to(session, (LANES, LANES)).T for session in shifted(session_ref)]
        for o in range(together):
            own_item, own_session = item_ref[pl.ds(first + o + 8, 1)], session_ref[pl.ds(first + o + 8, 1)]
            hot = jnp.concatenate([hots[o], hots[o + 1]], axis=1)
            linked = jnp.concatenate(
                [one_where((sessions[o + side] == own_session) & in_reach[side]) for side in range(2)], axis=0
            )
            links = jnp.dot(jnp.concatenate([hot, ones], axis=0), linked, preferred_element_type=jnp.float32)
            links_ref[...] += lax.dot_general(
                links.astype(jnp.bfloat16), one_where(ids == own_item), NT, preferred_element_type=jnp.float32
            )
            total_ref[...] += links[rows:]
        return unused

    inner = [blocks * n // 32 for n in (0, 16, 32)]

    def blocks_of(n):
        lax.fori_loop(inner[n] // together, inner[n + 1] // together, some_blocks, 0)

    step_columns = max(LANES, owned // 16)
    steps_in_all = owned // step_columns

    def signs(low_step, high_step):
        def step(t, unused):
            at = pl.multiple_of(t * step_columns, step_columns)
            sign_ref[:, pl.ds(at, step_columns)] = sign_table(own_bits[:, pl.ds(at, step_columns)], sign_ref.shape[0])
            return unused

        lax.fori_loop(low_step * steps_in_all // 16, high_step * steps_in_all // 16, step, 0)

    blocks_of(0)
    bit_copy.wait()
    pl.semaphore_wait(barrier, len(greeted))

    def along_line(there, here):
        return send(
            own_pack, all_ref.at[me], line_send.at[there], line_recv.at[here], there * PLANE + low
        )

    def in_plane(d, at_layer, own=False):
        slab = all_ref.at[at_layer * PLANE + low]
        sem = d * depth + at_layer
        return send(own_pack if own else slab, slab, plane_send.at[sem], plane_recv.at[sem], me + steps[d])

    def to_partner(r, at_layer, own=False):
        slab = all_ref.at[at_layer * PLANE + low + ((0,) + steps)[r]]
        sem = r * depth + at_layer
        return send(own_pack if own else slab, slab, near_send.at[sem], near_recv.at[sem], partner)

    for o in reversed(others):
        along_line(o, layer).start()
    for d in range(3):
        in_plane(d, layer, True).start()
    to_partner(0, layer, True).start()

    def forward_line(k):
        along_line(layer, others[k]).wait_recv()
        for d in range(3):
            in_plane(d, others[k]).start()
        to_partner(0, others[k]).start()

    def forward_plane(at_layer):
        for d in range(3):
            in_plane(d, at_layer).wait_recv()
            to_partner(d + 1, at_layer).start()

    blocks_of(1)
    forward_line(0)
    share = rows // slabs
    tail = jnp.concatenate(
        [links_ref[rows : rows + 1], total_ref[0:1], jnp.zeros((6 - share, LANES), jnp.float32)], axis=0
    )
    for d in range(slabs):
        at = (d % 2, d // PLANE, d // 2 % 4)
        pair_out[at + (slice(0, share),)] = links_ref[d * share : (d + 1) * share]
        pair_out[at + (slice(share, 8),)] = tail

    pair = send(pair_out.at[1 - parity], pair_in, pair_sems.at[0], pair_sems.at[1], partner)
    pair.start()
    forward_line(1)
    pair.wait()
    line_out[...] = pair_out[parity] + pair_in[...]

    def head_line(there, here):
        return send(
            line_out.at[there], line_in.at[layer], head_line_send.at[there], head_line_recv.at[here],
            there * PLANE + low,
        )

    for o in others:
        head_line(o, layer).start()
    line_in[layer] = line_out[layer]
    forward_plane(layer)
    for k in range(2, depth - 1):
        forward_line(k)
    count_ref[...] = jnp.zeros_like(count_ref)
    margin_ref[...] = jnp.zeros_like(margin_ref)
    signs(0, 4)
    forward_plane(others[0])
    signs(4, 8)
    for o in others[1:-1]:
        forward_plane(o)
    for o in others:
        head_line(o, o).wait_recv()
    plane_out[...] = jnp.sum(line_in[...], axis=0)

    def head_plane(d):
        to = me + steps[d]
        return send(
            plane_out.at[lax.rem(to // 2, 4)], plane_in.at[d], head_plane_send.at[d], head_plane_recv.at[d], to
        )

    for d in range(3):
        head_plane(d).start()
    signs(8, 12)
    for o in others[-1:]:
        forward_plane(o)
    signs(12, 16)
    for at_layer in [layer] + others:
        for r in range(4):
            to_partner(r, at_layer).wait()
        for d in range(3):
            in_plane(d, at_layer).wait_send()
    for o in others:
        along_line(o, layer).wait_send()
        head_line(o, o).wait_send()
    for d in range(3):
        head_plane(d).wait()
    head_ref[...] = plane_out[quad] + plane_in[0] + plane_in[1] + plane_in[2]


def take_windows(code_ref, length, start):
    whole, part = start >> 3, start & 7
    bits = max(1, (length // 8 - 1).bit_length())
    keep = 8 * ((1 << (bits - 1)) + 4)
    value = None
    for bit in reversed(range(bits)):
        step = 8 << bit
        keep = 8 * ((1 << bit) + 4)
        chosen = ((whole >> bit) & 1) == 1
        if value is None:
            low, high = code_ref[0:keep, :], code_ref[step : step + keep, :]
        else:
            low, high = value[0:keep], value[step : step + keep]
        value = jnp.where(chosen, high, low)
    for bit in (2, 1, 0):
        chosen = ((part >> bit) & 1) == 1
        value = jnp.where(chosen, pltpu.roll(value, value.shape[0] - (1 << bit), 0), value)
    return value[0:32]


def all_rows(value, combine):
    for shift in (4, 2, 1):
        value = combine(value, pltpu.roll(value, shift, 0))
    return value


def bytes_of_rows(tag):
    return tag[0:8] | (tag[8:16] << 8) | (tag[16:24] << 16) | (tag[24:32] << 24)


def plane_word(packed, k):
    sub = lax.broadcasted_iota(jnp.int32, (8, LANES), 0)
    spread = lax.shift_left(lax.shift_right_logical(packed, k) & 0x01010101, sub)
    return all_rows(spread, lambda x, y: x | y)


def head_counts(window, ok, near, rows):
    center = window[16:17]
    linked = ((window ^ center) >> ITEM_BITS == 0) & near & ok
    item = window & ((1 << ITEM_BITS) - 1)
    tag = jnp.where(linked & (item < rows), item | rows, 0)
    packed = bytes_of_rows(tag)
    one = jnp.where(linked, 1, 0)
    weight = all_rows(one[0:8] + one[8:16] + one[16:24] + one[24:32], lambda x, y: x + y)
    sub = lax.broadcasted_iota(jnp.int32, (8, LANES), 0)

    def plane(k):
        return plane_word(packed, k)

    bits = rows.bit_length() - 1
    node = plane(bits)
    for k in range(3):
        node = node & (plane(k) ^ (((sub >> k) & 1) - 1))
    nodes = [node]
    for k in reversed(range(3, bits)):
        word = plane(k)
        nodes = [part for node in nodes for part in (node & ~word, node & word)]
    counts = jnp.concatenate([lax.population_count(node).astype(jnp.float32) for node in nodes], axis=0)
    return counts.astype(jnp.bfloat16), weight[0:1].astype(jnp.float32), center & ((1 << ITEM_BITS) - 1)


def tile_kernel(rows, length, parts, base_ref, all_ref, unused_counts, unused_margins, count_ref, margin_ref, flat_ref, code_ref, mask_ref):
    item_mask = (1 << ITEM_BITS) - 1
    base = base_ref[0]
    bands, unused_rows, width = count_ref.shape
    band = parts * width
    slabs, blocks = all_ref.shape[0], all_ref.shape[1] * 2 // 3
    for n in range(slabs):
        paired = all_ref[n, blocks:]
        sessions = jnp.concatenate([paired & 0xFFFF, paired >> 16], axis=0)
        flat_ref[n * blocks : (n + 1) * blocks] = all_ref[n, 0:blocks] | (sessions << ITEM_BITS)
    per = length // LANES
    for r in range(per):
        code_ref[16 + r * LANES : 16 + (r + 1) * LANES] = flat_ref[pl.ds(r, LANES, stride=per), :].T
    lane = lax.broadcasted_iota(jnp.int32, (16, LANES), 1)
    code_ref[0:16] = jnp.where(lane == 0, -1, pltpu.roll(code_ref[length : length + 16], 1, 1))
    code_ref[length + 16 : length + 32] = jnp.where(
        lane == LANES - 1, -1, pltpu.roll(code_ref[16:32], LANES - 1, 1)
    )

    words = length // 32
    band_bits = (bands - 1).bit_length()
    for w in range(words):
        item = code_ref[16 + 32 * w : 48 + 32 * w] & item_mask
        local = item - base
        mine = (local >= 0) & (local < bands * band) & (item >= rows)
        packed = bytes_of_rows(jnp.where(mine, (local >> (band.bit_length() - 1)) | bands, 0))
        for k in range(band_bits + 1):
            mask_ref[k, w : w + 1] = plane_word(packed, k)[0:1]
    planes = [mask_ref[k] for k in range(band_bits + 1)]
    for s in range(bands):
        mask = planes[band_bits]
        for k in range(band_bits):
            mask = mask & (planes[k] if s >> k & 1 else ~planes[k])
        mask_ref[s] = mask
    tallies = [jnp.sum(lax.population_count(mask_ref[s]), axis=0, keepdims=True) for s in range(bands)]

    word_ids = lax.broadcasted_iota(jnp.int32, (words, LANES), 0)
    d_ids = lax.broadcasted_iota(jnp.int32, (32, LANES), 0)
    near = (d_ids >= 1) & (d_ids != 16)
    tile = min(width, 256)
    t_ids = lax.broadcasted_iota(jnp.int32, (tile, 2 * LANES), 0).astype(jnp.float32).astype(jnp.bfloat16)
    p_ids = lax.broadcasted_iota(jnp.int32, (16, 2 * LANES), 0)

    def ends(mask):
        some = mask != 0
        first_row = jnp.min(jnp.where(some, word_ids, words), axis=0, keepdims=True)
        last_row = jnp.max(jnp.where(some, word_ids, -1), axis=0, keepdims=True)
        at_first, at_last = word_ids == first_row, word_ids == last_row
        first_word = jnp.sum(jnp.where(at_first, mask, 0), axis=0, keepdims=True)
        last_word = jnp.sum(jnp.where(at_last, mask, 0), axis=0, keepdims=True)
        first_bit = first_word & -first_word
        last_place = 31 - lax.clz(last_word)
        last_bit = jnp.where(last_word == 0, 0, jnp.left_shift(1, last_place & 31))
        first = 32 * first_row + lax.population_count(first_bit - 1)
        last = 32 * last_row + last_place
        first_ok = first_word != 0
        last_ok = first_ok & (last > first)
        mask = mask & ~(jnp.where(at_first, first_bit, 0) | jnp.where(at_last, last_bit, 0))
        return mask, ((first, first_ok), (last, last_ok))

    def find(s, mask):
        mask, found = ends(mask)
        links, weights, locals_ = [], [], []
        for at, ok in found:
            window = take_windows(code_ref, length, jnp.where(ok, at, 0))
            counts, weight, item = head_counts(window, ok, near, rows)
            links.append(counts)
            weights.append(weight)
            locals_.append(item - base - s * band)
        return mask, *(jnp.concatenate(x, axis=1) for x in (links, weights, locals_))

    def count(s, links, weight, local):
        part = local >> (width.bit_length() - 1)
        inner = local & (width - 1)
        pieces = []
        for p in range(parts):
            chosen = jnp.broadcast_to(jnp.where(part == p, 1.0, 0.0), (16, 2 * LANES)).astype(jnp.bfloat16)
            pieces += [links[n : n + 16] * chosen for n in range(0, rows, 16)]
        pieces.append(jnp.where(p_ids == part, weight, 0.0).astype(jnp.bfloat16))
        left = jnp.concatenate(pieces, axis=0)
        for t in range(width // tile):
            inside = (inner >= t * tile) & (inner < (t + 1) * tile)
            hot = hot_columns(t_ids, jnp.where(inside, inner - t * tile, -1).astype(jnp.float32))
            cols = slice(t * tile, (t + 1) * tile)
            value = lax.dot_general(left, hot, NT, preferred_element_type=jnp.float32)
            count_ref[s, :, cols] += value[0 : parts * rows]
            margin_ref[s, :, cols] += value[parts * rows :]

    for low in range(0, bands, 2):
        both = range(low, min(low + 2, bands))
        most = functools.reduce(jnp.maximum, [tallies[s] for s in both])

        def body(unused, masks, both=both):
            out = []
            for s, mask in zip(both, masks):
                mask, *found = find(s, mask)
                out.append(mask)
                count(s, *found)
            return tuple(out)

        lax.fori_loop(0, (jnp.max(most) + 1) // 2, body, tuple(mask_ref[s] for s in both))


def sign_table(words, width):
    size = words.shape[1]

    def wide(value):
        return jnp.concatenate([value] * (size // LANES), axis=1)

    shift = lax.broadcasted_iota(jnp.int32, (8, LANES), 0)
    parts = []
    for g in range(width // 8):
        word = 8 * g // BITS_PER_WORD
        split, offset = (word + 1) * BITS_PER_WORD - 8 * g, 8 * g - word * BITS_PER_WORD
        now = jnp.broadcast_to(words[word : word + 1], (8, size))
        where_bit = jnp.left_shift(1, shift + offset)
        if split < 8:
            later = jnp.broadcast_to(words[word + 1 : word + 2], (8, size))
            now = jnp.where(wide(shift) >= split, later, now)
            place = jnp.where(shift >= split, shift - split, shift + offset)
            where_bit = jnp.left_shift(1, place)
        parts.append(jnp.where((now & wide(where_bit)) != 0, 1.0, -1.0))
    return jnp.concatenate(parts, axis=0).astype(jnp.bfloat16)


def boundary_counts(rows, share, me, all_ref, extra_ref):
    slabs, blocks = all_ref.shape[0], all_ref.shape[1] * 2 // 3
    half = blocks // 2
    group = slabs // 4
    sub = lax.broadcasted_iota(jnp.int32, (LANES, LANES), 0)
    lane = lax.broadcasted_iota(jnp.int32, (LANES, LANES), 1)
    ids = lax.broadcasted_iota(jnp.int32, (rows, LANES), 0)
    small = lax.broadcasted_iota(jnp.int32, (group, LANES), 1)
    last_items, last_sessions = all_ref[:, blocks - 1, :], all_ref[:, blocks + half - 1, :] >> 16
    next_items, next_sessions = all_ref[:, 0, :], all_ref[:, blocks, :] & 0xFFFF

    def meet(last, following):
        joined = None
        for g in range(4):
            shift = 32 * g + 16
            pieces = (pltpu.roll(x[g * group : (g + 1) * group], shift, 1) for x in (last, following))
            both = jnp.where(small % 32 < 16, *pieces)
            joined = both if joined is None else jnp.where(small // 32 == g, both, joined)
        return joined

    slab_ids = lax.broadcasted_iota(jnp.int32, (slabs, LANES), 0)
    next_sessions = jnp.where(slab_ids == slabs - 1, -1, pltpu.roll(next_sessions, slabs - 1, 0))
    met_items = meet(last_items, pltpu.roll(next_items, slabs - 1, 0))
    met_sessions = meet(last_sessions, next_sessions)
    crossing = ((sub >> 5) == (lane >> 5)) & (((sub ^ lane) & 16) != 0) & (jnp.abs(sub - lane) <= WINDOW)
    ones = jnp.ones((8, LANES), jnp.float32).astype(jnp.bfloat16)
    extra = jnp.zeros((rows + 8, LANES), jnp.float32)
    total = jnp.zeros((8, LANES), jnp.float32)
    for g in range(group):
        item, session = met_items[g : g + 1], met_sessions[g : g + 1]
        linked = one_where((jnp.broadcast_to(session, (LANES, LANES)).T == session) & crossing)
        hot = one_where(ids == item)
        links = jnp.dot(jnp.concatenate([hot, ones], axis=0), linked, preferred_element_type=jnp.float32)
        extra += lax.dot_general(links.astype(jnp.bfloat16), hot, NT, preferred_element_type=jnp.float32)
        total += links[rows:]
    extra_ref[...] = extra
    return jnp.concatenate(
        [
            extra_ref[pl.ds(me * share, share)],
            extra_ref[rows : rows + 1],
            total[0:1],
            jnp.zeros((6 - share, LANES), jnp.float32),
        ],
        axis=0,
    )


def sketch_kernel(
    slabs, rows, parts, width, scale, count_ref, margin_ref, head_ref, sign_ref, all_ref, bits_ref, out_ref,
    extra_ref, log_ref, head_bits, acc_ref, send_ref, recv_ref, bit_sem, send_sems, recv_sems,
):
    me = lax.axis_index("stream")
    barrier = greet_all(slabs, me)
    bands, unused_rows, part = count_ref.shape
    share = rows // slabs
    tile = min(part, 512)
    head_copy = pltpu.make_async_copy(bits_ref.at[:, 0:rows], head_bits, bit_sem.at[0])
    head_copy.start()

    log_ref[...] = jnp.log(jnp.maximum(margin_ref[...], 1.0))
    head = head_ref[...] + boundary_counts(rows, share, me, all_ref, extra_ref)
    row_log = jnp.log(jnp.maximum(head[share : share + 1], 1.0))
    column_log = jnp.broadcast_to(row_log, (rows, LANES)).T
    total_log = jnp.log(jnp.sum(head[share + 1 : share + 2], axis=1, keepdims=True))
    row_term = total_log - column_log[:, 0:1]
    def product(positive, signs):
        upper = positive.astype(jnp.bfloat16)
        lower = (positive - upper.astype(jnp.float32)).astype(jnp.bfloat16)
        both = jnp.concatenate([upper, lower], axis=0)
        value = lax.dot_general(both, signs, NT, preferred_element_type=jnp.float32)
        return value[0:rows] + value[rows:]

    head_copy.wait()
    row = lax.broadcasted_iota(jnp.int32, (8, LANES), 0)
    shared = jnp.concatenate(
        [jnp.where(row < share, head, 0.0), jnp.zeros((rows - 8, LANES), jnp.float32)], axis=0
    )
    shared = pltpu.roll(shared, me * share, 0)
    ratio = jnp.log(jnp.maximum(shared, 1.0)) + total_log - row_log - column_log
    first_band = jnp.where(lax.axis_index("item") == 0, 1.0, 0.0)
    positive = jnp.where(shared > 0, jnp.maximum(ratio, 0.0), 0.0) * first_band
    acc_ref[...] = product(positive.T, sign_table(head_bits[...], width))

    for s in range(bands):
        for h in range(parts):
            for at in range(0, part, tile):
                counts = count_ref[s, h * rows : (h + 1) * rows, at : at + tile]
                ratio = jnp.log(jnp.maximum(counts, NONE)) + row_term - log_ref[s, h : h + 1, at : at + tile]
                positive = jnp.maximum(ratio, 0.0)
                bit_at = (s * parts + h) * part + at
                acc_ref[...] += product(positive, sign_ref[:, bit_at : bit_at + tile])

    cuts = width // LANES
    for d in range(slabs):
        for c in range(cuts):
            send_ref[d, c * share : (c + 1) * share] = (
                acc_ref[d * share : (d + 1) * share, c * LANES : (c + 1) * LANES] * scale
            )
    pl.semaphore_wait(barrier, slabs - 1)
    exchange(slabs, me, send_ref, recv_ref, send_sems, recv_sems, True)
    exchange(slabs, me, send_ref, recv_ref, send_sems, recv_sems, False)
    summed = jnp.sum(recv_ref[...], axis=0)
    out_ref[...] = jnp.concatenate([summed[c * share : (c + 1) * share] for c in range(cuts)], axis=1)


def local(event_items, event_sessions, sketch_bits):
    slabs = lax.axis_size("stream")
    slab = event_items.shape[0]
    total_events = slab * slabs
    words, band_size = sketch_bits.shape
    owned = band_size // slabs
    rows, width = 128, 256
    part = max(LANES, owned // 16)
    bands = BANDS
    parts = owned // (bands * part)
    me = lax.axis_index("stream")
    own_start = me * owned
    first_id = lax.axis_index("item") * band_size + own_start
    blocks = slab // LANES
    length = total_events // LANES

    dma = pltpu.SemaphoreType.DMA
    depth = slabs // PLANE
    count_shapes = (
        jax.ShapeDtypeStruct((bands, parts * rows, part), jnp.float32),
        jax.ShapeDtypeStruct((bands, 16, part), jnp.float32),
    )
    events, head, signs, no_counts, no_margins = pl.pallas_call(
        functools.partial(gather_kernel, slabs, rows, blocks),
        out_shape=(
            jax.ShapeDtypeStruct((slabs, blocks * 3 // 2, LANES), jnp.int32),
            jax.ShapeDtypeStruct((8, LANES), jnp.float32),
            jax.ShapeDtypeStruct((width, owned), jnp.bfloat16),
            *count_shapes,
        ),
        in_specs=[pl.BlockSpec(memory_space=pltpu.HBM)] * 3,
        out_specs=(VMEM,) * 5,
        scratch_shapes=[
            pltpu.VMEM((blocks * 3 // 2, LANES), jnp.int32),
            pltpu.VMEM((words, owned), jnp.int32),
            pltpu.VMEM((blocks, LANES), jnp.int32),
            pltpu.VMEM((blocks, LANES), jnp.int32),
            pltpu.VMEM((blocks + 16, LANES), jnp.int32),
            pltpu.VMEM((blocks + 16, LANES), jnp.int32),
            pltpu.VMEM((rows + 8, LANES), jnp.float32),
            pltpu.VMEM((8, LANES), jnp.float32),
            pltpu.VMEM((2, depth, 4, 8, LANES), jnp.float32),
            pltpu.VMEM((depth, 4, 8, LANES), jnp.float32),
            pltpu.VMEM((4, 8, LANES), jnp.float32),
            pltpu.VMEM((3, 8, LANES), jnp.float32),
            pltpu.VMEM((depth, 4, 8, LANES), jnp.float32),
            pltpu.VMEM((depth, 4, 8, LANES), jnp.float32),
            dma((3,)),
            dma((depth,)),
            dma((depth,)),
            dma((3 * depth,)),
            dma((3 * depth,)),
            dma((4 * depth,)),
            dma((4 * depth,)),
            dma((2,)),
            dma((3,)),
            dma((3,)),
            dma((depth,)),
            dma((depth,)),
        ],
        compiler_params=pltpu.CompilerParams(
            collective_id=0, has_side_effects=True, vmem_limit_bytes=VMEM_GRANT
        ),
        name="gather_events",
    )(*(pltpu.with_memory_space_constraint(x.reshape(blocks, LANES), pltpu.HBM) for x in (event_items, event_sessions)), sketch_bits)

    counts, margins = pl.pallas_call(
        functools.partial(tile_kernel, rows, length, parts),
        out_shape=count_shapes,
        in_specs=[pl.BlockSpec(memory_space=pltpu.SMEM), VMEM, VMEM, VMEM],
        input_output_aliases={2: 0, 3: 1},
        out_specs=(VMEM, VMEM),
        scratch_shapes=[
            pltpu.VMEM((length, LANES), jnp.int32),
            pltpu.VMEM((length + 32, LANES), jnp.int32),
            pltpu.VMEM((bands, length // 32, LANES), jnp.int32),
        ],
        compiler_params=pltpu.CompilerParams(vmem_limit_bytes=VMEM_GRANT),
        name="tile_counts",
    )(first_id.astype(jnp.int32)[None], events, no_counts, no_margins)

    own_rows = pl.pallas_call(
        functools.partial(sketch_kernel, slabs, rows, parts, width, 1.0 / math.sqrt(total_events)),
        out_shape=jax.ShapeDtypeStruct((rows // slabs, width), jnp.float32),
        in_specs=[VMEM] * 5 + [pl.BlockSpec(memory_space=pl.ANY)],
        out_specs=VMEM,
        scratch_shapes=[
            pltpu.VMEM((rows + 8, LANES), jnp.float32),
            pltpu.VMEM((bands, 16, part), jnp.float32),
            pltpu.VMEM((words, rows), jnp.int32),
            pltpu.VMEM((rows, width), jnp.float32),
            pltpu.VMEM((slabs, 8, LANES), jnp.float32),
            pltpu.VMEM((slabs, 8, LANES), jnp.float32),
            dma((1,)),
            dma((slabs,)),
            dma((slabs,)),
        ],
        compiler_params=pltpu.CompilerParams(
            collective_id=1, has_side_effects=True, vmem_limit_bytes=VMEM_GRANT
        ),
        name="sketch_tile",
    )(counts, margins, head, signs, events, sketch_bits)
    if lax.axis_size("item") > 1:
        own_rows = lax.psum(own_rows, "item")
    return own_rows


def solution(mesh):
    placed = (P("stream"), P("stream"), P(None, "item"))
    return jax.shard_map(
        local, mesh=mesh, in_specs=placed, out_specs=P("stream", None), check_vma=False
    )
```

```python
import functools
import math

import jax
import jax.numpy as jnp
from jax import lax
from jax.experimental import pallas as pl
from jax.experimental.pallas import tpu as pltpu
from jax.sharding import PartitionSpec as P

WINDOW = 15
ITEM_BITS = 18
LANES = 128
BITS_PER_WORD = 18
PLANE = 8
BANDS = 4
NONE = 1.0e-30
VMEM_GRANT = 45 * 1024 * 1024
NT = (((1,), (1,)), ((), ()))
VMEM = pl.BlockSpec(memory_space=pltpu.VMEM)


def one_where(mask):
    return jnp.where(mask, 1.0, 0.0).astype(jnp.bfloat16)


def hot_columns(ids, values):
    row = jnp.broadcast_to(values, (16, values.shape[1])).astype(jnp.bfloat16)
    one, zero = jnp.ones((), jnp.bfloat16), jnp.zeros((), jnp.bfloat16)
    return jnp.concatenate(
        [jnp.where(ids[n : n + 16] == row, one, zero) for n in range(0, ids.shape[0], 16)], axis=0
    )


def greet_all(slabs, me):
    barrier = pltpu.get_barrier_semaphore()

    for k in range(1, slabs):
        pl.semaphore_signal(
            barrier, inc=1, device_id={"stream": lax.rem(me + k, slabs)}, device_id_type=pl.DeviceIdType.MESH
        )
    return barrier


def send(src, dst, send_sem, recv_sem, to):
    return pltpu.make_async_remote_copy(
        src_ref=src,
        dst_ref=dst,
        send_sem=send_sem,
        recv_sem=recv_sem,
        device_id={"stream": to},
        device_id_type=pl.DeviceIdType.MESH,
    )


def each(low, high, do):
    for k in range(low, high):
        do(k)


def exchange(slabs, me, out_ref, in_ref, send_sems, recv_sems, start):
    def copy(k):
        to = lax.rem(me + k, slabs)
        return send(out_ref.at[to], in_ref.at[me], send_sems.at[k], recv_sems.at[k], to)

    if start:
        each(1, slabs, lambda k: copy(k).start())
        in_ref[me] = out_ref[me]
    else:
        each(1, slabs, lambda k: copy(k).wait())


def gather_kernel(
    slabs, rows, blocks, items_ref, sessions_ref, bits_ref, all_ref, head_ref, sign_ref, count_ref, margin_ref,
    own_pack, own_bits, own_items, own_sessions, item_ref, session_ref, links_ref, total_ref,
    pair_out, pair_in, plane_out, plane_in, line_out, line_in,
    bit_sem, line_send, line_recv, plane_send, plane_recv, near_send, near_recv,
    pair_sems, head_plane_send, head_plane_recv, head_line_send, head_line_recv,
):
    me = lax.axis_index("stream")
    depth = slabs // PLANE
    layer, low = me // PLANE, lax.rem(me, PLANE)
    parity, quad = lax.rem(me, 2), lax.rem(me // 2, 4)

    def flip(bit):
        return bit - 2 * bit * lax.rem(me // bit, 2)

    partner = me + flip(1)
    steps = (flip(2), flip(4), flip(2) + flip(4))
    def other_layer(k):
        rising = k + (k - layer + depth) // depth
        mirrored = depth - 1 - layer
        falling = depth - 1 - k - (k - mirrored + depth) // depth
        high = layer // ((depth + 1) // 2)
        return rising + (falling - rising) * lax.rem(high, 2)

    others = [other_layer(k) for k in range(depth - 1)]
    loads = [
        pltpu.make_async_copy(items_ref, own_items, bit_sem.at[1]),
        pltpu.make_async_copy(sessions_ref, own_sessions, bit_sem.at[2]),
    ]
    for copy in loads:
        copy.start()
    barrier = pltpu.get_barrier_semaphore()
    owned = own_bits.shape[1]
    bit_copy = pltpu.make_async_copy(
        bits_ref.at[:, pl.ds(pl.multiple_of(me * owned, owned), owned)], own_bits, bit_sem.at[0]
    )
    greeted = [partner] + [me + step for step in steps] + [o * PLANE + low for o in others]
    for to in greeted:
        pl.semaphore_signal(
            barrier, inc=1, device_id={"stream": to}, device_id_type=pl.DeviceIdType.MESH
        )
    for copy in loads:
        copy.wait()
    bit_copy.start()
    half = blocks // 2
    own_pack[0:blocks] = own_items[...]
    own_pack[blocks : blocks + half] = own_sessions[0:half] | (own_sessions[half:blocks] << 16)
    all_ref[me] = own_pack[...]
    item_ref[8 : 8 + blocks] = own_items[...]
    session_ref[8 : 8 + blocks] = own_sessions[...]
    for edge in (slice(0, 8), slice(8 + blocks, 16 + blocks)):
        item_ref[edge] = jnp.zeros((8, LANES), jnp.int32)
        session_ref[edge] = jnp.full((8, LANES), -1, jnp.int32)
    sub = lax.broadcasted_iota(jnp.int32, (LANES, LANES), 0)
    lane = lax.broadcasted_iota(jnp.int32, (LANES, LANES), 1)
    low_lane = lax.broadcasted_iota(jnp.int32, (1, LANES), 1) < LANES // 2
    ids = lax.broadcasted_iota(jnp.int32, (rows, LANES), 0)
    gaps = (sub - LANES // 2 - lane, sub + LANES // 2 - lane)
    in_reach = [(jnp.abs(gap) <= WINDOW) & (gap != 0) for gap in gaps]
    ones = jnp.ones((8, 2 * LANES), jnp.float32).astype(jnp.bfloat16)
    links_ref[...] = jnp.zeros_like(links_ref)
    total_ref[...] = jnp.zeros_like(total_ref)

    together = 8

    def some_blocks(n, unused):
        first = n * together

        def shifted(ref):
            turned = [pltpu.roll(ref[pl.ds(first + 7 + o, 1)], LANES // 2, 1) for o in range(together + 2)]
            return [jnp.where(low_lane, turned[o], turned[o + 1]) for o in range(together + 1)]

        hots = [one_where(ids == item) for item in shifted(item_ref)]
        sessions = [jnp.broadcast_to(session, (LANES, LANES)).T for session in shifted(session_ref)]
        for o in range(together):
            own_item, own_session = item_ref[pl.ds(first + o + 8, 1)], session_ref[pl.ds(first + o + 8, 1)]
            hot = jnp.concatenate([hots[o], hots[o + 1]], axis=1)
            linked = jnp.concatenate(
                [one_where((sessions[o + side] == own_session) & in_reach[side]) for side in range(2)], axis=0
            )
            links = jnp.dot(jnp.concatenate([hot, ones], axis=0), linked, preferred_element_type=jnp.float32)
            links_ref[...] += lax.dot_general(
                links.astype(jnp.bfloat16), one_where(ids == own_item), NT, preferred_element_type=jnp.float32
            )
            total_ref[...] += links[rows:]
        return unused

    inner = [blocks * n // 32 for n in (0, 0, 32)]

    def blocks_of(n):
        lax.fori_loop(inner[n] // together, inner[n + 1] // together, some_blocks, 0)

    step_columns = max(LANES, owned // 16)
    steps_in_all = owned // step_columns

    def signs(low_step, high_step):
        def step(t, unused):
            at = pl.multiple_of(t * step_columns, step_columns)
            sign_ref[:, pl.ds(at, step_columns)] = sign_table(own_bits[:, pl.ds(at, step_columns)], sign_ref.shape[0])
            return unused

        lax.fori_loop(low_step * steps_in_all // 16, high_step * steps_in_all // 16, step, 0)

    blocks_of(0)
    pl.semaphore_wait(barrier, len(greeted))

    def along_line(there, here):
        return send(
            own_pack, all_ref.at[me], line_send.at[there], line_recv.at[here], there * PLANE + low
        )

    def in_plane(d, at_layer, own=False):
        slab = all_ref.at[at_layer * PLANE + low]
        sem = d * depth + at_layer
        return send(own_pack if own else slab, slab, plane_send.at[sem], plane_recv.at[sem], me + steps[d])

    def to_partner(r, at_layer, own=False):
        slab = all_ref.at[at_layer * PLANE + low + ((0,) + steps)[r]]
        sem = r * depth + at_layer
        return send(own_pack if own else slab, slab, near_send.at[sem], near_recv.at[sem], partner)

    for o in reversed(others):
        along_line(o, layer).start()
    for d in range(3):
        in_plane(d, layer, True).start()
    to_partner(0, layer, True).start()

    def forward_line(k):
        along_line(layer, others[k]).wait_recv()
        for d in range(3):
            in_plane(d, others[k]).start()
        to_partner(0, others[k]).start()

    def forward_plane(at_layer):
        for d in range(3):
            in_plane(d, at_layer).wait_recv()
            to_partner(d + 1, at_layer).start()

    blocks_of(1)
    forward_line(0)
    share = rows // slabs
    tail = jnp.concatenate(
        [links_ref[rows : rows + 1], total_ref[0:1], jnp.zeros((6 - share, LANES), jnp.float32)], axis=0
    )
    for d in range(slabs):
        at = (d % 2, d // PLANE, d // 2 % 4)
        pair_out[at + (slice(0, share),)] = links_ref[d * share : (d + 1) * share]
        pair_out[at + (slice(share, 8),)] = tail

    pair = send(pair_out.at[1 - parity], pair_in, pair_sems.at[0], pair_sems.at[1], partner)
    pair.start()
    forward_line(1)
    pair.wait()
    line_out[...] = pair_out[parity] + pair_in[...]

    def head_line(there, here):
        return send(
            line_out.at[there], line_in.at[layer], head_line_send.at[there], head_line_recv.at[here],
            there * PLANE + low,
        )

    for o in others:
        head_line(o, layer).start()
    line_in[layer] = line_out[layer]
    forward_plane(layer)
    for k in range(2, depth - 1):
        forward_line(k)
    count_ref[...] = jnp.zeros_like(count_ref)
    margin_ref[...] = jnp.zeros_like(margin_ref)
    bit_copy.wait()
    signs(0, 4)
    forward_plane(others[0])
    signs(4, 8)
    for o in others[1:-1]:
        forward_plane(o)
    for o in others:
        head_line(o, o).wait_recv()
    plane_out[...] = jnp.sum(line_in[...], axis=0)

    def head_plane(d):
        to = me + steps[d]
        return send(
            plane_out.at[lax.rem(to // 2, 4)], plane_in.at[d], head_plane_send.at[d], head_plane_recv.at[d], to
        )

    for d in range(3):
        head_plane(d).start()
    signs(8, 12)
    for o in others[-1:]:
        forward_plane(o)
    signs(12, 16)
    for at_layer in [layer] + others:
        for r in range(4):
            to_partner(r, at_layer).wait()
        for d in range(3):
            in_plane(d, at_layer).wait_send()
    for o in others:
        along_line(o, layer).wait_send()
        head_line(o, o).wait_send()
    for d in range(3):
        head_plane(d).wait()
    head_ref[...] = plane_out[quad] + plane_in[0] + plane_in[1] + plane_in[2]


def take_windows(code_ref, length, start):
    whole, part = start >> 3, start & 7
    bits = max(1, (length // 8 - 1).bit_length())
    keep = 8 * ((1 << (bits - 1)) + 4)
    value = None
    for bit in reversed(range(bits)):
        step = 8 << bit
        keep = 8 * ((1 << bit) + 4)
        chosen = ((whole >> bit) & 1) == 1
        if value is None:
            low, high = code_ref[0:keep, :], code_ref[step : step + keep, :]
        else:
            low, high = value[0:keep], value[step : step + keep]
        value = jnp.where(chosen, high, low)
    for bit in (2, 1, 0):
        chosen = ((part >> bit) & 1) == 1
        value = jnp.where(chosen, pltpu.roll(value, value.shape[0] - (1 << bit), 0), value)
    return value[0:32]


def all_rows(value, combine):
    for shift in (4, 2, 1):
        value = combine(value, pltpu.roll(value, shift, 0))
    return value


def bytes_of_rows(tag):
    return tag[0:8] | (tag[8:16] << 8) | (tag[16:24] << 16) | (tag[24:32] << 24)


def plane_word(packed, k):
    sub = lax.broadcasted_iota(jnp.int32, (8, LANES), 0)
    spread = lax.shift_left(lax.shift_right_logical(packed, k) & 0x01010101, sub)
    return all_rows(spread, lambda x, y: x | y)


def head_counts(window, ok, near, rows):
    center = window[16:17]
    linked = ((window ^ center) >> ITEM_BITS == 0) & near & ok
    item = window & ((1 << ITEM_BITS) - 1)
    tag = jnp.where(linked & (item < rows), item | rows, 0)
    packed = bytes_of_rows(tag)
    one = jnp.where(linked, 1, 0)
    weight = all_rows(one[0:8] + one[8:16] + one[16:24] + one[24:32], lambda x, y: x + y)
    sub = lax.broadcasted_iota(jnp.int32, (8, LANES), 0)

    def plane(k):
        return plane_word(packed, k)

    bits = rows.bit_length() - 1
    node = plane(bits)
    for k in range(3):
        node = node & (plane(k) ^ (((sub >> k) & 1) - 1))
    nodes = [node]
    for k in reversed(range(3, bits)):
        word = plane(k)
        nodes = [part for node in nodes for part in (node & ~word, node & word)]
    counts = jnp.concatenate([lax.population_count(node).astype(jnp.float32) for node in nodes], axis=0)
    return counts.astype(jnp.bfloat16), weight[0:1].astype(jnp.float32), center & ((1 << ITEM_BITS) - 1)


def tile_kernel(rows, length, parts, base_ref, all_ref, unused_counts, unused_margins, count_ref, margin_ref, flat_ref, code_ref, mask_ref):
    item_mask = (1 << ITEM_BITS) - 1
    base = base_ref[0]
    bands, unused_rows, width = count_ref.shape
    band = parts * width
    slabs, blocks = all_ref.shape[0], all_ref.shape[1] * 2 // 3
    for n in range(slabs):
        paired = all_ref[n, blocks:]
        sessions = jnp.concatenate([paired & 0xFFFF, paired >> 16], axis=0)
        flat_ref[n * blocks : (n + 1) * blocks] = all_ref[n, 0:blocks] | (sessions << ITEM_BITS)
    per = length // LANES
    for r in range(per):
        code_ref[16 + r * LANES : 16 + (r + 1) * LANES] = flat_ref[pl.ds(r, LANES, stride=per), :].T
    lane = lax.broadcasted_iota(jnp.int32, (16, LANES), 1)
    code_ref[0:16] = jnp.where(lane == 0, -1, pltpu.roll(code_ref[length : length + 16], 1, 1))
    code_ref[length + 16 : length + 32] = jnp.where(
        lane == LANES - 1, -1, pltpu.roll(code_ref[16:32], LANES - 1, 1)
    )

    words = length // 32
    band_bits = (bands - 1).bit_length()
    for w in range(words):
        item = code_ref[16 + 32 * w : 48 + 32 * w] & item_mask
        local = item - base
        mine = (local >= 0) & (local < bands * band) & (item >= rows)
        packed = bytes_of_rows(jnp.where(mine, (local >> (band.bit_length() - 1)) | bands, 0))
        for k in range(band_bits + 1):
            mask_ref[k, w : w + 1] = plane_word(packed, k)[0:1]
    planes = [mask_ref[k] for k in range(band_bits + 1)]
    for s in range(bands):
        mask = planes[band_bits]
        for k in range(band_bits):
            mask = mask & (planes[k] if s >> k & 1 else ~planes[k])
        mask_ref[s] = mask
    tallies = [jnp.sum(lax.population_count(mask_ref[s]), axis=0, keepdims=True) for s in range(bands)]

    word_ids = lax.broadcasted_iota(jnp.int32, (words, LANES), 0)
    d_ids = lax.broadcasted_iota(jnp.int32, (32, LANES), 0)
    near = (d_ids >= 1) & (d_ids != 16)
    tile = min(width, 256)
    t_ids = lax.broadcasted_iota(jnp.int32, (tile, 2 * LANES), 0).astype(jnp.float32).astype(jnp.bfloat16)
    p_ids = lax.broadcasted_iota(jnp.int32, (16, 2 * LANES), 0)

    def ends(mask):
        some = mask != 0
        first_row = jnp.min(jnp.where(some, word_ids, words), axis=0, keepdims=True)
        last_row = jnp.max(jnp.where(some, word_ids, -1), axis=0, keepdims=True)
        at_first, at_last = word_ids == first_row, word_ids == last_row
        first_word = jnp.sum(jnp.where(at_first, mask, 0), axis=0, keepdims=True)
        last_word = jnp.sum(jnp.where(at_last, mask, 0), axis=0, keepdims=True)
        first_bit = first_word & -first_word
        last_place = 31 - lax.clz(last_word)
        last_bit = jnp.where(last_word == 0, 0, jnp.left_shift(1, last_place & 31))
        first = 32 * first_row + lax.population_count(first_bit - 1)
        last = 32 * last_row + last_place
        first_ok = first_word != 0
        last_ok = first_ok & (last > first)
        mask = mask & ~(jnp.where(at_first, first_bit, 0) | jnp.where(at_last, last_bit, 0))
        return mask, ((first, first_ok), (last, last_ok))

    def find(s, mask):
        mask, found = ends(mask)
        links, weights, locals_ = [], [], []
        for at, ok in found:
            window = take_windows(code_ref, length, jnp.where(ok, at, 0))
            counts, weight, item = head_counts(window, ok, near, rows)
            links.append(counts)
            weights.append(weight)
            locals_.append(item - base - s * band)
        return mask, *(jnp.concatenate(x, axis=1) for x in (links, weights, locals_))

    def count(s, links, weight, local):
        part = local >> (width.bit_length() - 1)
        inner = local & (width - 1)
        pieces = []
        for p in range(parts):
            chosen = jnp.broadcast_to(jnp.where(part == p, 1.0, 0.0), (16, 2 * LANES)).astype(jnp.bfloat16)
            pieces += [links[n : n + 16] * chosen for n in range(0, rows, 16)]
        pieces.append(jnp.where(p_ids == part, weight, 0.0).astype(jnp.bfloat16))
        left = jnp.concatenate(pieces, axis=0)
        for t in range(width // tile):
            inside = (inner >= t * tile) & (inner < (t + 1) * tile)
            hot = hot_columns(t_ids, jnp.where(inside, inner - t * tile, -1).astype(jnp.float32))
            cols = slice(t * tile, (t + 1) * tile)
            value = lax.dot_general(left, hot, NT, preferred_element_type=jnp.float32)
            count_ref[s, :, cols] += value[0 : parts * rows]
            margin_ref[s, :, cols] += value[parts * rows :]

    for low in range(0, bands, 2):
        both = range(low, min(low + 2, bands))
        most = functools.reduce(jnp.maximum, [tallies[s] for s in both])

        def body(unused, masks, both=both):
            out = []
            for s, mask in zip(both, masks):
                mask, *found = find(s, mask)
                out.append(mask)
                count(s, *found)
            return tuple(out)

        lax.fori_loop(0, (jnp.max(most) + 1) // 2, body, tuple(mask_ref[s] for s in both))


def sign_table(words, width):
    size = words.shape[1]

    def wide(value):
        return jnp.concatenate([value] * (size // LANES), axis=1)

    shift = lax.broadcasted_iota(jnp.int32, (8, LANES), 0)
    parts = []
    for g in range(width // 8):
        word = 8 * g // BITS_PER_WORD
        split, offset = (word + 1) * BITS_PER_WORD - 8 * g, 8 * g - word * BITS_PER_WORD
        now = jnp.broadcast_to(words[word : word + 1], (8, size))
        where_bit = jnp.left_shift(1, shift + offset)
        if split < 8:
            later = jnp.broadcast_to(words[word + 1 : word + 2], (8, size))
            now = jnp.where(wide(shift) >= split, later, now)
            place = jnp.where(shift >= split, shift - split, shift + offset)
            where_bit = jnp.left_shift(1, place)
        parts.append(jnp.where((now & wide(where_bit)) != 0, 1.0, -1.0))
    return jnp.concatenate(parts, axis=0).astype(jnp.bfloat16)


def boundary_counts(rows, share, me, all_ref, extra_ref):
    slabs, blocks = all_ref.shape[0], all_ref.shape[1] * 2 // 3
    half = blocks // 2
    group = slabs // 4
    sub = lax.broadcasted_iota(jnp.int32, (LANES, LANES), 0)
    lane = lax.broadcasted_iota(jnp.int32, (LANES, LANES), 1)
    ids = lax.broadcasted_iota(jnp.int32, (rows, LANES), 0)
    small = lax.broadcasted_iota(jnp.int32, (group, LANES), 1)
    last_items, last_sessions = all_ref[:, blocks - 1, :], all_ref[:, blocks + half - 1, :] >> 16
    next_items, next_sessions = all_ref[:, 0, :], all_ref[:, blocks, :] & 0xFFFF

    def meet(last, following):
        joined = None
        for g in range(4):
            shift = 32 * g + 16
            pieces = (pltpu.roll(x[g * group : (g + 1) * group], shift, 1) for x in (last, following))
            both = jnp.where(small % 32 < 16, *pieces)
            joined = both if joined is None else jnp.where(small // 32 == g, both, joined)
        return joined

    slab_ids = lax.broadcasted_iota(jnp.int32, (slabs, LANES), 0)
    next_sessions = jnp.where(slab_ids == slabs - 1, -1, pltpu.roll(next_sessions, slabs - 1, 0))
    met_items = meet(last_items, pltpu.roll(next_items, slabs - 1, 0))
    met_sessions = meet(last_sessions, next_sessions)
    crossing = ((sub >> 5) == (lane >> 5)) & (((sub ^ lane) & 16) != 0) & (jnp.abs(sub - lane) <= WINDOW)
    ones = jnp.ones((8, LANES), jnp.float32).astype(jnp.bfloat16)
    extra = jnp.zeros((rows + 8, LANES), jnp.float32)
    total = jnp.zeros((8, LANES), jnp.float32)
    for g in range(group):
        item, session = met_items[g : g + 1], met_sessions[g : g + 1]
        linked = one_where((jnp.broadcast_to(session, (LANES, LANES)).T == session) & crossing)
        hot = one_where(ids == item)
        links = jnp.dot(jnp.concatenate([hot, ones], axis=0), linked, preferred_element_type=jnp.float32)
        extra += lax.dot_general(links.astype(jnp.bfloat16), hot, NT, preferred_element_type=jnp.float32)
        total += links[rows:]
    extra_ref[...] = extra
    return jnp.concatenate(
        [
            extra_ref[pl.ds(me * share, share)],
            extra_ref[rows : rows + 1],
            total[0:1],
            jnp.zeros((6 - share, LANES), jnp.float32),
        ],
        axis=0,
    )


def sketch_kernel(
    slabs, rows, parts, width, scale, count_ref, margin_ref, head_ref, sign_ref, all_ref, bits_ref, out_ref,
    extra_ref, log_ref, head_bits, acc_ref, send_ref, recv_ref, bit_sem, send_sems, recv_sems,
):
    me = lax.axis_index("stream")
    barrier = greet_all(slabs, me)
    bands, unused_rows, part = count_ref.shape
    share = rows // slabs
    tile = min(part, 512)
    head_copy = pltpu.make_async_copy(bits_ref.at[:, 0:rows], head_bits, bit_sem.at[0])
    head_copy.start()

    log_ref[...] = jnp.log(jnp.maximum(margin_ref[...], 1.0))
    head = head_ref[...] + boundary_counts(rows, share, me, all_ref, extra_ref)
    row_log = jnp.log(jnp.maximum(head[share : share + 1], 1.0))
    column_log = jnp.broadcast_to(row_log, (rows, LANES)).T
    total_log = jnp.log(jnp.sum(head[share + 1 : share + 2], axis=1, keepdims=True))
    row_term = total_log - column_log[:, 0:1]
    def product(positive, signs):
        upper = positive.astype(jnp.bfloat16)
        lower = (positive - upper.astype(jnp.float32)).astype(jnp.bfloat16)
        both = jnp.concatenate([upper, lower], axis=0)
        value = lax.dot_general(both, signs, NT, preferred_element_type=jnp.float32)
        return value[0:rows] + value[rows:]

    head_copy.wait()
    row = lax.broadcasted_iota(jnp.int32, (8, LANES), 0)
    shared = jnp.concatenate(
        [jnp.where(row < share, head, 0.0), jnp.zeros((rows - 8, LANES), jnp.float32)], axis=0
    )
    shared = pltpu.roll(shared, me * share, 0)
    ratio = jnp.log(jnp.maximum(shared, 1.0)) + total_log - row_log - column_log
    first_band = jnp.where(lax.axis_index("item") == 0, 1.0, 0.0)
    positive = jnp.where(shared > 0, jnp.maximum(ratio, 0.0), 0.0) * first_band
    acc_ref[...] = product(positive.T, sign_table(head_bits[...], width))

    for s in range(bands):
        for h in range(parts):
            for at in range(0, part, tile):
                counts = count_ref[s, h * rows : (h + 1) * rows, at : at + tile]
                ratio = jnp.log(jnp.maximum(counts, NONE)) + row_term - log_ref[s, h : h + 1, at : at + tile]
                positive = jnp.maximum(ratio, 0.0)
                bit_at = (s * parts + h) * part + at
                acc_ref[...] += product(positive, sign_ref[:, bit_at : bit_at + tile])

    cuts = width // LANES
    for d in range(slabs):
        for c in range(cuts):
            send_ref[d, c * share : (c + 1) * share] = (
                acc_ref[d * share : (d + 1) * share, c * LANES : (c + 1) * LANES] * scale
            )
    pl.semaphore_wait(barrier, slabs - 1)
    exchange(slabs, me, send_ref, recv_ref, send_sems, recv_sems, True)
    exchange(slabs, me, send_ref, recv_ref, send_sems, recv_sems, False)
    summed = jnp.sum(recv_ref[...], axis=0)
    out_ref[...] = jnp.concatenate([summed[c * share : (c + 1) * share] for c in range(cuts)], axis=1)


def local(event_items, event_sessions, sketch_bits):
    slabs = lax.axis_size("stream")
    slab = event_items.shape[0]
    total_events = slab * slabs
    words, band_size = sketch_bits.shape
    owned = band_size // slabs
    rows, width = 128, 256
    part = max(LANES, owned // 16)
    bands = BANDS
    parts = owned // (bands * part)
    me = lax.axis_index("stream")
    own_start = me * owned
    first_id = lax.axis_index("item") * band_size + own_start
    blocks = slab // LANES
    length = total_events // LANES

    dma = pltpu.SemaphoreType.DMA
    depth = slabs // PLANE
    count_shapes = (
        jax.ShapeDtypeStruct((bands, parts * rows, part), jnp.float32),
        jax.ShapeDtypeStruct((bands, 16, part), jnp.float32),
    )
    events, head, signs, no_counts, no_margins = pl.pallas_call(
        functools.partial(gather_kernel, slabs, rows, blocks),
        out_shape=(
            jax.ShapeDtypeStruct((slabs, blocks * 3 // 2, LANES), jnp.int32),
            jax.ShapeDtypeStruct((8, LANES), jnp.float32),
            jax.ShapeDtypeStruct((width, owned), jnp.bfloat16),
            *count_shapes,
        ),
        in_specs=[pl.BlockSpec(memory_space=pltpu.HBM)] * 3,
        out_specs=(VMEM,) * 5,
        scratch_shapes=[
            pltpu.VMEM((blocks * 3 // 2, LANES), jnp.int32),
            pltpu.VMEM((words, owned), jnp.int32),
            pltpu.VMEM((blocks, LANES), jnp.int32),
            pltpu.VMEM((blocks, LANES), jnp.int32),
            pltpu.VMEM((blocks + 16, LANES), jnp.int32),
            pltpu.VMEM((blocks + 16, LANES), jnp.int32),
            pltpu.VMEM((rows + 8, LANES), jnp.float32),
            pltpu.VMEM((8, LANES), jnp.float32),
            pltpu.VMEM((2, depth, 4, 8, LANES), jnp.float32),
            pltpu.VMEM((depth, 4, 8, LANES), jnp.float32),
            pltpu.VMEM((4, 8, LANES), jnp.float32),
            pltpu.VMEM((3, 8, LANES), jnp.float32),
            pltpu.VMEM((depth, 4, 8, LANES), jnp.float32),
            pltpu.VMEM((depth, 4, 8, LANES), jnp.float32),
            dma((3,)),
            dma((depth,)),
            dma((depth,)),
            dma((3 * depth,)),
            dma((3 * depth,)),
            dma((4 * depth,)),
            dma((4 * depth,)),
            dma((2,)),
            dma((3,)),
            dma((3,)),
            dma((depth,)),
            dma((depth,)),
        ],
        compiler_params=pltpu.CompilerParams(
            collective_id=0, has_side_effects=True, vmem_limit_bytes=VMEM_GRANT
        ),
        name="gather_events",
    )(*(pltpu.with_memory_space_constraint(x.reshape(blocks, LANES), pltpu.HBM) for x in (event_items, event_sessions)), sketch_bits)

    counts, margins = pl.pallas_call(
        functools.partial(tile_kernel, rows, length, parts),
        out_shape=count_shapes,
        in_specs=[pl.BlockSpec(memory_space=pltpu.SMEM), VMEM, VMEM, VMEM],
        input_output_aliases={2: 0, 3: 1},
        out_specs=(VMEM, VMEM),
        scratch_shapes=[
            pltpu.VMEM((length, LANES), jnp.int32),
            pltpu.VMEM((length + 32, LANES), jnp.int32),
            pltpu.VMEM((bands, length // 32, LANES), jnp.int32),
        ],
        compiler_params=pltpu.CompilerParams(vmem_limit_bytes=VMEM_GRANT),
        name="tile_counts",
    )(first_id.astype(jnp.int32)[None], events, no_counts, no_margins)

    own_rows = pl.pallas_call(
        functools.partial(sketch_kernel, slabs, rows, parts, width, 1.0 / math.sqrt(total_events)),
        out_shape=jax.ShapeDtypeStruct((rows // slabs, width), jnp.float32),
        in_specs=[VMEM] * 5 + [pl.BlockSpec(memory_space=pl.ANY)],
        out_specs=VMEM,
        scratch_shapes=[
            pltpu.VMEM((rows + 8, LANES), jnp.float32),
            pltpu.VMEM((bands, 16, part), jnp.float32),
            pltpu.VMEM((words, rows), jnp.int32),
            pltpu.VMEM((rows, width), jnp.float32),
            pltpu.VMEM((slabs, 8, LANES), jnp.float32),
            pltpu.VMEM((slabs, 8, LANES), jnp.float32),
            dma((1,)),
            dma((slabs,)),
            dma((slabs,)),
        ],
        compiler_params=pltpu.CompilerParams(
            collective_id=1, has_side_effects=True, vmem_limit_bytes=VMEM_GRANT
        ),
        name="sketch_tile",
    )(counts, margins, head, signs, events, sketch_bits)
    if lax.axis_size("item") > 1:
        own_rows = lax.psum(own_rows, "item")
    return own_rows


def solution(mesh):
    placed = (P("stream"), P("stream"), P(None, "item"))
    return jax.shard_map(
        local, mesh=mesh, in_specs=placed, out_specs=P("stream", None), check_vma=False
    )
```

```python
import functools
import math

import jax
import jax.numpy as jnp
from jax import lax
from jax.experimental import pallas as pl
from jax.experimental.pallas import tpu as pltpu
from jax.sharding import PartitionSpec as P

WINDOW = 15
ITEM_BITS = 18
LANES = 128
BITS_PER_WORD = 18
PLANE = 8
BANDS = 4
NONE = 1.0e-30
VMEM_GRANT = 45 * 1024 * 1024
NT = (((1,), (1,)), ((), ()))
VMEM = pl.BlockSpec(memory_space=pltpu.VMEM)


def one_where(mask):
    return jnp.where(mask, 1.0, 0.0).astype(jnp.bfloat16)


def hot_columns(ids, values):
    row = jnp.broadcast_to(values, (16, values.shape[1])).astype(jnp.bfloat16)
    one, zero = jnp.ones((), jnp.bfloat16), jnp.zeros((), jnp.bfloat16)
    return jnp.concatenate(
        [jnp.where(ids[n : n + 16] == row, one, zero) for n in range(0, ids.shape[0], 16)], axis=0
    )


def greet_all(slabs, me):
    barrier = pltpu.get_barrier_semaphore()

    for k in range(1, slabs):
        pl.semaphore_signal(
            barrier, inc=1, device_id={"stream": lax.rem(me + k, slabs)}, device_id_type=pl.DeviceIdType.MESH
        )
    return barrier


def send(src, dst, send_sem, recv_sem, to):
    return pltpu.make_async_remote_copy(
        src_ref=src,
        dst_ref=dst,
        send_sem=send_sem,
        recv_sem=recv_sem,
        device_id={"stream": to},
        device_id_type=pl.DeviceIdType.MESH,
    )


def each(low, high, do):
    for k in range(low, high):
        do(k)


def exchange(slabs, me, out_ref, in_ref, send_sems, recv_sems, start):
    def copy(k):
        to = lax.rem(me + k, slabs)
        return send(out_ref.at[to], in_ref.at[me], send_sems.at[k], recv_sems.at[k], to)

    if start:
        each(1, slabs, lambda k: copy(k).start())
        in_ref[me] = out_ref[me]
    else:
        each(1, slabs, lambda k: copy(k).wait())


def gather_kernel(
    slabs, rows, blocks, items_ref, sessions_ref, bits_ref, all_ref, head_ref, sign_ref, count_ref, margin_ref,
    own_pack, own_bits, own_items, own_sessions, item_ref, session_ref, links_ref, total_ref,
    pair_out, pair_in, plane_out, plane_in, line_out, line_in,
    bit_sem, line_send, line_recv, plane_send, plane_recv, near_send, near_recv,
    pair_sems, head_plane_send, head_plane_recv, head_line_send, head_line_recv,
):
    me = lax.axis_index("stream")
    depth = slabs // PLANE
    layer, low = me // PLANE, lax.rem(me, PLANE)
    parity, quad = lax.rem(me, 2), lax.rem(me // 2, 4)

    def flip(bit):
        return bit - 2 * bit * lax.rem(me // bit, 2)

    partner = me + flip(1)
    steps = (flip(2), flip(4), flip(2) + flip(4))
    def other_layer(k):
        rising = k + (k - layer + depth) // depth
        mirrored = depth - 1 - layer
        falling = depth - 1 - k - (k - mirrored + depth) // depth
        high = layer // ((depth + 1) // 2)
        return rising + (falling - rising) * lax.rem(high, 2)

    others = [other_layer(k) for k in range(depth - 1)]
    loads = [
        pltpu.make_async_copy(items_ref, own_items, bit_sem.at[1]),
        pltpu.make_async_copy(sessions_ref, own_sessions, bit_sem.at[2]),
    ]
    for copy in loads:
        copy.start()
    barrier = pltpu.get_barrier_semaphore()
    owned = own_bits.shape[1]
    bit_copy = pltpu.make_async_copy(
        bits_ref.at[:, pl.ds(pl.multiple_of(me * owned, owned), owned)], own_bits, bit_sem.at[0]
    )
    greeted = [partner] + [me + step for step in steps] + [o * PLANE + low for o in others]
    for to in greeted:
        pl.semaphore_signal(
            barrier, inc=1, device_id={"stream": to}, device_id_type=pl.DeviceIdType.MESH
        )
    for copy in loads:
        copy.wait()
    bit_copy.start()
    half = blocks // 2
    own_pack[0:blocks] = own_items[...]
    own_pack[blocks : blocks + half] = own_sessions[0:half] | (own_sessions[half:blocks] << 16)
    all_ref[me] = own_pack[...]
    item_ref[8 : 8 + blocks] = own_items[...]
    session_ref[8 : 8 + blocks] = own_sessions[...]
    for edge in (slice(0, 8), slice(8 + blocks, 16 + blocks)):
        item_ref[edge] = jnp.zeros((8, LANES), jnp.int32)
        session_ref[edge] = jnp.full((8, LANES), -1, jnp.int32)
    sub = lax.broadcasted_iota(jnp.int32, (LANES, LANES), 0)
    lane = lax.broadcasted_iota(jnp.int32, (LANES, LANES), 1)
    low_lane = lax.broadcasted_iota(jnp.int32, (1, LANES), 1) < LANES // 2
    ids = lax.broadcasted_iota(jnp.int32, (rows, LANES), 0)
    gaps = (sub - LANES // 2 - lane, sub + LANES // 2 - lane)
    in_reach = [(jnp.abs(gap) <= WINDOW) & (gap != 0) for gap in gaps]
    ones = jnp.ones((8, 2 * LANES), jnp.float32).astype(jnp.bfloat16)
    links_ref[...] = jnp.zeros_like(links_ref)
    total_ref[...] = jnp.zeros_like(total_ref)

    together = 8

    def some_blocks(n, unused):
        first = n * together

        def shifted(ref):
            turned = [pltpu.roll(ref[pl.ds(first + 7 + o, 1)], LANES // 2, 1) for o in range(together + 2)]
            return [jnp.where(low_lane, turned[o], turned[o + 1]) for o in range(together + 1)]

        hots = [one_where(ids == item) for item in shifted(item_ref)]
        sessions = [jnp.broadcast_to(session, (LANES, LANES)).T for session in shifted(session_ref)]
        for o in range(together):
            own_item, own_session = item_ref[pl.ds(first + o + 8, 1)], session_ref[pl.ds(first + o + 8, 1)]
            hot = jnp.concatenate([hots[o], hots[o + 1]], axis=1)
            linked = jnp.concatenate(
                [one_where((sessions[o + side] == own_session) & in_reach[side]) for side in range(2)], axis=0
            )
            links = jnp.dot(jnp.concatenate([hot, ones], axis=0), linked, preferred_element_type=jnp.float32)
            links_ref[...] += lax.dot_general(
                links.astype(jnp.bfloat16), one_where(ids == own_item), NT, preferred_element_type=jnp.float32
            )
            total_ref[...] += links[rows:]
        return unused

    inner = [blocks * n // 32 for n in (0, 0, 32)]

    def blocks_of(n):
        lax.fori_loop(inner[n] // together, inner[n + 1] // together, some_blocks, 0)

    step_columns = max(LANES, owned // 16)
    steps_in_all = owned // step_columns

    def signs(low_step, high_step):
        def step(t, unused):
            at = pl.multiple_of(t * step_columns, step_columns)
            sign_ref[:, pl.ds(at, step_columns)] = sign_table(own_bits[:, pl.ds(at, step_columns)], sign_ref.shape[0])
            return unused

        lax.fori_loop(low_step * steps_in_all // 16, high_step * steps_in_all // 16, step, 0)

    blocks_of(0)
    pl.semaphore_wait(barrier, len(greeted))

    def along_line(there, here):
        return send(
            own_pack, all_ref.at[me], line_send.at[there], line_recv.at[here], there * PLANE + low
        )

    def in_plane(d, at_layer, own=False):
        slab = all_ref.at[at_layer * PLANE + low]
        sem = d * depth + at_layer
        return send(own_pack if own else slab, slab, plane_send.at[sem], plane_recv.at[sem], me + steps[d])

    def to_partner(r, at_layer, own=False):
        slab = all_ref.at[at_layer * PLANE + low + ((0,) + steps)[r]]
        sem = r * depth + at_layer
        return send(own_pack if own else slab, slab, near_send.at[sem], near_recv.at[sem], partner)

    for o in reversed(others):
        along_line(o, layer).start()
    for d in range(3):
        in_plane(d, layer, True).start()
    to_partner(0, layer, True).start()

    def forward_line(k):
        along_line(layer, others[k]).wait_recv()
        for d in range(3):
            in_plane(d, others[k]).start()
        to_partner(0, others[k]).start()

    def forward_plane(at_layer):
        for d in range(3):
            in_plane(d, at_layer).wait_recv()
            to_partner(d + 1, at_layer).start()

    blocks_of(1)
    share = rows // slabs
    tail = jnp.concatenate(
        [links_ref[rows : rows + 1], total_ref[0:1], jnp.zeros((6 - share, LANES), jnp.float32)], axis=0
    )
    for d in range(slabs):
        at = (d % 2, d // PLANE, d // 2 % 4)
        pair_out[at + (slice(0, share),)] = links_ref[d * share : (d + 1) * share]
        pair_out[at + (slice(share, 8),)] = tail

    pair = send(pair_out.at[1 - parity], pair_in, pair_sems.at[0], pair_sems.at[1], partner)
    pair.start()
    forward_line(0)
    forward_line(1)
    pair.wait()
    line_out[...] = pair_out[parity] + pair_in[...]

    def head_line(there, here):
        return send(
            line_out.at[there], line_in.at[layer], head_line_send.at[there], head_line_recv.at[here],
            there * PLANE + low,
        )

    for o in others:
        head_line(o, layer).start()
    line_in[layer] = line_out[layer]
    forward_plane(layer)
    for k in range(2, depth - 1):
        forward_line(k)
    count_ref[...] = jnp.zeros_like(count_ref)
    margin_ref[...] = jnp.zeros_like(margin_ref)
    bit_copy.wait()
    signs(0, 4)
    forward_plane(others[0])
    signs(4, 8)
    for o in others[1:-1]:
        forward_plane(o)
    for o in others:
        head_line(o, o).wait_recv()
    plane_out[...] = jnp.sum(line_in[...], axis=0)

    def head_plane(d):
        to = me + steps[d]
        return send(
            plane_out.at[lax.rem(to // 2, 4)], plane_in.at[d], head_plane_send.at[d], head_plane_recv.at[d], to
        )

    for d in range(3):
        head_plane(d).start()
    signs(8, 12)
    for o in others[-1:]:
        forward_plane(o)
    signs(12, 16)
    for at_layer in [layer] + others:
        for r in range(4):
            to_partner(r, at_layer).wait()
        for d in range(3):
            in_plane(d, at_layer).wait_send()
    for o in others:
        along_line(o, layer).wait_send()
        head_line(o, o).wait_send()
    for d in range(3):
        head_plane(d).wait()
    head_ref[...] = plane_out[quad] + plane_in[0] + plane_in[1] + plane_in[2]


def take_windows(code_ref, length, start):
    whole, part = start >> 3, start & 7
    bits = max(1, (length // 8 - 1).bit_length())
    keep = 8 * ((1 << (bits - 1)) + 4)
    value = None
    for bit in reversed(range(bits)):
        step = 8 << bit
        keep = 8 * ((1 << bit) + 4)
        chosen = ((whole >> bit) & 1) == 1
        if value is None:
            low, high = code_ref[0:keep, :], code_ref[step : step + keep, :]
        else:
            low, high = value[0:keep], value[step : step + keep]
        value = jnp.where(chosen, high, low)
    for bit in (2, 1, 0):
        chosen = ((part >> bit) & 1) == 1
        value = jnp.where(chosen, pltpu.roll(value, value.shape[0] - (1 << bit), 0), value)
    return value[0:32]


def all_rows(value, combine):
    for shift in (4, 2, 1):
        value = combine(value, pltpu.roll(value, shift, 0))
    return value


def bytes_of_rows(tag):
    return tag[0:8] | (tag[8:16] << 8) | (tag[16:24] << 16) | (tag[24:32] << 24)


def plane_word(packed, k):
    sub = lax.broadcasted_iota(jnp.int32, (8, LANES), 0)
    spread = lax.shift_left(lax.shift_right_logical(packed, k) & 0x01010101, sub)
    return all_rows(spread, lambda x, y: x | y)


def head_counts(window, ok, near, rows):
    center = window[16:17]
    linked = ((window ^ center) >> ITEM_BITS == 0) & near & ok
    item = window & ((1 << ITEM_BITS) - 1)
    tag = jnp.where(linked & (item < rows), item | rows, 0)
    packed = bytes_of_rows(tag)
    one = jnp.where(linked, 1, 0)
    weight = all_rows(one[0:8] + one[8:16] + one[16:24] + one[24:32], lambda x, y: x + y)
    sub = lax.broadcasted_iota(jnp.int32, (8, LANES), 0)

    def plane(k):
        return plane_word(packed, k)

    bits = rows.bit_length() - 1
    node = plane(bits)
    for k in range(3):
        node = node & (plane(k) ^ (((sub >> k) & 1) - 1))
    nodes = [node]
    for k in reversed(range(3, bits)):
        word = plane(k)
        nodes = [part for node in nodes for part in (node & ~word, node & word)]
    counts = jnp.concatenate([lax.population_count(node).astype(jnp.float32) for node in nodes], axis=0)
    return counts.astype(jnp.bfloat16), weight[0:1].astype(jnp.float32), center & ((1 << ITEM_BITS) - 1)


def tile_kernel(rows, length, parts, base_ref, all_ref, unused_counts, unused_margins, count_ref, margin_ref, flat_ref, code_ref, mask_ref):
    item_mask = (1 << ITEM_BITS) - 1
    base = base_ref[0]
    bands, unused_rows, width = count_ref.shape
    band = parts * width
    slabs, blocks = all_ref.shape[0], all_ref.shape[1] * 2 // 3
    for n in range(slabs):
        paired = all_ref[n, blocks:]
        sessions = jnp.concatenate([paired & 0xFFFF, paired >> 16], axis=0)
        flat_ref[n * blocks : (n + 1) * blocks] = all_ref[n, 0:blocks] | (sessions << ITEM_BITS)
    per = length // LANES
    for r in range(per):
        code_ref[16 + r * LANES : 16 + (r + 1) * LANES] = flat_ref[pl.ds(r, LANES, stride=per), :].T
    lane = lax.broadcasted_iota(jnp.int32, (16, LANES), 1)
    code_ref[0:16] = jnp.where(lane == 0, -1, pltpu.roll(code_ref[length : length + 16], 1, 1))
    code_ref[length + 16 : length + 32] = jnp.where(
        lane == LANES - 1, -1, pltpu.roll(code_ref[16:32], LANES - 1, 1)
    )

    words = length // 32
    band_bits = (bands - 1).bit_length()
    for w in range(words):
        item = code_ref[16 + 32 * w : 48 + 32 * w] & item_mask
        local = item - base
        mine = (local >= 0) & (local < bands * band) & (item >= rows)
        packed = bytes_of_rows(jnp.where(mine, (local >> (band.bit_length() - 1)) | bands, 0))
        for k in range(band_bits + 1):
            mask_ref[k, w : w + 1] = plane_word(packed, k)[0:1]
    planes = [mask_ref[k] for k in range(band_bits + 1)]
    for s in range(bands):
        mask = planes[band_bits]
        for k in range(band_bits):
            mask = mask & (planes[k] if s >> k & 1 else ~planes[k])
        mask_ref[s] = mask
    keys = []
    for s in range(bands):
        tally = jnp.sum(lax.population_count(mask_ref[s]), axis=0, keepdims=True)
        keys.append((jnp.max(tally) + 1) // 2 * bands + s)
    for low, high in ((0, 1), (2, 3), (0, 2), (1, 3), (1, 2)):
        keys[low], keys[high] = jnp.minimum(keys[low], keys[high]), jnp.maximum(keys[low], keys[high])
    streams = ((keys[3], keys[0]), (keys[2], keys[1]))

    word_ids = lax.broadcasted_iota(jnp.int32, (words, LANES), 0)
    d_ids = lax.broadcasted_iota(jnp.int32, (32, LANES), 0)
    near = (d_ids >= 1) & (d_ids != 16)
    tile = min(width, 256)
    t_ids = lax.broadcasted_iota(jnp.int32, (tile, 2 * LANES), 0).astype(jnp.float32).astype(jnp.bfloat16)
    p_ids = lax.broadcasted_iota(jnp.int32, (16, 2 * LANES), 0)

    def ends(mask):
        some = mask != 0
        first_row = jnp.min(jnp.where(some, word_ids, words), axis=0, keepdims=True)
        last_row = jnp.max(jnp.where(some, word_ids, -1), axis=0, keepdims=True)
        at_first, at_last = word_ids == first_row, word_ids == last_row
        first_word = jnp.sum(jnp.where(at_first, mask, 0), axis=0, keepdims=True)
        last_word = jnp.sum(jnp.where(at_last, mask, 0), axis=0, keepdims=True)
        first_bit = first_word & -first_word
        last_place = 31 - lax.clz(last_word)
        last_bit = jnp.where(last_word == 0, 0, jnp.left_shift(1, last_place & 31))
        first = 32 * first_row + lax.population_count(first_bit - 1)
        last = 32 * last_row + last_place
        first_ok = first_word != 0
        last_ok = first_ok & (last > first)
        mask = mask & ~(jnp.where(at_first, first_bit, 0) | jnp.where(at_last, last_bit, 0))
        return mask, ((first, first_ok), (last, last_ok))

    def find(s, mask):
        mask, found = ends(mask)
        links, weights, locals_ = [], [], []
        for at, ok in found:
            window = take_windows(code_ref, length, jnp.where(ok, at, 0))
            counts, weight, item = head_counts(window, ok, near, rows)
            links.append(counts)
            weights.append(weight)
            locals_.append(item - base - s * band)
        return mask, *(jnp.concatenate(x, axis=1) for x in (links, weights, locals_))

    def count(s, links, weight, local):
        part = local >> (width.bit_length() - 1)
        inner = local & (width - 1)
        pieces = []
        for p in range(parts):
            chosen = jnp.broadcast_to(jnp.where(part == p, 1.0, 0.0), (16, 2 * LANES)).astype(jnp.bfloat16)
            pieces += [links[n : n + 16] * chosen for n in range(0, rows, 16)]
        pieces.append(jnp.where(p_ids == part, weight, 0.0).astype(jnp.bfloat16))
        left = jnp.concatenate(pieces, axis=0)
        for t in range(width // tile):
            inside = (inner >= t * tile) & (inner < (t + 1) * tile)
            hot = hot_columns(t_ids, jnp.where(inside, inner - t * tile, -1).astype(jnp.float32))
            cols = slice(t * tile, (t + 1) * tile)
            value = lax.dot_general(left, hot, NT, preferred_element_type=jnp.float32)
            count_ref[s, :, cols] += value[0 : parts * rows]
            margin_ref[s, :, cols] += value[parts * rows :]

    def body(trip, masks):
        out = []
        for (early, late), mask in zip(streams, masks):
            switch = early // bands
            s = jnp.where(trip < switch, lax.rem(early, bands), lax.rem(late, bands))
            mask = jnp.where(trip == switch, mask_ref[lax.rem(late, bands)], mask)
            mask, *found = find(s, mask)
            out.append(mask)
            count(s, *found)
        return tuple(out)

    trips = [early // bands + late // bands for early, late in streams]
    starts = tuple(mask_ref[lax.rem(early, bands)] for early, late in streams)
    lax.fori_loop(0, jnp.maximum(*trips), body, starts)


def sign_table(words, width):
    size = words.shape[1]

    def wide(value):
        return jnp.concatenate([value] * (size // LANES), axis=1)

    shift = lax.broadcasted_iota(jnp.int32, (8, LANES), 0)
    parts = []
    for g in range(width // 8):
        word = 8 * g // BITS_PER_WORD
        split, offset = (word + 1) * BITS_PER_WORD - 8 * g, 8 * g - word * BITS_PER_WORD
        now = jnp.broadcast_to(words[word : word + 1], (8, size))
        where_bit = jnp.left_shift(1, shift + offset)
        if split < 8:
            later = jnp.broadcast_to(words[word + 1 : word + 2], (8, size))
            now = jnp.where(wide(shift) >= split, later, now)
            place = jnp.where(shift >= split, shift - split, shift + offset)
            where_bit = jnp.left_shift(1, place)
        parts.append(jnp.where((now & wide(where_bit)) != 0, 1.0, -1.0))
    return jnp.concatenate(parts, axis=0).astype(jnp.bfloat16)


def boundary_counts(rows, share, me, all_ref, extra_ref):
    slabs, blocks = all_ref.shape[0], all_ref.shape[1] * 2 // 3
    half = blocks // 2
    group = slabs // 4
    sub = lax.broadcasted_iota(jnp.int32, (LANES, LANES), 0)
    lane = lax.broadcasted_iota(jnp.int32, (LANES, LANES), 1)
    ids = lax.broadcasted_iota(jnp.int32, (rows, LANES), 0)
    small = lax.broadcasted_iota(jnp.int32, (group, LANES), 1)
    last_items, last_sessions = all_ref[:, blocks - 1, :], all_ref[:, blocks + half - 1, :] >> 16
    next_items, next_sessions = all_ref[:, 0, :], all_ref[:, blocks, :] & 0xFFFF

    def meet(last, following):
        joined = None
        for g in range(4):
            shift = 32 * g + 16
            pieces = (pltpu.roll(x[g * group : (g + 1) * group], shift, 1) for x in (last, following))
            both = jnp.where(small % 32 < 16, *pieces)
            joined = both if joined is None else jnp.where(small // 32 == g, both, joined)
        return joined

    slab_ids = lax.broadcasted_iota(jnp.int32, (slabs, LANES), 0)
    next_sessions = jnp.where(slab_ids == slabs - 1, -1, pltpu.roll(next_sessions, slabs - 1, 0))
    met_items = meet(last_items, pltpu.roll(next_items, slabs - 1, 0))
    met_sessions = meet(last_sessions, next_sessions)
    crossing = ((sub >> 5) == (lane >> 5)) & (((sub ^ lane) & 16) != 0) & (jnp.abs(sub - lane) <= WINDOW)
    ones = jnp.ones((8, LANES), jnp.float32).astype(jnp.bfloat16)
    extra = jnp.zeros((rows + 8, LANES), jnp.float32)
    total = jnp.zeros((8, LANES), jnp.float32)
    for g in range(group):
        item, session = met_items[g : g + 1], met_sessions[g : g + 1]
        linked = one_where((jnp.broadcast_to(session, (LANES, LANES)).T == session) & crossing)
        hot = one_where(ids == item)
        links = jnp.dot(jnp.concatenate([hot, ones], axis=0), linked, preferred_element_type=jnp.float32)
        extra += lax.dot_general(links.astype(jnp.bfloat16), hot, NT, preferred_element_type=jnp.float32)
        total += links[rows:]
    extra_ref[...] = extra
    return jnp.concatenate(
        [
            extra_ref[pl.ds(me * share, share)],
            extra_ref[rows : rows + 1],
            total[0:1],
            jnp.zeros((6 - share, LANES), jnp.float32),
        ],
        axis=0,
    )


def sketch_kernel(
    slabs, rows, parts, width, scale, count_ref, margin_ref, head_ref, sign_ref, all_ref, bits_ref, out_ref,
    extra_ref, log_ref, head_bits, acc_ref, send_ref, recv_ref, bit_sem, send_sems, recv_sems,
):
    me = lax.axis_index("stream")
    barrier = greet_all(slabs, me)
    bands, unused_rows, part = count_ref.shape
    share = rows // slabs
    tile = min(part, 512)
    head_copy = pltpu.make_async_copy(bits_ref.at[:, 0:rows], head_bits, bit_sem.at[0])
    head_copy.start()

    log_ref[...] = jnp.log(jnp.maximum(margin_ref[...], 1.0))
    head = head_ref[...] + boundary_counts(rows, share, me, all_ref, extra_ref)
    row_log = jnp.log(jnp.maximum(head[share : share + 1], 1.0))
    column_log = jnp.broadcast_to(row_log, (rows, LANES)).T
    total_log = jnp.log(jnp.sum(head[share + 1 : share + 2], axis=1, keepdims=True))
    row_term = total_log - column_log[:, 0:1]
    def product(positive, signs):
        upper = positive.astype(jnp.bfloat16)
        lower = (positive - upper.astype(jnp.float32)).astype(jnp.bfloat16)
        both = jnp.concatenate([upper, lower], axis=0)
        value = lax.dot_general(both, signs, NT, preferred_element_type=jnp.float32)
        return value[0:rows] + value[rows:]

    head_copy.wait()
    row = lax.broadcasted_iota(jnp.int32, (8, LANES), 0)
    shared = jnp.concatenate(
        [jnp.where(row < share, head, 0.0), jnp.zeros((rows - 8, LANES), jnp.float32)], axis=0
    )
    shared = pltpu.roll(shared, me * share, 0)
    ratio = jnp.log(jnp.maximum(shared, 1.0)) + total_log - row_log - column_log
    first_band = jnp.where(lax.axis_index("item") == 0, 1.0, 0.0)
    positive = jnp.where(shared > 0, jnp.maximum(ratio, 0.0), 0.0) * first_band
    acc_ref[...] = product(positive.T, sign_table(head_bits[...], width))

    for s in range(bands):
        for h in range(parts):
            for at in range(0, part, tile):
                counts = count_ref[s, h * rows : (h + 1) * rows, at : at + tile]
                ratio = jnp.log(jnp.maximum(counts, NONE)) + row_term - log_ref[s, h : h + 1, at : at + tile]
                positive = jnp.maximum(ratio, 0.0)
                bit_at = (s * parts + h) * part + at
                acc_ref[...] += product(positive, sign_ref[:, bit_at : bit_at + tile])

    cuts = width // LANES
    for d in range(slabs):
        for c in range(cuts):
            send_ref[d, c * share : (c + 1) * share] = (
                acc_ref[d * share : (d + 1) * share, c * LANES : (c + 1) * LANES] * scale
            )
    pl.semaphore_wait(barrier, slabs - 1)
    exchange(slabs, me, send_ref, recv_ref, send_sems, recv_sems, True)
    exchange(slabs, me, send_ref, recv_ref, send_sems, recv_sems, False)
    summed = jnp.sum(recv_ref[...], axis=0)
    out_ref[...] = jnp.concatenate([summed[c * share : (c + 1) * share] for c in range(cuts)], axis=1)


def local(event_items, event_sessions, sketch_bits):
    slabs = lax.axis_size("stream")
    slab = event_items.shape[0]
    total_events = slab * slabs
    words, band_size = sketch_bits.shape
    owned = band_size // slabs
    rows, width = 128, 256
    part = max(LANES, owned // 16)
    bands = BANDS
    parts = owned // (bands * part)
    me = lax.axis_index("stream")
    own_start = me * owned
    first_id = lax.axis_index("item") * band_size + own_start
    blocks = slab // LANES
    length = total_events // LANES

    dma = pltpu.SemaphoreType.DMA
    depth = slabs // PLANE
    count_shapes = (
        jax.ShapeDtypeStruct((bands, parts * rows, part), jnp.float32),
        jax.ShapeDtypeStruct((bands, 16, part), jnp.float32),
    )
    events, head, signs, no_counts, no_margins = pl.pallas_call(
        functools.partial(gather_kernel, slabs, rows, blocks),
        out_shape=(
            jax.ShapeDtypeStruct((slabs, blocks * 3 // 2, LANES), jnp.int32),
            jax.ShapeDtypeStruct((8, LANES), jnp.float32),
            jax.ShapeDtypeStruct((width, owned), jnp.bfloat16),
            *count_shapes,
        ),
        in_specs=[pl.BlockSpec(memory_space=pltpu.HBM)] * 3,
        out_specs=(VMEM,) * 5,
        scratch_shapes=[
            pltpu.VMEM((blocks * 3 // 2, LANES), jnp.int32),
            pltpu.VMEM((words, owned), jnp.int32),
            pltpu.VMEM((blocks, LANES), jnp.int32),
            pltpu.VMEM((blocks, LANES), jnp.int32),
            pltpu.VMEM((blocks + 16, LANES), jnp.int32),
            pltpu.VMEM((blocks + 16, LANES), jnp.int32),
            pltpu.VMEM((rows + 8, LANES), jnp.float32),
            pltpu.VMEM((8, LANES), jnp.float32),
            pltpu.VMEM((2, depth, 4, 8, LANES), jnp.float32),
            pltpu.VMEM((depth, 4, 8, LANES), jnp.float32),
            pltpu.VMEM((4, 8, LANES), jnp.float32),
            pltpu.VMEM((3, 8, LANES), jnp.float32),
            pltpu.VMEM((depth, 4, 8, LANES), jnp.float32),
            pltpu.VMEM((depth, 4, 8, LANES), jnp.float32),
            dma((3,)),
            dma((depth,)),
            dma((depth,)),
            dma((3 * depth,)),
            dma((3 * depth,)),
            dma((4 * depth,)),
            dma((4 * depth,)),
            dma((2,)),
            dma((3,)),
            dma((3,)),
            dma((depth,)),
            dma((depth,)),
        ],
        compiler_params=pltpu.CompilerParams(
            collective_id=0, has_side_effects=True, vmem_limit_bytes=VMEM_GRANT
        ),
        name="gather_events",
    )(*(pltpu.with_memory_space_constraint(x.reshape(blocks, LANES), pltpu.HBM) for x in (event_items, event_sessions)), sketch_bits)

    counts, margins = pl.pallas_call(
        functools.partial(tile_kernel, rows, length, parts),
        out_shape=count_shapes,
        in_specs=[pl.BlockSpec(memory_space=pltpu.SMEM), VMEM, VMEM, VMEM],
        input_output_aliases={2: 0, 3: 1},
        out_specs=(VMEM, VMEM),
        scratch_shapes=[
            pltpu.VMEM((length, LANES), jnp.int32),
            pltpu.VMEM((length + 32, LANES), jnp.int32),
            pltpu.VMEM((bands, length // 32, LANES), jnp.int32),
        ],
        compiler_params=pltpu.CompilerParams(vmem_limit_bytes=VMEM_GRANT),
        name="tile_counts",
    )(first_id.astype(jnp.int32)[None], events, no_counts, no_margins)

    own_rows = pl.pallas_call(
        functools.partial(sketch_kernel, slabs, rows, parts, width, 1.0 / math.sqrt(total_events)),
        out_shape=jax.ShapeDtypeStruct((rows // slabs, width), jnp.float32),
        in_specs=[VMEM] * 5 + [pl.BlockSpec(memory_space=pl.ANY)],
        out_specs=VMEM,
        scratch_shapes=[
            pltpu.VMEM((rows + 8, LANES), jnp.float32),
            pltpu.VMEM((bands, 16, part), jnp.float32),
            pltpu.VMEM((words, rows), jnp.int32),
            pltpu.VMEM((rows, width), jnp.float32),
            pltpu.VMEM((slabs, 8, LANES), jnp.float32),
            pltpu.VMEM((slabs, 8, LANES), jnp.float32),
            dma((1,)),
            dma((slabs,)),
            dma((slabs,)),
        ],
        compiler_params=pltpu.CompilerParams(
            collective_id=1, has_side_effects=True, vmem_limit_bytes=VMEM_GRANT
        ),
        name="sketch_tile",
    )(counts, margins, head, signs, events, sketch_bits)
    if lax.axis_size("item") > 1:
        own_rows = lax.psum(own_rows, "item")
    return own_rows


def solution(mesh):
    placed = (P("stream"), P("stream"), P(None, "item"))
    return jax.shard_map(
        local, mesh=mesh, in_specs=placed, out_specs=P("stream", None), check_vma=False
    )
```

```python
import functools
import math

import jax
import jax.numpy as jnp
from jax import lax
from jax.experimental import pallas as pl
from jax.experimental.pallas import tpu as pltpu
from jax.sharding import PartitionSpec as P

WINDOW = 15
ITEM_BITS = 18
LANES = 128
BITS_PER_WORD = 18
PLANE = 8
BANDS = 4
NONE = 1.0e-30
VMEM_GRANT = 32 * 1024 * 1024
NT = (((1,), (1,)), ((), ()))
VMEM = pl.BlockSpec(memory_space=pltpu.VMEM)


def one_where(mask):
    return jnp.where(mask, 1.0, 0.0).astype(jnp.bfloat16)


def hot_columns(ids, values):
    row = jnp.broadcast_to(values, (16, values.shape[1])).astype(jnp.bfloat16)
    one, zero = jnp.ones((), jnp.bfloat16), jnp.zeros((), jnp.bfloat16)
    return jnp.concatenate(
        [jnp.where(ids[n : n + 16] == row, one, zero) for n in range(0, ids.shape[0], 16)], axis=0
    )


def greet_all(slabs, me):
    barrier = pltpu.get_barrier_semaphore()

    for k in range(1, slabs):
        pl.semaphore_signal(
            barrier, inc=1, device_id={"stream": lax.rem(me + k, slabs)}, device_id_type=pl.DeviceIdType.MESH
        )
    return barrier


def send(src, dst, send_sem, recv_sem, to):
    return pltpu.make_async_remote_copy(
        src_ref=src,
        dst_ref=dst,
        send_sem=send_sem,
        recv_sem=recv_sem,
        device_id={"stream": to},
        device_id_type=pl.DeviceIdType.MESH,
    )


def each(low, high, do):
    for k in range(low, high):
        do(k)


def exchange(slabs, me, out_ref, in_ref, send_sems, recv_sems, start):
    def copy(k):
        to = lax.rem(me + k, slabs)
        return send(out_ref.at[to], in_ref.at[me], send_sems.at[k], recv_sems.at[k], to)

    if start:
        each(1, slabs, lambda k: copy(k).start())
        in_ref[me] = out_ref[me]
    else:
        each(1, slabs, lambda k: copy(k).wait())


def lay_out(rows, owned, base, all_ref, flat_ref, code_ref, mask_ref):
    item_mask = (1 << ITEM_BITS) - 1
    bands = mask_ref.shape[0]
    band = owned // bands
    length = code_ref.shape[0] - 32
    slabs, blocks = all_ref.shape[0], all_ref.shape[1] * 2 // 3
    for n in range(slabs):
        paired = all_ref[n, blocks:]
        sessions = jnp.concatenate([paired & 0xFFFF, paired >> 16], axis=0)
        flat_ref[n * blocks : (n + 1) * blocks] = all_ref[n, 0:blocks] | (sessions << ITEM_BITS)
    per = length // LANES
    for r in range(per):
        code_ref[16 + r * LANES : 16 + (r + 1) * LANES] = flat_ref[pl.ds(r, LANES, stride=per), :].T
    lane = lax.broadcasted_iota(jnp.int32, (16, LANES), 1)
    code_ref[0:16] = jnp.where(lane == 0, -1, pltpu.roll(code_ref[length : length + 16], 1, 1))
    code_ref[length + 16 : length + 32] = jnp.where(
        lane == LANES - 1, -1, pltpu.roll(code_ref[16:32], LANES - 1, 1)
    )

    words = length // 32
    band_bits = (bands - 1).bit_length()
    for w in range(words):
        item = code_ref[16 + 32 * w : 48 + 32 * w] & item_mask
        local = item - base
        mine = (local >= 0) & (local < owned) & (item >= rows)
        packed = bytes_of_rows(jnp.where(mine, (local >> (band.bit_length() - 1)) | bands, 0))
        for k in range(band_bits + 1):
            mask_ref[k, w : w + 1] = plane_word(packed, k)[0:1]
    planes = [mask_ref[k] for k in range(band_bits + 1)]
    for s in range(bands):
        mask = planes[band_bits]
        for k in range(band_bits):
            mask = mask & (planes[k] if s >> k & 1 else ~planes[k])
        mask_ref[s] = mask


def gather_kernel(
    slabs, rows, blocks, items_ref, sessions_ref, bits_ref, all_ref, head_ref, sign_ref, count_ref, margin_ref, code_ref, mask_ref,
    flat_ref,    own_pack, own_bits, own_items, own_sessions, item_ref, session_ref, links_ref, total_ref,
    pair_out, pair_in, plane_out, plane_in, line_out, line_in,
    bit_sem, line_send, line_recv, plane_send, plane_recv, near_send, near_recv,
    pair_sems, head_plane_send, head_plane_recv, head_line_send, head_line_recv,
):
    me = lax.axis_index("stream")
    depth = slabs // PLANE
    layer, low = me // PLANE, lax.rem(me, PLANE)
    parity, quad = lax.rem(me, 2), lax.rem(me // 2, 4)

    def flip(bit):
        return bit - 2 * bit * lax.rem(me // bit, 2)

    partner = me + flip(1)
    steps = (flip(2), flip(4), flip(2) + flip(4))
    def other_layer(k):
        rising = k + (k - layer + depth) // depth
        mirrored = depth - 1 - layer
        falling = depth - 1 - k - (k - mirrored + depth) // depth
        high = layer // ((depth + 1) // 2)
        return rising + (falling - rising) * lax.rem(high, 2)

    others = [other_layer(k) for k in range(depth - 1)]
    loads = [
        pltpu.make_async_copy(items_ref, own_items, bit_sem.at[1]),
        pltpu.make_async_copy(sessions_ref, own_sessions, bit_sem.at[2]),
    ]
    for copy in loads:
        copy.start()
    barrier = pltpu.get_barrier_semaphore()
    owned = own_bits.shape[1]
    bit_copy = pltpu.make_async_copy(
        bits_ref.at[:, pl.ds(pl.multiple_of(me * owned, owned), owned)], own_bits, bit_sem.at[0]
    )
    greeted = [partner] + [me + step for step in steps] + [o * PLANE + low for o in others]
    for to in greeted:
        pl.semaphore_signal(
            barrier, inc=1, device_id={"stream": to}, device_id_type=pl.DeviceIdType.MESH
        )
    for copy in loads:
        copy.wait()
    bit_copy.start()
    half = blocks // 2
    own_pack[0:blocks] = own_items[...]
    own_pack[blocks : blocks + half] = own_sessions[0:half] | (own_sessions[half:blocks] << 16)
    all_ref[me] = own_pack[...]
    item_ref[8 : 8 + blocks] = own_items[...]
    session_ref[8 : 8 + blocks] = own_sessions[...]
    for edge in (slice(0, 8), slice(8 + blocks, 16 + blocks)):
        item_ref[edge] = jnp.zeros((8, LANES), jnp.int32)
        session_ref[edge] = jnp.full((8, LANES), -1, jnp.int32)
    sub = lax.broadcasted_iota(jnp.int32, (LANES, LANES), 0)
    lane = lax.broadcasted_iota(jnp.int32, (LANES, LANES), 1)
    low_lane = lax.broadcasted_iota(jnp.int32, (1, LANES), 1) < LANES // 2
    ids = lax.broadcasted_iota(jnp.int32, (rows, LANES), 0)
    gaps = (sub - LANES // 2 - lane, sub + LANES // 2 - lane)
    in_reach = [(jnp.abs(gap) <= WINDOW) & (gap != 0) for gap in gaps]
    ones = jnp.ones((8, 2 * LANES), jnp.float32).astype(jnp.bfloat16)
    links_ref[...] = jnp.zeros_like(links_ref)
    total_ref[...] = jnp.zeros_like(total_ref)

    together = 8

    def some_blocks(n, unused):
        first = n * together

        def shifted(ref):
            turned = [pltpu.roll(ref[pl.ds(first + 7 + o, 1)], LANES // 2, 1) for o in range(together + 2)]
            return [jnp.where(low_lane, turned[o], turned[o + 1]) for o in range(together + 1)]

        hots = [one_where(ids == item) for item in shifted(item_ref)]
        sessions = [jnp.broadcast_to(session, (LANES, LANES)).T for session in shifted(session_ref)]
        for o in range(together):
            own_item, own_session = item_ref[pl.ds(first + o + 8, 1)], session_ref[pl.ds(first + o + 8, 1)]
            hot = jnp.concatenate([hots[o], hots[o + 1]], axis=1)
            linked = jnp.concatenate(
                [one_where((sessions[o + side] == own_session) & in_reach[side]) for side in range(2)], axis=0
            )
            links = jnp.dot(jnp.concatenate([hot, ones], axis=0), linked, preferred_element_type=jnp.float32)
            links_ref[...] += lax.dot_general(
                links.astype(jnp.bfloat16), one_where(ids == own_item), NT, preferred_element_type=jnp.float32
            )
            total_ref[...] += links[rows:]
        return unused

    inner = [blocks * n // 32 for n in (0, 0, 32)]

    def blocks_of(n):
        lax.fori_loop(inner[n] // together, inner[n + 1] // together, some_blocks, 0)

    step_columns = max(LANES, owned // 16)
    steps_in_all = owned // step_columns

    def signs(low_step, high_step):
        def step(t, unused):
            at = pl.multiple_of(t * step_columns, step_columns)
            sign_ref[:, pl.ds(at, step_columns)] = sign_table(own_bits[:, pl.ds(at, step_columns)], sign_ref.shape[0])
            return unused

        lax.fori_loop(low_step * steps_in_all // 16, high_step * steps_in_all // 16, step, 0)

    blocks_of(0)
    pl.semaphore_wait(barrier, len(greeted))

    def along_line(there, here):
        return send(
            own_pack, all_ref.at[me], line_send.at[there], line_recv.at[here], there * PLANE + low
        )

    def in_plane(d, at_layer, own=False):
        slab = all_ref.at[at_layer * PLANE + low]
        sem = d * depth + at_layer
        return send(own_pack if own else slab, slab, plane_send.at[sem], plane_recv.at[sem], me + steps[d])

    def to_partner(r, at_layer, own=False):
        slab = all_ref.at[at_layer * PLANE + low + ((0,) + steps)[r]]
        sem = r * depth + at_layer
        return send(own_pack if own else slab, slab, near_send.at[sem], near_recv.at[sem], partner)

    for o in reversed(others):
        along_line(o, layer).start()
    for d in range(3):
        in_plane(d, layer, True).start()
    to_partner(0, layer, True).start()

    def forward_line(k):
        along_line(layer, others[k]).wait_recv()
        for d in range(3):
            in_plane(d, others[k]).start()
        to_partner(0, others[k]).start()

    def forward_plane(at_layer):
        for d in range(3):
            in_plane(d, at_layer).wait_recv()
            to_partner(d + 1, at_layer).start()

    blocks_of(1)
    share = rows // slabs
    tail = jnp.concatenate(
        [links_ref[rows : rows + 1], total_ref[0:1], jnp.zeros((6 - share, LANES), jnp.float32)], axis=0
    )
    for d in range(slabs):
        at = (d % 2, d // PLANE, d // 2 % 4)
        pair_out[at + (slice(0, share),)] = links_ref[d * share : (d + 1) * share]
        pair_out[at + (slice(share, 8),)] = tail

    pair = send(pair_out.at[1 - parity], pair_in, pair_sems.at[0], pair_sems.at[1], partner)
    pair.start()
    forward_line(0)
    forward_line(1)
    pair.wait()
    line_out[...] = pair_out[parity] + pair_in[...]

    def head_line(there, here):
        return send(
            line_out.at[there], line_in.at[layer], head_line_send.at[there], head_line_recv.at[here],
            there * PLANE + low,
        )

    for o in others:
        head_line(o, layer).start()
    line_in[layer] = line_out[layer]
    forward_plane(layer)
    for k in range(2, depth - 1):
        forward_line(k)
    count_ref[...] = jnp.zeros_like(count_ref)
    margin_ref[...] = jnp.zeros_like(margin_ref)
    bit_copy.wait()
    signs(0, 4)
    forward_plane(others[0])
    signs(4, 8)
    for o in others[1:-1]:
        forward_plane(o)
    for o in others:
        head_line(o, o).wait_recv()
    plane_out[...] = jnp.sum(line_in[...], axis=0)

    def head_plane(d):
        to = me + steps[d]
        return send(
            plane_out.at[lax.rem(to // 2, 4)], plane_in.at[d], head_plane_send.at[d], head_plane_recv.at[d], to
        )

    for d in range(3):
        head_plane(d).start()
    signs(8, 12)
    for o in others[-1:]:
        forward_plane(o)
    signs(12, 16)
    for at_layer in [layer] + others:
        for r in range(4):
            to_partner(r, at_layer).wait()
    base = lax.axis_index("item") * bits_ref.shape[1] + me * owned
    lay_out(rows, owned, base, all_ref, flat_ref, code_ref, mask_ref)
    for at_layer in [layer] + others:
        for d in range(3):
            in_plane(d, at_layer).wait_send()
    for o in others:
        along_line(o, layer).wait_send()
        head_line(o, o).wait_send()
    for d in range(3):
        head_plane(d).wait()
    head_ref[...] = plane_out[quad] + plane_in[0] + plane_in[1] + plane_in[2]


def take_windows(code_ref, length, start):
    whole, part = start >> 3, start & 7
    bits = max(1, (length // 8 - 1).bit_length())
    keep = 8 * ((1 << (bits - 1)) + 4)
    value = None
    for bit in reversed(range(bits)):
        step = 8 << bit
        keep = 8 * ((1 << bit) + 4)
        chosen = ((whole >> bit) & 1) == 1
        if value is None:
            low, high = code_ref[0:keep, :], code_ref[step : step + keep, :]
        else:
            low, high = value[0:keep], value[step : step + keep]
        value = jnp.where(chosen, high, low)
    for bit in (2, 1, 0):
        chosen = ((part >> bit) & 1) == 1
        value = jnp.where(chosen, pltpu.roll(value, value.shape[0] - (1 << bit), 0), value)
    return value[0:32]


def all_rows(value, combine):
    for shift in (4, 2, 1):
        value = combine(value, pltpu.roll(value, shift, 0))
    return value


def bytes_of_rows(tag):
    return tag[0:8] | (tag[8:16] << 8) | (tag[16:24] << 16) | (tag[24:32] << 24)


def plane_word(packed, k):
    sub = lax.broadcasted_iota(jnp.int32, (8, LANES), 0)
    spread = lax.shift_left(lax.shift_right_logical(packed, k) & 0x01010101, sub)
    return all_rows(spread, lambda x, y: x | y)


def head_counts(window, ok, near, rows):
    center = window[16:17]
    linked = ((window ^ center) >> ITEM_BITS == 0) & near & ok
    item = window & ((1 << ITEM_BITS) - 1)
    tag = jnp.where(linked & (item < rows), item | rows, 0)
    packed = bytes_of_rows(tag)
    one = jnp.where(linked, 1, 0)
    weight = all_rows(one[0:8] + one[8:16] + one[16:24] + one[24:32], lambda x, y: x + y)
    sub = lax.broadcasted_iota(jnp.int32, (8, LANES), 0)

    def plane(k):
        return plane_word(packed, k)

    bits = rows.bit_length() - 1
    node = plane(bits)
    for k in range(3):
        node = node & (plane(k) ^ (((sub >> k) & 1) - 1))
    nodes = [node]
    for k in reversed(range(3, bits)):
        word = plane(k)
        nodes = [part for node in nodes for part in (node & ~word, node & word)]
    counts = jnp.concatenate([lax.population_count(node).astype(jnp.float32) for node in nodes], axis=0)
    return counts.astype(jnp.bfloat16), weight[0:1].astype(jnp.float32), center & ((1 << ITEM_BITS) - 1)


def tile_kernel(rows, length, parts, base_ref, code_ref, mask_ref, unused_counts, unused_margins, count_ref, margin_ref):
    base = base_ref[0]
    bands, unused_rows, width = count_ref.shape
    band = parts * width
    words = length // 32
    keys = []
    for s in range(bands):
        tally = jnp.sum(lax.population_count(mask_ref[s]), axis=0, keepdims=True)
        keys.append((jnp.max(tally) + 1) // 2 * bands + s)
    for low, high in ((0, 1), (2, 3), (0, 2), (1, 3), (1, 2)):
        keys[low], keys[high] = jnp.minimum(keys[low], keys[high]), jnp.maximum(keys[low], keys[high])
    streams = ((keys[3], keys[0]), (keys[2], keys[1]))

    word_ids = lax.broadcasted_iota(jnp.int32, (words, LANES), 0)
    d_ids = lax.broadcasted_iota(jnp.int32, (32, LANES), 0)
    near = (d_ids >= 1) & (d_ids != 16)
    tile = min(width, 256)
    t_ids = lax.broadcasted_iota(jnp.int32, (tile, 2 * LANES), 0).astype(jnp.float32).astype(jnp.bfloat16)
    p_ids = lax.broadcasted_iota(jnp.int32, (16, 2 * LANES), 0)

    def ends(mask):
        some = mask != 0
        first_row = jnp.min(jnp.where(some, word_ids, words), axis=0, keepdims=True)
        last_row = jnp.max(jnp.where(some, word_ids, -1), axis=0, keepdims=True)
        at_first, at_last = word_ids == first_row, word_ids == last_row
        first_word = jnp.sum(jnp.where(at_first, mask, 0), axis=0, keepdims=True)
        last_word = jnp.sum(jnp.where(at_last, mask, 0), axis=0, keepdims=True)
        first_bit = first_word & -first_word
        last_place = 31 - lax.clz(last_word)
        last_bit = jnp.where(last_word == 0, 0, jnp.left_shift(1, last_place & 31))
        first = 32 * first_row + lax.population_count(first_bit - 1)
        last = 32 * last_row + last_place
        first_ok = first_word != 0
        last_ok = first_ok & (last > first)
        mask = mask & ~(jnp.where(at_first, first_bit, 0) | jnp.where(at_last, last_bit, 0))
        return mask, ((first, first_ok), (last, last_ok))

    def find(s, mask):
        mask, found = ends(mask)
        links, weights, locals_ = [], [], []
        for at, ok in found:
            window = take_windows(code_ref, length, jnp.where(ok, at, 0))
            counts, weight, item = head_counts(window, ok, near, rows)
            links.append(counts)
            weights.append(weight)
            locals_.append(item - base - s * band)
        return mask, *(jnp.concatenate(x, axis=1) for x in (links, weights, locals_))

    def count(s, links, weight, local):
        part = local >> (width.bit_length() - 1)
        inner = local & (width - 1)
        pieces = []
        for p in range(parts):
            chosen = jnp.broadcast_to(jnp.where(part == p, 1.0, 0.0), (16, 2 * LANES)).astype(jnp.bfloat16)
            pieces += [links[n : n + 16] * chosen for n in range(0, rows, 16)]
        pieces.append(jnp.where(p_ids == part, weight, 0.0).astype(jnp.bfloat16))
        left = jnp.concatenate(pieces, axis=0)
        for t in range(width // tile):
            inside = (inner >= t * tile) & (inner < (t + 1) * tile)
            hot = hot_columns(t_ids, jnp.where(inside, inner - t * tile, -1).astype(jnp.float32))
            cols = slice(t * tile, (t + 1) * tile)
            value = lax.dot_general(left, hot, NT, preferred_element_type=jnp.float32)
            count_ref[s, :, cols] += value[0 : parts * rows]
            margin_ref[s, :, cols] += value[parts * rows :]

    def body(trip, masks):
        out = []
        for (early, late), mask in zip(streams, masks):
            switch = early // bands
            s = jnp.where(trip < switch, lax.rem(early, bands), lax.rem(late, bands))
            mask = jnp.where(trip == switch, mask_ref[lax.rem(late, bands)], mask)
            mask, *found = find(s, mask)
            out.append(mask)
            count(s, *found)
        return tuple(out)

    trips = [early // bands + late // bands for early, late in streams]
    starts = tuple(mask_ref[lax.rem(early, bands)] for early, late in streams)
    lax.fori_loop(0, jnp.maximum(*trips), body, starts)


def sign_table(words, width):
    size = words.shape[1]

    def wide(value):
        return jnp.concatenate([value] * (size // LANES), axis=1)

    shift = lax.broadcasted_iota(jnp.int32, (8, LANES), 0)
    parts = []
    for g in range(width // 8):
        word = 8 * g // BITS_PER_WORD
        split, offset = (word + 1) * BITS_PER_WORD - 8 * g, 8 * g - word * BITS_PER_WORD
        now = jnp.broadcast_to(words[word : word + 1], (8, size))
        where_bit = jnp.left_shift(1, shift + offset)
        if split < 8:
            later = jnp.broadcast_to(words[word + 1 : word + 2], (8, size))
            now = jnp.where(wide(shift) >= split, later, now)
            place = jnp.where(shift >= split, shift - split, shift + offset)
            where_bit = jnp.left_shift(1, place)
        parts.append(jnp.where((now & wide(where_bit)) != 0, 1.0, -1.0))
    return jnp.concatenate(parts, axis=0).astype(jnp.bfloat16)


def boundary_counts(rows, share, me, all_ref, extra_ref):
    slabs, blocks = all_ref.shape[0], all_ref.shape[1] * 2 // 3
    half = blocks // 2
    group = slabs // 4
    sub = lax.broadcasted_iota(jnp.int32, (LANES, LANES), 0)
    lane = lax.broadcasted_iota(jnp.int32, (LANES, LANES), 1)
    ids = lax.broadcasted_iota(jnp.int32, (rows, LANES), 0)
    small = lax.broadcasted_iota(jnp.int32, (group, LANES), 1)
    last_items, last_sessions = all_ref[:, blocks - 1, :], all_ref[:, blocks + half - 1, :] >> 16
    next_items, next_sessions = all_ref[:, 0, :], all_ref[:, blocks, :] & 0xFFFF

    def meet(last, following):
        joined = None
        for g in range(4):
            shift = 32 * g + 16
            pieces = (pltpu.roll(x[g * group : (g + 1) * group], shift, 1) for x in (last, following))
            both = jnp.where(small % 32 < 16, *pieces)
            joined = both if joined is None else jnp.where(small // 32 == g, both, joined)
        return joined

    slab_ids = lax.broadcasted_iota(jnp.int32, (slabs, LANES), 0)
    next_sessions = jnp.where(slab_ids == slabs - 1, -1, pltpu.roll(next_sessions, slabs - 1, 0))
    met_items = meet(last_items, pltpu.roll(next_items, slabs - 1, 0))
    met_sessions = meet(last_sessions, next_sessions)
    crossing = ((sub >> 5) == (lane >> 5)) & (((sub ^ lane) & 16) != 0) & (jnp.abs(sub - lane) <= WINDOW)
    ones = jnp.ones((8, LANES), jnp.float32).astype(jnp.bfloat16)
    extra = jnp.zeros((rows + 8, LANES), jnp.float32)
    total = jnp.zeros((8, LANES), jnp.float32)
    for g in range(group):
        item, session = met_items[g : g + 1], met_sessions[g : g + 1]
        linked = one_where((jnp.broadcast_to(session, (LANES, LANES)).T == session) & crossing)
        hot = one_where(ids == item)
        links = jnp.dot(jnp.concatenate([hot, ones], axis=0), linked, preferred_element_type=jnp.float32)
        extra += lax.dot_general(links.astype(jnp.bfloat16), hot, NT, preferred_element_type=jnp.float32)
        total += links[rows:]
    extra_ref[...] = extra
    return jnp.concatenate(
        [
            extra_ref[pl.ds(me * share, share)],
            extra_ref[rows : rows + 1],
            total[0:1],
            jnp.zeros((6 - share, LANES), jnp.float32),
        ],
        axis=0,
    )


def sketch_kernel(
    slabs, rows, parts, width, scale, count_ref, margin_ref, head_ref, sign_ref, all_ref, bits_ref, out_ref,
    extra_ref, log_ref, head_bits, acc_ref, send_ref, recv_ref, bit_sem, send_sems, recv_sems,
):
    me = lax.axis_index("stream")
    barrier = greet_all(slabs, me)
    bands, unused_rows, part = count_ref.shape
    share = rows // slabs
    tile = min(part, 512)
    head_copy = pltpu.make_async_copy(bits_ref.at[:, 0:rows], head_bits, bit_sem.at[0])
    head_copy.start()

    log_ref[...] = jnp.log(jnp.maximum(margin_ref[...], 1.0))
    head = head_ref[...] + boundary_counts(rows, share, me, all_ref, extra_ref)
    row_log = jnp.log(jnp.maximum(head[share : share + 1], 1.0))
    column_log = jnp.broadcast_to(row_log, (rows, LANES)).T
    total_log = jnp.log(jnp.sum(head[share + 1 : share + 2], axis=1, keepdims=True))
    row_term = total_log - column_log[:, 0:1]
    def product(positive, signs):
        upper = positive.astype(jnp.bfloat16)
        lower = (positive - upper.astype(jnp.float32)).astype(jnp.bfloat16)
        both = jnp.concatenate([upper, lower], axis=0)
        value = lax.dot_general(both, signs, NT, preferred_element_type=jnp.float32)
        return value[0:rows] + value[rows:]

    head_copy.wait()
    row = lax.broadcasted_iota(jnp.int32, (8, LANES), 0)
    shared = jnp.concatenate(
        [jnp.where(row < share, head, 0.0), jnp.zeros((rows - 8, LANES), jnp.float32)], axis=0
    )
    shared = pltpu.roll(shared, me * share, 0)
    ratio = jnp.log(jnp.maximum(shared, 1.0)) + total_log - row_log - column_log
    first_band = jnp.where(lax.axis_index("item") == 0, 1.0, 0.0)
    positive = jnp.where(shared > 0, jnp.maximum(ratio, 0.0), 0.0) * first_band
    acc_ref[...] = product(positive.T, sign_table(head_bits[...], width))

    for s in range(bands):
        for h in range(parts):
            for at in range(0, part, tile):
                counts = count_ref[s, h * rows : (h + 1) * rows, at : at + tile]
                ratio = jnp.log(jnp.maximum(counts, NONE)) + row_term - log_ref[s, h : h + 1, at : at + tile]
                positive = jnp.maximum(ratio, 0.0)
                bit_at = (s * parts + h) * part + at
                acc_ref[...] += product(positive, sign_ref[:, bit_at : bit_at + tile])

    cuts = width // LANES
    for d in range(slabs):
        for c in range(cuts):
            send_ref[d, c * share : (c + 1) * share] = (
                acc_ref[d * share : (d + 1) * share, c * LANES : (c + 1) * LANES] * scale
            )
    pl.semaphore_wait(barrier, slabs - 1)
    exchange(slabs, me, send_ref, recv_ref, send_sems, recv_sems, True)
    exchange(slabs, me, send_ref, recv_ref, send_sems, recv_sems, False)
    summed = jnp.sum(recv_ref[...], axis=0)
    out_ref[...] = jnp.concatenate([summed[c * share : (c + 1) * share] for c in range(cuts)], axis=1)


def local(event_items, event_sessions, sketch_bits):
    slabs = lax.axis_size("stream")
    slab = event_items.shape[0]
    total_events = slab * slabs
    words, band_size = sketch_bits.shape
    owned = band_size // slabs
    rows, width = 128, 256
    part = max(LANES, owned // 16)
    bands = BANDS
    parts = owned // (bands * part)
    me = lax.axis_index("stream")
    own_start = me * owned
    first_id = lax.axis_index("item") * band_size + own_start
    blocks = slab // LANES
    length = total_events // LANES

    dma = pltpu.SemaphoreType.DMA
    depth = slabs // PLANE
    count_shapes = (
        jax.ShapeDtypeStruct((bands, parts * rows, part), jnp.float32),
        jax.ShapeDtypeStruct((bands, 16, part), jnp.float32),
    )
    events, head, signs, no_counts, no_margins, codes, masks = pl.pallas_call(
        functools.partial(gather_kernel, slabs, rows, blocks),
        out_shape=(
            jax.ShapeDtypeStruct((slabs, blocks * 3 // 2, LANES), jnp.int32),
            jax.ShapeDtypeStruct((8, LANES), jnp.float32),
            jax.ShapeDtypeStruct((width, owned), jnp.bfloat16),
            *count_shapes,
            jax.ShapeDtypeStruct((length + 32, LANES), jnp.int32),
            jax.ShapeDtypeStruct((bands, length // 32, LANES), jnp.int32),
        ),
        in_specs=[pl.BlockSpec(memory_space=pltpu.HBM)] * 3,
        out_specs=(VMEM,) * 7,
        scratch_shapes=[
            pltpu.VMEM((length, LANES), jnp.int32),
            pltpu.VMEM((blocks * 3 // 2, LANES), jnp.int32),
            pltpu.VMEM((words, owned), jnp.int32),
            pltpu.VMEM((blocks, LANES), jnp.int32),
            pltpu.VMEM((blocks, LANES), jnp.int32),
            pltpu.VMEM((blocks + 16, LANES), jnp.int32),
            pltpu.VMEM((blocks + 16, LANES), jnp.int32),
            pltpu.VMEM((rows + 8, LANES), jnp.float32),
            pltpu.VMEM((8, LANES), jnp.float32),
            pltpu.VMEM((2, depth, 4, 8, LANES), jnp.float32),
            pltpu.VMEM((depth, 4, 8, LANES), jnp.float32),
            pltpu.VMEM((4, 8, LANES), jnp.float32),
            pltpu.VMEM((3, 8, LANES), jnp.float32),
            pltpu.VMEM((depth, 4, 8, LANES), jnp.float32),
            pltpu.VMEM((depth, 4, 8, LANES), jnp.float32),
            dma((3,)),
            dma((depth,)),
            dma((depth,)),
            dma((3 * depth,)),
            dma((3 * depth,)),
            dma((4 * depth,)),
            dma((4 * depth,)),
            dma((2,)),
            dma((3,)),
            dma((3,)),
            dma((depth,)),
            dma((depth,)),
        ],
        compiler_params=pltpu.CompilerParams(
            collective_id=0, has_side_effects=True, vmem_limit_bytes=VMEM_GRANT
        ),
        name="gather_events",
    )(*(pltpu.with_memory_space_constraint(x.reshape(blocks, LANES), pltpu.HBM) for x in (event_items, event_sessions)), sketch_bits)

    counts, margins = pl.pallas_call(
        functools.partial(tile_kernel, rows, length, parts),
        out_shape=count_shapes,
        in_specs=[pl.BlockSpec(memory_space=pltpu.SMEM)] + [VMEM] * 4,
        input_output_aliases={3: 0, 4: 1},
        out_specs=(VMEM, VMEM),
        compiler_params=pltpu.CompilerParams(vmem_limit_bytes=VMEM_GRANT),
        name="tile_counts",
    )(first_id.astype(jnp.int32)[None], codes, masks, no_counts, no_margins)

    own_rows = pl.pallas_call(
        functools.partial(sketch_kernel, slabs, rows, parts, width, 1.0 / math.sqrt(total_events)),
        out_shape=jax.ShapeDtypeStruct((rows // slabs, width), jnp.float32),
        in_specs=[VMEM] * 5 + [pl.BlockSpec(memory_space=pl.ANY)],
        out_specs=VMEM,
        scratch_shapes=[
            pltpu.VMEM((rows + 8, LANES), jnp.float32),
            pltpu.VMEM((bands, 16, part), jnp.float32),
            pltpu.VMEM((words, rows), jnp.int32),
            pltpu.VMEM((rows, width), jnp.float32),
            pltpu.VMEM((slabs, 8, LANES), jnp.float32),
            pltpu.VMEM((slabs, 8, LANES), jnp.float32),
            dma((1,)),
            dma((slabs,)),
            dma((slabs,)),
        ],
        compiler_params=pltpu.CompilerParams(
            collective_id=1, has_side_effects=True, vmem_limit_bytes=VMEM_GRANT
        ),
        name="sketch_tile",
    )(counts, margins, head, signs, events, sketch_bits)
    if lax.axis_size("item") > 1:
        own_rows = lax.psum(own_rows, "item")
    return own_rows


def solution(mesh):
    placed = (P("stream"), P("stream"), P(None, "item"))
    return jax.shard_map(
        local, mesh=mesh, in_specs=placed, out_specs=P("stream", None), check_vma=False
    )
```

```python
import functools
import math

import jax
import jax.numpy as jnp
from jax import lax
from jax.experimental import pallas as pl
from jax.experimental.pallas import tpu as pltpu
from jax.sharding import PartitionSpec as P

WINDOW = 15
ITEM_BITS = 18
LANES = 128
BITS_PER_WORD = 18
PLANE = 8
BANDS = 4
NONE = 1.0e-30
VMEM_GRANT = 45 * 1024 * 1024
NT = (((1,), (1,)), ((), ()))
VMEM = pl.BlockSpec(memory_space=pltpu.VMEM)


def one_where(mask):
    return jnp.where(mask, 1.0, 0.0).astype(jnp.bfloat16)


def hot_columns(ids, values):
    row = jnp.broadcast_to(values, (16, values.shape[1])).astype(jnp.bfloat16)
    one, zero = jnp.ones((), jnp.bfloat16), jnp.zeros((), jnp.bfloat16)
    return jnp.concatenate(
        [jnp.where(ids[n : n + 16] == row, one, zero) for n in range(0, ids.shape[0], 16)], axis=0
    )


def greet_all(slabs, me):
    barrier = pltpu.get_barrier_semaphore()

    for k in range(1, slabs):
        pl.semaphore_signal(
            barrier, inc=1, device_id={"stream": lax.rem(me + k, slabs)}, device_id_type=pl.DeviceIdType.MESH
        )
    return barrier


def send(src, dst, send_sem, recv_sem, to):
    return pltpu.make_async_remote_copy(
        src_ref=src,
        dst_ref=dst,
        send_sem=send_sem,
        recv_sem=recv_sem,
        device_id={"stream": to},
        device_id_type=pl.DeviceIdType.MESH,
    )


def flip(me, bit):
    return bit - 2 * bit * lax.rem(me // bit, 2)


def other_layer(k, layer, depth):
    rising = k + (k - layer + depth) // depth
    mirrored = depth - 1 - layer
    falling = depth - 1 - k - (k - mirrored + depth) // depth
    high = layer // ((depth + 1) // 2)
    return rising + (falling - rising) * lax.rem(high, 2)


def far_first(slabs, me):
    depth = slabs // PLANE
    layer = me // PLANE
    turns = [sum(flip(me, bit) for bit in (1, 2, 4) if turn & bit) for turn in (6, 7, 4, 5, 2, 3, 0, 1)]
    shifts = [(other_layer(k, layer, depth) - layer) * PLANE for k in reversed(range(depth - 1))]
    away = [shift + turn for shift in shifts for turn in turns]
    return [me + step for step in away + turns[0:6] + turns[7:]]


def exchange(slabs, me, out_ref, in_ref, send_sems, recv_sems):
    targets = far_first(slabs, me)
    for k, to in enumerate(targets):
        send(out_ref.at[to], in_ref.at[me], send_sems.at[k], recv_sems.at[me], to).start()
    in_ref[me] = out_ref[me]
    for k, to in enumerate(targets):
        send(out_ref.at[to], in_ref.at[to], send_sems.at[k], recv_sems.at[to], to).wait()


def gather_kernel(
    slabs, rows, blocks, items_ref, sessions_ref, bits_ref, all_ref, head_ref, sign_ref, count_ref, margin_ref,
    own_pack, own_bits, own_items, own_sessions, item_ref, session_ref, links_ref, total_ref,
    pair_out, pair_in, plane_out, plane_in, line_out, line_in,
    bit_sem, line_send, line_recv, plane_send, plane_recv, near_send, near_recv,
    pair_sems, head_plane_send, head_plane_recv, head_line_send, head_line_recv,
):
    me = lax.axis_index("stream")
    depth = slabs // PLANE
    layer, low = me // PLANE, lax.rem(me, PLANE)
    parity, quad = lax.rem(me, 2), lax.rem(me // 2, 4)

    partner = me + flip(me, 1)
    steps = (flip(me, 2), flip(me, 4), flip(me, 2) + flip(me, 4))
    others = [other_layer(k, layer, depth) for k in range(depth - 1)]
    loads = [
        pltpu.make_async_copy(items_ref, own_items, bit_sem.at[1]),
        pltpu.make_async_copy(sessions_ref, own_sessions, bit_sem.at[2]),
    ]
    for copy in loads:
        copy.start()
    barrier = pltpu.get_barrier_semaphore()
    owned = own_bits.shape[1]
    bit_copy = pltpu.make_async_copy(
        bits_ref.at[:, pl.ds(pl.multiple_of(me * owned, owned), owned)], own_bits, bit_sem.at[0]
    )
    greeted = [partner] + [me + step for step in steps] + [o * PLANE + low for o in others]
    for to in greeted:
        pl.semaphore_signal(
            barrier, inc=1, device_id={"stream": to}, device_id_type=pl.DeviceIdType.MESH
        )
    for copy in loads:
        copy.wait()
    bit_copy.start()
    half = blocks // 2
    own_pack[0:blocks] = own_items[...]
    own_pack[blocks : blocks + half] = own_sessions[0:half] | (own_sessions[half:blocks] << 16)
    all_ref[me] = own_pack[...]
    item_ref[8 : 8 + blocks] = own_items[...]
    session_ref[8 : 8 + blocks] = own_sessions[...]
    for edge in (slice(0, 8), slice(8 + blocks, 16 + blocks)):
        item_ref[edge] = jnp.zeros((8, LANES), jnp.int32)
        session_ref[edge] = jnp.full((8, LANES), -1, jnp.int32)
    sub = lax.broadcasted_iota(jnp.int32, (LANES, LANES), 0)
    lane = lax.broadcasted_iota(jnp.int32, (LANES, LANES), 1)
    low_lane = lax.broadcasted_iota(jnp.int32, (1, LANES), 1) < LANES // 2
    ids = lax.broadcasted_iota(jnp.int32, (rows, LANES), 0)
    gaps = (sub - LANES // 2 - lane, sub + LANES // 2 - lane)
    in_reach = [(jnp.abs(gap) <= WINDOW) & (gap != 0) for gap in gaps]
    ones = jnp.ones((8, 2 * LANES), jnp.float32).astype(jnp.bfloat16)
    links_ref[...] = jnp.zeros_like(links_ref)
    total_ref[...] = jnp.zeros_like(total_ref)

    together = 8

    def some_blocks(n, unused):
        first = n * together

        def shifted(ref):
            turned = [pltpu.roll(ref[pl.ds(first + 7 + o, 1)], LANES // 2, 1) for o in range(together + 2)]
            return [jnp.where(low_lane, turned[o], turned[o + 1]) for o in range(together + 1)]

        hots = [one_where(ids == item) for item in shifted(item_ref)]
        sessions = [jnp.broadcast_to(session, (LANES, LANES)).T for session in shifted(session_ref)]
        for o in range(together):
            own_item, own_session = item_ref[pl.ds(first + o + 8, 1)], session_ref[pl.ds(first + o + 8, 1)]
            hot = jnp.concatenate([hots[o], hots[o + 1]], axis=1)
            linked = jnp.concatenate(
                [one_where((sessions[o + side] == own_session) & in_reach[side]) for side in range(2)], axis=0
            )
            links = jnp.dot(jnp.concatenate([hot, ones], axis=0), linked, preferred_element_type=jnp.float32)
            links_ref[...] += lax.dot_general(
                links.astype(jnp.bfloat16), one_where(ids == own_item), NT, preferred_element_type=jnp.float32
            )
            total_ref[...] += links[rows:]
        return unused

    inner = [blocks * n // 32 for n in (0, 0, 32)]

    def blocks_of(n):
        lax.fori_loop(inner[n] // together, inner[n + 1] // together, some_blocks, 0)

    step_columns = max(LANES, owned // 16)
    steps_in_all = owned // step_columns

    def signs(low_step, high_step):
        def step(t, unused):
            at = pl.multiple_of(t * step_columns, step_columns)
            sign_ref[:, pl.ds(at, step_columns)] = sign_table(own_bits[:, pl.ds(at, step_columns)], sign_ref.shape[0])
            return unused

        lax.fori_loop(low_step * steps_in_all // 16, high_step * steps_in_all // 16, step, 0)

    blocks_of(0)
    pl.semaphore_wait(barrier, len(greeted))

    def along_line(there, here):
        return send(
            own_pack, all_ref.at[me], line_send.at[there], line_recv.at[here], there * PLANE + low
        )

    def in_plane(d, at_layer, own=False):
        slab = all_ref.at[at_layer * PLANE + low]
        sem = d * depth + at_layer
        return send(own_pack if own else slab, slab, plane_send.at[sem], plane_recv.at[sem], me + steps[d])

    def to_partner(r, at_layer, own=False):
        slab = all_ref.at[at_layer * PLANE + low + ((0,) + steps)[r]]
        sem = r * depth + at_layer
        return send(own_pack if own else slab, slab, near_send.at[sem], near_recv.at[sem], partner)

    for o in reversed(others):
        along_line(o, layer).start()
    for d in range(3):
        in_plane(d, layer, True).start()
    to_partner(0, layer, True).start()

    def forward_line(k):
        along_line(layer, others[k]).wait_recv()
        for d in range(3):
            in_plane(d, others[k]).start()
        to_partner(0, others[k]).start()

    def forward_plane(at_layer):
        for d in range(3):
            in_plane(d, at_layer).wait_recv()
            to_partner(d + 1, at_layer).start()

    blocks_of(1)
    share = rows // slabs
    tail = jnp.concatenate(
        [links_ref[rows : rows + 1], total_ref[0:1], jnp.zeros((6 - share, LANES), jnp.float32)], axis=0
    )
    for d in range(slabs):
        at = (d % 2, d // PLANE, d // 2 % 4)
        pair_out[at + (slice(0, share),)] = links_ref[d * share : (d + 1) * share]
        pair_out[at + (slice(share, 8),)] = tail

    pair = send(pair_out.at[1 - parity], pair_in, pair_sems.at[0], pair_sems.at[1], partner)
    pair.start()
    forward_line(0)
    forward_line(1)
    pair.wait()
    line_out[...] = pair_out[parity] + pair_in[...]

    def head_line(there, here):
        return send(
            line_out.at[there], line_in.at[layer], head_line_send.at[there], head_line_recv.at[here],
            there * PLANE + low,
        )

    for o in others:
        head_line(o, layer).start()
    line_in[layer] = line_out[layer]
    forward_plane(layer)
    for k in range(2, depth - 1):
        forward_line(k)
    count_ref[...] = jnp.zeros_like(count_ref)
    margin_ref[...] = jnp.zeros_like(margin_ref)
    bit_copy.wait()
    signs(0, 4)
    forward_plane(others[0])
    signs(4, 8)
    for o in others[1:-1]:
        forward_plane(o)
    for o in others:
        head_line(o, o).wait_recv()
    plane_out[...] = jnp.sum(line_in[...], axis=0)

    def head_plane(d):
        to = me + steps[d]
        return send(
            plane_out.at[lax.rem(to // 2, 4)], plane_in.at[d], head_plane_send.at[d], head_plane_recv.at[d], to
        )

    for d in range(3):
        head_plane(d).start()
    signs(8, 12)
    for o in others[-1:]:
        forward_plane(o)
    signs(12, 16)
    for at_layer in [layer] + others:
        for r in range(4):
            to_partner(r, at_layer).wait()
        for d in range(3):
            in_plane(d, at_layer).wait_send()
    for o in others:
        along_line(o, layer).wait_send()
        head_line(o, o).wait_send()
    for d in range(3):
        head_plane(d).wait()
    head_ref[...] = plane_out[quad] + plane_in[0] + plane_in[1] + plane_in[2]


def take_windows(code_ref, length, start):
    whole, part = start >> 3, start & 7
    bits = max(1, (length // 8 - 1).bit_length())
    keep = 8 * ((1 << (bits - 1)) + 4)
    value = None
    for bit in reversed(range(bits)):
        step = 8 << bit
        keep = 8 * ((1 << bit) + 4)
        chosen = ((whole >> bit) & 1) == 1
        if value is None:
            low, high = code_ref[0:keep, :], code_ref[step : step + keep, :]
        else:
            low, high = value[0:keep], value[step : step + keep]
        value = jnp.where(chosen, high, low)
    for bit in (2, 1, 0):
        chosen = ((part >> bit) & 1) == 1
        value = jnp.where(chosen, pltpu.roll(value, value.shape[0] - (1 << bit), 0), value)
    return value[0:32]


def all_rows(value, combine):
    for shift in (4, 2, 1):
        value = combine(value, pltpu.roll(value, shift, 0))
    return value


def bytes_of_rows(tag):
    return tag[0:8] | (tag[8:16] << 8) | (tag[16:24] << 16) | (tag[24:32] << 24)


def plane_word(packed, k):
    sub = lax.broadcasted_iota(jnp.int32, (8, LANES), 0)
    spread = lax.shift_left(lax.shift_right_logical(packed, k) & 0x01010101, sub)
    return all_rows(spread, lambda x, y: x | y)


def head_counts(window, ok, near, rows):
    center = window[16:17]
    linked = ((window ^ center) >> ITEM_BITS == 0) & near & ok
    item = window & ((1 << ITEM_BITS) - 1)
    tag = jnp.where(linked & (item < rows), item | rows, 0)
    packed = bytes_of_rows(tag)
    one = jnp.where(linked, 1, 0)
    weight = all_rows(one[0:8] + one[8:16] + one[16:24] + one[24:32], lambda x, y: x + y)
    sub = lax.broadcasted_iota(jnp.int32, (8, LANES), 0)

    def plane(k):
        return plane_word(packed, k)

    bits = rows.bit_length() - 1
    node = plane(bits)
    for k in range(3):
        node = node & (plane(k) ^ (((sub >> k) & 1) - 1))
    nodes = [node]
    for k in reversed(range(3, bits)):
        word = plane(k)
        nodes = [part for node in nodes for part in (node & ~word, node & word)]
    counts = jnp.concatenate([lax.population_count(node).astype(jnp.float32) for node in nodes], axis=0)
    return counts.astype(jnp.bfloat16), weight[0:1].astype(jnp.float32), center & ((1 << ITEM_BITS) - 1)


def tile_kernel(rows, length, parts, base_ref, all_ref, unused_counts, unused_margins, count_ref, margin_ref, flat_ref, code_ref, mask_ref):
    item_mask = (1 << ITEM_BITS) - 1
    base = base_ref[0]
    bands, unused_rows, width = count_ref.shape
    band = parts * width
    slabs, blocks = all_ref.shape[0], all_ref.shape[1] * 2 // 3
    for n in range(slabs):
        paired = all_ref[n, blocks:]
        sessions = jnp.concatenate([paired & 0xFFFF, paired >> 16], axis=0)
        flat_ref[n * blocks : (n + 1) * blocks] = all_ref[n, 0:blocks] | (sessions << ITEM_BITS)
    per = length // LANES
    for r in range(per):
        code_ref[16 + r * LANES : 16 + (r + 1) * LANES] = flat_ref[pl.ds(r, LANES, stride=per), :].T
    lane = lax.broadcasted_iota(jnp.int32, (16, LANES), 1)
    code_ref[0:16] = jnp.where(lane == 0, -1, pltpu.roll(code_ref[length : length + 16], 1, 1))
    code_ref[length + 16 : length + 32] = jnp.where(
        lane == LANES - 1, -1, pltpu.roll(code_ref[16:32], LANES - 1, 1)
    )

    words = length // 32
    band_bits = (bands - 1).bit_length()
    for w in range(words):
        item = code_ref[16 + 32 * w : 48 + 32 * w] & item_mask
        local = item - base
        mine = (local >= 0) & (local < bands * band) & (item >= rows)
        packed = bytes_of_rows(jnp.where(mine, (local >> (band.bit_length() - 1)) | bands, 0))
        for k in range(band_bits + 1):
            mask_ref[k, w : w + 1] = plane_word(packed, k)[0:1]
    planes = [mask_ref[k] for k in range(band_bits + 1)]
    for s in range(bands):
        mask = planes[band_bits]
        for k in range(band_bits):
            mask = mask & (planes[k] if s >> k & 1 else ~planes[k])
        mask_ref[s] = mask
    keys = []
    for s in range(bands):
        tally = jnp.sum(lax.population_count(mask_ref[s]), axis=0, keepdims=True)
        keys.append((jnp.max(tally) + 1) // 2 * bands + s)
    for low, high in ((0, 1), (2, 3), (0, 2), (1, 3), (1, 2)):
        keys[low], keys[high] = jnp.minimum(keys[low], keys[high]), jnp.maximum(keys[low], keys[high])
    streams = ((keys[3], keys[0]), (keys[2], keys[1]))

    word_ids = lax.broadcasted_iota(jnp.int32, (words, LANES), 0)
    d_ids = lax.broadcasted_iota(jnp.int32, (32, LANES), 0)
    near = (d_ids >= 1) & (d_ids != 16)
    tile = min(width, 256)
    t_ids = lax.broadcasted_iota(jnp.int32, (tile, 2 * LANES), 0).astype(jnp.float32).astype(jnp.bfloat16)
    p_ids = lax.broadcasted_iota(jnp.int32, (16, 2 * LANES), 0)

    def ends(mask):
        some = mask != 0
        first_row = jnp.min(jnp.where(some, word_ids, words), axis=0, keepdims=True)
        last_row = jnp.max(jnp.where(some, word_ids, -1), axis=0, keepdims=True)
        at_first, at_last = word_ids == first_row, word_ids == last_row
        first_word = jnp.sum(jnp.where(at_first, mask, 0), axis=0, keepdims=True)
        last_word = jnp.sum(jnp.where(at_last, mask, 0), axis=0, keepdims=True)
        first_bit = first_word & -first_word
        last_place = 31 - lax.clz(last_word)
        last_bit = jnp.where(last_word == 0, 0, jnp.left_shift(1, last_place & 31))
        first = 32 * first_row + lax.population_count(first_bit - 1)
        last = 32 * last_row + last_place
        first_ok = first_word != 0
        last_ok = first_ok & (last > first)
        mask = mask & ~(jnp.where(at_first, first_bit, 0) | jnp.where(at_last, last_bit, 0))
        return mask, ((first, first_ok), (last, last_ok))

    def find(s, mask):
        mask, found = ends(mask)
        links, weights, locals_ = [], [], []
        for at, ok in found:
            window = take_windows(code_ref, length, jnp.where(ok, at, 0))
            counts, weight, item = head_counts(window, ok, near, rows)
            links.append(counts)
            weights.append(weight)
            locals_.append(item - base - s * band)
        return mask, *(jnp.concatenate(x, axis=1) for x in (links, weights, locals_))

    def count(s, links, weight, local):
        part = local >> (width.bit_length() - 1)
        inner = local & (width - 1)
        pieces = []
        for p in range(parts):
            chosen = jnp.broadcast_to(jnp.where(part == p, 1.0, 0.0), (16, 2 * LANES)).astype(jnp.bfloat16)
            pieces += [links[n : n + 16] * chosen for n in range(0, rows, 16)]
        pieces.append(jnp.where(p_ids == part, weight, 0.0).astype(jnp.bfloat16))
        left = jnp.concatenate(pieces, axis=0)
        for t in range(width // tile):
            inside = (inner >= t * tile) & (inner < (t + 1) * tile)
            hot = hot_columns(t_ids, jnp.where(inside, inner - t * tile, -1).astype(jnp.float32))
            cols = slice(t * tile, (t + 1) * tile)
            value = lax.dot_general(left, hot, NT, preferred_element_type=jnp.float32)
            count_ref[s, :, cols] += value[0 : parts * rows]
            margin_ref[s, :, cols] += value[parts * rows :]

    def body(trip, masks):
        out = []
        for (early, late), mask in zip(streams, masks):
            switch = early // bands
            s = jnp.where(trip < switch, lax.rem(early, bands), lax.rem(late, bands))
            mask = jnp.where(trip == switch, mask_ref[lax.rem(late, bands)], mask)
            mask, *found = find(s, mask)
            out.append(mask)
            count(s, *found)
        return tuple(out)

    trips = [early // bands + late // bands for early, late in streams]
    starts = tuple(mask_ref[lax.rem(early, bands)] for early, late in streams)
    lax.fori_loop(0, jnp.maximum(*trips), body, starts)


def sign_table(words, width):
    size = words.shape[1]

    def wide(value):
        return jnp.concatenate([value] * (size // LANES), axis=1)

    shift = lax.broadcasted_iota(jnp.int32, (8, LANES), 0)
    parts = []
    for g in range(width // 8):
        word = 8 * g // BITS_PER_WORD
        split, offset = (word + 1) * BITS_PER_WORD - 8 * g, 8 * g - word * BITS_PER_WORD
        now = jnp.broadcast_to(words[word : word + 1], (8, size))
        where_bit = jnp.left_shift(1, shift + offset)
        if split < 8:
            later = jnp.broadcast_to(words[word + 1 : word + 2], (8, size))
            now = jnp.where(wide(shift) >= split, later, now)
            place = jnp.where(shift >= split, shift - split, shift + offset)
            where_bit = jnp.left_shift(1, place)
        parts.append(jnp.where((now & wide(where_bit)) != 0, 1.0, -1.0))
    return jnp.concatenate(parts, axis=0).astype(jnp.bfloat16)


def boundary_counts(rows, share, me, all_ref, extra_ref):
    slabs, blocks = all_ref.shape[0], all_ref.shape[1] * 2 // 3
    half = blocks // 2
    group = slabs // 4
    sub = lax.broadcasted_iota(jnp.int32, (LANES, LANES), 0)
    lane = lax.broadcasted_iota(jnp.int32, (LANES, LANES), 1)
    ids = lax.broadcasted_iota(jnp.int32, (rows, LANES), 0)
    small = lax.broadcasted_iota(jnp.int32, (group, LANES), 1)
    last_items, last_sessions = all_ref[:, blocks - 1, :], all_ref[:, blocks + half - 1, :] >> 16
    next_items, next_sessions = all_ref[:, 0, :], all_ref[:, blocks, :] & 0xFFFF

    def meet(last, following):
        joined = None
        for g in range(4):
            shift = 32 * g + 16
            pieces = (pltpu.roll(x[g * group : (g + 1) * group], shift, 1) for x in (last, following))
            both = jnp.where(small % 32 < 16, *pieces)
            joined = both if joined is None else jnp.where(small // 32 == g, both, joined)
        return joined

    slab_ids = lax.broadcasted_iota(jnp.int32, (slabs, LANES), 0)
    next_sessions = jnp.where(slab_ids == slabs - 1, -1, pltpu.roll(next_sessions, slabs - 1, 0))
    met_items = meet(last_items, pltpu.roll(next_items, slabs - 1, 0))
    met_sessions = meet(last_sessions, next_sessions)
    crossing = ((sub >> 5) == (lane >> 5)) & (((sub ^ lane) & 16) != 0) & (jnp.abs(sub - lane) <= WINDOW)
    ones = jnp.ones((8, LANES), jnp.float32).astype(jnp.bfloat16)
    extra = jnp.zeros((rows + 8, LANES), jnp.float32)
    total = jnp.zeros((8, LANES), jnp.float32)
    for g in range(group):
        item, session = met_items[g : g + 1], met_sessions[g : g + 1]
        linked = one_where((jnp.broadcast_to(session, (LANES, LANES)).T == session) & crossing)
        hot = one_where(ids == item)
        links = jnp.dot(jnp.concatenate([hot, ones], axis=0), linked, preferred_element_type=jnp.float32)
        extra += lax.dot_general(links.astype(jnp.bfloat16), hot, NT, preferred_element_type=jnp.float32)
        total += links[rows:]
    extra_ref[...] = extra
    return jnp.concatenate(
        [
            extra_ref[pl.ds(me * share, share)],
            extra_ref[rows : rows + 1],
            total[0:1],
            jnp.zeros((6 - share, LANES), jnp.float32),
        ],
        axis=0,
    )


def sketch_kernel(
    slabs, rows, parts, width, scale, count_ref, margin_ref, head_ref, sign_ref, all_ref, bits_ref, out_ref,
    extra_ref, log_ref, head_bits, acc_ref, send_ref, recv_ref, bit_sem, send_sems, recv_sems,
):
    me = lax.axis_index("stream")
    barrier = greet_all(slabs, me)
    bands, unused_rows, part = count_ref.shape
    share = rows // slabs
    tile = min(part, 512)
    head_copy = pltpu.make_async_copy(bits_ref.at[:, 0:rows], head_bits, bit_sem.at[0])
    head_copy.start()

    log_ref[...] = jnp.log(jnp.maximum(margin_ref[...], 1.0))
    head = head_ref[...] + boundary_counts(rows, share, me, all_ref, extra_ref)
    row_log = jnp.log(jnp.maximum(head[share : share + 1], 1.0))
    column_log = jnp.broadcast_to(row_log, (rows, LANES)).T
    total_log = jnp.log(jnp.sum(head[share + 1 : share + 2], axis=1, keepdims=True))
    row_term = total_log - column_log[:, 0:1]
    def product(positive, signs):
        upper = positive.astype(jnp.bfloat16)
        lower = (positive - upper.astype(jnp.float32)).astype(jnp.bfloat16)
        both = jnp.concatenate([upper, lower], axis=0)
        value = lax.dot_general(both, signs, NT, preferred_element_type=jnp.float32)
        return value[0:rows] + value[rows:]

    head_copy.wait()
    row = lax.broadcasted_iota(jnp.int32, (8, LANES), 0)
    shared = jnp.concatenate(
        [jnp.where(row < share, head, 0.0), jnp.zeros((rows - 8, LANES), jnp.float32)], axis=0
    )
    shared = pltpu.roll(shared, me * share, 0)
    ratio = jnp.log(jnp.maximum(shared, 1.0)) + total_log - row_log - column_log
    first_band = jnp.where(lax.axis_index("item") == 0, 1.0, 0.0)
    positive = jnp.where(shared > 0, jnp.maximum(ratio, 0.0), 0.0) * first_band
    acc_ref[...] = product(positive.T, sign_table(head_bits[...], width))

    for s in range(bands):
        for h in range(parts):
            for at in range(0, part, tile):
                counts = count_ref[s, h * rows : (h + 1) * rows, at : at + tile]
                ratio = jnp.log(jnp.maximum(counts, NONE)) + row_term - log_ref[s, h : h + 1, at : at + tile]
                positive = jnp.maximum(ratio, 0.0)
                bit_at = (s * parts + h) * part + at
                acc_ref[...] += product(positive, sign_ref[:, bit_at : bit_at + tile])

    cuts = width // LANES
    for d in range(slabs):
        for c in range(cuts):
            send_ref[d, c * share : (c + 1) * share] = (
                acc_ref[d * share : (d + 1) * share, c * LANES : (c + 1) * LANES] * scale
            )
    pl.semaphore_wait(barrier, slabs - 1)
    exchange(slabs, me, send_ref, recv_ref, send_sems, recv_sems)
    summed = jnp.sum(recv_ref[...], axis=0)
    out_ref[...] = jnp.concatenate([summed[c * share : (c + 1) * share] for c in range(cuts)], axis=1)


def local(event_items, event_sessions, sketch_bits):
    slabs = lax.axis_size("stream")
    slab = event_items.shape[0]
    total_events = slab * slabs
    words, band_size = sketch_bits.shape
    owned = band_size // slabs
    rows, width = 128, 256
    part = max(LANES, owned // 16)
    bands = BANDS
    parts = owned // (bands * part)
    me = lax.axis_index("stream")
    own_start = me * owned
    first_id = lax.axis_index("item") * band_size + own_start
    blocks = slab // LANES
    length = total_events // LANES

    dma = pltpu.SemaphoreType.DMA
    depth = slabs // PLANE
    count_shapes = (
        jax.ShapeDtypeStruct((bands, parts * rows, part), jnp.float32),
        jax.ShapeDtypeStruct((bands, 16, part), jnp.float32),
    )
    events, head, signs, no_counts, no_margins = pl.pallas_call(
        functools.partial(gather_kernel, slabs, rows, blocks),
        out_shape=(
            jax.ShapeDtypeStruct((slabs, blocks * 3 // 2, LANES), jnp.int32),
            jax.ShapeDtypeStruct((8, LANES), jnp.float32),
            jax.ShapeDtypeStruct((width, owned), jnp.bfloat16),
            *count_shapes,
        ),
        in_specs=[pl.BlockSpec(memory_space=pltpu.HBM)] * 3,
        out_specs=(VMEM,) * 5,
        scratch_shapes=[
            pltpu.VMEM((blocks * 3 // 2, LANES), jnp.int32),
            pltpu.VMEM((words, owned), jnp.int32),
            pltpu.VMEM((blocks, LANES), jnp.int32),
            pltpu.VMEM((blocks, LANES), jnp.int32),
            pltpu.VMEM((blocks + 16, LANES), jnp.int32),
            pltpu.VMEM((blocks + 16, LANES), jnp.int32),
            pltpu.VMEM((rows + 8, LANES), jnp.float32),
            pltpu.VMEM((8, LANES), jnp.float32),
            pltpu.VMEM((2, depth, 4, 8, LANES), jnp.float32),
            pltpu.VMEM((depth, 4, 8, LANES), jnp.float32),
            pltpu.VMEM((4, 8, LANES), jnp.float32),
            pltpu.VMEM((3, 8, LANES), jnp.float32),
            pltpu.VMEM((depth, 4, 8, LANES), jnp.float32),
            pltpu.VMEM((depth, 4, 8, LANES), jnp.float32),
            dma((3,)),
            dma((depth,)),
            dma((depth,)),
            dma((3 * depth,)),
            dma((3 * depth,)),
            dma((4 * depth,)),
            dma((4 * depth,)),
            dma((2,)),
            dma((3,)),
            dma((3,)),
            dma((depth,)),
            dma((depth,)),
        ],
        compiler_params=pltpu.CompilerParams(
            collective_id=0, has_side_effects=True, vmem_limit_bytes=VMEM_GRANT
        ),
        name="gather_events",
    )(*(pltpu.with_memory_space_constraint(x.reshape(blocks, LANES), pltpu.HBM) for x in (event_items, event_sessions)), sketch_bits)

    counts, margins = pl.pallas_call(
        functools.partial(tile_kernel, rows, length, parts),
        out_shape=count_shapes,
        in_specs=[pl.BlockSpec(memory_space=pltpu.SMEM), VMEM, VMEM, VMEM],
        input_output_aliases={2: 0, 3: 1},
        out_specs=(VMEM, VMEM),
        scratch_shapes=[
            pltpu.VMEM((length, LANES), jnp.int32),
            pltpu.VMEM((length + 32, LANES), jnp.int32),
            pltpu.VMEM((bands, length // 32, LANES), jnp.int32),
        ],
        compiler_params=pltpu.CompilerParams(vmem_limit_bytes=VMEM_GRANT),
        name="tile_counts",
    )(first_id.astype(jnp.int32)[None], events, no_counts, no_margins)

    own_rows = pl.pallas_call(
        functools.partial(sketch_kernel, slabs, rows, parts, width, 1.0 / math.sqrt(total_events)),
        out_shape=jax.ShapeDtypeStruct((rows // slabs, width), jnp.float32),
        in_specs=[VMEM] * 5 + [pl.BlockSpec(memory_space=pl.ANY)],
        out_specs=VMEM,
        scratch_shapes=[
            pltpu.VMEM((rows + 8, LANES), jnp.float32),
            pltpu.VMEM((bands, 16, part), jnp.float32),
            pltpu.VMEM((words, rows), jnp.int32),
            pltpu.VMEM((rows, width), jnp.float32),
            pltpu.VMEM((slabs, 8, LANES), jnp.float32),
            pltpu.VMEM((slabs, 8, LANES), jnp.float32),
            dma((1,)),
            dma((slabs,)),
            dma((slabs,)),
        ],
        compiler_params=pltpu.CompilerParams(
            collective_id=1, has_side_effects=True, vmem_limit_bytes=VMEM_GRANT
        ),
        name="sketch_tile",
    )(counts, margins, head, signs, events, sketch_bits)
    if lax.axis_size("item") > 1:
        own_rows = lax.psum(own_rows, "item")
    return own_rows


def solution(mesh):
    placed = (P("stream"), P("stream"), P(None, "item"))
    return jax.shard_map(
        local, mesh=mesh, in_specs=placed, out_specs=P("stream", None), check_vma=False
    )
```

```python
import functools
import math

import jax
import jax.numpy as jnp
from jax import lax
from jax.experimental import pallas as pl
from jax.experimental.pallas import tpu as pltpu
from jax.sharding import PartitionSpec as P

WINDOW = 15
ITEM_BITS = 18
LANES = 128
BITS_PER_WORD = 18
PLANE = 8
BANDS = 4
NONE = 1.0e-30
VMEM_GRANT = 45 * 1024 * 1024
NT = (((1,), (1,)), ((), ()))
VMEM = pl.BlockSpec(memory_space=pltpu.VMEM)


def one_where(mask):
    return jnp.where(mask, 1.0, 0.0).astype(jnp.bfloat16)


def hot_columns(ids, values):
    row = jnp.broadcast_to(values, (16, values.shape[1])).astype(jnp.bfloat16)
    one, zero = jnp.ones((), jnp.bfloat16), jnp.zeros((), jnp.bfloat16)
    return jnp.concatenate(
        [jnp.where(ids[n : n + 16] == row, one, zero) for n in range(0, ids.shape[0], 16)], axis=0
    )


def greet_all(slabs, me):
    barrier = pltpu.get_barrier_semaphore()

    for to in far_first(slabs, me):
        pl.semaphore_signal(barrier, inc=1, device_id={"stream": to}, device_id_type=pl.DeviceIdType.MESH)
    return barrier


def send(src, dst, send_sem, recv_sem, to):
    return pltpu.make_async_remote_copy(
        src_ref=src,
        dst_ref=dst,
        send_sem=send_sem,
        recv_sem=recv_sem,
        device_id={"stream": to},
        device_id_type=pl.DeviceIdType.MESH,
    )


def flip(me, bit):
    return bit - 2 * bit * lax.rem(me // bit, 2)


def other_layer(k, layer, depth):
    rising = k + (k - layer + depth) // depth
    mirrored = depth - 1 - layer
    falling = depth - 1 - k - (k - mirrored + depth) // depth
    high = layer // ((depth + 1) // 2)
    return rising + (falling - rising) * lax.rem(high, 2)


def far_first(slabs, me):
    depth = slabs // PLANE
    layer = me // PLANE
    turns = [sum(flip(me, bit) for bit in (1, 2, 4) if turn & bit) for turn in (6, 7, 4, 5, 2, 3, 0, 1)]
    shifts = [(other_layer(k, layer, depth) - layer) * PLANE for k in reversed(range(depth - 1))]
    away = [shift + turn for shift in shifts for turn in turns]
    return [me + step for step in away + turns[0:6] + turns[7:]]


def exchange(slabs, me, out_ref, in_ref, send_sems, recv_sems):
    targets = far_first(slabs, me)
    for k, to in enumerate(targets):
        send(out_ref.at[to], in_ref.at[me], send_sems.at[k], recv_sems.at[me], to).start()
    in_ref[me] = out_ref[me]
    for k, to in enumerate(targets):
        send(out_ref.at[to], in_ref.at[to], send_sems.at[k], recv_sems.at[to], to).wait()


def gather_kernel(
    slabs, rows, blocks, items_ref, sessions_ref, bits_ref, all_ref, head_ref, sign_ref, count_ref, margin_ref,
    own_pack, own_bits, own_items, own_sessions, item_ref, session_ref, links_ref, total_ref,
    pair_out, pair_in, plane_out, plane_in, line_out, line_in,
    bit_sem, line_send, line_recv, plane_send, plane_recv, near_send, near_recv,
    pair_sems, head_plane_send, head_plane_recv, head_line_send, head_line_recv,
):
    me = lax.axis_index("stream")
    depth = slabs // PLANE
    layer, low = me // PLANE, lax.rem(me, PLANE)
    parity, quad = lax.rem(me, 2), lax.rem(me // 2, 4)

    partner = me + flip(me, 1)
    steps = (flip(me, 2), flip(me, 4), flip(me, 2) + flip(me, 4))
    others = [other_layer(k, layer, depth) for k in range(depth - 1)]
    loads = [
        pltpu.make_async_copy(items_ref, own_items, bit_sem.at[1]),
        pltpu.make_async_copy(sessions_ref, own_sessions, bit_sem.at[2]),
    ]
    for copy in loads:
        copy.start()
    barrier = pltpu.get_barrier_semaphore()
    owned = own_bits.shape[1]
    bit_copy = pltpu.make_async_copy(
        bits_ref.at[:, pl.ds(pl.multiple_of(me * owned, owned), owned)], own_bits, bit_sem.at[0]
    )
    greeted = [o * PLANE + low for o in reversed(others)] + [me + step for step in reversed(steps)] + [partner]
    for to in greeted:
        pl.semaphore_signal(
            barrier, inc=1, device_id={"stream": to}, device_id_type=pl.DeviceIdType.MESH
        )
    for copy in loads:
        copy.wait()
    bit_copy.start()
    half = blocks // 2
    own_pack[0:blocks] = own_items[...]
    own_pack[blocks : blocks + half] = own_sessions[0:half] | (own_sessions[half:blocks] << 16)
    all_ref[me] = own_pack[...]
    item_ref[8 : 8 + blocks] = own_items[...]
    session_ref[8 : 8 + blocks] = own_sessions[...]
    for edge in (slice(0, 8), slice(8 + blocks, 16 + blocks)):
        item_ref[edge] = jnp.zeros((8, LANES), jnp.int32)
        session_ref[edge] = jnp.full((8, LANES), -1, jnp.int32)
    sub = lax.broadcasted_iota(jnp.int32, (LANES, LANES), 0)
    lane = lax.broadcasted_iota(jnp.int32, (LANES, LANES), 1)
    low_lane = lax.broadcasted_iota(jnp.int32, (1, LANES), 1) < LANES // 2
    ids = lax.broadcasted_iota(jnp.int32, (rows, LANES), 0)
    gaps = (sub - LANES // 2 - lane, sub + LANES // 2 - lane)
    in_reach = [(jnp.abs(gap) <= WINDOW) & (gap != 0) for gap in gaps]
    ones = jnp.ones((8, 2 * LANES), jnp.float32).astype(jnp.bfloat16)
    links_ref[...] = jnp.zeros_like(links_ref)
    total_ref[...] = jnp.zeros_like(total_ref)

    together = 8

    def some_blocks(n, unused):
        first = n * together

        def shifted(ref):
            turned = [pltpu.roll(ref[pl.ds(first + 7 + o, 1)], LANES // 2, 1) for o in range(together + 2)]
            return [jnp.where(low_lane, turned[o], turned[o + 1]) for o in range(together + 1)]

        hots = [one_where(ids == item) for item in shifted(item_ref)]
        sessions = [jnp.broadcast_to(session, (LANES, LANES)).T for session in shifted(session_ref)]
        for o in range(together):
            own_item, own_session = item_ref[pl.ds(first + o + 8, 1)], session_ref[pl.ds(first + o + 8, 1)]
            hot = jnp.concatenate([hots[o], hots[o + 1]], axis=1)
            linked = jnp.concatenate(
                [one_where((sessions[o + side] == own_session) & in_reach[side]) for side in range(2)], axis=0
            )
            links = jnp.dot(jnp.concatenate([hot, ones], axis=0), linked, preferred_element_type=jnp.float32)
            links_ref[...] += lax.dot_general(
                links.astype(jnp.bfloat16), one_where(ids == own_item), NT, preferred_element_type=jnp.float32
            )
            total_ref[...] += links[rows:]
        return unused

    inner = [blocks * n // 32 for n in (0, 0, 32)]

    def blocks_of(n):
        lax.fori_loop(inner[n] // together, inner[n + 1] // together, some_blocks, 0)

    step_columns = max(LANES, owned // 16)
    steps_in_all = owned // step_columns

    def signs(low_step, high_step):
        def step(t, unused):
            at = pl.multiple_of(t * step_columns, step_columns)
            sign_ref[:, pl.ds(at, step_columns)] = sign_table(own_bits[:, pl.ds(at, step_columns)], sign_ref.shape[0])
            return unused

        lax.fori_loop(low_step * steps_in_all // 16, high_step * steps_in_all // 16, step, 0)

    blocks_of(0)
    pl.semaphore_wait(barrier, len(greeted))

    def along_line(there, here):
        return send(
            own_pack, all_ref.at[me], line_send.at[there], line_recv.at[here], there * PLANE + low
        )

    def in_plane(d, at_layer, own=False):
        slab = all_ref.at[at_layer * PLANE + low]
        sem = d * depth + at_layer
        return send(own_pack if own else slab, slab, plane_send.at[sem], plane_recv.at[sem], me + steps[d])

    def to_partner(r, at_layer, own=False):
        slab = all_ref.at[at_layer * PLANE + low + ((0,) + steps)[r]]
        sem = r * depth + at_layer
        return send(own_pack if own else slab, slab, near_send.at[sem], near_recv.at[sem], partner)

    for o in reversed(others):
        along_line(o, layer).start()
    for d in range(3):
        in_plane(d, layer, True).start()
    to_partner(0, layer, True).start()

    def forward_line(k):
        along_line(layer, others[k]).wait_recv()
        for d in range(3):
            in_plane(d, others[k]).start()
        to_partner(0, others[k]).start()

    def forward_plane(at_layer):
        for d in range(3):
            in_plane(d, at_layer).wait_recv()
            to_partner(d + 1, at_layer).start()

    blocks_of(1)
    share = rows // slabs
    tail = jnp.concatenate(
        [links_ref[rows : rows + 1], total_ref[0:1], jnp.zeros((6 - share, LANES), jnp.float32)], axis=0
    )
    for d in range(slabs):
        at = (d % 2, d // PLANE, d // 2 % 4)
        pair_out[at + (slice(0, share),)] = links_ref[d * share : (d + 1) * share]
        pair_out[at + (slice(share, 8),)] = tail

    pair = send(pair_out.at[1 - parity], pair_in, pair_sems.at[0], pair_sems.at[1], partner)
    pair.start()
    forward_line(0)
    forward_line(1)
    pair.wait()
    line_out[...] = pair_out[parity] + pair_in[...]

    def head_line(there, here):
        return send(
            line_out.at[there], line_in.at[layer], head_line_send.at[there], head_line_recv.at[here],
            there * PLANE + low,
        )

    for o in others:
        head_line(o, layer).start()
    line_in[layer] = line_out[layer]
    forward_plane(layer)
    for k in range(2, depth - 1):
        forward_line(k)
    count_ref[...] = jnp.zeros_like(count_ref)
    margin_ref[...] = jnp.zeros_like(margin_ref)
    bit_copy.wait()
    signs(0, 4)
    forward_plane(others[0])
    signs(4, 8)
    for o in others[1:-1]:
        forward_plane(o)
    for o in others:
        head_line(o, o).wait_recv()
    plane_out[...] = jnp.sum(line_in[...], axis=0)

    def head_plane(d):
        to = me + steps[d]
        return send(
            plane_out.at[lax.rem(to // 2, 4)], plane_in.at[d], head_plane_send.at[d], head_plane_recv.at[d], to
        )

    for d in range(3):
        head_plane(d).start()
    signs(8, 12)
    for o in others[-1:]:
        forward_plane(o)
    signs(12, 16)
    for at_layer in [layer] + others:
        for r in range(4):
            to_partner(r, at_layer).wait()
        for d in range(3):
            in_plane(d, at_layer).wait_send()
    for o in others:
        along_line(o, layer).wait_send()
        head_line(o, o).wait_send()
    for d in range(3):
        head_plane(d).wait()
    head_ref[...] = plane_out[quad] + plane_in[0] + plane_in[1] + plane_in[2]


def take_windows(code_ref, length, start):
    whole, part = start >> 3, start & 7
    bits = max(1, (length // 8 - 1).bit_length())
    keep = 8 * ((1 << (bits - 1)) + 4)
    value = None
    for bit in reversed(range(bits)):
        step = 8 << bit
        keep = 8 * ((1 << bit) + 4)
        chosen = ((whole >> bit) & 1) == 1
        if value is None:
            low, high = code_ref[0:keep, :], code_ref[step : step + keep, :]
        else:
            low, high = value[0:keep], value[step : step + keep]
        value = jnp.where(chosen, high, low)
    for bit in (2, 1, 0):
        chosen = ((part >> bit) & 1) == 1
        value = jnp.where(chosen, pltpu.roll(value, value.shape[0] - (1 << bit), 0), value)
    return value[0:32]


def all_rows(value, combine):
    for shift in (4, 2, 1):
        value = combine(value, pltpu.roll(value, shift, 0))
    return value


def bytes_of_rows(tag):
    return tag[0:8] | (tag[8:16] << 8) | (tag[16:24] << 16) | (tag[24:32] << 24)


def plane_word(packed, k):
    sub = lax.broadcasted_iota(jnp.int32, (8, LANES), 0)
    spread = lax.shift_left(lax.shift_right_logical(packed, k) & 0x01010101, sub)
    return all_rows(spread, lambda x, y: x | y)


def head_counts(window, ok, near, rows):
    center = window[16:17]
    linked = ((window ^ center) >> ITEM_BITS == 0) & near & ok
    item = window & ((1 << ITEM_BITS) - 1)
    tag = jnp.where(linked & (item < rows), item | rows, 0)
    packed = bytes_of_rows(tag)
    one = jnp.where(linked, 1, 0)
    weight = all_rows(one[0:8] + one[8:16] + one[16:24] + one[24:32], lambda x, y: x + y)
    sub = lax.broadcasted_iota(jnp.int32, (8, LANES), 0)

    def plane(k):
        return plane_word(packed, k)

    bits = rows.bit_length() - 1
    node = plane(bits)
    for k in range(3):
        node = node & (plane(k) ^ (((sub >> k) & 1) - 1))
    nodes = [node]
    for k in reversed(range(3, bits)):
        word = plane(k)
        nodes = [part for node in nodes for part in (node & ~word, node & word)]
    counts = jnp.concatenate([lax.population_count(node).astype(jnp.float32) for node in nodes], axis=0)
    return counts.astype(jnp.bfloat16), weight[0:1].astype(jnp.float32), center & ((1 << ITEM_BITS) - 1)


def tile_kernel(rows, length, parts, base_ref, all_ref, unused_counts, unused_margins, count_ref, margin_ref, flat_ref, code_ref, mask_ref):
    item_mask = (1 << ITEM_BITS) - 1
    base = base_ref[0]
    bands, unused_rows, width = count_ref.shape
    band = parts * width
    slabs, blocks = all_ref.shape[0], all_ref.shape[1] * 2 // 3
    for n in range(slabs):
        paired = all_ref[n, blocks:]
        sessions = jnp.concatenate([paired & 0xFFFF, paired >> 16], axis=0)
        flat_ref[n * blocks : (n + 1) * blocks] = all_ref[n, 0:blocks] | (sessions << ITEM_BITS)
    per = length // LANES
    for r in range(per):
        code_ref[16 + r * LANES : 16 + (r + 1) * LANES] = flat_ref[pl.ds(r, LANES, stride=per), :].T
    lane = lax.broadcasted_iota(jnp.int32, (16, LANES), 1)
    code_ref[0:16] = jnp.where(lane == 0, -1, pltpu.roll(code_ref[length : length + 16], 1, 1))
    code_ref[length + 16 : length + 32] = jnp.where(
        lane == LANES - 1, -1, pltpu.roll(code_ref[16:32], LANES - 1, 1)
    )

    words = length // 32
    band_bits = (bands - 1).bit_length()
    for w in range(words):
        item = code_ref[16 + 32 * w : 48 + 32 * w] & item_mask
        local = item - base
        mine = (local >= 0) & (local < bands * band) & (item >= rows)
        packed = bytes_of_rows(jnp.where(mine, (local >> (band.bit_length() - 1)) | bands, 0))
        for k in range(band_bits + 1):
            mask_ref[k, w : w + 1] = plane_word(packed, k)[0:1]
    planes = [mask_ref[k] for k in range(band_bits + 1)]
    for s in range(bands):
        mask = planes[band_bits]
        for k in range(band_bits):
            mask = mask & (planes[k] if s >> k & 1 else ~planes[k])
        mask_ref[s] = mask
    keys = []
    for s in range(bands):
        tally = jnp.sum(lax.population_count(mask_ref[s]), axis=0, keepdims=True)
        keys.append((jnp.max(tally) + 1) // 2 * bands + s)
    for low, high in ((0, 1), (2, 3), (0, 2), (1, 3), (1, 2)):
        keys[low], keys[high] = jnp.minimum(keys[low], keys[high]), jnp.maximum(keys[low], keys[high])
    streams = ((keys[3], keys[0]), (keys[2], keys[1]))

    word_ids = lax.broadcasted_iota(jnp.int32, (words, LANES), 0)
    d_ids = lax.broadcasted_iota(jnp.int32, (32, LANES), 0)
    near = (d_ids >= 1) & (d_ids != 16)
    tile = min(width, 256)
    t_ids = lax.broadcasted_iota(jnp.int32, (tile, 2 * LANES), 0).astype(jnp.float32).astype(jnp.bfloat16)
    p_ids = lax.broadcasted_iota(jnp.int32, (16, 2 * LANES), 0)

    def ends(mask):
        some = mask != 0
        first_row = jnp.min(jnp.where(some, word_ids, words), axis=0, keepdims=True)
        last_row = jnp.max(jnp.where(some, word_ids, -1), axis=0, keepdims=True)
        at_first, at_last = word_ids == first_row, word_ids == last_row
        first_word = jnp.sum(jnp.where(at_first, mask, 0), axis=0, keepdims=True)
        last_word = jnp.sum(jnp.where(at_last, mask, 0), axis=0, keepdims=True)
        first_bit = first_word & -first_word
        last_place = 31 - lax.clz(last_word)
        last_bit = jnp.where(last_word == 0, 0, jnp.left_shift(1, last_place & 31))
        first = 32 * first_row + lax.population_count(first_bit - 1)
        last = 32 * last_row + last_place
        first_ok = first_word != 0
        last_ok = first_ok & (last > first)
        mask = mask & ~(jnp.where(at_first, first_bit, 0) | jnp.where(at_last, last_bit, 0))
        return mask, ((first, first_ok), (last, last_ok))

    def find(s, mask):
        mask, found = ends(mask)
        links, weights, locals_ = [], [], []
        for at, ok in found:
            window = take_windows(code_ref, length, jnp.where(ok, at, 0))
            counts, weight, item = head_counts(window, ok, near, rows)
            links.append(counts)
            weights.append(weight)
            locals_.append(item - base - s * band)
        return mask, *(jnp.concatenate(x, axis=1) for x in (links, weights, locals_))

    def count(s, links, weight, local):
        part = local >> (width.bit_length() - 1)
        inner = local & (width - 1)
        pieces = []
        for p in range(parts):
            chosen = jnp.broadcast_to(jnp.where(part == p, 1.0, 0.0), (16, 2 * LANES)).astype(jnp.bfloat16)
            pieces += [links[n : n + 16] * chosen for n in range(0, rows, 16)]
        pieces.append(jnp.where(p_ids == part, weight, 0.0).astype(jnp.bfloat16))
        left = jnp.concatenate(pieces, axis=0)
        for t in range(width // tile):
            inside = (inner >= t * tile) & (inner < (t + 1) * tile)
            hot = hot_columns(t_ids, jnp.where(inside, inner - t * tile, -1).astype(jnp.float32))
            cols = slice(t * tile, (t + 1) * tile)
            value = lax.dot_general(left, hot, NT, preferred_element_type=jnp.float32)
            count_ref[s, :, cols] += value[0 : parts * rows]
            margin_ref[s, :, cols] += value[parts * rows :]

    def body(trip, masks):
        out = []
        for (early, late), mask in zip(streams, masks):
            switch = early // bands
            s = jnp.where(trip < switch, lax.rem(early, bands), lax.rem(late, bands))
            mask = jnp.where(trip == switch, mask_ref[lax.rem(late, bands)], mask)
            mask, *found = find(s, mask)
            out.append(mask)
            count(s, *found)
        return tuple(out)

    trips = [early // bands + late // bands for early, late in streams]
    starts = tuple(mask_ref[lax.rem(early, bands)] for early, late in streams)
    lax.fori_loop(0, jnp.maximum(*trips), body, starts)


def sign_table(words, width):
    size = words.shape[1]

    def wide(value):
        return jnp.concatenate([value] * (size // LANES), axis=1)

    shift = lax.broadcasted_iota(jnp.int32, (8, LANES), 0)
    parts = []
    for g in range(width // 8):
        word = 8 * g // BITS_PER_WORD
        split, offset = (word + 1) * BITS_PER_WORD - 8 * g, 8 * g - word * BITS_PER_WORD
        now = jnp.broadcast_to(words[word : word + 1], (8, size))
        where_bit = jnp.left_shift(1, shift + offset)
        if split < 8:
            later = jnp.broadcast_to(words[word + 1 : word + 2], (8, size))
            now = jnp.where(wide(shift) >= split, later, now)
            place = jnp.where(shift >= split, shift - split, shift + offset)
            where_bit = jnp.left_shift(1, place)
        parts.append(jnp.where((now & wide(where_bit)) != 0, 1.0, -1.0))
    return jnp.concatenate(parts, axis=0).astype(jnp.bfloat16)


def boundary_counts(rows, share, me, all_ref, extra_ref):
    slabs, blocks = all_ref.shape[0], all_ref.shape[1] * 2 // 3
    half = blocks // 2
    group = slabs // 4
    sub = lax.broadcasted_iota(jnp.int32, (LANES, LANES), 0)
    lane = lax.broadcasted_iota(jnp.int32, (LANES, LANES), 1)
    ids = lax.broadcasted_iota(jnp.int32, (rows, LANES), 0)
    small = lax.broadcasted_iota(jnp.int32, (group, LANES), 1)
    last_items, last_sessions = all_ref[:, blocks - 1, :], all_ref[:, blocks + half - 1, :] >> 16
    next_items, next_sessions = all_ref[:, 0, :], all_ref[:, blocks, :] & 0xFFFF

    def meet(last, following):
        joined = None
        for g in range(4):
            shift = 32 * g + 16
            pieces = (pltpu.roll(x[g * group : (g + 1) * group], shift, 1) for x in (last, following))
            both = jnp.where(small % 32 < 16, *pieces)
            joined = both if joined is None else jnp.where(small // 32 == g, both, joined)
        return joined

    slab_ids = lax.broadcasted_iota(jnp.int32, (slabs, LANES), 0)
    next_sessions = jnp.where(slab_ids == slabs - 1, -1, pltpu.roll(next_sessions, slabs - 1, 0))
    met_items = meet(last_items, pltpu.roll(next_items, slabs - 1, 0))
    met_sessions = meet(last_sessions, next_sessions)
    crossing = ((sub >> 5) == (lane >> 5)) & (((sub ^ lane) & 16) != 0) & (jnp.abs(sub - lane) <= WINDOW)
    ones = jnp.ones((8, LANES), jnp.float32).astype(jnp.bfloat16)
    extra = jnp.zeros((rows + 8, LANES), jnp.float32)
    total = jnp.zeros((8, LANES), jnp.float32)
    for g in range(group):
        item, session = met_items[g : g + 1], met_sessions[g : g + 1]
        linked = one_where((jnp.broadcast_to(session, (LANES, LANES)).T == session) & crossing)
        hot = one_where(ids == item)
        links = jnp.dot(jnp.concatenate([hot, ones], axis=0), linked, preferred_element_type=jnp.float32)
        extra += lax.dot_general(links.astype(jnp.bfloat16), hot, NT, preferred_element_type=jnp.float32)
        total += links[rows:]
    extra_ref[...] = extra
    return jnp.concatenate(
        [
            extra_ref[pl.ds(me * share, share)],
            extra_ref[rows : rows + 1],
            total[0:1],
            jnp.zeros((6 - share, LANES), jnp.float32),
        ],
        axis=0,
    )


def sketch_kernel(
    slabs, rows, parts, width, scale, count_ref, margin_ref, head_ref, sign_ref, all_ref, bits_ref, out_ref,
    extra_ref, log_ref, head_bits, acc_ref, send_ref, recv_ref, bit_sem, send_sems, recv_sems,
):
    me = lax.axis_index("stream")
    barrier = greet_all(slabs, me)
    bands, unused_rows, part = count_ref.shape
    share = rows // slabs
    tile = min(part, 512)
    head_copy = pltpu.make_async_copy(bits_ref.at[:, 0:rows], head_bits, bit_sem.at[0])
    head_copy.start()

    log_ref[...] = jnp.log(jnp.maximum(margin_ref[...], 1.0))
    head = head_ref[...] + boundary_counts(rows, share, me, all_ref, extra_ref)
    row_log = jnp.log(jnp.maximum(head[share : share + 1], 1.0))
    column_log = jnp.broadcast_to(row_log, (rows, LANES)).T
    total_log = jnp.log(jnp.sum(head[share + 1 : share + 2], axis=1, keepdims=True))
    row_term = total_log - column_log[:, 0:1]
    def product(positive, signs):
        upper = positive.astype(jnp.bfloat16)
        lower = (positive - upper.astype(jnp.float32)).astype(jnp.bfloat16)
        both = jnp.concatenate([upper, lower], axis=0)
        value = lax.dot_general(both, signs, NT, preferred_element_type=jnp.float32)
        return value[0:rows] + value[rows:]

    head_copy.wait()
    row = lax.broadcasted_iota(jnp.int32, (8, LANES), 0)
    shared = jnp.concatenate(
        [jnp.where(row < share, head, 0.0), jnp.zeros((rows - 8, LANES), jnp.float32)], axis=0
    )
    shared = pltpu.roll(shared, me * share, 0)
    ratio = jnp.log(jnp.maximum(shared, 1.0)) + total_log - row_log - column_log
    first_band = jnp.where(lax.axis_index("item") == 0, 1.0, 0.0)
    positive = jnp.where(shared > 0, jnp.maximum(ratio, 0.0), 0.0) * first_band
    acc_ref[...] = product(positive.T, sign_table(head_bits[...], width))

    for s in range(bands):
        for h in range(parts):
            for at in range(0, part, tile):
                counts = count_ref[s, h * rows : (h + 1) * rows, at : at + tile]
                ratio = jnp.log(jnp.maximum(counts, NONE)) + row_term - log_ref[s, h : h + 1, at : at + tile]
                positive = jnp.maximum(ratio, 0.0)
                bit_at = (s * parts + h) * part + at
                acc_ref[...] += product(positive, sign_ref[:, bit_at : bit_at + tile])

    cuts = width // LANES
    for d in range(slabs):
        for c in range(cuts):
            send_ref[d, c * share : (c + 1) * share] = (
                acc_ref[d * share : (d + 1) * share, c * LANES : (c + 1) * LANES] * scale
            )
    pl.semaphore_wait(barrier, slabs - 1)
    exchange(slabs, me, send_ref, recv_ref, send_sems, recv_sems)
    summed = jnp.sum(recv_ref[...], axis=0)
    out_ref[...] = jnp.concatenate([summed[c * share : (c + 1) * share] for c in range(cuts)], axis=1)


def local(event_items, event_sessions, sketch_bits):
    slabs = lax.axis_size("stream")
    slab = event_items.shape[0]
    total_events = slab * slabs
    words, band_size = sketch_bits.shape
    owned = band_size // slabs
    rows, width = 128, 256
    part = max(LANES, owned // 16)
    bands = BANDS
    parts = owned // (bands * part)
    me = lax.axis_index("stream")
    own_start = me * owned
    first_id = lax.axis_index("item") * band_size + own_start
    blocks = slab // LANES
    length = total_events // LANES

    dma = pltpu.SemaphoreType.DMA
    depth = slabs // PLANE
    count_shapes = (
        jax.ShapeDtypeStruct((bands, parts * rows, part), jnp.float32),
        jax.ShapeDtypeStruct((bands, 16, part), jnp.float32),
    )
    events, head, signs, no_counts, no_margins = pl.pallas_call(
        functools.partial(gather_kernel, slabs, rows, blocks),
        out_shape=(
            jax.ShapeDtypeStruct((slabs, blocks * 3 // 2, LANES), jnp.int32),
            jax.ShapeDtypeStruct((8, LANES), jnp.float32),
            jax.ShapeDtypeStruct((width, owned), jnp.bfloat16),
            *count_shapes,
        ),
        in_specs=[pl.BlockSpec(memory_space=pltpu.HBM)] * 3,
        out_specs=(VMEM,) * 5,
        scratch_shapes=[
            pltpu.VMEM((blocks * 3 // 2, LANES), jnp.int32),
            pltpu.VMEM((words, owned), jnp.int32),
            pltpu.VMEM((blocks, LANES), jnp.int32),
            pltpu.VMEM((blocks, LANES), jnp.int32),
            pltpu.VMEM((blocks + 16, LANES), jnp.int32),
            pltpu.VMEM((blocks + 16, LANES), jnp.int32),
            pltpu.VMEM((rows + 8, LANES), jnp.float32),
            pltpu.VMEM((8, LANES), jnp.float32),
            pltpu.VMEM((2, depth, 4, 8, LANES), jnp.float32),
            pltpu.VMEM((depth, 4, 8, LANES), jnp.float32),
            pltpu.VMEM((4, 8, LANES), jnp.float32),
            pltpu.VMEM((3, 8, LANES), jnp.float32),
            pltpu.VMEM((depth, 4, 8, LANES), jnp.float32),
            pltpu.VMEM((depth, 4, 8, LANES), jnp.float32),
            dma((3,)),
            dma((depth,)),
            dma((depth,)),
            dma((3 * depth,)),
            dma((3 * depth,)),
            dma((4 * depth,)),
            dma((4 * depth,)),
            dma((2,)),
            dma((3,)),
            dma((3,)),
            dma((depth,)),
            dma((depth,)),
        ],
        compiler_params=pltpu.CompilerParams(
            collective_id=0, has_side_effects=True, vmem_limit_bytes=VMEM_GRANT
        ),
        name="gather_events",
    )(*(pltpu.with_memory_space_constraint(x.reshape(blocks, LANES), pltpu.HBM) for x in (event_items, event_sessions)), sketch_bits)

    counts, margins = pl.pallas_call(
        functools.partial(tile_kernel, rows, length, parts),
        out_shape=count_shapes,
        in_specs=[pl.BlockSpec(memory_space=pltpu.SMEM), VMEM, VMEM, VMEM],
        input_output_aliases={2: 0, 3: 1},
        out_specs=(VMEM, VMEM),
        scratch_shapes=[
            pltpu.VMEM((length, LANES), jnp.int32),
            pltpu.VMEM((length + 32, LANES), jnp.int32),
            pltpu.VMEM((bands, length // 32, LANES), jnp.int32),
        ],
        compiler_params=pltpu.CompilerParams(vmem_limit_bytes=VMEM_GRANT),
        name="tile_counts",
    )(first_id.astype(jnp.int32)[None], events, no_counts, no_margins)

    own_rows = pl.pallas_call(
        functools.partial(sketch_kernel, slabs, rows, parts, width, 1.0 / math.sqrt(total_events)),
        out_shape=jax.ShapeDtypeStruct((rows // slabs, width), jnp.float32),
        in_specs=[VMEM] * 5 + [pl.BlockSpec(memory_space=pl.ANY)],
        out_specs=VMEM,
        scratch_shapes=[
            pltpu.VMEM((rows + 8, LANES), jnp.float32),
            pltpu.VMEM((bands, 16, part), jnp.float32),
            pltpu.VMEM((words, rows), jnp.int32),
            pltpu.VMEM((rows, width), jnp.float32),
            pltpu.VMEM((slabs, 8, LANES), jnp.float32),
            pltpu.VMEM((slabs, 8, LANES), jnp.float32),
            dma((1,)),
            dma((slabs,)),
            dma((slabs,)),
        ],
        compiler_params=pltpu.CompilerParams(
            collective_id=1, has_side_effects=True, vmem_limit_bytes=VMEM_GRANT
        ),
        name="sketch_tile",
    )(counts, margins, head, signs, events, sketch_bits)
    if lax.axis_size("item") > 1:
        own_rows = lax.psum(own_rows, "item")
    return own_rows


def solution(mesh):
    placed = (P("stream"), P("stream"), P(None, "item"))
    return jax.shard_map(
        local, mesh=mesh, in_specs=placed, out_specs=P("stream", None), check_vma=False
    )
```

```python
import functools
import math

import jax
import jax.numpy as jnp
from jax import lax
from jax.experimental import pallas as pl
from jax.experimental.pallas import tpu as pltpu
from jax.sharding import PartitionSpec as P

WINDOW = 15
ITEM_BITS = 18
LANES = 128
BITS_PER_WORD = 18
PLANE = 8
BANDS = 4
NONE = 1.0e-30
VMEM_GRANT = 45 * 1024 * 1024
NT = (((1,), (1,)), ((), ()))
VMEM = pl.BlockSpec(memory_space=pltpu.VMEM)


def one_where(mask):
    return jnp.where(mask, 1.0, 0.0).astype(jnp.bfloat16)


def hot_columns(ids, values):
    row = jnp.broadcast_to(values, (16, values.shape[1])).astype(jnp.bfloat16)
    one, zero = jnp.ones((), jnp.bfloat16), jnp.zeros((), jnp.bfloat16)
    return jnp.concatenate(
        [jnp.where(ids[n : n + 16] == row, one, zero) for n in range(0, ids.shape[0], 16)], axis=0
    )


def greet_all(slabs, me):
    barrier = pltpu.get_barrier_semaphore()

    for k in range(1, slabs):
        pl.semaphore_signal(
            barrier, inc=1, device_id={"stream": lax.rem(me + k, slabs)}, device_id_type=pl.DeviceIdType.MESH
        )
    return barrier


def send(src, dst, send_sem, recv_sem, to):
    return pltpu.make_async_remote_copy(
        src_ref=src,
        dst_ref=dst,
        send_sem=send_sem,
        recv_sem=recv_sem,
        device_id={"stream": to},
        device_id_type=pl.DeviceIdType.MESH,
    )


def each(low, high, do):
    for k in range(low, high):
        do(k)


def exchange(slabs, me, out_ref, in_ref, send_sems, recv_sems, start):
    def copy(k):
        to = lax.rem(me + k, slabs)
        return send(out_ref.at[to], in_ref.at[me], send_sems.at[k], recv_sems.at[k], to)

    if start:
        each(1, slabs, lambda k: copy(k).start())
        in_ref[me] = out_ref[me]
    else:
        each(1, slabs, lambda k: copy(k).wait())


def gather_kernel(
    slabs, rows, blocks, items_ref, sessions_ref, bits_ref, all_ref, head_ref, sign_ref, count_ref, margin_ref,
    own_pack, own_bits, own_items, own_sessions, item_ref, session_ref, links_ref, total_ref,
    pair_out, pair_in, plane_out, plane_in, line_out, line_in,
    bit_sem, line_send, line_recv, plane_send, plane_recv, near_send, near_recv,
    pair_sems, head_plane_send, head_plane_recv, head_line_send, head_line_recv,
):
    me = lax.axis_index("stream")
    depth = slabs // PLANE
    layer, low = me // PLANE, lax.rem(me, PLANE)
    parity, quad = lax.rem(me, 2), lax.rem(me // 2, 4)

    def flip(bit):
        return bit - 2 * bit * lax.rem(me // bit, 2)

    partner = me + flip(1)
    steps = (flip(2), flip(4), flip(2) + flip(4))
    def other_layer(k):
        rising = k + (k - layer + depth) // depth
        mirrored = depth - 1 - layer
        falling = depth - 1 - k - (k - mirrored + depth) // depth
        high = layer // ((depth + 1) // 2)
        return rising + (falling - rising) * lax.rem(high, 2)

    others = [other_layer(k) for k in range(depth - 1)]
    loads = [
        pltpu.make_async_copy(items_ref, own_items, bit_sem.at[1]),
        pltpu.make_async_copy(sessions_ref, own_sessions, bit_sem.at[2]),
    ]
    for copy in loads:
        copy.start()
    barrier = pltpu.get_barrier_semaphore()
    owned = own_bits.shape[1]
    bit_copy = pltpu.make_async_copy(
        bits_ref.at[:, pl.ds(pl.multiple_of(me * owned, owned), owned)], own_bits, bit_sem.at[0]
    )
    greeted = [partner] + [me + step for step in steps] + [o * PLANE + low for o in others]
    for to in greeted:
        pl.semaphore_signal(
            barrier, inc=1, device_id={"stream": to}, device_id_type=pl.DeviceIdType.MESH
        )
    for copy in loads:
        copy.wait()
    bit_copy.start()
    half = blocks // 2
    own_pack[0:blocks] = own_items[...]
    own_pack[blocks : blocks + half] = own_sessions[0:half] | (own_sessions[half:blocks] << 16)
    all_ref[me] = own_pack[...]
    item_ref[8 : 8 + blocks] = own_items[...]
    session_ref[8 : 8 + blocks] = own_sessions[...]
    for edge in (slice(0, 8), slice(8 + blocks, 16 + blocks)):
        item_ref[edge] = jnp.zeros((8, LANES), jnp.int32)
        session_ref[edge] = jnp.full((8, LANES), -1, jnp.int32)
    sub = lax.broadcasted_iota(jnp.int32, (LANES, LANES), 0)
    lane = lax.broadcasted_iota(jnp.int32, (LANES, LANES), 1)
    low_lane = lax.broadcasted_iota(jnp.int32, (1, LANES), 1) < LANES // 2
    ids = lax.broadcasted_iota(jnp.int32, (rows, LANES), 0)
    gaps = (sub - LANES // 2 - lane, sub + LANES // 2 - lane)
    in_reach = [(jnp.abs(gap) <= WINDOW) & (gap != 0) for gap in gaps]
    ones = jnp.ones((8, 2 * LANES), jnp.float32).astype(jnp.bfloat16)
    links_ref[...] = jnp.zeros_like(links_ref)
    total_ref[...] = jnp.zeros_like(total_ref)

    together = 8

    def some_blocks(n, unused):
        first = n * together

        def shifted(ref):
            turned = [pltpu.roll(ref[pl.ds(first + 7 + o, 1)], LANES // 2, 1) for o in range(together + 2)]
            return [jnp.where(low_lane, turned[o], turned[o + 1]) for o in range(together + 1)]

        hots = [one_where(ids == item) for item in shifted(item_ref)]
        sessions = [jnp.broadcast_to(session, (LANES, LANES)).T for session in shifted(session_ref)]
        for o in range(together):
            own_item, own_session = item_ref[pl.ds(first + o + 8, 1)], session_ref[pl.ds(first + o + 8, 1)]
            hot = jnp.concatenate([hots[o], hots[o + 1]], axis=1)
            linked = jnp.concatenate(
                [one_where((sessions[o + side] == own_session) & in_reach[side]) for side in range(2)], axis=0
            )
            links = jnp.dot(jnp.concatenate([hot, ones], axis=0), linked, preferred_element_type=jnp.float32)
            links_ref[...] += lax.dot_general(
                links.astype(jnp.bfloat16), one_where(ids == own_item), NT, preferred_element_type=jnp.float32
            )
            total_ref[...] += links[rows:]
        return unused

    inner = [blocks * n // 32 for n in (0, 0, 32)]

    def blocks_of(n):
        lax.fori_loop(inner[n] // together, inner[n + 1] // together, some_blocks, 0)

    step_columns = max(LANES, owned // 16)
    steps_in_all = owned // step_columns

    def signs(low_step, high_step):
        def step(t, unused):
            at = pl.multiple_of(t * step_columns, step_columns)
            sign_ref[:, pl.ds(at, step_columns)] = sign_table(own_bits[:, pl.ds(at, step_columns)], sign_ref.shape[0])
            return unused

        lax.fori_loop(low_step * steps_in_all // 16, high_step * steps_in_all // 16, step, 0)

    blocks_of(0)
    pl.semaphore_wait(barrier, len(greeted))

    def along_line(there, here):
        return send(
            own_pack, all_ref.at[me], line_send.at[there], line_recv.at[here], there * PLANE + low
        )

    def in_plane(d, at_layer, own=False):
        slab = all_ref.at[at_layer * PLANE + low]
        sem = d * depth + at_layer
        return send(own_pack if own else slab, slab, plane_send.at[sem], plane_recv.at[sem], me + steps[d])

    def to_partner(r, at_layer, own=False):
        slab = all_ref.at[at_layer * PLANE + low + ((0,) + steps)[r]]
        sem = r * depth + at_layer
        return send(own_pack if own else slab, slab, near_send.at[sem], near_recv.at[sem], partner)

    for o in reversed(others):
        along_line(o, layer).start()
    for d in range(3):
        in_plane(d, layer, True).start()
    to_partner(0, layer, True).start()

    def forward_line(k):
        along_line(layer, others[k]).wait_recv()
        for d in range(3):
            in_plane(d, others[k]).start()
        to_partner(0, others[k]).start()

    def forward_plane(at_layer):
        for d in range(3):
            in_plane(d, at_layer).wait_recv()
            to_partner(d + 1, at_layer).start()

    blocks_of(1)
    share = rows // slabs
    tail = jnp.concatenate(
        [links_ref[rows : rows + 1], total_ref[0:1], jnp.zeros((6 - share, LANES), jnp.float32)], axis=0
    )
    for d in range(slabs):
        at = (d % 2, d // PLANE, d // 2 % 4)
        pair_out[at + (slice(0, share),)] = links_ref[d * share : (d + 1) * share]
        pair_out[at + (slice(share, 8),)] = tail

    pair = send(pair_out.at[1 - parity], pair_in, pair_sems.at[0], pair_sems.at[1], partner)
    pair.start()
    forward_line(0)
    forward_line(1)
    pair.wait()
    line_out[...] = pair_out[parity] + pair_in[...]

    def head_line(there, here):
        return send(
            line_out.at[there], line_in.at[layer], head_line_send.at[there], head_line_recv.at[here],
            there * PLANE + low,
        )

    for o in others:
        head_line(o, layer).start()
    line_in[layer] = line_out[layer]
    for k in range(2, depth - 1):
        forward_line(k)
    forward_plane(layer)
    count_ref[...] = jnp.zeros_like(count_ref)
    margin_ref[...] = jnp.zeros_like(margin_ref)
    bit_copy.wait()
    signs(0, 4)
    forward_plane(others[0])
    signs(4, 8)
    for o in others[1:-1]:
        forward_plane(o)
    for o in others:
        head_line(o, o).wait_recv()
    plane_out[...] = jnp.sum(line_in[...], axis=0)

    def head_plane(d):
        to = me + steps[d]
        return send(
            plane_out.at[lax.rem(to // 2, 4)], plane_in.at[d], head_plane_send.at[d], head_plane_recv.at[d], to
        )

    for d in range(3):
        head_plane(d).start()
    signs(8, 12)
    for o in others[-1:]:
        forward_plane(o)
    signs(12, 16)
    for at_layer in [layer] + others:
        for r in range(4):
            to_partner(r, at_layer).wait()
        for d in range(3):
            in_plane(d, at_layer).wait_send()
    for o in others:
        along_line(o, layer).wait_send()
        head_line(o, o).wait_send()
    for d in range(3):
        head_plane(d).wait()
    head_ref[...] = plane_out[quad] + plane_in[0] + plane_in[1] + plane_in[2]


def take_windows(code_ref, length, start):
    whole, part = start >> 3, start & 7
    bits = max(1, (length // 8 - 1).bit_length())
    keep = 8 * ((1 << (bits - 1)) + 4)
    value = None
    for bit in reversed(range(bits)):
        step = 8 << bit
        keep = 8 * ((1 << bit) + 4)
        chosen = ((whole >> bit) & 1) == 1
        if value is None:
            low, high = code_ref[0:keep, :], code_ref[step : step + keep, :]
        else:
            low, high = value[0:keep], value[step : step + keep]
        value = jnp.where(chosen, high, low)
    for bit in (2, 1, 0):
        chosen = ((part >> bit) & 1) == 1
        value = jnp.where(chosen, pltpu.roll(value, value.shape[0] - (1 << bit), 0), value)
    return value[0:32]


def all_rows(value, combine):
    for shift in (4, 2, 1):
        value = combine(value, pltpu.roll(value, shift, 0))
    return value


def bytes_of_rows(tag):
    return tag[0:8] | (tag[8:16] << 8) | (tag[16:24] << 16) | (tag[24:32] << 24)


def plane_word(packed, k):
    sub = lax.broadcasted_iota(jnp.int32, (8, LANES), 0)
    spread = lax.shift_left(lax.shift_right_logical(packed, k) & 0x01010101, sub)
    return all_rows(spread, lambda x, y: x | y)


def head_counts(window, ok, near, rows):
    center = window[16:17]
    linked = ((window ^ center) >> ITEM_BITS == 0) & near & ok
    item = window & ((1 << ITEM_BITS) - 1)
    tag = jnp.where(linked & (item < rows), item | rows, 0)
    packed = bytes_of_rows(tag)
    one = jnp.where(linked, 1, 0)
    weight = all_rows(one[0:8] + one[8:16] + one[16:24] + one[24:32], lambda x, y: x + y)
    sub = lax.broadcasted_iota(jnp.int32, (8, LANES), 0)

    def plane(k):
        return plane_word(packed, k)

    bits = rows.bit_length() - 1
    node = plane(bits)
    for k in range(3):
        node = node & (plane(k) ^ (((sub >> k) & 1) - 1))
    nodes = [node]
    for k in reversed(range(3, bits)):
        word = plane(k)
        nodes = [part for node in nodes for part in (node & ~word, node & word)]
    counts = jnp.concatenate([lax.population_count(node).astype(jnp.float32) for node in nodes], axis=0)
    return counts.astype(jnp.bfloat16), weight[0:1].astype(jnp.float32), center & ((1 << ITEM_BITS) - 1)


def tile_kernel(rows, length, parts, base_ref, all_ref, unused_counts, unused_margins, count_ref, margin_ref, flat_ref, code_ref, mask_ref):
    item_mask = (1 << ITEM_BITS) - 1
    base = base_ref[0]
    bands, unused_rows, width = count_ref.shape
    band = parts * width
    slabs, blocks = all_ref.shape[0], all_ref.shape[1] * 2 // 3
    for n in range(slabs):
        paired = all_ref[n, blocks:]
        sessions = jnp.concatenate([paired & 0xFFFF, paired >> 16], axis=0)
        flat_ref[n * blocks : (n + 1) * blocks] = all_ref[n, 0:blocks] | (sessions << ITEM_BITS)
    per = length // LANES
    for r in range(per):
        code_ref[16 + r * LANES : 16 + (r + 1) * LANES] = flat_ref[pl.ds(r, LANES, stride=per), :].T
    lane = lax.broadcasted_iota(jnp.int32, (16, LANES), 1)
    code_ref[0:16] = jnp.where(lane == 0, -1, pltpu.roll(code_ref[length : length + 16], 1, 1))
    code_ref[length + 16 : length + 32] = jnp.where(
        lane == LANES - 1, -1, pltpu.roll(code_ref[16:32], LANES - 1, 1)
    )

    words = length // 32
    band_bits = (bands - 1).bit_length()
    for w in range(words):
        item = code_ref[16 + 32 * w : 48 + 32 * w] & item_mask
        local = item - base
        mine = (local >= 0) & (local < bands * band) & (item >= rows)
        packed = bytes_of_rows(jnp.where(mine, (local >> (band.bit_length() - 1)) | bands, 0))
        for k in range(band_bits + 1):
            mask_ref[k, w : w + 1] = plane_word(packed, k)[0:1]
    planes = [mask_ref[k] for k in range(band_bits + 1)]
    for s in range(bands):
        mask = planes[band_bits]
        for k in range(band_bits):
            mask = mask & (planes[k] if s >> k & 1 else ~planes[k])
        mask_ref[s] = mask
    keys = []
    for s in range(bands):
        tally = jnp.sum(lax.population_count(mask_ref[s]), axis=0, keepdims=True)
        keys.append((jnp.max(tally) + 1) // 2 * bands + s)
    for low, high in ((0, 1), (2, 3), (0, 2), (1, 3), (1, 2)):
        keys[low], keys[high] = jnp.minimum(keys[low], keys[high]), jnp.maximum(keys[low], keys[high])
    streams = ((keys[3], keys[0]), (keys[2], keys[1]))

    word_ids = lax.broadcasted_iota(jnp.int32, (words, LANES), 0)
    d_ids = lax.broadcasted_iota(jnp.int32, (32, LANES), 0)
    near = (d_ids >= 1) & (d_ids != 16)
    tile = min(width, 256)
    t_ids = lax.broadcasted_iota(jnp.int32, (tile, 2 * LANES), 0).astype(jnp.float32).astype(jnp.bfloat16)
    p_ids = lax.broadcasted_iota(jnp.int32, (16, 2 * LANES), 0)

    def ends(mask):
        some = mask != 0
        first_row = jnp.min(jnp.where(some, word_ids, words), axis=0, keepdims=True)
        last_row = jnp.max(jnp.where(some, word_ids, -1), axis=0, keepdims=True)
        at_first, at_last = word_ids == first_row, word_ids == last_row
        first_word = jnp.sum(jnp.where(at_first, mask, 0), axis=0, keepdims=True)
        last_word = jnp.sum(jnp.where(at_last, mask, 0), axis=0, keepdims=True)
        first_bit = first_word & -first_word
        last_place = 31 - lax.clz(last_word)
        last_bit = jnp.where(last_word == 0, 0, jnp.left_shift(1, last_place & 31))
        first = 32 * first_row + lax.population_count(first_bit - 1)
        last = 32 * last_row + last_place
        first_ok = first_word != 0
        last_ok = first_ok & (last > first)
        mask = mask & ~(jnp.where(at_first, first_bit, 0) | jnp.where(at_last, last_bit, 0))
        return mask, ((first, first_ok), (last, last_ok))

    def find(s, mask):
        mask, found = ends(mask)
        links, weights, locals_ = [], [], []
        for at, ok in found:
            window = take_windows(code_ref, length, jnp.where(ok, at, 0))
            counts, weight, item = head_counts(window, ok, near, rows)
            links.append(counts)
            weights.append(weight)
            locals_.append(item - base - s * band)
        return mask, *(jnp.concatenate(x, axis=1) for x in (links, weights, locals_))

    def count(s, links, weight, local):
        part = local >> (width.bit_length() - 1)
        inner = local & (width - 1)
        pieces = []
        for p in range(parts):
            chosen = jnp.broadcast_to(jnp.where(part == p, 1.0, 0.0), (16, 2 * LANES)).astype(jnp.bfloat16)
            pieces += [links[n : n + 16] * chosen for n in range(0, rows, 16)]
        pieces.append(jnp.where(p_ids == part, weight, 0.0).astype(jnp.bfloat16))
        left = jnp.concatenate(pieces, axis=0)
        for t in range(width // tile):
            inside = (inner >= t * tile) & (inner < (t + 1) * tile)
            hot = hot_columns(t_ids, jnp.where(inside, inner - t * tile, -1).astype(jnp.float32))
            cols = slice(t * tile, (t + 1) * tile)
            value = lax.dot_general(left, hot, NT, preferred_element_type=jnp.float32)
            count_ref[s, :, cols] += value[0 : parts * rows]
            margin_ref[s, :, cols] += value[parts * rows :]

    def body(trip, masks):
        out = []
        for (early, late), mask in zip(streams, masks):
            switch = early // bands
            s = jnp.where(trip < switch, lax.rem(early, bands), lax.rem(late, bands))
            mask = jnp.where(trip == switch, mask_ref[lax.rem(late, bands)], mask)
            mask, *found = find(s, mask)
            out.append(mask)
            count(s, *found)
        return tuple(out)

    trips = [early // bands + late // bands for early, late in streams]
    starts = tuple(mask_ref[lax.rem(early, bands)] for early, late in streams)
    lax.fori_loop(0, jnp.maximum(*trips), body, starts)


def sign_table(words, width):
    size = words.shape[1]

    def wide(value):
        return jnp.concatenate([value] * (size // LANES), axis=1)

    shift = lax.broadcasted_iota(jnp.int32, (8, LANES), 0)
    parts = []
    for g in range(width // 8):
        word = 8 * g // BITS_PER_WORD
        split, offset = (word + 1) * BITS_PER_WORD - 8 * g, 8 * g - word * BITS_PER_WORD
        now = jnp.broadcast_to(words[word : word + 1], (8, size))
        where_bit = jnp.left_shift(1, shift + offset)
        if split < 8:
            later = jnp.broadcast_to(words[word + 1 : word + 2], (8, size))
            now = jnp.where(wide(shift) >= split, later, now)
            place = jnp.where(shift >= split, shift - split, shift + offset)
            where_bit = jnp.left_shift(1, place)
        parts.append(jnp.where((now & wide(where_bit)) != 0, 1.0, -1.0))
    return jnp.concatenate(parts, axis=0).astype(jnp.bfloat16)


def boundary_counts(rows, share, me, all_ref, extra_ref):
    slabs, blocks = all_ref.shape[0], all_ref.shape[1] * 2 // 3
    half = blocks // 2
    group = slabs // 4
    sub = lax.broadcasted_iota(jnp.int32, (LANES, LANES), 0)
    lane = lax.broadcasted_iota(jnp.int32, (LANES, LANES), 1)
    ids = lax.broadcasted_iota(jnp.int32, (rows, LANES), 0)
    small = lax.broadcasted_iota(jnp.int32, (group, LANES), 1)
    last_items, last_sessions = all_ref[:, blocks - 1, :], all_ref[:, blocks + half - 1, :] >> 16
    next_items, next_sessions = all_ref[:, 0, :], all_ref[:, blocks, :] & 0xFFFF

    def meet(last, following):
        joined = None
        for g in range(4):
            shift = 32 * g + 16
            pieces = (pltpu.roll(x[g * group : (g + 1) * group], shift, 1) for x in (last, following))
            both = jnp.where(small % 32 < 16, *pieces)
            joined = both if joined is None else jnp.where(small // 32 == g, both, joined)
        return joined

    slab_ids = lax.broadcasted_iota(jnp.int32, (slabs, LANES), 0)
    next_sessions = jnp.where(slab_ids == slabs - 1, -1, pltpu.roll(next_sessions, slabs - 1, 0))
    met_items = meet(last_items, pltpu.roll(next_items, slabs - 1, 0))
    met_sessions = meet(last_sessions, next_sessions)
    crossing = ((sub >> 5) == (lane >> 5)) & (((sub ^ lane) & 16) != 0) & (jnp.abs(sub - lane) <= WINDOW)
    ones = jnp.ones((8, LANES), jnp.float32).astype(jnp.bfloat16)
    extra = jnp.zeros((rows + 8, LANES), jnp.float32)
    total = jnp.zeros((8, LANES), jnp.float32)
    for g in range(group):
        item, session = met_items[g : g + 1], met_sessions[g : g + 1]
        linked = one_where((jnp.broadcast_to(session, (LANES, LANES)).T == session) & crossing)
        hot = one_where(ids == item)
        links = jnp.dot(jnp.concatenate([hot, ones], axis=0), linked, preferred_element_type=jnp.float32)
        extra += lax.dot_general(links.astype(jnp.bfloat16), hot, NT, preferred_element_type=jnp.float32)
        total += links[rows:]
    extra_ref[...] = extra
    return jnp.concatenate(
        [
            extra_ref[pl.ds(me * share, share)],
            extra_ref[rows : rows + 1],
            total[0:1],
            jnp.zeros((6 - share, LANES), jnp.float32),
        ],
        axis=0,
    )


def sketch_kernel(
    slabs, rows, parts, width, scale, count_ref, margin_ref, head_ref, sign_ref, all_ref, bits_ref, out_ref,
    extra_ref, log_ref, head_bits, acc_ref, send_ref, recv_ref, bit_sem, send_sems, recv_sems,
):
    me = lax.axis_index("stream")
    barrier = greet_all(slabs, me)
    bands, unused_rows, part = count_ref.shape
    share = rows // slabs
    tile = min(part, 512)
    head_copy = pltpu.make_async_copy(bits_ref.at[:, 0:rows], head_bits, bit_sem.at[0])
    head_copy.start()

    log_ref[...] = jnp.log(jnp.maximum(margin_ref[...], 1.0))
    head = head_ref[...] + boundary_counts(rows, share, me, all_ref, extra_ref)
    row_log = jnp.log(jnp.maximum(head[share : share + 1], 1.0))
    column_log = jnp.broadcast_to(row_log, (rows, LANES)).T
    total_log = jnp.log(jnp.sum(head[share + 1 : share + 2], axis=1, keepdims=True))
    row_term = total_log - column_log[:, 0:1]
    def product(positive, signs):
        upper = positive.astype(jnp.bfloat16)
        lower = (positive - upper.astype(jnp.float32)).astype(jnp.bfloat16)
        both = jnp.concatenate([upper, lower], axis=0)
        value = lax.dot_general(both, signs, NT, preferred_element_type=jnp.float32)
        return value[0:rows] + value[rows:]

    head_copy.wait()
    row = lax.broadcasted_iota(jnp.int32, (8, LANES), 0)
    shared = jnp.concatenate(
        [jnp.where(row < share, head, 0.0), jnp.zeros((rows - 8, LANES), jnp.float32)], axis=0
    )
    shared = pltpu.roll(shared, me * share, 0)
    ratio = jnp.log(jnp.maximum(shared, 1.0)) + total_log - row_log - column_log
    first_band = jnp.where(lax.axis_index("item") == 0, 1.0, 0.0)
    positive = jnp.where(shared > 0, jnp.maximum(ratio, 0.0), 0.0) * first_band
    acc_ref[...] = product(positive.T, sign_table(head_bits[...], width))

    for s in range(bands):
        for h in range(parts):
            for at in range(0, part, tile):
                counts = count_ref[s, h * rows : (h + 1) * rows, at : at + tile]
                ratio = jnp.log(jnp.maximum(counts, NONE)) + row_term - log_ref[s, h : h + 1, at : at + tile]
                positive = jnp.maximum(ratio, 0.0)
                bit_at = (s * parts + h) * part + at
                acc_ref[...] += product(positive, sign_ref[:, bit_at : bit_at + tile])

    cuts = width // LANES
    for d in range(slabs):
        for c in range(cuts):
            send_ref[d, c * share : (c + 1) * share] = (
                acc_ref[d * share : (d + 1) * share, c * LANES : (c + 1) * LANES] * scale
            )
    pl.semaphore_wait(barrier, slabs - 1)
    exchange(slabs, me, send_ref, recv_ref, send_sems, recv_sems, True)
    exchange(slabs, me, send_ref, recv_ref, send_sems, recv_sems, False)
    summed = jnp.sum(recv_ref[...], axis=0)
    out_ref[...] = jnp.concatenate([summed[c * share : (c + 1) * share] for c in range(cuts)], axis=1)


def local(event_items, event_sessions, sketch_bits):
    slabs = lax.axis_size("stream")
    slab = event_items.shape[0]
    total_events = slab * slabs
    words, band_size = sketch_bits.shape
    owned = band_size // slabs
    rows, width = 128, 256
    part = max(LANES, owned // 16)
    bands = BANDS
    parts = owned // (bands * part)
    me = lax.axis_index("stream")
    own_start = me * owned
    first_id = lax.axis_index("item") * band_size + own_start
    blocks = slab // LANES
    length = total_events // LANES

    dma = pltpu.SemaphoreType.DMA
    depth = slabs // PLANE
    count_shapes = (
        jax.ShapeDtypeStruct((bands, parts * rows, part), jnp.float32),
        jax.ShapeDtypeStruct((bands, 16, part), jnp.float32),
    )
    events, head, signs, no_counts, no_margins = pl.pallas_call(
        functools.partial(gather_kernel, slabs, rows, blocks),
        out_shape=(
            jax.ShapeDtypeStruct((slabs, blocks * 3 // 2, LANES), jnp.int32),
            jax.ShapeDtypeStruct((8, LANES), jnp.float32),
            jax.ShapeDtypeStruct((width, owned), jnp.bfloat16),
            *count_shapes,
        ),
        in_specs=[pl.BlockSpec(memory_space=pltpu.HBM)] * 3,
        out_specs=(VMEM,) * 5,
        scratch_shapes=[
            pltpu.VMEM((blocks * 3 // 2, LANES), jnp.int32),
            pltpu.VMEM((words, owned), jnp.int32),
            pltpu.VMEM((blocks, LANES), jnp.int32),
            pltpu.VMEM((blocks, LANES), jnp.int32),
            pltpu.VMEM((blocks + 16, LANES), jnp.int32),
            pltpu.VMEM((blocks + 16, LANES), jnp.int32),
            pltpu.VMEM((rows + 8, LANES), jnp.float32),
            pltpu.VMEM((8, LANES), jnp.float32),
            pltpu.VMEM((2, depth, 4, 8, LANES), jnp.float32),
            pltpu.VMEM((depth, 4, 8, LANES), jnp.float32),
            pltpu.VMEM((4, 8, LANES), jnp.float32),
            pltpu.VMEM((3, 8, LANES), jnp.float32),
            pltpu.VMEM((depth, 4, 8, LANES), jnp.float32),
            pltpu.VMEM((depth, 4, 8, LANES), jnp.float32),
            dma((3,)),
            dma((depth,)),
            dma((depth,)),
            dma((3 * depth,)),
            dma((3 * depth,)),
            dma((4 * depth,)),
            dma((4 * depth,)),
            dma((2,)),
            dma((3,)),
            dma((3,)),
            dma((depth,)),
            dma((depth,)),
        ],
        compiler_params=pltpu.CompilerParams(
            collective_id=0, has_side_effects=True, vmem_limit_bytes=VMEM_GRANT
        ),
        name="gather_events",
    )(*(pltpu.with_memory_space_constraint(x.reshape(blocks, LANES), pltpu.HBM) for x in (event_items, event_sessions)), sketch_bits)

    counts, margins = pl.pallas_call(
        functools.partial(tile_kernel, rows, length, parts),
        out_shape=count_shapes,
        in_specs=[pl.BlockSpec(memory_space=pltpu.SMEM), VMEM, VMEM, VMEM],
        input_output_aliases={2: 0, 3: 1},
        out_specs=(VMEM, VMEM),
        scratch_shapes=[
            pltpu.VMEM((length, LANES), jnp.int32),
            pltpu.VMEM((length + 32, LANES), jnp.int32),
            pltpu.VMEM((bands, length // 32, LANES), jnp.int32),
        ],
        compiler_params=pltpu.CompilerParams(vmem_limit_bytes=VMEM_GRANT),
        name="tile_counts",
    )(first_id.astype(jnp.int32)[None], events, no_counts, no_margins)

    own_rows = pl.pallas_call(
        functools.partial(sketch_kernel, slabs, rows, parts, width, 1.0 / math.sqrt(total_events)),
        out_shape=jax.ShapeDtypeStruct((rows // slabs, width), jnp.float32),
        in_specs=[VMEM] * 5 + [pl.BlockSpec(memory_space=pl.ANY)],
        out_specs=VMEM,
        scratch_shapes=[
            pltpu.VMEM((rows + 8, LANES), jnp.float32),
            pltpu.VMEM((bands, 16, part), jnp.float32),
            pltpu.VMEM((words, rows), jnp.int32),
            pltpu.VMEM((rows, width), jnp.float32),
            pltpu.VMEM((slabs, 8, LANES), jnp.float32),
            pltpu.VMEM((slabs, 8, LANES), jnp.float32),
            dma((1,)),
            dma((slabs,)),
            dma((slabs,)),
        ],
        compiler_params=pltpu.CompilerParams(
            collective_id=1, has_side_effects=True, vmem_limit_bytes=VMEM_GRANT
        ),
        name="sketch_tile",
    )(counts, margins, head, signs, events, sketch_bits)
    if lax.axis_size("item") > 1:
        own_rows = lax.psum(own_rows, "item")
    return own_rows


def solution(mesh):
    placed = (P("stream"), P("stream"), P(None, "item"))
    return jax.shard_map(
        local, mesh=mesh, in_specs=placed, out_specs=P("stream", None), check_vma=False
    )
```

```python
import functools
import math

import jax
import jax.numpy as jnp
from jax import lax
from jax.experimental import pallas as pl
from jax.experimental.pallas import tpu as pltpu
from jax.sharding import PartitionSpec as P

WINDOW = 15
ITEM_BITS = 18
LANES = 128
BITS_PER_WORD = 18
PLANE = 8
BANDS = 4
NONE = 1.0e-30
VMEM_GRANT = 45 * 1024 * 1024
NT = (((1,), (1,)), ((), ()))
VMEM = pl.BlockSpec(memory_space=pltpu.VMEM)


def one_where(mask):
    return jnp.where(mask, 1.0, 0.0).astype(jnp.bfloat16)


def hot_columns(ids, values):
    row = jnp.broadcast_to(values, (16, values.shape[1])).astype(jnp.bfloat16)
    one, zero = jnp.ones((), jnp.bfloat16), jnp.zeros((), jnp.bfloat16)
    return jnp.concatenate(
        [jnp.where(ids[n : n + 16] == row, one, zero) for n in range(0, ids.shape[0], 16)], axis=0
    )


def greet_all(slabs, me):
    barrier = pltpu.get_barrier_semaphore()

    for k in range(1, slabs):
        pl.semaphore_signal(
            barrier, inc=1, device_id={"stream": lax.rem(me + k, slabs)}, device_id_type=pl.DeviceIdType.MESH
        )
    return barrier


def send(src, dst, send_sem, recv_sem, to):
    return pltpu.make_async_remote_copy(
        src_ref=src,
        dst_ref=dst,
        send_sem=send_sem,
        recv_sem=recv_sem,
        device_id={"stream": to},
        device_id_type=pl.DeviceIdType.MESH,
    )


def each(low, high, do):
    for k in range(low, high):
        do(k)


def exchange(slabs, me, out_ref, in_ref, send_sems, recv_sems, start):
    def copy(k):
        to = lax.rem(me + k, slabs)
        return send(out_ref.at[to], in_ref.at[me], send_sems.at[k], recv_sems.at[k], to)

    if start:
        each(1, slabs, lambda k: copy(k).start())
        in_ref[me] = out_ref[me]
    else:
        each(1, slabs, lambda k: copy(k).wait())


def gather_kernel(
    slabs, rows, blocks, items_ref, sessions_ref, bits_ref, all_ref, head_ref, sign_ref, count_ref, margin_ref,
    own_pack, own_bits, own_items, own_sessions, item_ref, session_ref, links_ref, total_ref,
    pair_out, pair_in, plane_out, plane_in, line_out, line_in,
    bit_sem, line_send, line_recv, plane_send, plane_recv, near_send, near_recv,
    pair_sems, head_plane_send, head_plane_recv, head_line_send, head_line_recv,
):
    me = lax.axis_index("stream")
    depth = slabs // PLANE
    layer, low = me // PLANE, lax.rem(me, PLANE)
    parity, quad = lax.rem(me, 2), lax.rem(me // 2, 4)

    def flip(bit):
        return bit - 2 * bit * lax.rem(me // bit, 2)

    partner = me + flip(1)
    steps = (flip(2), flip(4), flip(2) + flip(4))
    def other_layer(k):
        rising = k + (k - layer + depth) // depth
        mirrored = depth - 1 - layer
        falling = depth - 1 - k - (k - mirrored + depth) // depth
        high = layer // ((depth + 1) // 2)
        return rising + (falling - rising) * lax.rem(high, 2)

    others = [other_layer(k) for k in range(depth - 1)]
    loads = [
        pltpu.make_async_copy(items_ref, own_items, bit_sem.at[1]),
        pltpu.make_async_copy(sessions_ref, own_sessions, bit_sem.at[2]),
    ]
    for copy in loads:
        copy.start()
    barrier = pltpu.get_barrier_semaphore()
    owned = own_bits.shape[1]
    bit_copy = pltpu.make_async_copy(
        bits_ref.at[:, pl.ds(pl.multiple_of(me * owned, owned), owned)], own_bits, bit_sem.at[0]
    )
    greeted = [partner] + [me + step for step in steps] + [o * PLANE + low for o in others]
    for to in greeted:
        pl.semaphore_signal(
            barrier, inc=1, device_id={"stream": to}, device_id_type=pl.DeviceIdType.MESH
        )
    for copy in loads:
        copy.wait()
    bit_copy.start()
    half = blocks // 2
    own_pack[0:blocks] = own_items[...]
    own_pack[blocks : blocks + half] = own_sessions[0:half] | (own_sessions[half:blocks] << 16)
    all_ref[me] = own_pack[...]
    item_ref[8 : 8 + blocks] = own_items[...]
    session_ref[8 : 8 + blocks] = own_sessions[...]
    for edge in (slice(0, 8), slice(8 + blocks, 16 + blocks)):
        item_ref[edge] = jnp.zeros((8, LANES), jnp.int32)
        session_ref[edge] = jnp.full((8, LANES), -1, jnp.int32)
    sub = lax.broadcasted_iota(jnp.int32, (LANES, LANES), 0)
    lane = lax.broadcasted_iota(jnp.int32, (LANES, LANES), 1)
    low_lane = lax.broadcasted_iota(jnp.int32, (1, LANES), 1) < LANES // 2
    ids = lax.broadcasted_iota(jnp.int32, (rows, LANES), 0)
    gaps = (sub - LANES // 2 - lane, sub + LANES // 2 - lane)
    in_reach = [(jnp.abs(gap) <= WINDOW) & (gap != 0) for gap in gaps]
    ones = jnp.ones((8, 2 * LANES), jnp.float32).astype(jnp.bfloat16)
    links_ref[...] = jnp.zeros_like(links_ref)
    total_ref[...] = jnp.zeros_like(total_ref)

    together = 8

    def some_blocks(n, unused):
        first = n * together

        def shifted(ref):
            turned = [pltpu.roll(ref[pl.ds(first + 7 + o, 1)], LANES // 2, 1) for o in range(together + 2)]
            return [jnp.where(low_lane, turned[o], turned[o + 1]) for o in range(together + 1)]

        hots = [one_where(ids == item) for item in shifted(item_ref)]
        sessions = [jnp.broadcast_to(session, (LANES, LANES)).T for session in shifted(session_ref)]
        for o in range(together):
            own_item, own_session = item_ref[pl.ds(first + o + 8, 1)], session_ref[pl.ds(first + o + 8, 1)]
            hot = jnp.concatenate([hots[o], hots[o + 1]], axis=1)
            linked = jnp.concatenate(
                [one_where((sessions[o + side] == own_session) & in_reach[side]) for side in range(2)], axis=0
            )
            links = jnp.dot(jnp.concatenate([hot, ones], axis=0), linked, preferred_element_type=jnp.float32)
            links_ref[...] += lax.dot_general(
                links.astype(jnp.bfloat16), one_where(ids == own_item), NT, preferred_element_type=jnp.float32
            )
            total_ref[...] += links[rows:]
        return unused

    inner = [blocks * n // 32 for n in (0, 0, 32)]

    def blocks_of(n):
        lax.fori_loop(inner[n] // together, inner[n + 1] // together, some_blocks, 0)

    step_columns = max(LANES, owned // 16)
    steps_in_all = owned // step_columns

    def signs(low_step, high_step):
        def step(t, unused):
            at = pl.multiple_of(t * step_columns, step_columns)
            sign_ref[:, pl.ds(at, step_columns)] = sign_table(own_bits[:, pl.ds(at, step_columns)], sign_ref.shape[0])
            return unused

        lax.fori_loop(low_step * steps_in_all // 16, high_step * steps_in_all // 16, step, 0)

    blocks_of(0)
    pl.semaphore_wait(barrier, len(greeted))

    def along_line(there, here):
        return send(
            own_pack, all_ref.at[me], line_send.at[there], line_recv.at[here], there * PLANE + low
        )

    def in_plane(d, at_layer, own=False):
        slab = all_ref.at[at_layer * PLANE + low]
        sem = d * depth + at_layer
        return send(own_pack if own else slab, slab, plane_send.at[sem], plane_recv.at[sem], me + steps[d])

    def to_partner(r, at_layer, own=False):
        slab = all_ref.at[at_layer * PLANE + low + ((0,) + steps)[r]]
        sem = r * depth + at_layer
        return send(own_pack if own else slab, slab, near_send.at[sem], near_recv.at[sem], partner)

    for o in reversed(others):
        along_line(o, layer).start()
    for d in range(3):
        in_plane(d, layer, True).start()
    to_partner(0, layer, True).start()

    def forward_line(k):
        along_line(layer, others[k]).wait_recv()
        for d in range(3):
            in_plane(d, others[k]).start()
        to_partner(0, others[k]).start()

    def forward_plane(at_layer):
        for d in range(3):
            in_plane(d, at_layer).wait_recv()
            to_partner(d + 1, at_layer).start()

    blocks_of(1)
    share = rows // slabs
    tail = jnp.concatenate(
        [links_ref[rows : rows + 1], total_ref[0:1], jnp.zeros((6 - share, LANES), jnp.float32)], axis=0
    )
    for d in range(slabs):
        at = (d % 2, d // PLANE, d // 2 % 4)
        pair_out[at + (slice(0, share),)] = links_ref[d * share : (d + 1) * share]
        pair_out[at + (slice(share, 8),)] = tail

    pair = send(pair_out.at[1 - parity], pair_in, pair_sems.at[0], pair_sems.at[1], partner)
    pair.start()
    forward_line(0)
    forward_line(1)
    pair.wait()
    line_out[...] = pair_out[parity] + pair_in[...]

    def head_line(there, here):
        return send(
            line_out.at[there], line_in.at[layer], head_line_send.at[there], head_line_recv.at[here],
            there * PLANE + low,
        )

    for o in others:
        head_line(o, layer).start()
    line_in[layer] = line_out[layer]
    forward_plane(layer)
    for k in range(2, depth - 1):
        forward_line(k)
    count_ref[...] = jnp.zeros_like(count_ref)
    margin_ref[...] = jnp.zeros_like(margin_ref)
    bit_copy.wait()
    signs(0, 4)
    forward_plane(others[0])
    signs(4, 8)
    for o in others:
        head_line(o, o).wait_recv()
    plane_out[...] = jnp.sum(line_in[...], axis=0)

    def head_plane(d):
        to = me + steps[d]
        return send(
            plane_out.at[lax.rem(to // 2, 4)], plane_in.at[d], head_plane_send.at[d], head_plane_recv.at[d], to
        )

    for d in range(3):
        head_plane(d).start()
    signs(8, 12)
    for o in others[1:]:
        forward_plane(o)
    signs(12, 16)
    for at_layer in [layer] + others:
        for r in range(4):
            to_partner(r, at_layer).wait()
        for d in range(3):
            in_plane(d, at_layer).wait_send()
    for o in others:
        along_line(o, layer).wait_send()
        head_line(o, o).wait_send()
    for d in range(3):
        head_plane(d).wait()
    head_ref[...] = plane_out[quad] + plane_in[0] + plane_in[1] + plane_in[2]


def take_windows(code_ref, length, start):
    whole, part = start >> 3, start & 7
    bits = max(1, (length // 8 - 1).bit_length())
    keep = 8 * ((1 << (bits - 1)) + 4)
    value = None
    for bit in reversed(range(bits)):
        step = 8 << bit
        keep = 8 * ((1 << bit) + 4)
        chosen = ((whole >> bit) & 1) == 1
        if value is None:
            low, high = code_ref[0:keep, :], code_ref[step : step + keep, :]
        else:
            low, high = value[0:keep], value[step : step + keep]
        value = jnp.where(chosen, high, low)
    for bit in (2, 1, 0):
        chosen = ((part >> bit) & 1) == 1
        value = jnp.where(chosen, pltpu.roll(value, value.shape[0] - (1 << bit), 0), value)
    return value[0:32]


def all_rows(value, combine):
    for shift in (4, 2, 1):
        value = combine(value, pltpu.roll(value, shift, 0))
    return value


def bytes_of_rows(tag):
    return tag[0:8] | (tag[8:16] << 8) | (tag[16:24] << 16) | (tag[24:32] << 24)


def plane_word(packed, k):
    sub = lax.broadcasted_iota(jnp.int32, (8, LANES), 0)
    spread = lax.shift_left(lax.shift_right_logical(packed, k) & 0x01010101, sub)
    return all_rows(spread, lambda x, y: x | y)


def head_counts(window, ok, near, rows):
    center = window[16:17]
    linked = ((window ^ center) >> ITEM_BITS == 0) & near & ok
    item = window & ((1 << ITEM_BITS) - 1)
    tag = jnp.where(linked & (item < rows), item | rows, 0)
    packed = bytes_of_rows(tag)
    one = jnp.where(linked, 1, 0)
    weight = all_rows(one[0:8] + one[8:16] + one[16:24] + one[24:32], lambda x, y: x + y)
    sub = lax.broadcasted_iota(jnp.int32, (8, LANES), 0)

    def plane(k):
        return plane_word(packed, k)

    bits = rows.bit_length() - 1
    node = plane(bits)
    for k in range(3):
        node = node & (plane(k) ^ (((sub >> k) & 1) - 1))
    nodes = [node]
    for k in reversed(range(3, bits)):
        word = plane(k)
        nodes = [part for node in nodes for part in (node & ~word, node & word)]
    counts = jnp.concatenate([lax.population_count(node).astype(jnp.float32) for node in nodes], axis=0)
    return counts.astype(jnp.bfloat16), weight[0:1].astype(jnp.float32), center & ((1 << ITEM_BITS) - 1)


def tile_kernel(rows, length, parts, base_ref, all_ref, unused_counts, unused_margins, count_ref, margin_ref, flat_ref, code_ref, mask_ref):
    item_mask = (1 << ITEM_BITS) - 1
    base = base_ref[0]
    bands, unused_rows, width = count_ref.shape
    band = parts * width
    slabs, blocks = all_ref.shape[0], all_ref.shape[1] * 2 // 3
    for n in range(slabs):
        paired = all_ref[n, blocks:]
        sessions = jnp.concatenate([paired & 0xFFFF, paired >> 16], axis=0)
        flat_ref[n * blocks : (n + 1) * blocks] = all_ref[n, 0:blocks] | (sessions << ITEM_BITS)
    per = length // LANES
    for r in range(per):
        code_ref[16 + r * LANES : 16 + (r + 1) * LANES] = flat_ref[pl.ds(r, LANES, stride=per), :].T
    lane = lax.broadcasted_iota(jnp.int32, (16, LANES), 1)
    code_ref[0:16] = jnp.where(lane == 0, -1, pltpu.roll(code_ref[length : length + 16], 1, 1))
    code_ref[length + 16 : length + 32] = jnp.where(
        lane == LANES - 1, -1, pltpu.roll(code_ref[16:32], LANES - 1, 1)
    )

    words = length // 32
    band_bits = (bands - 1).bit_length()
    for w in range(words):
        item = code_ref[16 + 32 * w : 48 + 32 * w] & item_mask
        local = item - base
        mine = (local >= 0) & (local < bands * band) & (item >= rows)
        packed = bytes_of_rows(jnp.where(mine, (local >> (band.bit_length() - 1)) | bands, 0))
        for k in range(band_bits + 1):
            mask_ref[k, w : w + 1] = plane_word(packed, k)[0:1]
    planes = [mask_ref[k] for k in range(band_bits + 1)]
    for s in range(bands):
        mask = planes[band_bits]
        for k in range(band_bits):
            mask = mask & (planes[k] if s >> k & 1 else ~planes[k])
        mask_ref[s] = mask
    keys = []
    for s in range(bands):
        tally = jnp.sum(lax.population_count(mask_ref[s]), axis=0, keepdims=True)
        keys.append((jnp.max(tally) + 1) // 2 * bands + s)
    for low, high in ((0, 1), (2, 3), (0, 2), (1, 3), (1, 2)):
        keys[low], keys[high] = jnp.minimum(keys[low], keys[high]), jnp.maximum(keys[low], keys[high])
    streams = ((keys[3], keys[0]), (keys[2], keys[1]))

    word_ids = lax.broadcasted_iota(jnp.int32, (words, LANES), 0)
    d_ids = lax.broadcasted_iota(jnp.int32, (32, LANES), 0)
    near = (d_ids >= 1) & (d_ids != 16)
    tile = min(width, 256)
    t_ids = lax.broadcasted_iota(jnp.int32, (tile, 2 * LANES), 0).astype(jnp.float32).astype(jnp.bfloat16)
    p_ids = lax.broadcasted_iota(jnp.int32, (16, 2 * LANES), 0)

    def ends(mask):
        some = mask != 0
        first_row = jnp.min(jnp.where(some, word_ids, words), axis=0, keepdims=True)
        last_row = jnp.max(jnp.where(some, word_ids, -1), axis=0, keepdims=True)
        at_first, at_last = word_ids == first_row, word_ids == last_row
        first_word = jnp.sum(jnp.where(at_first, mask, 0), axis=0, keepdims=True)
        last_word = jnp.sum(jnp.where(at_last, mask, 0), axis=0, keepdims=True)
        first_bit = first_word & -first_word
        last_place = 31 - lax.clz(last_word)
        last_bit = jnp.where(last_word == 0, 0, jnp.left_shift(1, last_place & 31))
        first = 32 * first_row + lax.population_count(first_bit - 1)
        last = 32 * last_row + last_place
        first_ok = first_word != 0
        last_ok = first_ok & (last > first)
        mask = mask & ~(jnp.where(at_first, first_bit, 0) | jnp.where(at_last, last_bit, 0))
        return mask, ((first, first_ok), (last, last_ok))

    def find(s, mask):
        mask, found = ends(mask)
        links, weights, locals_ = [], [], []
        for at, ok in found:
            window = take_windows(code_ref, length, jnp.where(ok, at, 0))
            counts, weight, item = head_counts(window, ok, near, rows)
            links.append(counts)
            weights.append(weight)
            locals_.append(item - base - s * band)
        return mask, *(jnp.concatenate(x, axis=1) for x in (links, weights, locals_))

    def count(s, links, weight, local):
        part = local >> (width.bit_length() - 1)
        inner = local & (width - 1)
        pieces = []
        for p in range(parts):
            chosen = jnp.broadcast_to(jnp.where(part == p, 1.0, 0.0), (16, 2 * LANES)).astype(jnp.bfloat16)
            pieces += [links[n : n + 16] * chosen for n in range(0, rows, 16)]
        pieces.append(jnp.where(p_ids == part, weight, 0.0).astype(jnp.bfloat16))
        left = jnp.concatenate(pieces, axis=0)
        for t in range(width // tile):
            inside = (inner >= t * tile) & (inner < (t + 1) * tile)
            hot = hot_columns(t_ids, jnp.where(inside, inner - t * tile, -1).astype(jnp.float32))
            cols = slice(t * tile, (t + 1) * tile)
            value = lax.dot_general(left, hot, NT, preferred_element_type=jnp.float32)
            count_ref[s, :, cols] += value[0 : parts * rows]
            margin_ref[s, :, cols] += value[parts * rows :]

    def body(trip, masks):
        out = []
        for (early, late), mask in zip(streams, masks):
            switch = early // bands
            s = jnp.where(trip < switch, lax.rem(early, bands), lax.rem(late, bands))
            mask = jnp.where(trip == switch, mask_ref[lax.rem(late, bands)], mask)
            mask, *found = find(s, mask)
            out.append(mask)
            count(s, *found)
        return tuple(out)

    trips = [early // bands + late // bands for early, late in streams]
    starts = tuple(mask_ref[lax.rem(early, bands)] for early, late in streams)
    lax.fori_loop(0, jnp.maximum(*trips), body, starts)


def sign_table(words, width):
    size = words.shape[1]

    def wide(value):
        return jnp.concatenate([value] * (size // LANES), axis=1)

    shift = lax.broadcasted_iota(jnp.int32, (8, LANES), 0)
    parts = []
    for g in range(width // 8):
        word = 8 * g // BITS_PER_WORD
        split, offset = (word + 1) * BITS_PER_WORD - 8 * g, 8 * g - word * BITS_PER_WORD
        now = jnp.broadcast_to(words[word : word + 1], (8, size))
        where_bit = jnp.left_shift(1, shift + offset)
        if split < 8:
            later = jnp.broadcast_to(words[word + 1 : word + 2], (8, size))
            now = jnp.where(wide(shift) >= split, later, now)
            place = jnp.where(shift >= split, shift - split, shift + offset)
            where_bit = jnp.left_shift(1, place)
        parts.append(jnp.where((now & wide(where_bit)) != 0, 1.0, -1.0))
    return jnp.concatenate(parts, axis=0).astype(jnp.bfloat16)


def boundary_counts(rows, share, me, all_ref, extra_ref):
    slabs, blocks = all_ref.shape[0], all_ref.shape[1] * 2 // 3
    half = blocks // 2
    group = slabs // 4
    sub = lax.broadcasted_iota(jnp.int32, (LANES, LANES), 0)
    lane = lax.broadcasted_iota(jnp.int32, (LANES, LANES), 1)
    ids = lax.broadcasted_iota(jnp.int32, (rows, LANES), 0)
    small = lax.broadcasted_iota(jnp.int32, (group, LANES), 1)
    last_items, last_sessions = all_ref[:, blocks - 1, :], all_ref[:, blocks + half - 1, :] >> 16
    next_items, next_sessions = all_ref[:, 0, :], all_ref[:, blocks, :] & 0xFFFF

    def meet(last, following):
        joined = None
        for g in range(4):
            shift = 32 * g + 16
            pieces = (pltpu.roll(x[g * group : (g + 1) * group], shift, 1) for x in (last, following))
            both = jnp.where(small % 32 < 16, *pieces)
            joined = both if joined is None else jnp.where(small // 32 == g, both, joined)
        return joined

    slab_ids = lax.broadcasted_iota(jnp.int32, (slabs, LANES), 0)
    next_sessions = jnp.where(slab_ids == slabs - 1, -1, pltpu.roll(next_sessions, slabs - 1, 0))
    met_items = meet(last_items, pltpu.roll(next_items, slabs - 1, 0))
    met_sessions = meet(last_sessions, next_sessions)
    crossing = ((sub >> 5) == (lane >> 5)) & (((sub ^ lane) & 16) != 0) & (jnp.abs(sub - lane) <= WINDOW)
    ones = jnp.ones((8, LANES), jnp.float32).astype(jnp.bfloat16)
    extra = jnp.zeros((rows + 8, LANES), jnp.float32)
    total = jnp.zeros((8, LANES), jnp.float32)
    for g in range(group):
        item, session = met_items[g : g + 1], met_sessions[g : g + 1]
        linked = one_where((jnp.broadcast_to(session, (LANES, LANES)).T == session) & crossing)
        hot = one_where(ids == item)
        links = jnp.dot(jnp.concatenate([hot, ones], axis=0), linked, preferred_element_type=jnp.float32)
        extra += lax.dot_general(links.astype(jnp.bfloat16), hot, NT, preferred_element_type=jnp.float32)
        total += links[rows:]
    extra_ref[...] = extra
    return jnp.concatenate(
        [
            extra_ref[pl.ds(me * share, share)],
            extra_ref[rows : rows + 1],
            total[0:1],
            jnp.zeros((6 - share, LANES), jnp.float32),
        ],
        axis=0,
    )


def sketch_kernel(
    slabs, rows, parts, width, scale, count_ref, margin_ref, head_ref, sign_ref, all_ref, bits_ref, out_ref,
    extra_ref, log_ref, head_bits, acc_ref, send_ref, recv_ref, bit_sem, send_sems, recv_sems,
):
    me = lax.axis_index("stream")
    barrier = greet_all(slabs, me)
    bands, unused_rows, part = count_ref.shape
    share = rows // slabs
    tile = min(part, 512)
    head_copy = pltpu.make_async_copy(bits_ref.at[:, 0:rows], head_bits, bit_sem.at[0])
    head_copy.start()

    log_ref[...] = jnp.log(jnp.maximum(margin_ref[...], 1.0))
    head = head_ref[...] + boundary_counts(rows, share, me, all_ref, extra_ref)
    row_log = jnp.log(jnp.maximum(head[share : share + 1], 1.0))
    column_log = jnp.broadcast_to(row_log, (rows, LANES)).T
    total_log = jnp.log(jnp.sum(head[share + 1 : share + 2], axis=1, keepdims=True))
    row_term = total_log - column_log[:, 0:1]
    def product(positive, signs):
        upper = positive.astype(jnp.bfloat16)
        lower = (positive - upper.astype(jnp.float32)).astype(jnp.bfloat16)
        both = jnp.concatenate([upper, lower], axis=0)
        value = lax.dot_general(both, signs, NT, preferred_element_type=jnp.float32)
        return value[0:rows] + value[rows:]

    head_copy.wait()
    row = lax.broadcasted_iota(jnp.int32, (8, LANES), 0)
    shared = jnp.concatenate(
        [jnp.where(row < share, head, 0.0), jnp.zeros((rows - 8, LANES), jnp.float32)], axis=0
    )
    shared = pltpu.roll(shared, me * share, 0)
    ratio = jnp.log(jnp.maximum(shared, 1.0)) + total_log - row_log - column_log
    first_band = jnp.where(lax.axis_index("item") == 0, 1.0, 0.0)
    positive = jnp.where(shared > 0, jnp.maximum(ratio, 0.0), 0.0) * first_band
    acc_ref[...] = product(positive.T, sign_table(head_bits[...], width))

    for s in range(bands):
        for h in range(parts):
            for at in range(0, part, tile):
                counts = count_ref[s, h * rows : (h + 1) * rows, at : at + tile]
                ratio = jnp.log(jnp.maximum(counts, NONE)) + row_term - log_ref[s, h : h + 1, at : at + tile]
                positive = jnp.maximum(ratio, 0.0)
                bit_at = (s * parts + h) * part + at
                acc_ref[...] += product(positive, sign_ref[:, bit_at : bit_at + tile])

    cuts = width // LANES
    for d in range(slabs):
        for c in range(cuts):
            send_ref[d, c * share : (c + 1) * share] = (
                acc_ref[d * share : (d + 1) * share, c * LANES : (c + 1) * LANES] * scale
            )
    pl.semaphore_wait(barrier, slabs - 1)
    exchange(slabs, me, send_ref, recv_ref, send_sems, recv_sems, True)
    exchange(slabs, me, send_ref, recv_ref, send_sems, recv_sems, False)
    summed = jnp.sum(recv_ref[...], axis=0)
    out_ref[...] = jnp.concatenate([summed[c * share : (c + 1) * share] for c in range(cuts)], axis=1)


def local(event_items, event_sessions, sketch_bits):
    slabs = lax.axis_size("stream")
    slab = event_items.shape[0]
    total_events = slab * slabs
    words, band_size = sketch_bits.shape
    owned = band_size // slabs
    rows, width = 128, 256
    part = max(LANES, owned // 16)
    bands = BANDS
    parts = owned // (bands * part)
    me = lax.axis_index("stream")
    own_start = me * owned
    first_id = lax.axis_index("item") * band_size + own_start
    blocks = slab // LANES
    length = total_events // LANES

    dma = pltpu.SemaphoreType.DMA
    depth = slabs // PLANE
    count_shapes = (
        jax.ShapeDtypeStruct((bands, parts * rows, part), jnp.float32),
        jax.ShapeDtypeStruct((bands, 16, part), jnp.float32),
    )
    events, head, signs, no_counts, no_margins = pl.pallas_call(
        functools.partial(gather_kernel, slabs, rows, blocks),
        out_shape=(
            jax.ShapeDtypeStruct((slabs, blocks * 3 // 2, LANES), jnp.int32),
            jax.ShapeDtypeStruct((8, LANES), jnp.float32),
            jax.ShapeDtypeStruct((width, owned), jnp.bfloat16),
            *count_shapes,
        ),
        in_specs=[pl.BlockSpec(memory_space=pltpu.HBM)] * 3,
        out_specs=(VMEM,) * 5,
        scratch_shapes=[
            pltpu.VMEM((blocks * 3 // 2, LANES), jnp.int32),
            pltpu.VMEM((words, owned), jnp.int32),
            pltpu.VMEM((blocks, LANES), jnp.int32),
            pltpu.VMEM((blocks, LANES), jnp.int32),
            pltpu.VMEM((blocks + 16, LANES), jnp.int32),
            pltpu.VMEM((blocks + 16, LANES), jnp.int32),
            pltpu.VMEM((rows + 8, LANES), jnp.float32),
            pltpu.VMEM((8, LANES), jnp.float32),
            pltpu.VMEM((2, depth, 4, 8, LANES), jnp.float32),
            pltpu.VMEM((depth, 4, 8, LANES), jnp.float32),
            pltpu.VMEM((4, 8, LANES), jnp.float32),
            pltpu.VMEM((3, 8, LANES), jnp.float32),
            pltpu.VMEM((depth, 4, 8, LANES), jnp.float32),
            pltpu.VMEM((depth, 4, 8, LANES), jnp.float32),
            dma((3,)),
            dma((depth,)),
            dma((depth,)),
            dma((3 * depth,)),
            dma((3 * depth,)),
            dma((4 * depth,)),
            dma((4 * depth,)),
            dma((2,)),
            dma((3,)),
            dma((3,)),
            dma((depth,)),
            dma((depth,)),
        ],
        compiler_params=pltpu.CompilerParams(
            collective_id=0, has_side_effects=True, vmem_limit_bytes=VMEM_GRANT
        ),
        name="gather_events",
    )(*(pltpu.with_memory_space_constraint(x.reshape(blocks, LANES), pltpu.HBM) for x in (event_items, event_sessions)), sketch_bits)

    counts, margins = pl.pallas_call(
        functools.partial(tile_kernel, rows, length, parts),
        out_shape=count_shapes,
        in_specs=[pl.BlockSpec(memory_space=pltpu.SMEM), VMEM, VMEM, VMEM],
        input_output_aliases={2: 0, 3: 1},
        out_specs=(VMEM, VMEM),
        scratch_shapes=[
            pltpu.VMEM((length, LANES), jnp.int32),
            pltpu.VMEM((length + 32, LANES), jnp.int32),
            pltpu.VMEM((bands, length // 32, LANES), jnp.int32),
        ],
        compiler_params=pltpu.CompilerParams(vmem_limit_bytes=VMEM_GRANT),
        name="tile_counts",
    )(first_id.astype(jnp.int32)[None], events, no_counts, no_margins)

    own_rows = pl.pallas_call(
        functools.partial(sketch_kernel, slabs, rows, parts, width, 1.0 / math.sqrt(total_events)),
        out_shape=jax.ShapeDtypeStruct((rows // slabs, width), jnp.float32),
        in_specs=[VMEM] * 5 + [pl.BlockSpec(memory_space=pl.ANY)],
        out_specs=VMEM,
        scratch_shapes=[
            pltpu.VMEM((rows + 8, LANES), jnp.float32),
            pltpu.VMEM((bands, 16, part), jnp.float32),
            pltpu.VMEM((words, rows), jnp.int32),
            pltpu.VMEM((rows, width), jnp.float32),
            pltpu.VMEM((slabs, 8, LANES), jnp.float32),
            pltpu.VMEM((slabs, 8, LANES), jnp.float32),
            dma((1,)),
            dma((slabs,)),
            dma((slabs,)),
        ],
        compiler_params=pltpu.CompilerParams(
            collective_id=1, has_side_effects=True, vmem_limit_bytes=VMEM_GRANT
        ),
        name="sketch_tile",
    )(counts, margins, head, signs, events, sketch_bits)
    if lax.axis_size("item") > 1:
        own_rows = lax.psum(own_rows, "item")
    return own_rows


def solution(mesh):
    placed = (P("stream"), P("stream"), P(None, "item"))
    return jax.shard_map(
        local, mesh=mesh, in_specs=placed, out_specs=P("stream", None), check_vma=False
    )
```
